32 devices in a mesh: dp: 4 (over x, core), tensor: 8 (over z, y).
Axes of the slice: x: 2, y: 2, z: 4, core: 2. Of those that a mesh axis runs over, the one named last changes fastest.
Arguments:
- tokens: bfloat16 [2, 4, 1024, 1024], P(None, 'dp', 'tensor'), may hold values from -6 to 6
- resets: int32 [2, 4, 1024], P(None, 'dp', 'tensor'), may hold values from 0 to 1, as said below
- out_grads: bfloat16 [2, 4, 1024, 1024], P(None, 'dp', 'tensor'), may hold values from -6 to 6
- mixer_key: bfloat16 [1024, 1024], P(('dp', 'tensor')), may hold values from -0.1875 to 0.1875
- mixer_value: bfloat16 [1024, 1024], P(('dp', 'tensor')), may hold values from -0.1875 to 0.1875
- mixer_recept: bfloat16 [1024, 1024], P(('dp', 'tensor')), may hold values from -0.1875 to 0.1875
- mixer_output: bfloat16 [1024, 1024], P(('dp', 'tensor')), may hold values from -1.5 to 1.5
- feed_recept: bfloat16 [1024, 1024], P(('dp', 'tensor')), may hold values from -0.1875 to 0.1875
- feed_key: bfloat16 [4096, 1024], P('tensor'), may hold values from -0.1875 to 0.1875
- feed_value: bfloat16 [4096, 1024], P('tensor'), may hold values from -0.09375 to 0.09375
- first_gain: bfloat16 [1024], P(('dp', 'tensor')), may hold values from 0.099609375 to 1.8984375
- first_bias: bfloat16 [1024], P(('dp', 'tensor')), may hold values from -3 to 3
- second_gain: bfloat16 [1024], P(('dp', 'tensor')), may hold values from 0.099609375 to 1.8984375
- second_bias: bfloat16 [1024], P(('dp', 'tensor')), may hold values from -3 to 3
- mixing_key: bfloat16 [1024], P(('dp', 'tensor')), may hold values from 0.049804688 to 0.94921875
- mixing_value: bfloat16 [1024], P(('dp', 'tensor')), may hold values from 0.049804688 to 0.94921875
- mixing_recept: bfloat16 [1024], P(('dp', 'tensor')), may hold values from 0.049804688 to 0.94921875
- time_decay: bfloat16 [1024], P(('dp', 'tensor')), as said below
- time_first: bfloat16 [1024], P(('dp', 'tensor')), may hold values from -0.5 to 1.5
- feeding_key: bfloat16 [1024], P(('dp', 'tensor')), may hold values from 0.049804688 to 0.94921875
- feeding_recept: bfloat16 [1024], P(('dp', 'tensor')), may hold values from 0.049804688 to 0.94921875
Outputs:
- result: float32 [2, 4, 1024, 1024], P(None, 'dp', 'tensor')
- token_grads: float32 [2, 4, 1024, 1024], P(None, 'dp', 'tensor')
- mixer_key_grad: float32 [1024, 1024], P(('dp', 'tensor'))
- mixer_value_grad: float32 [1024, 1024], P(('dp', 'tensor'))
- mixer_recept_grad: float32 [1024, 1024], P(('dp', 'tensor'))
- mixer_output_grad: float32 [1024, 1024], P(('dp', 'tensor'))
- feed_recept_grad: float32 [1024, 1024], P(('dp', 'tensor'))
- feed_key_grad: float32 [4096, 1024], P('tensor')
- feed_value_grad: float32 [4096, 1024], P('tensor')
- first_gain_grad: float32 [1024], P(('dp', 'tensor'))
- first_bias_grad: float32 [1024], P(('dp', 'tensor'))
- second_gain_grad: float32 [1024], P(('dp', 'tensor'))
- second_bias_grad: float32 [1024], P(('dp', 'tensor'))
- mixing_key_grad: float32 [1024], P(('dp', 'tensor'))
- mixing_value_grad: float32 [1024], P(('dp', 'tensor'))
- mixing_recept_grad: float32 [1024], P(('dp', 'tensor'))
- time_decay_grad: float32 [1024], P(('dp', 'tensor'))
- time_first_grad: float32 [1024], P(('dp', 'tensor'))
- feeding_key_grad: float32 [1024], P(('dp', 'tensor'))
- feeding_recept_grad: float32 [1024], P(('dp', 'tensor'))
The draws below stay inside these ranges and needn't reach their ends.
Inputs may be any that keep to these rules, and one draw needn't show every extreme that they name: `resets`: the first token of every row is 1; further document starts fall anywhere. exp(time_decay) lies between 0.05 / 1024 and 0.25.
All inputs are finite; a program needn't handle non-finite values.
Results may differ from the reference program's by a relative error of at most 0.012.
Values may be sent and summed in bfloat16 or wider, within the bound.
A program may use at most 320 MiB of HBM per device.

```python
import math
import jax
import jax.numpy as jnp
from jax import lax

D = 1024
FF = 4096
MICRO = 2
ROWS = 4
ROW_LEN = 1024


def draw_resets(key, part):
    shape = (MICRO, ROWS, ROW_LEN)
    marks = jax.random.randint(key, shape, 0, max(ROW_LEN // 4, 2))
    position = lax.broadcasted_iota(jnp.int32, shape, 2)
    return jnp.where((marks == 0) | (position == 0), 1, 0).astype(jnp.int32)


def draw_time_decay(key, part):
    first, second, third = jax.random.split(jax.random.fold_in(key, 7), 3)
    slow_share = 5
    choose_slow = jax.random.randint(first, (D,), 0, 10) < slow_share
    slow_log = jax.random.uniform(second, (D,), jnp.float32, math.log(0.05 / ROW_LEN), math.log(2.0 / ROW_LEN))
    fast_log = jax.random.uniform(third, (D,), jnp.float32, math.log(0.02), math.log(0.25))
    return jnp.where(choose_slow, slow_log, fast_log).astype(jnp.bfloat16)


def block_scale(own_key, shape, cuts, low, top_value):
    factor_of = 1.0
    for dim, shards_of in cuts:
        draws = jax.random.uniform(jax.random.fold_in(jax.random.fold_in(own_key, 6), dim), (shards_of,), jnp.float32, low / len(cuts), top_value / len(cuts))
        factor_of = factor_of * jnp.repeat(jnp.exp(draws), shape[dim] // shards_of).reshape((-1,) + (1,) * (len(shape) - 1 - dim))
    return factor_of


def gaussian(rng, extent, width, bound, cuts=(), dtype=jnp.bfloat16):
    array = jax.random.normal(rng, extent, jnp.float32) * width
    if len(cuts) > 0:
        array = block_scale(rng, extent, cuts, -0.22, 0.18) * array
    return jnp.clip(array, min=-bound, max=bound).astype(dtype)


def setup_inputs(seed: int = 0) -> dict:
    streams_of = jax.random.split(jax.random.key(seed), 22)
    return {
        "tokens": gaussian(streams_of[0], (MICRO, ROWS, ROW_LEN, D), 1.0, 6.0, ((1, 4), (2, 8))),
        "resets": draw_resets(jax.random.fold_in(streams_of[21], 71), 0),
        "out_grads": gaussian(streams_of[2], (MICRO, ROWS, ROW_LEN, D), 1.0, 6.0, ((1, 4), (2, 8))),
        "mixer_key": gaussian(streams_of[3], (D, D), D ** -0.5, 0.1875, ((0, 32),)),
        "mixer_value": gaussian(streams_of[4], (D, D), D ** -0.5, 0.1875, ((0, 32),)),
        "mixer_recept": gaussian(streams_of[5], (D, D), D ** -0.5, 0.1875, ((0, 32),)),
        "mixer_output": gaussian(streams_of[6], (D, D), (D // 64) ** -0.5, 1.5, ((0, 32),)),
        "feed_recept": gaussian(streams_of[7], (D, D), D ** -0.5, 0.1875, ((0, 32),)),
        "feed_key": gaussian(streams_of[8], (FF, D), D ** -0.5, 0.1875, ((0, 8),)),
        "feed_value": gaussian(streams_of[9], (FF, D), FF ** -0.5, 0.09375, ((0, 8),)),
        "first_gain": jnp.clip(1.0 + 0.18 * jax.random.normal(streams_of[10], (D,), jnp.float32), 0.099609375, 1.8984375).astype(jnp.bfloat16),
        "first_bias": gaussian(streams_of[11], (D,), 0.3, 3.0, ((0, 32),)),
        "second_gain": jnp.clip(1.0 + 0.18 * jax.random.normal(streams_of[12], (D,), jnp.float32), 0.099609375, 1.8984375).astype(jnp.bfloat16),
        "second_bias": gaussian(streams_of[13], (D,), 0.3, 3.0, ((0, 32),)),
        "mixing_key": jnp.clip(0.049804688 + 0.89941406 * jax.random.uniform(streams_of[14], (D,), jnp.float32) ** block_scale(streams_of[14], (D,), ((0, 32),), -0.2, 0.2), 0.049804688, 0.94921875).astype(jnp.bfloat16),
        "mixing_value": jnp.clip(0.049804688 + 0.89941406 * jax.random.uniform(streams_of[15], (D,), jnp.float32) ** block_scale(streams_of[15], (D,), ((0, 32),), -0.2, 0.2), 0.049804688, 0.94921875).astype(jnp.bfloat16),
        "mixing_recept": jnp.clip(0.049804688 + 0.89941406 * jax.random.uniform(streams_of[16], (D,), jnp.float32) ** block_scale(streams_of[16], (D,), ((0, 32),), -0.2, 0.2), 0.049804688, 0.94921875).astype(jnp.bfloat16),
        "time_decay": draw_time_decay(jax.random.fold_in(streams_of[21], 71), 0),
        "time_first": jnp.clip(-0.5 + 2.0 * jax.random.uniform(streams_of[18], (D,), jnp.float32) ** block_scale(streams_of[18], (D,), ((0, 32),), -0.2, 0.2), -0.5, 1.5).astype(jnp.bfloat16),
        "feeding_key": jnp.clip(0.049804688 + 0.89941406 * jax.random.uniform(streams_of[19], (D,), jnp.float32) ** block_scale(streams_of[19], (D,), ((0, 32),), -0.2, 0.2), 0.049804688, 0.94921875).astype(jnp.bfloat16),
        "feeding_recept": jnp.clip(0.049804688 + 0.89941406 * jax.random.uniform(streams_of[20], (D,), jnp.float32) ** block_scale(streams_of[20], (D,), ((0, 32),), -0.2, 0.2), 0.049804688, 0.94921875).astype(jnp.bfloat16),
    }


EPSILON = 1e-05

@jax.custom_vjp
def low(v):
    return lax.optimization_barrier(v.astype(jnp.bfloat16)).astype(jnp.float32)

@jax.custom_vjp
def low_back(v):
    return v

def low_keep(v):
    return (low(v), None)

def low_pass(kept, grad):
    return (grad,)

def back_keep(v):
    return (v, None)

def back_low(kept, grad):
    return (low(grad),)
low.defvjp(low_keep, low_pass)
low_back.defvjp(back_keep, back_low)

def norm_rows(payload_series, gain, bias):
    center = payload_series - lax.optimization_barrier(jnp.mean(payload_series, axis=-1, keepdims=True))
    inverse = lax.rsqrt(lax.optimization_barrier(jnp.mean(center * center, axis=-1, keepdims=True)) + EPSILON)
    return center * inverse * gain + bias

def shifted(payload_series, restart_retain_flags):
    earlier = jnp.concatenate([jnp.zeros_like(payload_series[:, :1]), payload_series[:, :-1]], axis=1)
    return earlier * restart_retain_flags

def matmul(left, right):
    return jnp.einsum('rld,de->rle', left, right, precision=lax.Precision.HIGHEST)

def scaled_lookup_payload_lines(lookup_series, payload_series, restart_retain_flags, fading_multiplier, opening_premium):

    def advance(carry, item):
        upper_running_state, lower_running_state = carry
        present_lookup, present_payload, retain_present = item
        premium_plus_lookup = jnp.exp(opening_premium + present_lookup)
        powered_lookup = jnp.exp(present_lookup)
        upper_quotient_part = retain_present * upper_running_state + premium_plus_lookup * present_payload
        lower_quotient_part = retain_present * lower_running_state + premium_plus_lookup
        next_a = retain_present * fading_multiplier * upper_running_state + powered_lookup * present_payload
        next_b = retain_present * fading_multiplier * lower_running_state + powered_lookup
        return ((next_a, next_b), upper_quotient_part / lower_quotient_part)
    zeros = jnp.zeros((lookup_series.shape[0], lookup_series.shape[2]), jnp.float32)
    items = (jnp.swapaxes(lookup_series, 0, 1), jnp.swapaxes(payload_series, 0, 1), jnp.swapaxes(restart_retain_flags, 0, 1))
    _, blended = lax.scan(advance, (zeros, zeros), items)
    return jnp.swapaxes(blended, 0, 1)

def forward(inputs, restart_retain_flags, params):
    mixer_key, mixer_value, mixer_recept, mixer_output, feed_recept, feed_key, feed_value, first_gain, first_bias, second_gain, second_bias, mixing_key, mixing_value, mixing_recept, time_decay, time_first, feeding_key, feeding_recept = params
    fading_multiplier = jnp.exp(-jnp.exp(time_decay))
    z_one = low(norm_rows(inputs, first_gain, first_bias))
    before_one = shifted(z_one, restart_retain_flags)
    in_key = low(z_one * mixing_key + before_one * (1.0 - mixing_key))
    in_value = low(z_one * mixing_value + before_one * (1.0 - mixing_value))
    in_recept = low(z_one * mixing_recept + before_one * (1.0 - mixing_recept))
    lookup_series = low_back(matmul(in_key, mixer_key))
    payload_series = low_back(matmul(in_value, mixer_value))
    recept = jax.nn.sigmoid(low_back(matmul(in_recept, mixer_recept)))
    blended = scaled_lookup_payload_lines(lookup_series, payload_series, restart_retain_flags, fading_multiplier, time_first)
    attention = low_back(matmul(low(recept * blended), mixer_output))
    residual = inputs + attention
    z_two = low(norm_rows(residual, second_gain, second_bias))
    before_two = shifted(z_two, restart_retain_flags)
    feed_in = low(z_two * feeding_key + before_two * (1.0 - feeding_key))
    feed_rin = low(z_two * feeding_recept + before_two * (1.0 - feeding_recept))
    hidden_pre = low_back(jnp.einsum('rld,fd->rlf', feed_in, feed_key, precision=lax.Precision.HIGHEST))
    hidden = low(jnp.square(jnp.maximum(hidden_pre, 0.0)))
    value_out = low_back(jnp.einsum('rlf,fd->rld', hidden, feed_value, precision=lax.Precision.HIGHEST))
    gate = jax.nn.sigmoid(low_back(matmul(feed_rin, feed_recept)))
    return residual + gate * value_out

def reference(tokens, resets, out_grads, mixer_key, mixer_value, mixer_recept, mixer_output, feed_recept, feed_key, feed_value, first_gain, first_bias, second_gain, second_bias, mixing_key, mixing_value, mixing_recept, time_decay, time_first, feeding_key, feeding_recept):
    params = tuple((item.astype(jnp.float32) for item in (mixer_key, mixer_value, mixer_recept, mixer_output, feed_recept, feed_key, feed_value, first_gain, first_bias, second_gain, second_bias, mixing_key, mixing_value, mixing_recept, time_decay, time_first, feeding_key, feeding_recept)))
    totals = [jnp.zeros(item.shape, jnp.float32) for item in params]
    results = []
    input_grads = []
    for micro_index in range(MICRO):
        inputs = tokens[micro_index].astype(jnp.float32)
        restart_retain_flags = (1 - resets[micro_index]).astype(jnp.float32)[..., None]

        def apply_block(block_in, *block_params):
            return forward(block_in, restart_retain_flags, block_params)
        output, pullback = jax.vjp(apply_block, inputs, *params)
        grads = pullback(out_grads[micro_index].astype(jnp.float32))
        results.append(output)
        input_grads.append(grads[0])
        totals = [total + grad for total, grad in zip(totals, grads[1:])]
    return (jnp.stack(results), jnp.stack(input_grads), totals[0], totals[1], totals[2], totals[3], totals[4], totals[5], totals[6], totals[7], totals[8], totals[9], totals[10], totals[11], totals[12], totals[13], totals[14], totals[15], totals[16], totals[17])
```

```python
import functools

import jax
import jax.numpy as jnp
from jax import lax
from jax.experimental import pallas as pl
from jax.experimental.pallas import tpu as pltpu
from jax.sharding import PartitionSpec as P

EPSILON = 1e-05


def entering(shard, axis, combine, identity, reverse):
    size, here = (lax.axis_size(axis), lax.axis_index(axis))
    everything = jax.tree.map(lambda part: lax.all_gather(part, axis), shard)
    start = jax.tree.map(
        lambda part, zero: jnp.broadcast_to(jnp.asarray(zero, part.dtype), part.shape),
        shard,
        identity,
    )

    def turn(k, before):
        at = size - 1 - k if reverse else k
        reached = at > here if reverse else at < here
        new = combine(before, jax.tree.map(lambda part: part[at], everything))
        return jax.tree.map(lambda a, b: jnp.where(reached, a, b), new, before)

    return lax.fori_loop(0, size, turn, start)


def shifted(block, axis, distance):
    devices = range(lax.axis_size(axis))
    route = [(i - distance, i) for i in devices if i - distance in devices]
    return lax.ppermute(block, axis, route)


def norm_rows(payload_series, gain, bias):
    center = payload_series - jnp.mean(payload_series, axis=-1, keepdims=True)
    inverse = lax.rsqrt(jnp.mean(center * center, axis=-1, keepdims=True) + EPSILON)
    normed = center * inverse
    return (normed * gain + bias, normed, inverse)


def norm_back(grad_out, normed, inverse, gain):
    scaled = grad_out * gain
    centred = scaled - jnp.mean(scaled, axis=-1, keepdims=True)
    grad_in = inverse * (centred - normed * jnp.mean(scaled * normed, axis=-1, keepdims=True))
    return (grad_in, jnp.sum(grad_out * normed, axis=0), jnp.sum(grad_out, axis=0))


def affine(earlier, later):
    return (
        earlier[0] * later[0],
        later[0] * earlier[1] + later[1],
        later[0] * earlier[2] + later[2],
    )


def carry_across(summary, backward):
    width = summary[0].shape[0]
    identity = (
        jnp.ones((width,), jnp.float32),
        jnp.zeros((width,), jnp.float32),
        jnp.zeros((width,), jnp.float32),
    )
    return entering(summary, "tensor", affine, identity, backward)


def matmul(left, right):
    return jnp.dot(left, right, preferred_element_type=jnp.float32)


def matmul_lead(left, right):
    return lax.dot_general(
        left, right, (((0,), (0,)), ((), ())), preferred_element_type=jnp.float32
    )


def matmul_last(left, right):
    return lax.dot_general(
        left, right, (((1,), (1,)), ((), ())), preferred_element_type=jnp.float32
    )


def shards(
    tokens,
    resets,
    out_grads,
    mixer_key,
    mixer_value,
    mixer_recept,
    mixer_output,
    feed_recept,
    feed_key,
    feed_value,
    first_gain,
    first_bias,
    second_gain,
    second_bias,
    mixing_key,
    mixing_value,
    mixing_recept,
    time_decay,
    time_first,
    feeding_key,
    feeding_recept,
):
    gathered = (
        lax.all_gather(mixer_key, ("dp", "tensor"), axis=0, tiled=True),
        lax.all_gather(mixer_value, ("dp", "tensor"), axis=0, tiled=True),
        lax.all_gather(mixer_recept, ("dp", "tensor"), axis=0, tiled=True),
        lax.all_gather(mixer_output, ("dp", "tensor"), axis=0, tiled=True),
        lax.all_gather(feed_recept, ("dp", "tensor"), axis=0, tiled=True),
        lax.all_gather(first_gain, ("dp", "tensor"), axis=0, tiled=True),
        lax.all_gather(first_bias, ("dp", "tensor"), axis=0, tiled=True),
        lax.all_gather(second_gain, ("dp", "tensor"), axis=0, tiled=True),
        lax.all_gather(second_bias, ("dp", "tensor"), axis=0, tiled=True),
        lax.all_gather(mixing_key, ("dp", "tensor"), axis=0, tiled=True),
        lax.all_gather(mixing_value, ("dp", "tensor"), axis=0, tiled=True),
        lax.all_gather(mixing_recept, ("dp", "tensor"), axis=0, tiled=True),
        lax.all_gather(time_decay, ("dp", "tensor"), axis=0, tiled=True),
        lax.all_gather(time_first, ("dp", "tensor"), axis=0, tiled=True),
        lax.all_gather(feeding_key, ("dp", "tensor"), axis=0, tiled=True),
        lax.all_gather(feeding_recept, ("dp", "tensor"), axis=0, tiled=True),
    )
    w_key, w_value, w_recept, w_output, w_feedr = (
        gathered[0],
        gathered[1],
        gathered[2],
        gathered[3],
        gathered[4],
    )
    parameter_vectors = [piece.astype(jnp.float32) for piece in gathered[5:]]
    gain_one, bias_one, gain_two, bias_two = (
        parameter_vectors[0],
        parameter_vectors[1],
        parameter_vectors[2],
        parameter_vectors[3],
    )
    mix_key, mix_value, mix_recept = (
        parameter_vectors[4],
        parameter_vectors[5],
        parameter_vectors[6],
    )
    (
        fading_speed_logarithm,
        opening_premium_logarithm,
        channel_lookup_blend,
        channel_gating_blend,
    ) = (parameter_vectors[7], parameter_vectors[8], parameter_vectors[9], parameter_vectors[10])
    rates = jnp.exp(fading_speed_logarithm)
    fading_multiplier = jnp.exp(-rates)
    micro_count = tokens.shape[0]
    width = tokens.shape[3]
    grad_keyw = jnp.zeros(feed_key.shape, jnp.float32)
    grad_valuew = jnp.zeros(feed_value.shape, jnp.float32)
    square_grads = [jnp.zeros((width, width), jnp.float32) for index_one in range(5)]
    parameter_vector_gradients = [jnp.zeros((width,), jnp.float32) for index_two in range(11)]
    results = []
    input_grads = []
    for micro_index in range(micro_count):
        inputs = tokens[micro_index, 0].astype(jnp.float32)
        restart_retain_flags = (1 - resets[micro_index, 0]).astype(jnp.float32)[:, None]
        cotangent = out_grads[micro_index, 0].astype(jnp.float32)
        normed_one, unit_one, inverse_one = norm_rows(inputs, gain_one, bias_one)
        z_one = normed_one.astype(jnp.bfloat16)
        prior_one = shifted(z_one[-1:], "tensor", 1)
        before_one = (
            jnp.concatenate([prior_one, z_one[:-1]], axis=0).astype(jnp.float32)
            * restart_retain_flags
        )
        z_onef = z_one.astype(jnp.float32)
        in_key = (z_onef * mix_key + before_one * (1.0 - mix_key)).astype(jnp.bfloat16)
        in_value = (z_onef * mix_value + before_one * (1.0 - mix_value)).astype(jnp.bfloat16)
        in_recept = (z_onef * mix_recept + before_one * (1.0 - mix_recept)).astype(jnp.bfloat16)
        lookup_series = matmul(in_key, w_key)
        payload_series = matmul(in_value, w_value)
        recept = jax.nn.sigmoid(matmul(in_recept, w_recept))
        powered_lookup = jnp.exp(lookup_series)
        premium_plus_lookup = jnp.exp(opening_premium_logarithm + lookup_series)
        factor = restart_retain_flags * fading_multiplier
        cum_factor, local_a, local_b = lax.associative_scan(
            affine, (factor, powered_lookup * payload_series, powered_lookup), axis=0
        )
        incoming = carry_across((cum_factor[-1], local_a[-1], local_b[-1]), False)
        upper_running_state = local_a + cum_factor * incoming[1]
        lower_running_state = local_b + cum_factor * incoming[2]
        earlier_upper_state = jnp.concatenate([incoming[1][None], upper_running_state[:-1]], axis=0)
        earlier_lower_state = jnp.concatenate([incoming[2][None], lower_running_state[:-1]], axis=0)
        lower_quotient_part = restart_retain_flags * earlier_lower_state + premium_plus_lookup
        blended = (
            restart_retain_flags * earlier_upper_state + premium_plus_lookup * payload_series
        ) / lower_quotient_part
        weighted = (recept * blended).astype(jnp.bfloat16)
        residual = inputs + matmul(weighted, w_output)
        normed_two, unit_two, inverse_two = norm_rows(residual, gain_two, bias_two)
        z_two = normed_two.astype(jnp.bfloat16)
        prior_two = shifted(z_two[-1:], "tensor", 1)
        before_two = (
            jnp.concatenate([prior_two, z_two[:-1]], axis=0).astype(jnp.float32)
            * restart_retain_flags
        )
        z_twof = z_two.astype(jnp.float32)
        feed_in = (
            z_twof * channel_lookup_blend + before_two * (1.0 - channel_lookup_blend)
        ).astype(jnp.bfloat16)
        feed_rin = (
            z_twof * channel_gating_blend + before_two * (1.0 - channel_gating_blend)
        ).astype(jnp.bfloat16)
        gate = jax.nn.sigmoid(matmul(feed_rin, w_feedr))
        all_in = lax.all_gather(feed_in, "tensor", axis=0, tiled=True)
        hidden_pre = matmul_last(feed_key, all_in)
        hidden = jnp.square(jnp.maximum(hidden_pre, 0.0)).astype(jnp.bfloat16)
        value_out = lax.psum_scatter(
            matmul_lead(hidden, feed_value), "tensor", scatter_dimension=0, tiled=True
        )
        results.append(residual + gate * value_out)
        grad_value = (cotangent * gate).astype(jnp.bfloat16)
        grad_gate = (cotangent * value_out * gate * (1.0 - gate)).astype(jnp.bfloat16)
        square_grads[4] = square_grads[4] + matmul_lead(feed_rin, grad_gate)
        grad_rin = matmul_last(grad_gate, w_feedr)
        relu_twice = 2.0 * jnp.maximum(hidden_pre, 0.0)
        add_piece = lax.all_gather(grad_value, "tensor", axis=0, tiled=True)
        rows_total = matmul(hidden, add_piece)
        block = matmul_last(feed_value, add_piece)
        grad_valuew = grad_valuew + rows_total
        grad_pre = (block * relu_twice).astype(jnp.bfloat16)
        grad_keyw = grad_keyw + matmul(grad_pre, all_in)
        grad_in = lax.psum_scatter(
            matmul_lead(grad_pre, feed_key), "tensor", scatter_dimension=0, tiled=True
        )
        parameter_vector_gradients[9] = parameter_vector_gradients[9] + jnp.sum(
            grad_in * (z_twof - before_two), axis=0
        )
        parameter_vector_gradients[10] = parameter_vector_gradients[10] + jnp.sum(
            grad_rin * (z_twof - before_two), axis=0
        )
        shift_two = restart_retain_flags * (
            grad_in * (1.0 - channel_lookup_blend) + grad_rin * (1.0 - channel_gating_blend)
        )
        after_two = shifted(shift_two[:1], "tensor", -1)
        grad_z_two = (
            grad_in * channel_lookup_blend
            + grad_rin * channel_gating_blend
            + jnp.concatenate([shift_two[1:], after_two], axis=0)
        )
        back_two, gain_part, bias_part = norm_back(grad_z_two, unit_two, inverse_two, gain_two)
        parameter_vector_gradients[2] = parameter_vector_gradients[2] + gain_part
        parameter_vector_gradients[3] = parameter_vector_gradients[3] + bias_part
        grad_residual = cotangent + back_two
        grad_att = grad_residual.astype(jnp.bfloat16)
        square_grads[3] = square_grads[3] + matmul_lead(weighted, grad_att)
        grad_weighted = matmul_last(grad_att, w_output)
        grad_mixed = grad_weighted * recept
        grad_recept = (grad_weighted * blended * recept * (1.0 - recept)).astype(jnp.bfloat16)
        upper_adjoint = grad_mixed / lower_quotient_part
        denominator_gradient = -grad_mixed * blended / lower_quotient_part
        cum_back, local_xa, local_xb = lax.associative_scan(
            affine,
            (
                factor,
                restart_retain_flags * upper_adjoint,
                restart_retain_flags * denominator_gradient,
            ),
            reverse=True,
            axis=0,
        )
        beyond = carry_across((cum_back[0], local_xa[0], local_xb[0]), True)
        adjoint_a = local_xa + cum_back * beyond[1]
        adjoint_b = local_xb + cum_back * beyond[2]
        running_upper_total = jnp.concatenate([adjoint_a[1:], beyond[1][None]], axis=0)
        running_lower_total = jnp.concatenate([adjoint_b[1:], beyond[2][None]], axis=0)
        premium_power = premium_plus_lookup * (
            payload_series * upper_adjoint + denominator_gradient
        )
        adjoint_payloads = (
            premium_plus_lookup * upper_adjoint + powered_lookup * running_upper_total
        ).astype(jnp.bfloat16)
        key_gradient_rows = (
            premium_power
            + powered_lookup * (payload_series * running_upper_total + running_lower_total)
        ).astype(jnp.bfloat16)
        parameter_vector_gradients[8] = parameter_vector_gradients[8] + jnp.sum(
            premium_power, axis=0
        )
        decay_sum = jnp.sum(
            restart_retain_flags
            * (
                running_upper_total * earlier_upper_state
                + running_lower_total * earlier_lower_state
            ),
            axis=0,
        )
        parameter_vector_gradients[7] = (
            parameter_vector_gradients[7] - rates * fading_multiplier * decay_sum
        )
        square_grads[0] = square_grads[0] + matmul_lead(in_key, key_gradient_rows)
        square_grads[1] = square_grads[1] + matmul_lead(in_value, adjoint_payloads)
        square_grads[2] = square_grads[2] + matmul_lead(in_recept, grad_recept)
        grad_inkey = matmul_last(key_gradient_rows, w_key)
        grad_invalue = matmul_last(adjoint_payloads, w_value)
        grad_inrecept = matmul_last(grad_recept, w_recept)
        spread_one = z_onef - before_one
        parameter_vector_gradients[4] = parameter_vector_gradients[4] + jnp.sum(
            grad_inkey * spread_one, axis=0
        )
        parameter_vector_gradients[5] = parameter_vector_gradients[5] + jnp.sum(
            grad_invalue * spread_one, axis=0
        )
        parameter_vector_gradients[6] = parameter_vector_gradients[6] + jnp.sum(
            grad_inrecept * spread_one, axis=0
        )
        shift_one = restart_retain_flags * (
            grad_inkey * (1.0 - mix_key)
            + grad_invalue * (1.0 - mix_value)
            + grad_inrecept * (1.0 - mix_recept)
        )
        after_one = shifted(shift_one[:1], "tensor", -1)
        grad_z_one = (
            grad_inkey * mix_key
            + grad_invalue * mix_value
            + grad_inrecept * mix_recept
            + jnp.concatenate([shift_one[1:], after_one], axis=0)
        )
        back_one, gain_first, bias_first = norm_back(grad_z_one, unit_one, inverse_one, gain_one)
        parameter_vector_gradients[0] = parameter_vector_gradients[0] + gain_first
        parameter_vector_gradients[1] = parameter_vector_gradients[1] + bias_first
        input_grads.append(grad_residual + back_one)
    owned = (
        lax.psum_scatter(square_grads[0], ("dp", "tensor"), scatter_dimension=0, tiled=True),
        lax.psum_scatter(square_grads[1], ("dp", "tensor"), scatter_dimension=0, tiled=True),
        lax.psum_scatter(square_grads[2], ("dp", "tensor"), scatter_dimension=0, tiled=True),
        lax.psum_scatter(square_grads[3], ("dp", "tensor"), scatter_dimension=0, tiled=True),
        lax.psum_scatter(square_grads[4], ("dp", "tensor"), scatter_dimension=0, tiled=True),
        lax.psum_scatter(
            parameter_vector_gradients[0], ("dp", "tensor"), scatter_dimension=0, tiled=True
        ),
        lax.psum_scatter(
            parameter_vector_gradients[1], ("dp", "tensor"), scatter_dimension=0, tiled=True
        ),
        lax.psum_scatter(
            parameter_vector_gradients[2], ("dp", "tensor"), scatter_dimension=0, tiled=True
        ),
        lax.psum_scatter(
            parameter_vector_gradients[3], ("dp", "tensor"), scatter_dimension=0, tiled=True
        ),
        lax.psum_scatter(
            parameter_vector_gradients[4], ("dp", "tensor"), scatter_dimension=0, tiled=True
        ),
        lax.psum_scatter(
            parameter_vector_gradients[5], ("dp", "tensor"), scatter_dimension=0, tiled=True
        ),
        lax.psum_scatter(
            parameter_vector_gradients[6], ("dp", "tensor"), scatter_dimension=0, tiled=True
        ),
        lax.psum_scatter(
            parameter_vector_gradients[7], ("dp", "tensor"), scatter_dimension=0, tiled=True
        ),
        lax.psum_scatter(
            parameter_vector_gradients[8], ("dp", "tensor"), scatter_dimension=0, tiled=True
        ),
        lax.psum_scatter(
            parameter_vector_gradients[9], ("dp", "tensor"), scatter_dimension=0, tiled=True
        ),
        lax.psum_scatter(
            parameter_vector_gradients[10], ("dp", "tensor"), scatter_dimension=0, tiled=True
        ),
    )
    key_rows, value_rows_grad = (grad_keyw, grad_valuew)
    key_total, value_total = (
        lax.psum(key_rows.astype(jnp.bfloat16), "dp").astype(jnp.float32),
        lax.psum(value_rows_grad.astype(jnp.bfloat16), "dp").astype(jnp.float32),
    )
    result_all = jnp.stack(results)[:, None]
    grads_all = jnp.stack(input_grads)[:, None]
    return (
        result_all,
        grads_all,
        owned[0],
        owned[1],
        owned[2],
        owned[3],
        owned[4],
        key_total,
        value_total,
        owned[5],
        owned[6],
        owned[7],
        owned[8],
        owned[9],
        owned[10],
        owned[11],
        owned[12],
        owned[13],
        owned[14],
        owned[15],
    )


BF = jnp.bfloat16
F32 = jnp.float32
BOTH = ("dp", "tensor")
MESH_ID = pl.DeviceIdType.MESH
DEVICES = [(x, c, z, y) for x in range(2) for c in range(2) for z in range(4) for y in range(2)]


def flat(x, c, z, y):
    return (x * 2 + c) * 8 + z * 2 + y


TO_CORE = [(flat(*d), flat(d[0], 1 - d[1], d[2], d[3])) for d in DEVICES]
TO_X = [(flat(*d), flat(1 - d[0], d[1], d[2], d[3])) for d in DEVICES]
TO_FIRST = [(flat(x, c, z, y), flat(x, c, z, 1 - y) if c == 0 else flat(1 - x, c, z, y)) for x, c, z, y in DEVICES]
TO_SECOND = [(flat(x, c, z, y), flat(x, c, z, 1 - y) if c == 1 else flat(1 - x, c, z, y)) for x, c, z, y in DEVICES]
TO_Z = [[(flat(x, c, z, y), flat(x, c, (z + o) % 4, y)) for x, c, z, y in DEVICES] for o in (1, 2, 3)]


def place():
    dp, t = lax.axis_index("dp"), lax.axis_index("tensor")
    return dp // 2, dp % 2, t // 2, t % 2


def cost(flops, moved):
    return pl.CostEstimate(flops=flops, bytes_accessed=moved, transcendentals=0)


def whole():
    return pl.BlockSpec(memory_space=pltpu.VMEM)


def anywhere():
    return pl.BlockSpec(memory_space=pl.ANY)


def gather_kernel(count, chunks, *refs):
    ins, outs = refs[:count], refs[count : 2 * count]
    send, recv, local_sem = refs[2 * count :]
    dp, t = lax.axis_index("dp"), lax.axis_index("tensor")
    x, c, z, y = dp // 2, dp % 2, t // 2, t % 2
    over_x, over_y, over_core = (1 - x) * 2 + c, z * 2 + 1 - y, x * 2 + 1 - c
    first = (jnp.where(c == 0, dp, over_x), jnp.where(c == 0, over_y, t))
    second = (jnp.where(c == 0, over_x, dp), jnp.where(c == 0, t, over_y))
    x_first, y_first = jnp.where(c == 0, x, 1 - x), jnp.where(c == 0, 1 - y, y)
    along_z = [(dp, lax.rem(z + o, 4) * 2 + y) for o in (1, 2, 3)]
    barrier = pltpu.get_barrier_semaphore()
    peers = along_z + [(over_x, t), (dp, over_y), (over_core, t)]
    for peer in peers:
        pl.semaphore_signal(barrier, inc=1, device_id=peer, device_id_type=MESH_ID)
    pl.semaphore_wait(barrier, len(peers))

    def copy(source, target, k, j, device):
        return pltpu.make_async_remote_copy(
            src_ref=source,
            dst_ref=target,
            send_sem=send.at[k, j],
            recv_sem=recv.at[k, j],
            device_id=device,
            device_id_type=MESH_ID,
        )

    copies = {}

    def begin(k, j, source, target, device):
        copies[k, j] = copy(source, target, k, j, device)
        copies[k, j].start()

    def column(k, xx, yy):
        i, start, rows = chunks[k]
        return outs[i].at[xx, c, :, yy, pl.ds(start, rows)]

    own = []
    for i in range(count):
        own.append(pltpu.make_async_copy(ins[i], outs[i].at[x, c, z, y], local_sem.at[i]))
        own[i].start()
    steps = len(chunks)
    for k in range(steps):
        i, start, rows = chunks[k]
        for o in range(3):
            begin(k, o, ins[i].at[pl.ds(start, rows)], outs[i].at[x, c, z, y, pl.ds(start, rows)], along_z[o])
    for i in range(count):
        own[i].wait()
    for s in range(steps + 2):
        if s < steps:
            for o in range(3):
                copies[s, o].wait_recv()
            begin(s, 3, column(s, x, y), column(s, x, y), first)
            begin(s, 4, column(s, x, y), column(s, x, y), second)
        if 0 <= s - 1 < steps:
            k = s - 1
            copies[k, 3].wait_recv()
            begin(k, 5, column(k, x_first, y_first), column(k, x_first, y_first), second)
        if 0 <= s - 2 < steps:
            k = s - 2
            i, start, rows = chunks[k]
            copies[k, 4].wait_recv()
            copies[k, 5].wait_recv()
            half = outs[i].at[:, c, :, :, pl.ds(start, rows)]
            begin(k, 6, half, half, (over_core, t))
    for k in range(steps):
        copies[k, 6].wait_recv()
    for k in range(steps):
        for j in range(7):
            copies[k, j].wait_send()


def gather(parts):
    count = len(parts)
    chunks = []
    for i, part in enumerate(parts):
        for start in range(0, part.shape[0], 16):
            chunks.append((i, start, 16))
    outs = [jax.ShapeDtypeStruct((2, 2, 4, 2) + p.shape, p.dtype) for p in parts]
    moved = sum(2 * 32 * p.size for p in parts)
    return pl.pallas_call(
        functools.partial(gather_kernel, count, chunks),
        out_shape=outs,
        in_specs=[anywhere()] * count,
        out_specs=[anywhere()] * count,
        scratch_shapes=[
            pltpu.SemaphoreType.DMA((len(chunks), 7)),
            pltpu.SemaphoreType.DMA((len(chunks), 7)),
            pltpu.SemaphoreType.DMA((count,)),
        ],
        compiler_params=pltpu.CompilerParams(collective_id=0, has_side_effects=True),
        cost_estimate=cost(0, 8 * moved),
        name="gather",
    )(*parts)


def roll_rows(value, distance, fill, row):
    size = value.shape[0]
    moved = pltpu.roll(value, distance % size, 0)
    outside = row < distance if distance > 0 else row >= size + distance
    return jnp.where(outside, fill, moved)


def doubling(factor, up, low, row, sign):
    size, step = factor.shape[0], 1
    while step < size:
        up = up + factor * roll_rows(up, sign * step, 0.0, row)
        low = low + factor * roll_rows(low, sign * step, 0.0, row)
        factor = factor * roll_rows(factor, sign * step, 1.0, row)
        step *= 2
    return factor, up, low


def greet_row(t, dp, size):
    barrier = pltpu.get_barrier_semaphore()
    for o in range(1, size):
        pl.semaphore_signal(barrier, inc=1, device_id=(dp, lax.rem(t + o, size)), device_id_type=MESH_ID)
    pl.semaphore_wait(barrier, size - 1)


def share_row(summary, arrived, send, recv, t, dp, size):
    copies = []
    for o in range(1, size):
        copies.append(
            pltpu.make_async_remote_copy(
                src_ref=summary,
                dst_ref=arrived.at[o],
                send_sem=send.at[o],
                recv_sem=recv.at[o],
                device_id=(dp, lax.rem(t + o, size)),
                device_id_type=MESH_ID,
            )
        )
        copies[-1].start()
    for copy in copies:
        copy.wait_recv()
    return copies


def lanes(j):
    return pl.ds(pl.multiple_of(j * 128, 128), 128)


def forward_scan_kernel(
    keys, values, gates, keep, vectors, weighted, denom, mixed, prior_a, prior_b, recept,
    cum, up, low, summary, arrived, entering_rows, send, recv,
):
    dp, t = lax.axis_index("dp"), lax.axis_index("tensor")
    size = arrived.shape[0]
    micro, rows = keys.shape[:2]
    greet_row(t, dp, size)
    row = lax.broadcasted_iota(jnp.int32, (rows, 128), 0)
    summary[...] = jnp.zeros_like(summary)
    for m in range(micro):

        def first_pass(j, carry, m=m):
            at = lanes(j)
            power = jnp.exp(keys[m, :, at])
            factor = keep[m] * vectors[0:1, at]
            f, a, b = doubling(factor, power * values[m, :, at], power, row, 1)
            cum[m, :, at] = f
            up[m, :, at] = a
            low[m, :, at] = b
            summary[3 * m : 3 * m + 1, at] = f[rows - 1 :]
            summary[3 * m + 1 : 3 * m + 2, at] = a[rows - 1 :]
            summary[3 * m + 2 : 3 * m + 3, at] = b[rows - 1 :]
            return carry

        lax.fori_loop(0, keys.shape[2] // 128, first_pass, 0)
    copies = share_row(summary, arrived, send, recv, t, dp, size)
    for m in range(micro):
        a = jnp.zeros((1, keys.shape[2]), F32)
        b = jnp.zeros((1, keys.shape[2]), F32)
        for o in range(size - 1, 0, -1):
            f = arrived[o, 3 * m : 3 * m + 1]
            a = jnp.where(t >= o, f * a + arrived[o, 3 * m + 1 : 3 * m + 2], a)
            b = jnp.where(t >= o, f * b + arrived[o, 3 * m + 2 : 3 * m + 3], b)
        entering_rows[2 * m : 2 * m + 1] = a
        entering_rows[2 * m + 1 : 2 * m + 2] = b
    for m in range(micro):

        def second_pass(j, carry, m=m):
            at = lanes(j)
            enter_a = entering_rows[2 * m : 2 * m + 1, at]
            enter_b = entering_rows[2 * m + 1 : 2 * m + 2, at]
            f = cum[m, :, at]
            before_a = roll_rows(up[m, :, at] + f * enter_a, 1, enter_a, row)
            before_b = roll_rows(low[m, :, at] + f * enter_b, 1, enter_b, row)
            bonus = jnp.exp(vectors[1:2, at] + keys[m, :, at])
            below = keep[m] * before_b + bonus
            blended = (keep[m] * before_a + bonus * values[m, :, at]) / below
            gate = jax.nn.sigmoid(gates[m, :, at])
            weighted[m, :, at] = (gate * blended).astype(BF)
            denom[m, :, at] = below
            mixed[m, :, at] = blended
            prior_a[m, :, at] = before_a
            prior_b[m, :, at] = before_b
            recept[m, :, at] = gate
            return carry

        lax.fori_loop(0, keys.shape[2] // 128, second_pass, 0)
    for copy in copies:
        copy.wait_send()


def scan_scratch(shape, size):
    width = shape[-1]
    return [
        pltpu.VMEM(shape, F32),
        pltpu.VMEM(shape, F32),
        pltpu.VMEM(shape, F32),
        pltpu.VMEM((8, width), F32),
        pltpu.VMEM((size, 8, width), F32),
        pltpu.VMEM((8, width), F32),
        pltpu.SemaphoreType.DMA((size,)),
        pltpu.SemaphoreType.DMA((size,)),
    ]


def forward_scan(keys, values, gates, keep, vectors, size):
    shape = keys.shape
    full = jax.ShapeDtypeStruct(shape, F32)
    return pl.pallas_call(
        forward_scan_kernel,
        out_shape=[jax.ShapeDtypeStruct(shape, BF)] + [full] * 5,
        in_specs=[whole()] * 5,
        out_specs=[whole()] * 6,
        scratch_shapes=scan_scratch(shape, size),
        compiler_params=pltpu.CompilerParams(collective_id=1, has_side_effects=True),
        cost_estimate=cost(100 * keys.size, 36 * keys.size),
        name="forward_scan",
    )(keys, values, gates, keep, vectors)


def backward_scan_kernel(
    grads, keys, values, denom, mixed, prior_a, prior_b, recept, keep, vectors,
    grad_keys, grad_values, grad_recept, sums,
    cum, up, low, summary, arrived, entering_rows, send, recv,
):
    dp, t = lax.axis_index("dp"), lax.axis_index("tensor")
    size = arrived.shape[0]
    micro, rows = keys.shape[:2]
    greet_row(t, dp, size)
    row = lax.broadcasted_iota(jnp.int32, (rows, 128), 0)
    summary[...] = jnp.zeros_like(summary)
    sums[...] = jnp.zeros_like(sums)

    def quotient_grads(m, at):
        gate = recept[m, :, at]
        blended = mixed[m, :, at]
        inner = grads[m, :, at] * gate
        above = inner / denom[m, :, at]
        return above, -above * blended, inner * blended * (1.0 - gate)

    for m in range(micro):

        def first_pass(j, carry, m=m):
            at = lanes(j)
            above, below, rec = quotient_grads(m, at)
            grad_recept[m, :, at] = rec.astype(BF)
            factor = keep[m] * vectors[0:1, at]
            f, a, b = doubling(factor, keep[m] * above, keep[m] * below, row, -1)
            cum[m, :, at] = f
            up[m, :, at] = a
            low[m, :, at] = b
            summary[3 * m : 3 * m + 1, at] = f[:1]
            summary[3 * m + 1 : 3 * m + 2, at] = a[:1]
            summary[3 * m + 2 : 3 * m + 3, at] = b[:1]
            return carry

        lax.fori_loop(0, keys.shape[2] // 128, first_pass, 0)
    copies = share_row(summary, arrived, send, recv, t, dp, size)
    for m in range(micro):
        a = jnp.zeros((1, keys.shape[2]), F32)
        b = jnp.zeros((1, keys.shape[2]), F32)
        for ahead in range(size - 1, 0, -1):
            o = size - ahead
            f = arrived[o, 3 * m : 3 * m + 1]
            a = jnp.where(t + ahead < size, f * a + arrived[o, 3 * m + 1 : 3 * m + 2], a)
            b = jnp.where(t + ahead < size, f * b + arrived[o, 3 * m + 2 : 3 * m + 3], b)
        entering_rows[2 * m : 2 * m + 1] = a
        entering_rows[2 * m + 1 : 2 * m + 2] = b
    for m in range(micro):

        def second_pass(j, carry, m=m):
            at = lanes(j)
            enter_a = entering_rows[2 * m : 2 * m + 1, at]
            enter_b = entering_rows[2 * m + 1 : 2 * m + 2, at]
            f = cum[m, :, at]
            alpha = roll_rows(up[m, :, at] + f * enter_a, -1, enter_a, row)
            beta = roll_rows(low[m, :, at] + f * enter_b, -1, enter_b, row)
            above, below, _ = quotient_grads(m, at)
            power = jnp.exp(keys[m, :, at])
            bonus = jnp.exp(vectors[1:2, at] + keys[m, :, at])
            premium = bonus * (values[m, :, at] * above + below)
            grad_values[m, :, at] = (bonus * above + power * alpha).astype(BF)
            grad_keys[m, :, at] = (premium + power * (values[m, :, at] * alpha + beta)).astype(BF)
            fading = keep[m] * (alpha * prior_a[m, :, at] + beta * prior_b[m, :, at])
            sums[0:1, at] += jnp.sum(premium, axis=0, keepdims=True)
            sums[1:2, at] += jnp.sum(fading, axis=0, keepdims=True)
            return carry

        lax.fori_loop(0, keys.shape[2] // 128, second_pass, 0)
    for copy in copies:
        copy.wait_send()


def backward_scan(grads, keys, values, denom, mixed, prior_a, prior_b, recept, keep, vectors, size):
    shape = keys.shape
    half = jax.ShapeDtypeStruct(shape, BF)
    return pl.pallas_call(
        backward_scan_kernel,
        out_shape=[half, half, half, jax.ShapeDtypeStruct((8, shape[-1]), F32)],
        in_specs=[whole()] * 10,
        out_specs=[whole()] * 4,
        scratch_shapes=scan_scratch(shape, size),
        compiler_params=pltpu.CompilerParams(collective_id=2, has_side_effects=True),
        cost_estimate=cost(100 * keys.size, 38 * keys.size),
        name="backward_scan",
    )(grads, keys, values, denom, mixed, prior_a, prior_b, recept, keep, vectors)


def channel_forward_kernel(feed_in, key_block, value_block, positive, total):
    rows = 4 * key_block.shape[-2]
    keys = key_block[...].reshape(rows, key_block.shape[-1])
    hidden = jnp.maximum(matmul_last(feed_in[...], keys), 0.0)
    positive[0] = hidden
    squares = (hidden * hidden).astype(BF)
    part = matmul(squares, value_block[...].reshape(rows, value_block.shape[-1]))

    @pl.when(pl.program_id(0) == 0)
    def _():
        total[...] = part

    @pl.when(pl.program_id(0) > 0)
    def _():
        total[...] += part


def channel_forward(feed_in, weights):
    tokens, width = feed_in.shape
    rows = weights.shape[4]
    units = 32 * rows

    def block(side):
        return pl.BlockSpec((1, 1, 4, 1, rows, width), lambda i: (i // 4, (i // 2) % 2, 0, i % 2, 0, side))

    return pl.pallas_call(
        channel_forward_kernel,
        grid=(8,),
        out_shape=[jax.ShapeDtypeStruct((8, tokens, 4 * rows), F32), jax.ShapeDtypeStruct((tokens, width), F32)],
        in_specs=[pl.BlockSpec((tokens, width), lambda i: (0, 0)), block(0), block(1)],
        out_specs=[
            pl.BlockSpec((1, tokens, 4 * rows), lambda i: (i, 0, 0)),
            pl.BlockSpec((tokens, width), lambda i: (0, 0)),
        ],
        cost_estimate=cost(4 * tokens * units * width, 4 * units * width + 4 * tokens * units),
        name="channel_forward",
    )(feed_in, weights, weights)


def channel_backward_kernel(here, feed_in, grad_value, positive, start, key_block, value_block, key_grad, value_grad, total):
    rows = key_block.shape[-2]
    width = key_block.shape[-1]
    keys = key_block[...].reshape(4 * rows, width)
    weights = value_block[...].reshape(4 * rows, width)
    hidden = positive[0]
    squares = (hidden * hidden).astype(BF)
    value_part = matmul_lead(squares, grad_value[...]).astype(BF)
    grad_pre = (matmul_last(grad_value[...], weights) * (2.0 * hidden)).astype(BF)
    key_part = matmul_lead(grad_pre, feed_in[...]).astype(BF)
    part = matmul(grad_pre, keys)
    for k in range(4):
        at = lax.rem(k + 4 - here[3], 4)
        value_grad[0, at] = value_part[k * rows : (k + 1) * rows]
        key_grad[0, at] = key_part[k * rows : (k + 1) * rows]

    @pl.when(pl.program_id(0) == 0)
    def _():
        total[...] = start[...] + part

    @pl.when(pl.program_id(0) > 0)
    def _():
        total[...] += part


def owner(i, here, c):
    first, second = i // 2, i % 2
    x, y = here[0], here[2]
    flip_x = first * c + second * (1 - c)
    flip_y = first * (1 - c) + second * c
    return x + flip_x - 2 * x * flip_x, y + flip_y - 2 * y * flip_y


def channel_backward(here, feed_in, grad_value, positive, start, weights, own):
    tokens, width = feed_in.shape
    rows = weights.shape[4]

    def side_of(here):
        return here[1] if own else 1 - here[1]

    def block(side):
        def at(i, here):
            x, y = owner(i, here, side_of(here))
            return (x, side_of(here), 0, y, 0, side)

        return pl.BlockSpec((1, 1, 4, 1, rows, width), at)

    def saved(i, here):
        x, y = owner(i, here, side_of(here))
        return (x * 4 + side_of(here) * 2 + y, 0, 0)

    full = pl.BlockSpec((tokens, width), lambda i, here: (0, 0))
    grads = jax.ShapeDtypeStruct((4, 4, rows, width), BF)
    grads_spec = pl.BlockSpec((1, 4, rows, width), lambda i, here: (i, 0, 0, 0))
    return pl.pallas_call(
        channel_backward_kernel,
        out_shape=[grads, grads, jax.ShapeDtypeStruct((tokens, width), F32)],
        grid_spec=pltpu.PrefetchScalarGridSpec(
            num_scalar_prefetch=1,
            grid=(4,),
            in_specs=[full, full, pl.BlockSpec((1, tokens, 4 * rows), saved), full, block(0), block(1)],
            out_specs=[grads_spec, grads_spec, full],
        ),
        cost_estimate=cost(8 * tokens * 16 * rows * width, 8 * 16 * rows * width),
        name="channel_backward_own" if own else "channel_backward_other",
    )(here, feed_in, grad_value, positive, start, weights, weights)


def weight_grad_kernel(here, left, right, other, own, total):
    width = left.shape[-1]
    tile = 256

    def turn(j, carry):
        at = pl.multiple_of(j * tile, tile)
        total[pl.ds(at, tile), :] = matmul_lead(left[0, :, pl.ds(at, tile)], right[0])
        return carry

    lax.fori_loop(0, width // tile, turn, 0)
    rows = width // 32
    for i in range(4):
        for target, c in ((own, here[1]), (other, 1 - here[1])):
            x, y = owner(i, here, c)
            for o in range(4):
                z = lax.rem(here[3] + o, 4)
                at = pl.multiple_of((x * 16 + c * 8 + z * 2 + y) * rows, rows)
                target[0, i, o] = total[pl.ds(at, rows), :].astype(BF)


def weight_grads(here, lefts, rights):
    count = len(lefts)
    left, right = jnp.stack(lefts), jnp.stack(rights)
    tokens, width = left.shape[1:]
    out = jax.ShapeDtypeStruct((count, 4, 4, width // 32, width), BF)
    spec = pl.BlockSpec((1, tokens, width), lambda i, here: (i, 0, 0))
    out_spec = pl.BlockSpec((1, 4, 4, width // 32, width), lambda i, here: (i, 0, 0, 0, 0))
    return pl.pallas_call(
        weight_grad_kernel,
        out_shape=[out, out],
        grid_spec=pltpu.PrefetchScalarGridSpec(
            num_scalar_prefetch=1,
            grid=(count,),
            in_specs=[spec, spec],
            out_specs=[out_spec, out_spec],
            scratch_shapes=[pltpu.VMEM((width, width), F32)],
        ),
        cost_estimate=cost(2 * count * tokens * width * width, 2 * count * width * width),
        name="weight_grads",
    )(here, left, right)


def permute(value, route):
    return lax.ppermute(value, BOTH, route)


def reduce_to_owner(other, own):
    shape = (own.shape[0], 2, 2) + own.shape[2:]
    other, own = other.reshape(shape), own.reshape(shape)
    wide = lambda v: v.astype(F32)
    from_core = permute(other, TO_CORE)
    from_first = permute((wide(own[:, 1]) + wide(from_core[:, 1])).astype(BF), TO_FIRST)
    kept = wide(own[:, 0]) + wide(from_core[:, 0]) + wide(from_first)
    from_second = permute(kept[:, 1].astype(BF), TO_SECOND)
    kept = kept[:, 0] + wide(from_second)
    total = kept[:, 0]
    for o in (1, 2, 3):
        total = total + wide(permute(kept[:, o].astype(BF), TO_Z[o - 1]))
    return total


def vector_sum_kernel(part, total, held, send, recv):
    dp, t = lax.axis_index("dp"), lax.axis_index("tensor")
    x, c, z, y = dp // 2, dp % 2, t // 2, t % 2
    stages = [
        [(x * 2 + 1 - c, t)],
        [((1 - x) * 2 + c, t)],
        [(dp, z * 2 + 1 - y)],
        [(dp, lax.rem(z + o, 4) * 2 + y) for o in (1, 2, 3)],
    ]
    barrier = pltpu.get_barrier_semaphore()
    for stage in stages:
        for peer in stage:
            pl.semaphore_signal(barrier, inc=1, device_id=peer, device_id_type=MESH_ID)
    pl.semaphore_wait(barrier, 6)
    slot = 0
    sending = []
    source = part
    for s, stage in enumerate(stages):
        copies = []
        for peer in stage:
            copies.append(
                pltpu.make_async_remote_copy(
                    src_ref=source,
                    dst_ref=held.at[slot],
                    send_sem=send.at[slot],
                    recv_sem=recv.at[slot],
                    device_id=peer,
                    device_id_type=MESH_ID,
                )
            )
            copies[-1].start()
            slot += 1
        value = source[...]
        for i, copy in enumerate(copies):
            copy.wait_recv()
            value = value + held[slot - len(copies) + i]
        sending += copies
        if s < len(stages) - 1:
            held[6 + s] = value
            source = held.at[6 + s]
        else:
            total[...] = value
    for copy in sending:
        copy.wait_send()


def vector_sum(part):
    return pl.pallas_call(
        vector_sum_kernel,
        out_shape=jax.ShapeDtypeStruct(part.shape, F32),
        in_specs=[whole()],
        out_specs=whole(),
        scratch_shapes=[
            pltpu.VMEM((9,) + part.shape, F32),
            pltpu.SemaphoreType.DMA((6,)),
            pltpu.SemaphoreType.DMA((6,)),
        ],
        compiler_params=pltpu.CompilerParams(collective_id=3, has_side_effects=True),
        cost_estimate=cost(0, 4 * 16 * part.size),
        name="vector_sum",
    )(part)


def along_row(block, distance):
    return shifted(block, "tensor", distance)


def with_prior(value, prior):
    return jnp.concatenate([prior, value[:, :-1]], axis=1)


def with_next(value, following):
    return jnp.concatenate([value[:, 1:], following], axis=1)


def norm_back_rows(grad_out, normed, inverse, gain):
    scaled = grad_out * gain
    centred = scaled - jnp.mean(scaled, axis=-1, keepdims=True)
    grad_in = inverse * (centred - normed * jnp.mean(scaled * normed, axis=-1, keepdims=True))
    return grad_in, jnp.sum(grad_out * normed, axis=(0, 1)), jnp.sum(grad_out, axis=(0, 1))


def local_shards(tokens, resets, out_grads, *weights):
    (
        mixer_key, mixer_value, mixer_recept, mixer_output, feed_recept, feed_key, feed_value, *vector_shards
    ) = weights
    size = lax.axis_size("tensor")
    dp, t = lax.axis_index("dp"), lax.axis_index("tensor")
    x, c, z, y = place()
    here = jnp.stack([x, c, y, z]).astype(jnp.int32)
    micro, _, length, width = tokens.shape
    count = micro * length
    wide = lambda v: v.astype(F32)

    unit_rows = feed_key.shape[0] // 4
    feed_shard = jnp.concatenate(
        [lax.dynamic_slice_in_dim(w, dp * unit_rows, unit_rows, 0) for w in (feed_key, feed_value)], axis=1
    )
    feed = lax.all_gather(feed_shard, BOTH, axis=0, tiled=True).reshape(2, 2, 4, 2, unit_rows, 2 * width)
    share = vector_shards[0].shape[0]
    vector_pack = jnp.pad(jnp.stack(vector_shards), ((0, 16 - len(vector_shards)), (0, 128 - share)))
    token_block = tokens[:, 0]
    last_token = along_row(token_block[:, -1:], 1)
    packed, *squares = gather([vector_pack, mixer_key, mixer_value, mixer_recept, mixer_output, feed_recept])
    w_key, w_value, w_recept, w_output, w_feedr = [w.reshape(width, width) for w in squares]
    vectors = wide(packed.reshape(32, 16, 128)[:, : len(vector_shards), :share].transpose(1, 0, 2).reshape(-1, width))
    (
        gain_one, bias_one, gain_two, bias_two, mix_key, mix_value, mix_recept, fading, premium, blend_key, blend_recept
    ) = [vectors[i] for i in range(len(vector_shards))]
    rates = jnp.exp(fading)
    decay = jnp.exp(-rates)
    scan_vectors = jnp.pad(jnp.stack([decay, premium]), ((0, 6), (0, 0)))

    inputs = wide(token_block)
    cotangent = wide(out_grads[:, 0])
    keep = wide(1 - resets[:, 0])[:, :, None]
    keep_lanes = jnp.broadcast_to(keep, (micro, length, 128))
    normed_one, unit_one, inverse_one = norm_rows(inputs, gain_one, bias_one)
    z_one = wide(normed_one.astype(BF))
    prior_one = wide(norm_rows(wide(last_token), gain_one, bias_one)[0].astype(BF))
    before_one = with_prior(z_one, prior_one) * keep
    blend = lambda z, before, mix: (z * mix + before * (1.0 - mix)).astype(BF)
    in_key, in_value, in_recept = [
        blend(z_one, before_one, m).reshape(count, width) for m in (mix_key, mix_value, mix_recept)
    ]
    cube = (micro, length, width)
    keys = matmul(in_key, w_key).reshape(cube)
    values = matmul(in_value, w_value).reshape(cube)
    gates = matmul(in_recept, w_recept).reshape(cube)
    weighted, denom, mixed, prior_a, prior_b, recept = forward_scan(keys, values, gates, keep_lanes, scan_vectors, size)
    weighted = weighted.reshape(count, width)
    residual = inputs + matmul(weighted, w_output).reshape(cube)

    normed_two, unit_two, inverse_two = norm_rows(residual, gain_two, bias_two)
    low_two = normed_two.astype(BF)
    z_two = wide(low_two)
    before_two = with_prior(z_two, wide(along_row(low_two[:, -1:], 1))) * keep
    feed_in = blend(z_two, before_two, blend_key).reshape(count, width)
    feed_rin = blend(z_two, before_two, blend_recept).reshape(count, width)
    gate = jax.nn.sigmoid(matmul(feed_rin, w_feedr)).reshape(cube)
    positive, value_out = channel_forward(feed_in, feed)
    value_out = value_out.reshape(cube)
    result = residual + gate * value_out

    grad_value = (cotangent * gate).astype(BF).reshape(count, width)
    grad_gate = (cotangent * value_out * gate * (1.0 - gate)).astype(BF).reshape(count, width)
    nothing = jnp.zeros((count, width), F32)
    key_other, value_other, partial = channel_backward(here, feed_in, grad_value, positive, nothing, feed, False)
    key_own, value_own, grad_in = channel_backward(here, feed_in, grad_value, positive, partial, feed, True)
    value_total = reduce_to_owner(value_other[None], value_own[None])[0]
    key_total = reduce_to_owner(key_other[None], key_own[None])[0]
    grad_in = grad_in.reshape(cube)
    grad_rin = matmul_last(grad_gate, w_feedr).reshape(cube)
    spread_two = z_two - before_two
    blend_key_grad = jnp.sum(grad_in * spread_two, axis=(0, 1))
    blend_recept_grad = jnp.sum(grad_rin * spread_two, axis=(0, 1))
    shift_two = keep * (grad_in * (1.0 - blend_key) + grad_rin * (1.0 - blend_recept))
    after_two = along_row(shift_two[:, :1], -1)
    grad_z_two = grad_in * blend_key + grad_rin * blend_recept + with_next(shift_two, after_two)
    back_two, gain_two_grad, bias_two_grad = norm_back_rows(grad_z_two, unit_two, inverse_two, gain_two)
    grad_residual = cotangent + back_two
    grad_att = grad_residual.astype(BF).reshape(count, width)

    middle = reduce_to_owner(*weight_grads(here, [feed_rin, weighted], [grad_gate, grad_att]))
    grad_weighted = matmul_last(grad_att, w_output).reshape(cube)
    grad_keys, grad_values, grad_recept, sums = backward_scan(
        grad_weighted, keys, values, denom, mixed, prior_a, prior_b, recept, keep_lanes, scan_vectors, size
    )
    grad_keys, grad_values, grad_recept = [g.reshape(count, width) for g in (grad_keys, grad_values, grad_recept)]
    front = reduce_to_owner(
        *weight_grads(here, [in_key, in_value, in_recept], [grad_keys, grad_values, grad_recept])
    )
    grad_inkey = matmul_last(grad_keys, w_key).reshape(cube)
    grad_invalue = matmul_last(grad_values, w_value).reshape(cube)
    grad_inrecept = matmul_last(grad_recept, w_recept).reshape(cube)
    spread_one = z_one - before_one
    mix_grads = [jnp.sum(g * spread_one, axis=(0, 1)) for g in (grad_inkey, grad_invalue, grad_inrecept)]
    shift_one = keep * (
        grad_inkey * (1.0 - mix_key) + grad_invalue * (1.0 - mix_value) + grad_inrecept * (1.0 - mix_recept)
    )
    after_one = along_row(shift_one[:, :1], -1)
    grad_z_one = (
        grad_inkey * mix_key
        + grad_invalue * mix_value
        + grad_inrecept * mix_recept
        + with_next(shift_one, after_one)
    )
    back_one, gain_one_grad, bias_one_grad = norm_back_rows(grad_z_one, unit_one, inverse_one, gain_one)
    token_grads = grad_residual + back_one

    vector_parts = [
        gain_one_grad, bias_one_grad, gain_two_grad, bias_two_grad, *mix_grads,
        -rates * decay * sums[1], sums[0], blend_key_grad, blend_recept_grad,
    ]
    summed = vector_sum(jnp.pad(jnp.stack(vector_parts), ((0, 16 - len(vector_parts)), (0, 0))))
    mine = lax.dynamic_slice_in_dim(summed, (dp * size + t) * share, share, 1)

    own_units = jnp.stack([key_total, value_total]).astype(BF)
    x_units = permute(own_units, TO_X)
    core_units = permute(jnp.stack([own_units, x_units]), TO_CORE)
    unit_grads = []
    for i in range(2):
        blocks = []
        for d in range(4):
            pick = jnp.where(dp == d ^ 1, core_units[0, i], core_units[1, i])
            pick = jnp.where(dp == d ^ 2, x_units[i], pick)
            blocks.append(wide(jnp.where(dp == d, own_units[i], pick)))
        unit_grads.append(jnp.concatenate(blocks, axis=0))
    return (
        result[:, None], token_grads[:, None],
        front[0], front[1], front[2], middle[1], middle[0], unit_grads[0], unit_grads[1],
    ) + tuple(mine[i] for i in range(len(vector_parts)))


def is_two_by_two_by_four(mesh):
    return mesh.shape["dp"] == 4 and mesh.shape["tensor"] == 8


def solution(mesh):
    return jax.shard_map(
        local_shards if is_two_by_two_by_four(mesh) else shards,
        mesh=mesh,
        in_specs=(
            P(None, "dp", "tensor", None),
            P(None, "dp", "tensor"),
            P(None, "dp", "tensor", None),
            P(("dp", "tensor"), None),
            P(("dp", "tensor"), None),
            P(("dp", "tensor"), None),
            P(("dp", "tensor"), None),
            P(("dp", "tensor"), None),
            P("tensor", None),
            P("tensor", None),
            P(("dp", "tensor")),
            P(("dp", "tensor")),
            P(("dp", "tensor")),
            P(("dp", "tensor")),
            P(("dp", "tensor")),
            P(("dp", "tensor")),
            P(("dp", "tensor")),
            P(("dp", "tensor")),
            P(("dp", "tensor")),
            P(("dp", "tensor")),
            P(("dp", "tensor")),
        ),
        out_specs=(
            P(None, "dp", "tensor", None),
            P(None, "dp", "tensor", None),
            P(("dp", "tensor"), None),
            P(("dp", "tensor"), None),
            P(("dp", "tensor"), None),
            P(("dp", "tensor"), None),
            P(("dp", "tensor"), None),
            P("tensor", None),
            P("tensor", None),
            P(("dp", "tensor")),
            P(("dp", "tensor")),
            P(("dp", "tensor")),
            P(("dp", "tensor")),
            P(("dp", "tensor")),
            P(("dp", "tensor")),
            P(("dp", "tensor")),
            P(("dp", "tensor")),
            P(("dp", "tensor")),
            P(("dp", "tensor")),
            P(("dp", "tensor")),
        ),
        check_vma=False,
    )
```

```python
import functools

import jax
import jax.numpy as jnp
from jax import lax
from jax.experimental import pallas as pl
from jax.experimental.pallas import tpu as pltpu
from jax.sharding import PartitionSpec as P

EPSILON = 1e-05


def entering(shard, axis, combine, identity, reverse):
    size, here = (lax.axis_size(axis), lax.axis_index(axis))
    everything = jax.tree.map(lambda part: lax.all_gather(part, axis), shard)
    start = jax.tree.map(
        lambda part, zero: jnp.broadcast_to(jnp.asarray(zero, part.dtype), part.shape),
        shard,
        identity,
    )

    def turn(k, before):
        at = size - 1 - k if reverse else k
        reached = at > here if reverse else at < here
        new = combine(before, jax.tree.map(lambda part: part[at], everything))
        return jax.tree.map(lambda a, b: jnp.where(reached, a, b), new, before)

    return lax.fori_loop(0, size, turn, start)


def shifted(block, axis, distance):
    devices = range(lax.axis_size(axis))
    route = [(i - distance, i) for i in devices if i - distance in devices]
    return lax.ppermute(block, axis, route)


def norm_rows(payload_series, gain, bias):
    center = payload_series - jnp.mean(payload_series, axis=-1, keepdims=True)
    inverse = lax.rsqrt(jnp.mean(center * center, axis=-1, keepdims=True) + EPSILON)
    normed = center * inverse
    return (normed * gain + bias, normed, inverse)


def norm_back(grad_out, normed, inverse, gain):
    scaled = grad_out * gain
    centred = scaled - jnp.mean(scaled, axis=-1, keepdims=True)
    grad_in = inverse * (centred - normed * jnp.mean(scaled * normed, axis=-1, keepdims=True))
    return (grad_in, jnp.sum(grad_out * normed, axis=0), jnp.sum(grad_out, axis=0))


def affine(earlier, later):
    return (
        earlier[0] * later[0],
        later[0] * earlier[1] + later[1],
        later[0] * earlier[2] + later[2],
    )


def carry_across(summary, backward):
    width = summary[0].shape[0]
    identity = (
        jnp.ones((width,), jnp.float32),
        jnp.zeros((width,), jnp.float32),
        jnp.zeros((width,), jnp.float32),
    )
    return entering(summary, "tensor", affine, identity, backward)


def matmul(left, right):
    return jnp.dot(left, right, preferred_element_type=jnp.float32)


def matmul_lead(left, right):
    return lax.dot_general(
        left, right, (((0,), (0,)), ((), ())), preferred_element_type=jnp.float32
    )


def matmul_last(left, right):
    return lax.dot_general(
        left, right, (((1,), (1,)), ((), ())), preferred_element_type=jnp.float32
    )


def shards(
    tokens,
    resets,
    out_grads,
    mixer_key,
    mixer_value,
    mixer_recept,
    mixer_output,
    feed_recept,
    feed_key,
    feed_value,
    first_gain,
    first_bias,
    second_gain,
    second_bias,
    mixing_key,
    mixing_value,
    mixing_recept,
    time_decay,
    time_first,
    feeding_key,
    feeding_recept,
):
    gathered = (
        lax.all_gather(mixer_key, ("dp", "tensor"), axis=0, tiled=True),
        lax.all_gather(mixer_value, ("dp", "tensor"), axis=0, tiled=True),
        lax.all_gather(mixer_recept, ("dp", "tensor"), axis=0, tiled=True),
        lax.all_gather(mixer_output, ("dp", "tensor"), axis=0, tiled=True),
        lax.all_gather(feed_recept, ("dp", "tensor"), axis=0, tiled=True),
        lax.all_gather(first_gain, ("dp", "tensor"), axis=0, tiled=True),
        lax.all_gather(first_bias, ("dp", "tensor"), axis=0, tiled=True),
        lax.all_gather(second_gain, ("dp", "tensor"), axis=0, tiled=True),
        lax.all_gather(second_bias, ("dp", "tensor"), axis=0, tiled=True),
        lax.all_gather(mixing_key, ("dp", "tensor"), axis=0, tiled=True),
        lax.all_gather(mixing_value, ("dp", "tensor"), axis=0, tiled=True),
        lax.all_gather(mixing_recept, ("dp", "tensor"), axis=0, tiled=True),
        lax.all_gather(time_decay, ("dp", "tensor"), axis=0, tiled=True),
        lax.all_gather(time_first, ("dp", "tensor"), axis=0, tiled=True),
        lax.all_gather(feeding_key, ("dp", "tensor"), axis=0, tiled=True),
        lax.all_gather(feeding_recept, ("dp", "tensor"), axis=0, tiled=True),
    )
    w_key, w_value, w_recept, w_output, w_feedr = (
        gathered[0],
        gathered[1],
        gathered[2],
        gathered[3],
        gathered[4],
    )
    parameter_vectors = [piece.astype(jnp.float32) for piece in gathered[5:]]
    gain_one, bias_one, gain_two, bias_two = (
        parameter_vectors[0],
        parameter_vectors[1],
        parameter_vectors[2],
        parameter_vectors[3],
    )
    mix_key, mix_value, mix_recept = (
        parameter_vectors[4],
        parameter_vectors[5],
        parameter_vectors[6],
    )
    (
        fading_speed_logarithm,
        opening_premium_logarithm,
        channel_lookup_blend,
        channel_gating_blend,
    ) = (parameter_vectors[7], parameter_vectors[8], parameter_vectors[9], parameter_vectors[10])
    rates = jnp.exp(fading_speed_logarithm)
    fading_multiplier = jnp.exp(-rates)
    micro_count = tokens.shape[0]
    width = tokens.shape[3]
    grad_keyw = jnp.zeros(feed_key.shape, jnp.float32)
    grad_valuew = jnp.zeros(feed_value.shape, jnp.float32)
    square_grads = [jnp.zeros((width, width), jnp.float32) for index_one in range(5)]
    parameter_vector_gradients = [jnp.zeros((width,), jnp.float32) for index_two in range(11)]
    results = []
    input_grads = []
    for micro_index in range(micro_count):
        inputs = tokens[micro_index, 0].astype(jnp.float32)
        restart_retain_flags = (1 - resets[micro_index, 0]).astype(jnp.float32)[:, None]
        cotangent = out_grads[micro_index, 0].astype(jnp.float32)
        normed_one, unit_one, inverse_one = norm_rows(inputs, gain_one, bias_one)
        z_one = normed_one.astype(jnp.bfloat16)
        prior_one = shifted(z_one[-1:], "tensor", 1)
        before_one = (
            jnp.concatenate([prior_one, z_one[:-1]], axis=0).astype(jnp.float32)
            * restart_retain_flags
        )
        z_onef = z_one.astype(jnp.float32)
        in_key = (z_onef * mix_key + before_one * (1.0 - mix_key)).astype(jnp.bfloat16)
        in_value = (z_onef * mix_value + before_one * (1.0 - mix_value)).astype(jnp.bfloat16)
        in_recept = (z_onef * mix_recept + before_one * (1.0 - mix_recept)).astype(jnp.bfloat16)
        lookup_series = matmul(in_key, w_key)
        payload_series = matmul(in_value, w_value)
        recept = jax.nn.sigmoid(matmul(in_recept, w_recept))
        powered_lookup = jnp.exp(lookup_series)
        premium_plus_lookup = jnp.exp(opening_premium_logarithm + lookup_series)
        factor = restart_retain_flags * fading_multiplier
        cum_factor, local_a, local_b = lax.associative_scan(
            affine, (factor, powered_lookup * payload_series, powered_lookup), axis=0
        )
        incoming = carry_across((cum_factor[-1], local_a[-1], local_b[-1]), False)
        upper_running_state = local_a + cum_factor * incoming[1]
        lower_running_state = local_b + cum_factor * incoming[2]
        earlier_upper_state = jnp.concatenate([incoming[1][None], upper_running_state[:-1]], axis=0)
        earlier_lower_state = jnp.concatenate([incoming[2][None], lower_running_state[:-1]], axis=0)
        lower_quotient_part = restart_retain_flags * earlier_lower_state + premium_plus_lookup
        blended = (
            restart_retain_flags * earlier_upper_state + premium_plus_lookup * payload_series
        ) / lower_quotient_part
        weighted = (recept * blended).astype(jnp.bfloat16)
        residual = inputs + matmul(weighted, w_output)
        normed_two, unit_two, inverse_two = norm_rows(residual, gain_two, bias_two)
        z_two = normed_two.astype(jnp.bfloat16)
        prior_two = shifted(z_two[-1:], "tensor", 1)
        before_two = (
            jnp.concatenate([prior_two, z_two[:-1]], axis=0).astype(jnp.float32)
            * restart_retain_flags
        )
        z_twof = z_two.astype(jnp.float32)
        feed_in = (
            z_twof * channel_lookup_blend + before_two * (1.0 - channel_lookup_blend)
        ).astype(jnp.bfloat16)
        feed_rin = (
            z_twof * channel_gating_blend + before_two * (1.0 - channel_gating_blend)
        ).astype(jnp.bfloat16)
        gate = jax.nn.sigmoid(matmul(feed_rin, w_feedr))
        all_in = lax.all_gather(feed_in, "tensor", axis=0, tiled=True)
        hidden_pre = matmul_last(feed_key, all_in)
        hidden = jnp.square(jnp.maximum(hidden_pre, 0.0)).astype(jnp.bfloat16)
        value_out = lax.psum_scatter(
            matmul_lead(hidden, feed_value), "tensor", scatter_dimension=0, tiled=True
        )
        results.append(residual + gate * value_out)
        grad_value = (cotangent * gate).astype(jnp.bfloat16)
        grad_gate = (cotangent * value_out * gate * (1.0 - gate)).astype(jnp.bfloat16)
        square_grads[4] = square_grads[4] + matmul_lead(feed_rin, grad_gate)
        grad_rin = matmul_last(grad_gate, w_feedr)
        relu_twice = 2.0 * jnp.maximum(hidden_pre, 0.0)
        add_piece = lax.all_gather(grad_value, "tensor", axis=0, tiled=True)
        rows_total = matmul(hidden, add_piece)
        block = matmul_last(feed_value, add_piece)
        grad_valuew = grad_valuew + rows_total
        grad_pre = (block * relu_twice).astype(jnp.bfloat16)
        grad_keyw = grad_keyw + matmul(grad_pre, all_in)
        grad_in = lax.psum_scatter(
            matmul_lead(grad_pre, feed_key), "tensor", scatter_dimension=0, tiled=True
        )
        parameter_vector_gradients[9] = parameter_vector_gradients[9] + jnp.sum(
            grad_in * (z_twof - before_two), axis=0
        )
        parameter_vector_gradients[10] = parameter_vector_gradients[10] + jnp.sum(
            grad_rin * (z_twof - before_two), axis=0
        )
        shift_two = restart_retain_flags * (
            grad_in * (1.0 - channel_lookup_blend) + grad_rin * (1.0 - channel_gating_blend)
        )
        after_two = shifted(shift_two[:1], "tensor", -1)
        grad_z_two = (
            grad_in * channel_lookup_blend
            + grad_rin * channel_gating_blend
            + jnp.concatenate([shift_two[1:], after_two], axis=0)
        )
        back_two, gain_part, bias_part = norm_back(grad_z_two, unit_two, inverse_two, gain_two)
        parameter_vector_gradients[2] = parameter_vector_gradients[2] + gain_part
        parameter_vector_gradients[3] = parameter_vector_gradients[3] + bias_part
        grad_residual = cotangent + back_two
        grad_att = grad_residual.astype(jnp.bfloat16)
        square_grads[3] = square_grads[3] + matmul_lead(weighted, grad_att)
        grad_weighted = matmul_last(grad_att, w_output)
        grad_mixed = grad_weighted * recept
        grad_recept = (grad_weighted * blended * recept * (1.0 - recept)).astype(jnp.bfloat16)
        upper_adjoint = grad_mixed / lower_quotient_part
        denominator_gradient = -grad_mixed * blended / lower_quotient_part
        cum_back, local_xa, local_xb = lax.associative_scan(
            affine,
            (
                factor,
                restart_retain_flags * upper_adjoint,
                restart_retain_flags * denominator_gradient,
            ),
            reverse=True,
            axis=0,
        )
        beyond = carry_across((cum_back[0], local_xa[0], local_xb[0]), True)
        adjoint_a = local_xa + cum_back * beyond[1]
        adjoint_b = local_xb + cum_back * beyond[2]
        running_upper_total = jnp.concatenate([adjoint_a[1:], beyond[1][None]], axis=0)
        running_lower_total = jnp.concatenate([adjoint_b[1:], beyond[2][None]], axis=0)
        premium_power = premium_plus_lookup * (
            payload_series * upper_adjoint + denominator_gradient
        )
        adjoint_payloads = (
            premium_plus_lookup * upper_adjoint + powered_lookup * running_upper_total
        ).astype(jnp.bfloat16)
        key_gradient_rows = (
            premium_power
            + powered_lookup * (payload_series * running_upper_total + running_lower_total)
        ).astype(jnp.bfloat16)
        parameter_vector_gradients[8] = parameter_vector_gradients[8] + jnp.sum(
            premium_power, axis=0
        )
        decay_sum = jnp.sum(
            restart_retain_flags
            * (
                running_upper_total * earlier_upper_state
                + running_lower_total * earlier_lower_state
            ),
            axis=0,
        )
        parameter_vector_gradients[7] = (
            parameter_vector_gradients[7] - rates * fading_multiplier * decay_sum
        )
        square_grads[0] = square_grads[0] + matmul_lead(in_key, key_gradient_rows)
        square_grads[1] = square_grads[1] + matmul_lead(in_value, adjoint_payloads)
        square_grads[2] = square_grads[2] + matmul_lead(in_recept, grad_recept)
        grad_inkey = matmul_last(key_gradient_rows, w_key)
        grad_invalue = matmul_last(adjoint_payloads, w_value)
        grad_inrecept = matmul_last(grad_recept, w_recept)
        spread_one = z_onef - before_one
        parameter_vector_gradients[4] = parameter_vector_gradients[4] + jnp.sum(
            grad_inkey * spread_one, axis=0
        )
        parameter_vector_gradients[5] = parameter_vector_gradients[5] + jnp.sum(
            grad_invalue * spread_one, axis=0
        )
        parameter_vector_gradients[6] = parameter_vector_gradients[6] + jnp.sum(
            grad_inrecept * spread_one, axis=0
        )
        shift_one = restart_retain_flags * (
            grad_inkey * (1.0 - mix_key)
            + grad_invalue * (1.0 - mix_value)
            + grad_inrecept * (1.0 - mix_recept)
        )
        after_one = shifted(shift_one[:1], "tensor", -1)
        grad_z_one = (
            grad_inkey * mix_key
            + grad_invalue * mix_value
            + grad_inrecept * mix_recept
            + jnp.concatenate([shift_one[1:], after_one], axis=0)
        )
        back_one, gain_first, bias_first = norm_back(grad_z_one, unit_one, inverse_one, gain_one)
        parameter_vector_gradients[0] = parameter_vector_gradients[0] + gain_first
        parameter_vector_gradients[1] = parameter_vector_gradients[1] + bias_first
        input_grads.append(grad_residual + back_one)
    owned = (
        lax.psum_scatter(square_grads[0], ("dp", "tensor"), scatter_dimension=0, tiled=True),
        lax.psum_scatter(square_grads[1], ("dp", "tensor"), scatter_dimension=0, tiled=True),
        lax.psum_scatter(square_grads[2], ("dp", "tensor"), scatter_dimension=0, tiled=True),
        lax.psum_scatter(square_grads[3], ("dp", "tensor"), scatter_dimension=0, tiled=True),
        lax.psum_scatter(square_grads[4], ("dp", "tensor"), scatter_dimension=0, tiled=True),
        lax.psum_scatter(
            parameter_vector_gradients[0], ("dp", "tensor"), scatter_dimension=0, tiled=True
        ),
        lax.psum_scatter(
            parameter_vector_gradients[1], ("dp", "tensor"), scatter_dimension=0, tiled=True
        ),
        lax.psum_scatter(
            parameter_vector_gradients[2], ("dp", "tensor"), scatter_dimension=0, tiled=True
        ),
        lax.psum_scatter(
            parameter_vector_gradients[3], ("dp", "tensor"), scatter_dimension=0, tiled=True
        ),
        lax.psum_scatter(
            parameter_vector_gradients[4], ("dp", "tensor"), scatter_dimension=0, tiled=True
        ),
        lax.psum_scatter(
            parameter_vector_gradients[5], ("dp", "tensor"), scatter_dimension=0, tiled=True
        ),
        lax.psum_scatter(
            parameter_vector_gradients[6], ("dp", "tensor"), scatter_dimension=0, tiled=True
        ),
        lax.psum_scatter(
            parameter_vector_gradients[7], ("dp", "tensor"), scatter_dimension=0, tiled=True
        ),
        lax.psum_scatter(
            parameter_vector_gradients[8], ("dp", "tensor"), scatter_dimension=0, tiled=True
        ),
        lax.psum_scatter(
            parameter_vector_gradients[9], ("dp", "tensor"), scatter_dimension=0, tiled=True
        ),
        lax.psum_scatter(
            parameter_vector_gradients[10], ("dp", "tensor"), scatter_dimension=0, tiled=True
        ),
    )
    key_rows, value_rows_grad = (grad_keyw, grad_valuew)
    key_total, value_total = (
        lax.psum(key_rows.astype(jnp.bfloat16), "dp").astype(jnp.float32),
        lax.psum(value_rows_grad.astype(jnp.bfloat16), "dp").astype(jnp.float32),
    )
    result_all = jnp.stack(results)[:, None]
    grads_all = jnp.stack(input_grads)[:, None]
    return (
        result_all,
        grads_all,
        owned[0],
        owned[1],
        owned[2],
        owned[3],
        owned[4],
        key_total,
        value_total,
        owned[5],
        owned[6],
        owned[7],
        owned[8],
        owned[9],
        owned[10],
        owned[11],
        owned[12],
        owned[13],
        owned[14],
        owned[15],
    )


BF = jnp.bfloat16
F32 = jnp.float32
BOTH = ("dp", "tensor")
MESH_ID = pl.DeviceIdType.MESH


def cost(flops, moved):
    return pl.CostEstimate(flops=flops, bytes_accessed=moved, transcendentals=0)


def whole():
    return pl.BlockSpec(memory_space=pltpu.VMEM)


def anywhere():
    return pl.BlockSpec(memory_space=pl.ANY)


def gather_kernel(count, chunks, *refs):
    ins, outs = refs[:count], refs[count : 2 * count]
    send, recv, local_sem = refs[2 * count :]
    dp, t = lax.axis_index("dp"), lax.axis_index("tensor")
    x, c, z, y = dp // 2, dp % 2, t // 2, t % 2
    over_x, over_y, over_core = (1 - x) * 2 + c, z * 2 + 1 - y, x * 2 + 1 - c
    first = (jnp.where(c == 0, dp, over_x), jnp.where(c == 0, over_y, t))
    second = (jnp.where(c == 0, over_x, dp), jnp.where(c == 0, t, over_y))
    x_first, y_first = jnp.where(c == 0, x, 1 - x), jnp.where(c == 0, 1 - y, y)
    along_z = [(dp, lax.rem(z + o, 4) * 2 + y) for o in (1, 2, 3)]
    barrier = pltpu.get_barrier_semaphore()
    peers = along_z + [(over_x, t), (dp, over_y), (over_core, t)]
    for peer in peers:
        pl.semaphore_signal(barrier, inc=1, device_id=peer, device_id_type=MESH_ID)
    pl.semaphore_wait(barrier, len(peers))

    def copy(source, target, k, j, device):
        return pltpu.make_async_remote_copy(
            src_ref=source,
            dst_ref=target,
            send_sem=send.at[k, j],
            recv_sem=recv.at[k, j],
            device_id=device,
            device_id_type=MESH_ID,
        )

    copies = {}

    def begin(k, j, source, target, device):
        copies[k, j] = copy(source, target, k, j, device)
        copies[k, j].start()

    def column(k, xx, yy):
        i, start, rows = chunks[k]
        return outs[i].at[xx, c, :, yy, pl.ds(start, rows)]

    own = []
    for i in range(count):
        own.append(pltpu.make_async_copy(ins[i], outs[i].at[x, c, z, y], local_sem.at[i]))
        own[i].start()
    steps = len(chunks)
    for k in range(steps):
        i, start, rows = chunks[k]
        for o in range(3):
            begin(k, o, ins[i].at[pl.ds(start, rows)], outs[i].at[x, c, z, y, pl.ds(start, rows)], along_z[o])
    for i in range(count):
        own[i].wait()
    for s in range(steps + 2):
        if s < steps:
            for o in range(3):
                copies[s, o].wait_recv()
            begin(s, 3, column(s, x, y), column(s, x, y), first)
            begin(s, 4, column(s, x, y), column(s, x, y), second)
        if 0 <= s - 1 < steps:
            k = s - 1
            copies[k, 3].wait_recv()
            begin(k, 5, column(k, x_first, y_first), column(k, x_first, y_first), second)
        if 0 <= s - 2 < steps:
            k = s - 2
            i, start, rows = chunks[k]
            copies[k, 4].wait_recv()
            copies[k, 5].wait_recv()
            half = outs[i].at[:, c, :, :, pl.ds(start, rows)]
            begin(k, 6, half, half, (over_core, t))
    for k in range(steps):
        copies[k, 6].wait_recv()
    for k in range(steps):
        for j in range(7):
            copies[k, j].wait_send()


def gather(parts):
    count = len(parts)
    chunks = []
    for i, part in enumerate(parts):
        for start in range(0, part.shape[0], 16):
            chunks.append((i, start, 16))
    outs = [jax.ShapeDtypeStruct((2, 2, 4, 2) + p.shape, p.dtype) for p in parts]
    moved = sum(2 * 32 * p.size for p in parts)
    return pl.pallas_call(
        functools.partial(gather_kernel, count, chunks),
        out_shape=outs,
        in_specs=[anywhere()] * count,
        out_specs=[anywhere()] * count,
        scratch_shapes=[
            pltpu.SemaphoreType.DMA((len(chunks), 7)),
            pltpu.SemaphoreType.DMA((len(chunks), 7)),
            pltpu.SemaphoreType.DMA((count,)),
        ],
        compiler_params=pltpu.CompilerParams(collective_id=0, has_side_effects=True),
        cost_estimate=cost(0, 8 * moved),
        name="gather",
    )(*parts)


def roll_rows(value, distance, fill, row):
    size = value.shape[0]
    moved = pltpu.roll(value, distance % size, 0)
    outside = row < distance if distance > 0 else row >= size + distance
    return jnp.where(outside, fill, moved)


def doubling(factor, up, low, row, sign):
    size, step = factor.shape[0], 1
    while step < size:
        up = up + factor * roll_rows(up, sign * step, 0.0, row)
        low = low + factor * roll_rows(low, sign * step, 0.0, row)
        factor = factor * roll_rows(factor, sign * step, 1.0, row)
        step *= 2
    return factor, up, low


def greet_row(t, dp, size):
    barrier = pltpu.get_barrier_semaphore()
    for o in range(1, size):
        pl.semaphore_signal(barrier, inc=1, device_id=(dp, lax.rem(t + o, size)), device_id_type=MESH_ID)
    pl.semaphore_wait(barrier, size - 1)


def share_row(summary, arrived, send, recv, t, dp, size):
    copies = []
    for o in range(1, size):
        copies.append(
            pltpu.make_async_remote_copy(
                src_ref=summary,
                dst_ref=arrived.at[o],
                send_sem=send.at[o],
                recv_sem=recv.at[o],
                device_id=(dp, lax.rem(t + o, size)),
                device_id_type=MESH_ID,
            )
        )
        copies[-1].start()
    for copy in copies:
        copy.wait_recv()
    return copies


def lanes(j):
    return pl.ds(pl.multiple_of(j * 128, 128), 128)


def forward_scan_kernel(
    keys, values, gates, keep, vectors, weighted, denom, mixed, prior_a, prior_b, recept,
    cum, up, low, summary, arrived, entering_rows, send, recv,
):
    dp, t = lax.axis_index("dp"), lax.axis_index("tensor")
    size = arrived.shape[0]
    micro, rows = keys.shape[:2]
    greet_row(t, dp, size)
    row = lax.broadcasted_iota(jnp.int32, (rows, 128), 0)
    summary[...] = jnp.zeros_like(summary)
    for m in range(micro):

        def first_pass(j, carry, m=m):
            at = lanes(j)
            power = jnp.exp(keys[m, :, at])
            factor = keep[m] * vectors[0:1, at]
            f, a, b = doubling(factor, power * values[m, :, at], power, row, 1)
            cum[m, :, at] = f
            up[m, :, at] = a
            low[m, :, at] = b
            summary[3 * m : 3 * m + 1, at] = f[rows - 1 :]
            summary[3 * m + 1 : 3 * m + 2, at] = a[rows - 1 :]
            summary[3 * m + 2 : 3 * m + 3, at] = b[rows - 1 :]
            return carry

        lax.fori_loop(0, keys.shape[2] // 128, first_pass, 0)
    copies = share_row(summary, arrived, send, recv, t, dp, size)
    for m in range(micro):
        a = jnp.zeros((1, keys.shape[2]), F32)
        b = jnp.zeros((1, keys.shape[2]), F32)
        for o in range(size - 1, 0, -1):
            f = arrived[o, 3 * m : 3 * m + 1]
            a = jnp.where(t >= o, f * a + arrived[o, 3 * m + 1 : 3 * m + 2], a)
            b = jnp.where(t >= o, f * b + arrived[o, 3 * m + 2 : 3 * m + 3], b)
        entering_rows[2 * m : 2 * m + 1] = a
        entering_rows[2 * m + 1 : 2 * m + 2] = b
    for m in range(micro):

        def second_pass(j, carry, m=m):
            at = lanes(j)
            enter_a = entering_rows[2 * m : 2 * m + 1, at]
            enter_b = entering_rows[2 * m + 1 : 2 * m + 2, at]
            f = cum[m, :, at]
            before_a = roll_rows(up[m, :, at] + f * enter_a, 1, enter_a, row)
            before_b = roll_rows(low[m, :, at] + f * enter_b, 1, enter_b, row)
            bonus = jnp.exp(vectors[1:2, at] + keys[m, :, at])
            below = keep[m] * before_b + bonus
            blended = (keep[m] * before_a + bonus * values[m, :, at]) / below
            gate = jax.nn.sigmoid(gates[m, :, at])
            weighted[m, :, at] = (gate * blended).astype(BF)
            denom[m, :, at] = below
            mixed[m, :, at] = blended
            prior_a[m, :, at] = before_a
            prior_b[m, :, at] = before_b
            recept[m, :, at] = gate
            return carry

        lax.fori_loop(0, keys.shape[2] // 128, second_pass, 0)
    for copy in copies:
        copy.wait_send()


def scan_scratch(shape, size):
    width = shape[-1]
    return [
        pltpu.VMEM(shape, F32),
        pltpu.VMEM(shape, F32),
        pltpu.VMEM(shape, F32),
        pltpu.VMEM((8, width), F32),
        pltpu.VMEM((size, 8, width), F32),
        pltpu.VMEM((8, width), F32),
        pltpu.SemaphoreType.DMA((size,)),
        pltpu.SemaphoreType.DMA((size,)),
    ]


def forward_scan(keys, values, gates, keep, vectors, size):
    shape = keys.shape
    full = jax.ShapeDtypeStruct(shape, F32)
    return pl.pallas_call(
        forward_scan_kernel,
        out_shape=[jax.ShapeDtypeStruct(shape, BF)] + [full] * 5,
        in_specs=[whole()] * 5,
        out_specs=[whole()] * 6,
        scratch_shapes=scan_scratch(shape, size),
        compiler_params=pltpu.CompilerParams(collective_id=1, has_side_effects=True),
        cost_estimate=cost(100 * keys.size, 36 * keys.size),
        name="forward_scan",
    )(keys, values, gates, keep, vectors)


def channel_forward_kernel(feed_in, key_block, value_block, positive, total):
    rows = 4 * key_block.shape[-2]
    keys = key_block[...].reshape(rows, key_block.shape[-1])
    hidden = jnp.maximum(matmul_last(feed_in[...], keys), 0.0)
    positive[0] = hidden
    squares = (hidden * hidden).astype(BF)
    part = matmul(squares, value_block[...].reshape(rows, value_block.shape[-1]))

    @pl.when(pl.program_id(0) == 0)
    def _():
        total[...] = part

    @pl.when(pl.program_id(0) > 0)
    def _():
        total[...] += part


def channel_forward(feed_in, weights):
    tokens, width = feed_in.shape
    rows = weights.shape[4]
    units = 32 * rows

    def block(side):
        return pl.BlockSpec((1, 1, 4, 1, rows, width), lambda i: (i // 4, (i // 2) % 2, 0, i % 2, 0, side))

    return pl.pallas_call(
        channel_forward_kernel,
        grid=(8,),
        out_shape=[jax.ShapeDtypeStruct((8, tokens, 4 * rows), F32), jax.ShapeDtypeStruct((tokens, width), F32)],
        in_specs=[pl.BlockSpec((tokens, width), lambda i: (0, 0)), block(0), block(1)],
        out_specs=[
            pl.BlockSpec((1, tokens, 4 * rows), lambda i: (i, 0, 0)),
            pl.BlockSpec((tokens, width), lambda i: (0, 0)),
        ],
        cost_estimate=cost(4 * tokens * units * width, 4 * units * width + 4 * tokens * units),
        name="channel_forward",
    )(feed_in, weights, weights)


def owner(i, x, y, c):
    first, second = i // 2, i % 2
    flip_x = first * c + second * (1 - c)
    flip_y = first * (1 - c) + second * c
    return x + flip_x - 2 * x * flip_x, y + flip_y - 2 * y * flip_y


def position(xx, yy, x, y, c):
    flip_x = x + xx - 2 * x * xx
    flip_y = y + yy - 2 * y * yy
    return 2 * (flip_x * c + flip_y * (1 - c)) + flip_x * (1 - c) + flip_y * c


class Links:
    def __init__(self, size):
        dp, t = lax.axis_index("dp"), lax.axis_index("tensor")
        x, c, z, y = dp // 2, dp % 2, t // 2, t % 2
        self.x, self.c, self.z, self.y, self.dp, self.t, self.size = x, c, z, y, dp, t, size
        over_x, over_y = ((1 - x) * 2 + c, t), (dp, z * 2 + 1 - y)
        self.over_x = over_x
        self.core = (x * 2 + 1 - c, t)
        self.first = (jnp.where(c == 0, over_y[0], over_x[0]), jnp.where(c == 0, over_y[1], over_x[1]))
        self.second = (jnp.where(c == 0, over_x[0], over_y[0]), jnp.where(c == 0, over_x[1], over_y[1]))
        self.along_z = [(dp, lax.rem(z + o, 4) * 2 + y) for o in (1, 2, 3)]
        self.over_y = over_y

    def row(self, o):
        return (self.dp, lax.rem(self.t + o, self.size))

    def greet(self, whole_row):
        peers = [self.row(o) for o in range(1, self.size)] if whole_row else self.along_z + [self.over_y]
        peers = peers + [self.over_x, self.core]
        barrier = pltpu.get_barrier_semaphore()
        for peer in peers:
            pl.semaphore_signal(barrier, inc=1, device_id=peer, device_id_type=MESH_ID)
        pl.semaphore_wait(barrier, len(peers))


def remote(source, target, send, recv, device):
    return pltpu.make_async_remote_copy(
        src_ref=source, dst_ref=target, send_sem=send, recv_sem=recv, device_id=device, device_id_type=MESH_ID
    )


def add_blocks(target, sources):
    count, rows = target.shape[:2]
    tile = min(rows, 32)
    per = rows // tile

    def turn(k, carry):
        n, at = k // per, pl.ds(pl.multiple_of(lax.rem(k, per) * tile, tile), tile)
        value = sources[0][n, at].astype(F32)
        for source in sources[1:]:
            value = value + source[n, at].astype(F32)
        target[n, at] = value.astype(target.dtype)
        return carry

    lax.fori_loop(0, count * per, turn, 0)


def dot_rows(target, left, right):
    tile = 256

    def turn(n, carry):
        at = pl.ds(pl.multiple_of(n * tile, tile), tile)
        target[:, at] = matmul_last(left[...], right[at, :])
        return carry

    lax.fori_loop(0, right.shape[0] // tile, turn, 0)


def norm_back_tiles(target, grads, normed, inverse, gain, base, sums, gain_row):
    tile = 32
    width = grads.shape[1]

    def turn(k, carry):
        at = pl.ds(pl.multiple_of(k * tile, tile), tile)
        grad, unit = grads[at, :], normed[at, :]
        scaled = grad * gain
        middle = jnp.sum(scaled, axis=-1, keepdims=True) * (1.0 / width)
        along = jnp.sum(scaled * unit, axis=-1, keepdims=True) * (1.0 / width)
        target[at, :] = base[at, :].astype(F32) + inverse[at, 0:1] * (scaled - middle - unit * along)
        sums[gain_row : gain_row + 1, :] += jnp.sum(grad * unit, axis=0, keepdims=True)
        sums[gain_row + 1 : gain_row + 2, :] += jnp.sum(grad, axis=0, keepdims=True)
        return carry

    lax.fori_loop(0, grads.shape[0] // tile, turn, 0)


GAIN_ONE, BIAS_ONE, GAIN_TWO, BIAS_TWO, MIX_KEY, MIX_VALUE, MIX_RECEPT, DECAY, PREMIUM, BLEND_KEY, BLEND_RECEPT = range(11)


def channel_backward_kernel(
    feed_in, grad_value, grad_gate, vectors, keep, inverse, cotangent,
    weights, positive, w_feedr, w_output, spread, unit, keys, values, denom, mixed, prior_a, prior_b, recept,
    feed_part, grad_keys, grad_values, grad_recept, grad_att, grad_residual, sums,
    weight_slots, positive_slots, feedr, output, spread_in, unit_in, keys_in, values_in, denom_in, mixed_in,
    prior_a_in, prior_b_in, recept_in, value_part, key_part, outgoing, gathered, from_first, from_second,
    grad_in, grad_rin, grad_z, grad_w, cum, up, low, summary, arrived, entering_rows, halo_out, halo_in,
    slot_sem, load_sem, core_send, core_recv, first_send, first_recv, second_send, second_recv,
    scan_send, scan_recv, halo_send, halo_recv,
):
    size = arrived.shape[0]
    links = Links(size)
    x, c, z, y, t = links.x, links.c, links.z, links.y, links.t
    rows, width = weight_slots.shape[2], feed_in.shape[1]
    micro, length = keep.shape[:2]

    def fetches(s, slot):
        own = s // 4
        cc = own * c + (1 - own) * (1 - c)
        xx, yy = owner(3 - lax.rem(s, 4), x, y, cc)
        return (
            pltpu.make_async_copy(weights.at[xx, cc, :, yy], weight_slots.at[slot], slot_sem.at[0, slot]),
            pltpu.make_async_copy(positive.at[xx * 4 + cc * 2 + yy], positive_slots.at[slot], slot_sem.at[1, slot]),
        )

    for copy in fetches(0, 0):
        copy.start()
    late = [
        (w_feedr, feedr), (spread, spread_in), (unit, unit_in), (w_output, output), (recept, recept_in),
        (mixed, mixed_in), (denom, denom_in), (keys, keys_in), (values, values_in), (prior_a, prior_a_in),
        (prior_b, prior_b_in),
    ]
    loads = [pltpu.make_async_copy(source, target, load_sem.at[k]) for k, (source, target) in enumerate(late)]
    for load in loads:
        load.start()
    links.greet(True)
    grad_in[...] = jnp.zeros_like(grad_in)
    sums[...] = jnp.zeros_like(sums)
    summary[...] = jnp.zeros_like(summary)
    halo_out[...] = jnp.zeros_like(halo_out)

    def to_core(i, slot):
        return remote(outgoing.at[slot], gathered.at[i], core_send.at[i], core_recv.at[i], links.core)

    def to_first(q, side):
        return remote(
            gathered.at[2 + q, side], from_first.at[q, side], first_send.at[q, side], first_recv.at[q, side], links.first
        )

    def column(s, carry):
        slot = lax.rem(s, 2)
        i = 3 - lax.rem(s, 4)
        for copy in fetches(s, slot):
            copy.wait()

        @pl.when(s < 7)
        def _():
            for copy in fetches(s + 1, 1 - slot):
                copy.start()

        hidden = positive_slots[slot]
        squares = (hidden * hidden).astype(BF)
        key_rows = weight_slots[slot, :, :, :width].reshape(4 * rows, width)
        value_rows = weight_slots[slot, :, :, width:].reshape(4 * rows, width)
        value_part[...] = matmul_lead(squares, grad_value[...])
        grad_pre = (matmul_last(grad_value[...], value_rows) * (2.0 * hidden)).astype(BF)
        key_part[...] = matmul_lead(grad_pre, feed_in[...])
        grad_in[...] += matmul(grad_pre, key_rows)

        @pl.when(s < 4)
        def _():
            @pl.when(s >= 2)
            def _():
                to_core(i + 2, slot).wait_send()

            for k in range(4):
                at = lax.rem(k + 4 - z, 4)
                outgoing[slot, 0, at] = value_part[k * rows : (k + 1) * rows].astype(BF)
                outgoing[slot, 1, at] = key_part[k * rows : (k + 1) * rows].astype(BF)
            to_core(i, slot).start()

        @pl.when(s >= 4)
        def _():
            to_core(i, slot).wait_recv()
            for side, part in ((0, value_part), (1, key_part)):
                for k in range(4):
                    at = lax.rem(k + 4 - z, 4)
                    total = gathered[i, side, at].astype(F32) + part[k * rows : (k + 1) * rows]
                    gathered[i, side, at] = total.astype(BF)

        @pl.when(jnp.logical_and(s >= 4, s < 6))
        def _():
            for side in (0, 1):
                to_first(i - 2, side).start()

        return carry

    lax.fori_loop(0, 8, column, 0)
    to_core(1, 0).wait_send()
    to_core(0, 1).wait_send()

    def to_second(side):
        return remote(
            gathered.at[1, side], from_second.at[side], second_send.at[side], second_recv.at[side], links.second
        )

    def pass_second(side):
        to_first(1, side).wait_recv()
        add_blocks(gathered.at[1, side], [gathered.at[1, side], from_first.at[1, side]])
        to_second(side).start()

    row = lax.broadcasted_iota(jnp.int32, (length, 128), 0)
    loads[0].wait()
    dot_rows(grad_rin, grad_gate, feedr)

    def shift_two(m, rows_at, at, keeping):
        return keeping * (
            grad_in[rows_at, at] * (1.0 - vectors[BLEND_KEY : BLEND_KEY + 1, at])
            + grad_rin[rows_at, at] * (1.0 - vectors[BLEND_RECEPT : BLEND_RECEPT + 1, at])
        )

    for m in range(micro):
        start = m * length
        halo_out[m : m + 1] = shift_two(m, slice(start, start + 1), slice(None), keep[m, 0:1, 0:1])
    halo = remote(halo_out, halo_in, halo_send.at[0], halo_recv.at[0], links.row(size - 1))
    halo.start()
    pass_second(0)
    loads[1].wait()
    halo.wait_recv()
    for m in range(micro):
        rows_at = slice(m * length, (m + 1) * length)

        def shift_pass(j, carry, m=m, rows_at=rows_at):
            at = lanes(j)
            after = jnp.where(t < size - 1, halo_in[m : m + 1, at], 0.0)
            shift = shift_two(m, rows_at, at, keep[m])
            from_in, from_rin, apart = grad_in[rows_at, at], grad_rin[rows_at, at], spread_in[rows_at, at]
            grad_z[rows_at, at] = (
                from_in * vectors[BLEND_KEY : BLEND_KEY + 1, at]
                + from_rin * vectors[BLEND_RECEPT : BLEND_RECEPT + 1, at]
                + roll_rows(shift, -1, after, row)
            )
            sums[BLEND_KEY : BLEND_KEY + 1, at] += jnp.sum(from_in * apart, axis=0, keepdims=True)
            sums[BLEND_RECEPT : BLEND_RECEPT + 1, at] += jnp.sum(from_rin * apart, axis=0, keepdims=True)
            return carry

        lax.fori_loop(0, width // 128, shift_pass, 0)
    loads[2].wait()
    norm_back_tiles(
        grad_residual, grad_z, unit_in, inverse, vectors[GAIN_TWO : GAIN_TWO + 1, :], cotangent, sums, GAIN_TWO
    )
    grad_att[...] = grad_residual[...].astype(BF)
    pass_second(1)

    loads[3].wait()
    dot_rows(grad_w, grad_att, output)
    for load in loads[4:]:
        load.wait()

    def quotient_grads(rows_at, at):
        gate = recept_in[rows_at, at]
        blended = mixed_in[rows_at, at]
        inner = grad_w[rows_at, at] * gate
        above = inner / denom_in[rows_at, at]
        return above, -above * blended, inner * blended * (1.0 - gate)

    for m in range(micro):
        rows_at = slice(m * length, (m + 1) * length)

        def first_pass(j, carry, m=m, rows_at=rows_at):
            at = lanes(j)
            above, below, rec = quotient_grads(rows_at, at)
            grad_recept[rows_at, at] = rec.astype(BF)
            factor = keep[m] * vectors[DECAY : DECAY + 1, at]
            f, a, b = doubling(factor, keep[m] * above, keep[m] * below, row, -1)
            cum[rows_at, at] = f
            up[rows_at, at] = a
            low[rows_at, at] = b
            summary[3 * m : 3 * m + 1, at] = f[:1]
            summary[3 * m + 1 : 3 * m + 2, at] = a[:1]
            summary[3 * m + 2 : 3 * m + 3, at] = b[:1]
            return carry

        lax.fori_loop(0, width // 128, first_pass, 0)
    copies = share_row(summary, arrived, scan_send, scan_recv, t, links.dp, size)
    for m in range(micro):
        a = jnp.zeros((1, width), F32)
        b = jnp.zeros((1, width), F32)
        for ahead in range(size - 1, 0, -1):
            o = size - ahead
            f = arrived[o, 3 * m : 3 * m + 1]
            a = jnp.where(t + ahead < size, f * a + arrived[o, 3 * m + 1 : 3 * m + 2], a)
            b = jnp.where(t + ahead < size, f * b + arrived[o, 3 * m + 2 : 3 * m + 3], b)
        entering_rows[2 * m : 2 * m + 1] = a
        entering_rows[2 * m + 1 : 2 * m + 2] = b
    for m in range(micro):
        rows_at = slice(m * length, (m + 1) * length)

        def second_pass(j, carry, m=m, rows_at=rows_at):
            at = lanes(j)
            enter_a = entering_rows[2 * m : 2 * m + 1, at]
            enter_b = entering_rows[2 * m + 1 : 2 * m + 2, at]
            f = cum[rows_at, at]
            alpha = roll_rows(up[rows_at, at] + f * enter_a, -1, enter_a, row)
            beta = roll_rows(low[rows_at, at] + f * enter_b, -1, enter_b, row)
            above, below, _ = quotient_grads(rows_at, at)
            key, value = keys_in[rows_at, at], values_in[rows_at, at]
            power = jnp.exp(key)
            bonus = jnp.exp(vectors[PREMIUM : PREMIUM + 1, at] + key)
            premium = bonus * (value * above + below)
            grad_values[rows_at, at] = (bonus * above + power * alpha).astype(BF)
            grad_keys[rows_at, at] = (premium + power * (value * alpha + beta)).astype(BF)
            fading = keep[m] * (alpha * prior_a_in[rows_at, at] + beta * prior_b_in[rows_at, at])
            sums[PREMIUM : PREMIUM + 1, at] += jnp.sum(premium, axis=0, keepdims=True)
            sums[DECAY : DECAY + 1, at] += jnp.sum(fading, axis=0, keepdims=True)
            return carry

        lax.fori_loop(0, width // 128, second_pass, 0)

    for side in (0, 1):
        to_first(0, side).wait_recv()
        to_second(side).wait_recv()
        add_blocks(
            feed_part.at[side], [gathered.at[0, side], from_first.at[0, side], from_second.at[side]]
        )
    for side in (0, 1):
        to_first(0, side).wait_send()
        to_first(1, side).wait_send()
        to_second(side).wait_send()
    halo.wait_send()
    for copy in copies:
        copy.wait_send()


def channel_backward(near, far, size):
    feed_in = near[0]
    weights = far[0]
    tokens, width = feed_in.shape
    micro, length = near[4].shape[:2]
    rows = weights.shape[4]
    flat_f32, flat_bf = (tokens, width), jax.ShapeDtypeStruct((tokens, width), BF)
    dma = pltpu.SemaphoreType.DMA
    big = pltpu.VMEM(flat_f32, F32)
    return pl.pallas_call(
        channel_backward_kernel,
        out_shape=[
            jax.ShapeDtypeStruct((2, 4, rows, width), BF), flat_bf, flat_bf, flat_bf, flat_bf,
            jax.ShapeDtypeStruct(flat_f32, F32), jax.ShapeDtypeStruct((16, width), F32),
        ],
        in_specs=[whole()] * len(near) + [anywhere()] * len(far),
        out_specs=[whole()] * 7,
        scratch_shapes=[
            pltpu.VMEM((2, 4, rows, 2 * width), BF), pltpu.VMEM((2, tokens, 4 * rows), F32),
            pltpu.VMEM((width, width), BF), pltpu.VMEM((width, width), BF),
        ]
        + [big] * 9
        + [
            pltpu.VMEM((4 * rows, width), F32), pltpu.VMEM((4 * rows, width), F32),
            pltpu.VMEM((2, 2, 4, rows, width), BF), pltpu.VMEM((4, 2, 4, rows, width), BF),
            pltpu.VMEM((2, 2, 4, rows, width), BF), pltpu.VMEM((2, 4, rows, width), BF),
        ]
        + [big] * 7
        + [
            pltpu.VMEM((8, width), F32), pltpu.VMEM((size, 8, width), F32), pltpu.VMEM((8, width), F32),
            pltpu.VMEM((8, width), F32), pltpu.VMEM((8, width), F32),
            dma((2, 2)), dma((11,)), dma((4,)), dma((4,)), dma((2, 2)), dma((2, 2)), dma((2,)), dma((2,)),
            dma((size,)), dma((size,)), dma((1,)), dma((1,)),
        ],
        compiler_params=pltpu.CompilerParams(
            collective_id=2, has_side_effects=True, vmem_limit_bytes=66_000_000
        ),
        cost_estimate=cost(8 * tokens * 32 * rows * width, 16 * 32 * rows * width),
        name="channel_backward",
    )(*near, *far)


def front_backward_kernel(
    feed_part, lefts, rights, vectors, keep, inverse, grad_residual, sums_in, rates,
    w_key, w_value, w_recept, spread, unit,
    square_grads, unit_key, unit_value, token_grads, vector_grads,
    key_in, value_in, recept_in, spread_in, unit_in, outgoing, gathered, from_first, from_second, from_z, feed_z,
    own_units, x_units, core_units, grad_key, grad_value, grad_recept, grad_z, sums, held, halo_out, halo_in,
    load_sem, core_send, core_recv, first_send, first_recv, second_send, second_recv, z_send, z_recv,
    feed_send, feed_recv, unit_send, unit_recv, halo_send, halo_recv, sum_send, sum_recv,
):
    links = Links(8)
    x, c, z, y, t, size = links.x, links.c, links.z, links.y, links.t, links.size
    count = lefts.shape[0]
    width = lefts.shape[2]
    rows = width // 32
    micro, length = keep.shape[:2]
    late = [(w_key, key_in), (w_value, value_in), (w_recept, recept_in), (spread, spread_in), (unit, unit_in)]
    loads = [pltpu.make_async_copy(source, target, load_sem.at[k]) for k, (source, target) in enumerate(late)]
    for load in loads:
        load.start()
    links.greet(True)
    feed_copies = {}
    for side in (0, 1):
        for o in (1, 2, 3):
            feed_copies[side, o] = remote(
                feed_part.at[side, o], feed_z.at[side, o - 1], feed_send.at[side, o - 1], feed_recv.at[side, o - 1],
                links.along_z[o - 1],
            )
            feed_copies[side, o].start()
    halo_out[...] = jnp.zeros_like(halo_out)
    sums[...] = sums_in[...]

    def part(n, cc, xx):
        at = pl.ds(pl.multiple_of((xx * 2 + cc) * 8 * rows, 8 * rows), 8 * rows)
        return matmul_lead(lefts[n, :, at], rights[n])

    def blocks():
        for zz in range(4):
            for yy in range(2):
                yield zz, yy, slice((zz * 2 + yy) * rows, (zz * 2 + yy + 1) * rows)

    def to_core(n):
        return remote(outgoing.at[n], gathered.at[n], core_send.at[n], core_recv.at[n], links.core)

    def to_first(n):
        return remote(
            gathered.at[n, pl.ds(2, 2)], from_first.at[n], first_send.at[n], first_recv.at[n], links.first
        )

    def to_second(n):
        return remote(gathered.at[n, 1], from_second.at[n], second_send.at[n], second_recv.at[n], links.second)

    def to_z(n, o):
        return remote(
            gathered.at[n, 0, o], from_z.at[n, o - 1], z_send.at[n, o - 1], z_recv.at[n, o - 1], links.along_z[o - 1]
        )

    def other(n, carry):
        for xx in range(2):
            value = part(n, 1 - c, xx)
            for zz, yy, at in blocks():
                outgoing[n, position(xx, yy, x, y, 1 - c), lax.rem(zz + 4 - z, 4)] = value[at].astype(BF)
        to_core(n).start()
        return carry

    def own(n, carry):
        to_core(n).wait_recv()
        for xx in range(2):
            value = part(n, c, xx)
            for zz, yy, at in blocks():
                i, o = position(xx, yy, x, y, c), lax.rem(zz + 4 - z, 4)
                gathered[n, i, o] = (gathered[n, i, o].astype(F32) + value[at]).astype(BF)
        to_first(n).start()
        return carry

    lax.fori_loop(0, count, other, 0)
    lax.fori_loop(0, count, own, 0)

    def pass_second(n):
        to_first(n).wait_recv()
        add_blocks(gathered.at[n, 1], [gathered.at[n, 1], from_first.at[n, 1]])
        to_second(n).start()

    def pass_z(n):
        to_second(n).wait_recv()
        add_blocks(gathered.at[n, 0], [gathered.at[n, 0], from_first.at[n, 0], from_second.at[n]])
        for o in (1, 2, 3):
            to_z(n, o).start()

    def finish(n):
        value = gathered[n, 0, 0].astype(F32)
        for o in (1, 2, 3):
            to_z(n, o).wait_recv()
            value = value + from_z[n, o - 1].astype(F32)
        square_grads[n] = value

    for side in (0, 1):
        for o in (1, 2, 3):
            feed_copies[side, o].wait_recv()
        for r in range(0, feed_part.shape[2], 32):
            at = slice(r, r + 32)
            value = feed_part[side, 0, at].astype(F32)
            for o in range(3):
                value = value + feed_z[side, o, at].astype(F32)
            own_units[side, at] = value.astype(BF)
    units_over_x = remote(own_units, x_units, unit_send.at[0], unit_recv.at[0], links.over_x)
    units_over_x.start()
    units_over_core = remote(own_units, core_units.at[0], unit_send.at[1], unit_recv.at[1], links.core)
    units_over_core.start()

    loads[0].wait()
    dot_rows(grad_key, rights.at[2], key_in)
    pass_second(0)
    loads[1].wait()
    dot_rows(grad_value, rights.at[3], value_in)
    pass_second(1)
    loads[2].wait()
    dot_rows(grad_recept, rights.at[4], recept_in)
    units_over_x.wait_recv()
    both_over_core = remote(x_units, core_units.at[1], unit_send.at[2], unit_recv.at[2], links.core)
    both_over_core.start()
    grads = ((grad_key, MIX_KEY), (grad_value, MIX_VALUE), (grad_recept, MIX_RECEPT))

    def shift_one(rows_at, at, keeping):
        return keeping * sum(g[rows_at, at] * (1.0 - vectors[k : k + 1, at]) for g, k in grads)

    for m in range(micro):
        start = m * length
        halo_out[m : m + 1] = shift_one(slice(start, start + 1), slice(None), keep[m, 0:1, 0:1])
    halo = remote(halo_out, halo_in, halo_send.at[0], halo_recv.at[0], links.row(size - 1))
    halo.start()
    pass_second(2)
    pass_z(0)
    loads[3].wait()
    halo.wait_recv()
    row = lax.broadcasted_iota(jnp.int32, (length, 128), 0)
    for m in range(micro):
        rows_at = slice(m * length, (m + 1) * length)

        def shift_pass(j, carry, m=m, rows_at=rows_at):
            at = lanes(j)
            after = jnp.where(t < size - 1, halo_in[m : m + 1, at], 0.0)
            apart = spread_in[rows_at, at]
            value = roll_rows(shift_one(rows_at, at, keep[m]), -1, after, row)
            for g, k in grads:
                value = value + g[rows_at, at] * vectors[k : k + 1, at]
                sums[k : k + 1, at] += jnp.sum(g[rows_at, at] * apart, axis=0, keepdims=True)
            grad_z[rows_at, at] = value
            return carry

        lax.fori_loop(0, width // 128, shift_pass, 0)
    pass_second(3)
    pass_z(1)
    loads[4].wait()
    norm_back_tiles(
        token_grads, grad_z, unit_in, inverse, vectors[GAIN_ONE : GAIN_ONE + 1, :], grad_residual, sums, GAIN_ONE
    )
    sums[DECAY : DECAY + 1, :] = -sums[DECAY : DECAY + 1, :] * rates[0:1, :] * vectors[DECAY : DECAY + 1, :]
    pass_second(4)

    stages = [[links.core], [links.over_x], [links.over_y], links.along_z]
    pending = []
    source, slot = sums, 0

    def begin(stage, source, slot):
        copies = [
            remote(source, held.at[slot + k], sum_send.at[slot + k], sum_recv.at[slot + k], peer)
            for k, peer in enumerate(stage)
        ]
        for copy in copies:
            copy.start()
        return copies

    def collect(copies, source, slot, target):
        value = source[...]
        for k, copy in enumerate(copies):
            copy.wait_recv()
            value = value + held[slot + k]
        target[...] = value

    copies = begin(stages[0], sums, 0)
    pending += copies
    pass_z(2)
    collect(copies, sums, 0, held.at[6])
    copies = begin(stages[1], held.at[6], 1)
    pending += copies
    pass_z(3)
    finish(0)
    collect(copies, held.at[6], 1, held.at[7])
    copies = begin(stages[2], held.at[7], 2)
    pending += copies
    pass_z(4)
    finish(1)
    collect(copies, held.at[7], 2, held.at[8])
    copies = begin(stages[3], held.at[8], 3)
    pending += copies
    units_over_core.wait_recv()
    both_over_core.wait_recv()
    for side, target in ((1, unit_key), (0, unit_value)):
        for d in range(4):
            for r in range(0, own_units.shape[1], 32):
                at = slice(r, r + 32)
                pick = jnp.where(links.dp == d ^ 1, core_units[0, side, at], core_units[1, side, at])
                pick = jnp.where(links.dp == d ^ 2, x_units[side, at], pick)
                pick = jnp.where(links.dp == d, own_units[side, at], pick)
                target[d, at] = pick.astype(F32)
    collect(copies, held.at[8], 3, vector_grads)
    finish(2)
    finish(3)
    finish(4)
    for n in range(count):
        to_core(n).wait_send()
        to_first(n).wait_send()
        to_second(n).wait_send()
        for o in (1, 2, 3):
            to_z(n, o).wait_send()
    for copy in pending + list(feed_copies.values()) + [units_over_x, units_over_core, both_over_core, halo]:
        copy.wait_send()


def front_backward(near, far):
    feed_part, lefts = near[:2]
    rows = feed_part.shape[2]
    count, tokens, width = lefts.shape
    own = width // 32
    dma = pltpu.SemaphoreType.DMA
    big = pltpu.VMEM((tokens, width), F32)
    square = pltpu.VMEM((width, width), BF)
    return pl.pallas_call(
        front_backward_kernel,
        out_shape=[
            jax.ShapeDtypeStruct((count, own, width), F32),
            jax.ShapeDtypeStruct((4, rows, width), F32), jax.ShapeDtypeStruct((4, rows, width), F32),
            jax.ShapeDtypeStruct((tokens, width), F32), jax.ShapeDtypeStruct((16, width), F32),
        ],
        in_specs=[whole()] * len(near) + [anywhere()] * len(far),
        out_specs=[whole()] * 5,
        scratch_shapes=[square] * 3
        + [big] * 2
        + [
            pltpu.VMEM((count, 4, 4, own, width), BF), pltpu.VMEM((count, 4, 4, own, width), BF),
            pltpu.VMEM((count, 2, 4, own, width), BF), pltpu.VMEM((count, 4, own, width), BF),
            pltpu.VMEM((count, 3, own, width), BF), pltpu.VMEM((2, 3, rows, width), BF),
            pltpu.VMEM((2, rows, width), BF), pltpu.VMEM((2, rows, width), BF), pltpu.VMEM((2, 2, rows, width), BF),
        ]
        + [big] * 4
        + [
            pltpu.VMEM((16, width), F32), pltpu.VMEM((9, 16, width), F32), pltpu.VMEM((8, width), F32),
            pltpu.VMEM((8, width), F32),
            dma((5,)), dma((count,)), dma((count,)), dma((count,)), dma((count,)), dma((count,)), dma((count,)),
            dma((count, 3)), dma((count, 3)), dma((2, 3)), dma((2, 3)), dma((3,)), dma((3,)), dma((1,)), dma((1,)),
            dma((6,)), dma((6,)),
        ],
        compiler_params=pltpu.CompilerParams(
            collective_id=3, has_side_effects=True, vmem_limit_bytes=66_000_000
        ),
        cost_estimate=cost(4 * count * tokens * width * width, 40 * width * width),
        name="front_backward",
    )(*near, *far)


def along_row(block, distance):
    return shifted(block, "tensor", distance)


def with_prior(value, prior):
    return jnp.concatenate([prior, value[:, :-1]], axis=1)


def local_shards(tokens, resets, out_grads, *weights):
    (
        mixer_key, mixer_value, mixer_recept, mixer_output, feed_recept, feed_key, feed_value, *vector_shards
    ) = weights
    size = lax.axis_size("tensor")
    dp, t = lax.axis_index("dp"), lax.axis_index("tensor")
    micro, _, length, width = tokens.shape
    count = micro * length
    wide = lambda v: v.astype(F32)

    unit_rows = feed_key.shape[0] // 4
    feed_shard = jnp.concatenate(
        [lax.dynamic_slice_in_dim(w, dp * unit_rows, unit_rows, 0) for w in (feed_key, feed_value)], axis=1
    )
    feed = lax.all_gather(feed_shard, BOTH, axis=0, tiled=True).reshape(2, 2, 4, 2, unit_rows, 2 * width)
    share = vector_shards[0].shape[0]
    vector_pack = jnp.pad(jnp.stack(vector_shards), ((0, 16 - len(vector_shards)), (0, 128 - share)))
    token_block = tokens[:, 0]
    last_token = along_row(token_block[:, -1:], 1)
    packed, *squares = gather([vector_pack, mixer_key, mixer_value, mixer_recept, mixer_output, feed_recept])
    w_key, w_value, w_recept, w_output, w_feedr = [w.reshape(width, width) for w in squares]
    vectors = wide(packed.reshape(32, 16, 128)[:, : len(vector_shards), :share].transpose(1, 0, 2).reshape(-1, width))
    (
        gain_one, bias_one, gain_two, bias_two, mix_key, mix_value, mix_recept, fading, premium, blend_key, blend_recept
    ) = [vectors[i] for i in range(len(vector_shards))]
    rates = jnp.exp(fading)
    decay = jnp.exp(-rates)
    scan_vectors = jnp.pad(jnp.stack([decay, premium]), ((0, 6), (0, 0)))

    inputs = wide(token_block)
    cotangent = wide(out_grads[:, 0])
    keep = wide(1 - resets[:, 0])[:, :, None]
    keep_lanes = jnp.broadcast_to(keep, (micro, length, 128))
    normed_one, unit_one, inverse_one = norm_rows(inputs, gain_one, bias_one)
    z_one = wide(normed_one.astype(BF))
    prior_one = wide(norm_rows(wide(last_token), gain_one, bias_one)[0].astype(BF))
    before_one = with_prior(z_one, prior_one) * keep
    blend = lambda z, before, mix: (z * mix + before * (1.0 - mix)).astype(BF)
    in_key, in_value, in_recept = [
        blend(z_one, before_one, m).reshape(count, width) for m in (mix_key, mix_value, mix_recept)
    ]
    cube = (micro, length, width)
    keys = matmul(in_key, w_key).reshape(cube)
    values = matmul(in_value, w_value).reshape(cube)
    gates = matmul(in_recept, w_recept).reshape(cube)
    weighted, denom, mixed, prior_a, prior_b, recept = forward_scan(keys, values, gates, keep_lanes, scan_vectors, size)
    weighted = weighted.reshape(count, width)
    residual = inputs + matmul(weighted, w_output).reshape(cube)

    normed_two, unit_two, inverse_two = norm_rows(residual, gain_two, bias_two)
    low_two = normed_two.astype(BF)
    z_two = wide(low_two)
    before_two = with_prior(z_two, wide(along_row(low_two[:, -1:], 1))) * keep
    feed_in = blend(z_two, before_two, blend_key).reshape(count, width)
    feed_rin = blend(z_two, before_two, blend_recept).reshape(count, width)
    gate = jax.nn.sigmoid(matmul(feed_rin, w_feedr)).reshape(cube)
    positive, value_out = channel_forward(feed_in, feed)
    value_out = value_out.reshape(cube)
    result = residual + gate * value_out

    grad_value = (cotangent * gate).astype(BF).reshape(count, width)
    grad_gate = (cotangent * value_out * gate * (1.0 - gate)).astype(BF).reshape(count, width)
    table = jnp.pad(vectors.at[DECAY].set(decay), ((0, 5), (0, 0)))
    flat = lambda v: v.reshape(count, width)
    over_lanes = lambda v: jnp.broadcast_to(v.reshape(count, 1), (count, 128))
    near = [feed_in, grad_value, grad_gate, table, keep_lanes, over_lanes(inverse_two), flat(out_grads)]
    far = [feed, positive, w_feedr, w_output, flat(z_two - before_two), flat(unit_two)]
    far += [flat(v) for v in (keys, values, denom, mixed, prior_a, prior_b, recept)]
    feed_part, grad_keys, grad_values, grad_recept, grad_att, grad_residual, sums = channel_backward(near, far, size)
    lefts = jnp.stack([feed_rin, weighted, in_key, in_value, in_recept])
    rights = jnp.stack([grad_gate, grad_att, grad_keys, grad_values, grad_recept])
    near = [feed_part, lefts, rights, table, keep_lanes, over_lanes(inverse_one), grad_residual, sums]
    near += [jnp.broadcast_to(rates, (8, width))]
    far = [w_key, w_value, w_recept, flat(z_one - before_one), flat(unit_one)]
    square_grads, unit_key, unit_value, token_grads, vector_grads = front_backward(near, far)
    mine = lax.dynamic_slice_in_dim(vector_grads, (dp * size + t) * share, share, 1)
    return (
        result[:, None], token_grads.reshape(cube)[:, None],
        square_grads[2], square_grads[3], square_grads[4], square_grads[1], square_grads[0],
        unit_key.reshape(feed_key.shape), unit_value.reshape(feed_value.shape),
    ) + tuple(mine[i] for i in range(len(vector_shards)))


def is_two_by_two_by_four(mesh):
    return mesh.shape["dp"] == 4 and mesh.shape["tensor"] == 8


def solution(mesh):
    return jax.shard_map(
        local_shards if is_two_by_two_by_four(mesh) else shards,
        mesh=mesh,
        in_specs=(
            P(None, "dp", "tensor", None),
            P(None, "dp", "tensor"),
            P(None, "dp", "tensor", None),
            P(("dp", "tensor"), None),
            P(("dp", "tensor"), None),
            P(("dp", "tensor"), None),
            P(("dp", "tensor"), None),
            P(("dp", "tensor"), None),
            P("tensor", None),
            P("tensor", None),
            P(("dp", "tensor")),
            P(("dp", "tensor")),
            P(("dp", "tensor")),
            P(("dp", "tensor")),
            P(("dp", "tensor")),
            P(("dp", "tensor")),
            P(("dp", "tensor")),
            P(("dp", "tensor")),
            P(("dp", "tensor")),
            P(("dp", "tensor")),
            P(("dp", "tensor")),
        ),
        out_specs=(
            P(None, "dp", "tensor", None),
            P(None, "dp", "tensor", None),
            P(("dp", "tensor"), None),
            P(("dp", "tensor"), None),
            P(("dp", "tensor"), None),
            P(("dp", "tensor"), None),
            P(("dp", "tensor"), None),
            P("tensor", None),
            P("tensor", None),
            P(("dp", "tensor")),
            P(("dp", "tensor")),
            P(("dp", "tensor")),
            P(("dp", "tensor")),
            P(("dp", "tensor")),
            P(("dp", "tensor")),
            P(("dp", "tensor")),
            P(("dp", "tensor")),
            P(("dp", "tensor")),
            P(("dp", "tensor")),
            P(("dp", "tensor")),
        ),
        check_vma=False,
    )
```

```python
import functools

import jax
import jax.numpy as jnp
from jax import lax
from jax.experimental import pallas as pl
from jax.experimental.pallas import tpu as pltpu
from jax.sharding import PartitionSpec as P

EPSILON = 1e-05


def entering(shard, axis, combine, identity, reverse):
    size, here = (lax.axis_size(axis), lax.axis_index(axis))
    everything = jax.tree.map(lambda part: lax.all_gather(part, axis), shard)
    start = jax.tree.map(
        lambda part, zero: jnp.broadcast_to(jnp.asarray(zero, part.dtype), part.shape),
        shard,
        identity,
    )

    def turn(k, before):
        at = size - 1 - k if reverse else k
        reached = at > here if reverse else at < here
        new = combine(before, jax.tree.map(lambda part: part[at], everything))
        return jax.tree.map(lambda a, b: jnp.where(reached, a, b), new, before)

    return lax.fori_loop(0, size, turn, start)


def shifted(block, axis, distance):
    devices = range(lax.axis_size(axis))
    route = [(i - distance, i) for i in devices if i - distance in devices]
    return lax.ppermute(block, axis, route)


def norm_rows(payload_series, gain, bias):
    center = payload_series - jnp.mean(payload_series, axis=-1, keepdims=True)
    inverse = lax.rsqrt(jnp.mean(center * center, axis=-1, keepdims=True) + EPSILON)
    normed = center * inverse
    return (normed * gain + bias, normed, inverse)


def norm_back(grad_out, normed, inverse, gain):
    scaled = grad_out * gain
    centred = scaled - jnp.mean(scaled, axis=-1, keepdims=True)
    grad_in = inverse * (centred - normed * jnp.mean(scaled * normed, axis=-1, keepdims=True))
    return (grad_in, jnp.sum(grad_out * normed, axis=0), jnp.sum(grad_out, axis=0))


def affine(earlier, later):
    return (
        earlier[0] * later[0],
        later[0] * earlier[1] + later[1],
        later[0] * earlier[2] + later[2],
    )


def carry_across(summary, backward):
    width = summary[0].shape[0]
    identity = (
        jnp.ones((width,), jnp.float32),
        jnp.zeros((width,), jnp.float32),
        jnp.zeros((width,), jnp.float32),
    )
    return entering(summary, "tensor", affine, identity, backward)


def matmul(left, right):
    return jnp.dot(left, right, preferred_element_type=jnp.float32)


def matmul_lead(left, right):
    return lax.dot_general(
        left, right, (((0,), (0,)), ((), ())), preferred_element_type=jnp.float32
    )


def matmul_last(left, right):
    return lax.dot_general(
        left, right, (((1,), (1,)), ((), ())), preferred_element_type=jnp.float32
    )


def shards(
    tokens,
    resets,
    out_grads,
    mixer_key,
    mixer_value,
    mixer_recept,
    mixer_output,
    feed_recept,
    feed_key,
    feed_value,
    first_gain,
    first_bias,
    second_gain,
    second_bias,
    mixing_key,
    mixing_value,
    mixing_recept,
    time_decay,
    time_first,
    feeding_key,
    feeding_recept,
):
    gathered = (
        lax.all_gather(mixer_key, ("dp", "tensor"), axis=0, tiled=True),
        lax.all_gather(mixer_value, ("dp", "tensor"), axis=0, tiled=True),
        lax.all_gather(mixer_recept, ("dp", "tensor"), axis=0, tiled=True),
        lax.all_gather(mixer_output, ("dp", "tensor"), axis=0, tiled=True),
        lax.all_gather(feed_recept, ("dp", "tensor"), axis=0, tiled=True),
        lax.all_gather(first_gain, ("dp", "tensor"), axis=0, tiled=True),
        lax.all_gather(first_bias, ("dp", "tensor"), axis=0, tiled=True),
        lax.all_gather(second_gain, ("dp", "tensor"), axis=0, tiled=True),
        lax.all_gather(second_bias, ("dp", "tensor"), axis=0, tiled=True),
        lax.all_gather(mixing_key, ("dp", "tensor"), axis=0, tiled=True),
        lax.all_gather(mixing_value, ("dp", "tensor"), axis=0, tiled=True),
        lax.all_gather(mixing_recept, ("dp", "tensor"), axis=0, tiled=True),
        lax.all_gather(time_decay, ("dp", "tensor"), axis=0, tiled=True),
        lax.all_gather(time_first, ("dp", "tensor"), axis=0, tiled=True),
        lax.all_gather(feeding_key, ("dp", "tensor"), axis=0, tiled=True),
        lax.all_gather(feeding_recept, ("dp", "tensor"), axis=0, tiled=True),
    )
    w_key, w_value, w_recept, w_output, w_feedr = (
        gathered[0],
        gathered[1],
        gathered[2],
        gathered[3],
        gathered[4],
    )
    parameter_vectors = [piece.astype(jnp.float32) for piece in gathered[5:]]
    gain_one, bias_one, gain_two, bias_two = (
        parameter_vectors[0],
        parameter_vectors[1],
        parameter_vectors[2],
        parameter_vectors[3],
    )
    mix_key, mix_value, mix_recept = (
        parameter_vectors[4],
        parameter_vectors[5],
        parameter_vectors[6],
    )
    (
        fading_speed_logarithm,
        opening_premium_logarithm,
        channel_lookup_blend,
        channel_gating_blend,
    ) = (parameter_vectors[7], parameter_vectors[8], parameter_vectors[9], parameter_vectors[10])
    rates = jnp.exp(fading_speed_logarithm)
    fading_multiplier = jnp.exp(-rates)
    micro_count = tokens.shape[0]
    width = tokens.shape[3]
    grad_keyw = jnp.zeros(feed_key.shape, jnp.float32)
    grad_valuew = jnp.zeros(feed_value.shape, jnp.float32)
    square_grads = [jnp.zeros((width, width), jnp.float32) for index_one in range(5)]
    parameter_vector_gradients = [jnp.zeros((width,), jnp.float32) for index_two in range(11)]
    results = []
    input_grads = []
    for micro_index in range(micro_count):
        inputs = tokens[micro_index, 0].astype(jnp.float32)
        restart_retain_flags = (1 - resets[micro_index, 0]).astype(jnp.float32)[:, None]
        cotangent = out_grads[micro_index, 0].astype(jnp.float32)
        normed_one, unit_one, inverse_one = norm_rows(inputs, gain_one, bias_one)
        z_one = normed_one.astype(jnp.bfloat16)
        prior_one = shifted(z_one[-1:], "tensor", 1)
        before_one = (
            jnp.concatenate([prior_one, z_one[:-1]], axis=0).astype(jnp.float32)
            * restart_retain_flags
        )
        z_onef = z_one.astype(jnp.float32)
        in_key = (z_onef * mix_key + before_one * (1.0 - mix_key)).astype(jnp.bfloat16)
        in_value = (z_onef * mix_value + before_one * (1.0 - mix_value)).astype(jnp.bfloat16)
        in_recept = (z_onef * mix_recept + before_one * (1.0 - mix_recept)).astype(jnp.bfloat16)
        lookup_series = matmul(in_key, w_key)
        payload_series = matmul(in_value, w_value)
        recept = jax.nn.sigmoid(matmul(in_recept, w_recept))
        powered_lookup = jnp.exp(lookup_series)
        premium_plus_lookup = jnp.exp(opening_premium_logarithm + lookup_series)
        factor = restart_retain_flags * fading_multiplier
        cum_factor, local_a, local_b = lax.associative_scan(
            affine, (factor, powered_lookup * payload_series, powered_lookup), axis=0
        )
        incoming = carry_across((cum_factor[-1], local_a[-1], local_b[-1]), False)
        upper_running_state = local_a + cum_factor * incoming[1]
        lower_running_state = local_b + cum_factor * incoming[2]
        earlier_upper_state = jnp.concatenate([incoming[1][None], upper_running_state[:-1]], axis=0)
        earlier_lower_state = jnp.concatenate([incoming[2][None], lower_running_state[:-1]], axis=0)
        lower_quotient_part = restart_retain_flags * earlier_lower_state + premium_plus_lookup
        blended = (
            restart_retain_flags * earlier_upper_state + premium_plus_lookup * payload_series
        ) / lower_quotient_part
        weighted = (recept * blended).astype(jnp.bfloat16)
        residual = inputs + matmul(weighted, w_output)
        normed_two, unit_two, inverse_two = norm_rows(residual, gain_two, bias_two)
        z_two = normed_two.astype(jnp.bfloat16)
        prior_two = shifted(z_two[-1:], "tensor", 1)
        before_two = (
            jnp.concatenate([prior_two, z_two[:-1]], axis=0).astype(jnp.float32)
            * restart_retain_flags
        )
        z_twof = z_two.astype(jnp.float32)
        feed_in = (
            z_twof * channel_lookup_blend + before_two * (1.0 - channel_lookup_blend)
        ).astype(jnp.bfloat16)
        feed_rin = (
            z_twof * channel_gating_blend + before_two * (1.0 - channel_gating_blend)
        ).astype(jnp.bfloat16)
        gate = jax.nn.sigmoid(matmul(feed_rin, w_feedr))
        all_in = lax.all_gather(feed_in, "tensor", axis=0, tiled=True)
        hidden_pre = matmul_last(feed_key, all_in)
        hidden = jnp.square(jnp.maximum(hidden_pre, 0.0)).astype(jnp.bfloat16)
        value_out = lax.psum_scatter(
            matmul_lead(hidden, feed_value), "tensor", scatter_dimension=0, tiled=True
        )
        results.append(residual + gate * value_out)
        grad_value = (cotangent * gate).astype(jnp.bfloat16)
        grad_gate = (cotangent * value_out * gate * (1.0 - gate)).astype(jnp.bfloat16)
        square_grads[4] = square_grads[4] + matmul_lead(feed_rin, grad_gate)
        grad_rin = matmul_last(grad_gate, w_feedr)
        relu_twice = 2.0 * jnp.maximum(hidden_pre, 0.0)
        add_piece = lax.all_gather(grad_value, "tensor", axis=0, tiled=True)
        rows_total = matmul(hidden, add_piece)
        block = matmul_last(feed_value, add_piece)
        grad_valuew = grad_valuew + rows_total
        grad_pre = (block * relu_twice).astype(jnp.bfloat16)
        grad_keyw = grad_keyw + matmul(grad_pre, all_in)
        grad_in = lax.psum_scatter(
            matmul_lead(grad_pre, feed_key), "tensor", scatter_dimension=0, tiled=True
        )
        parameter_vector_gradients[9] = parameter_vector_gradients[9] + jnp.sum(
            grad_in * (z_twof - before_two), axis=0
        )
        parameter_vector_gradients[10] = parameter_vector_gradients[10] + jnp.sum(
            grad_rin * (z_twof - before_two), axis=0
        )
        shift_two = restart_retain_flags * (
            grad_in * (1.0 - channel_lookup_blend) + grad_rin * (1.0 - channel_gating_blend)
        )
        after_two = shifted(shift_two[:1], "tensor", -1)
        grad_z_two = (
            grad_in * channel_lookup_blend
            + grad_rin * channel_gating_blend
            + jnp.concatenate([shift_two[1:], after_two], axis=0)
        )
        back_two, gain_part, bias_part = norm_back(grad_z_two, unit_two, inverse_two, gain_two)
        parameter_vector_gradients[2] = parameter_vector_gradients[2] + gain_part
        parameter_vector_gradients[3] = parameter_vector_gradients[3] + bias_part
        grad_residual = cotangent + back_two
        grad_att = grad_residual.astype(jnp.bfloat16)
        square_grads[3] = square_grads[3] + matmul_lead(weighted, grad_att)
        grad_weighted = matmul_last(grad_att, w_output)
        grad_mixed = grad_weighted * recept
        grad_recept = (grad_weighted * blended * recept * (1.0 - recept)).astype(jnp.bfloat16)
        upper_adjoint = grad_mixed / lower_quotient_part
        denominator_gradient = -grad_mixed * blended / lower_quotient_part
        cum_back, local_xa, local_xb = lax.associative_scan(
            affine,
            (
                factor,
                restart_retain_flags * upper_adjoint,
                restart_retain_flags * denominator_gradient,
            ),
            reverse=True,
            axis=0,
        )
        beyond = carry_across((cum_back[0], local_xa[0], local_xb[0]), True)
        adjoint_a = local_xa + cum_back * beyond[1]
        adjoint_b = local_xb + cum_back * beyond[2]
        running_upper_total = jnp.concatenate([adjoint_a[1:], beyond[1][None]], axis=0)
        running_lower_total = jnp.concatenate([adjoint_b[1:], beyond[2][None]], axis=0)
        premium_power = premium_plus_lookup * (
            payload_series * upper_adjoint + denominator_gradient
        )
        adjoint_payloads = (
            premium_plus_lookup * upper_adjoint + powered_lookup * running_upper_total
        ).astype(jnp.bfloat16)
        key_gradient_rows = (
            premium_power
            + powered_lookup * (payload_series * running_upper_total + running_lower_total)
        ).astype(jnp.bfloat16)
        parameter_vector_gradients[8] = parameter_vector_gradients[8] + jnp.sum(
            premium_power, axis=0
        )
        decay_sum = jnp.sum(
            restart_retain_flags
            * (
                running_upper_total * earlier_upper_state
                + running_lower_total * earlier_lower_state
            ),
            axis=0,
        )
        parameter_vector_gradients[7] = (
            parameter_vector_gradients[7] - rates * fading_multiplier * decay_sum
        )
        square_grads[0] = square_grads[0] + matmul_lead(in_key, key_gradient_rows)
        square_grads[1] = square_grads[1] + matmul_lead(in_value, adjoint_payloads)
        square_grads[2] = square_grads[2] + matmul_lead(in_recept, grad_recept)
        grad_inkey = matmul_last(key_gradient_rows, w_key)
        grad_invalue = matmul_last(adjoint_payloads, w_value)
        grad_inrecept = matmul_last(grad_recept, w_recept)
        spread_one = z_onef - before_one
        parameter_vector_gradients[4] = parameter_vector_gradients[4] + jnp.sum(
            grad_inkey * spread_one, axis=0
        )
        parameter_vector_gradients[5] = parameter_vector_gradients[5] + jnp.sum(
            grad_invalue * spread_one, axis=0
        )
        parameter_vector_gradients[6] = parameter_vector_gradients[6] + jnp.sum(
            grad_inrecept * spread_one, axis=0
        )
        shift_one = restart_retain_flags * (
            grad_inkey * (1.0 - mix_key)
            + grad_invalue * (1.0 - mix_value)
            + grad_inrecept * (1.0 - mix_recept)
        )
        after_one = shifted(shift_one[:1], "tensor", -1)
        grad_z_one = (
            grad_inkey * mix_key
            + grad_invalue * mix_value
            + grad_inrecept * mix_recept
            + jnp.concatenate([shift_one[1:], after_one], axis=0)
        )
        back_one, gain_first, bias_first = norm_back(grad_z_one, unit_one, inverse_one, gain_one)
        parameter_vector_gradients[0] = parameter_vector_gradients[0] + gain_first
        parameter_vector_gradients[1] = parameter_vector_gradients[1] + bias_first
        input_grads.append(grad_residual + back_one)
    owned = (
        lax.psum_scatter(square_grads[0], ("dp", "tensor"), scatter_dimension=0, tiled=True),
        lax.psum_scatter(square_grads[1], ("dp", "tensor"), scatter_dimension=0, tiled=True),
        lax.psum_scatter(square_grads[2], ("dp", "tensor"), scatter_dimension=0, tiled=True),
        lax.psum_scatter(square_grads[3], ("dp", "tensor"), scatter_dimension=0, tiled=True),
        lax.psum_scatter(square_grads[4], ("dp", "tensor"), scatter_dimension=0, tiled=True),
        lax.psum_scatter(
            parameter_vector_gradients[0], ("dp", "tensor"), scatter_dimension=0, tiled=True
        ),
        lax.psum_scatter(
            parameter_vector_gradients[1], ("dp", "tensor"), scatter_dimension=0, tiled=True
        ),
        lax.psum_scatter(
            parameter_vector_gradients[2], ("dp", "tensor"), scatter_dimension=0, tiled=True
        ),
        lax.psum_scatter(
            parameter_vector_gradients[3], ("dp", "tensor"), scatter_dimension=0, tiled=True
        ),
        lax.psum_scatter(
            parameter_vector_gradients[4], ("dp", "tensor"), scatter_dimension=0, tiled=True
        ),
        lax.psum_scatter(
            parameter_vector_gradients[5], ("dp", "tensor"), scatter_dimension=0, tiled=True
        ),
        lax.psum_scatter(
            parameter_vector_gradients[6], ("dp", "tensor"), scatter_dimension=0, tiled=True
        ),
        lax.psum_scatter(
            parameter_vector_gradients[7], ("dp", "tensor"), scatter_dimension=0, tiled=True
        ),
        lax.psum_scatter(
            parameter_vector_gradients[8], ("dp", "tensor"), scatter_dimension=0, tiled=True
        ),
        lax.psum_scatter(
            parameter_vector_gradients[9], ("dp", "tensor"), scatter_dimension=0, tiled=True
        ),
        lax.psum_scatter(
            parameter_vector_gradients[10], ("dp", "tensor"), scatter_dimension=0, tiled=True
        ),
    )
    key_rows, value_rows_grad = (grad_keyw, grad_valuew)
    key_total, value_total = (
        lax.psum(key_rows.astype(jnp.bfloat16), "dp").astype(jnp.float32),
        lax.psum(value_rows_grad.astype(jnp.bfloat16), "dp").astype(jnp.float32),
    )
    result_all = jnp.stack(results)[:, None]
    grads_all = jnp.stack(input_grads)[:, None]
    return (
        result_all,
        grads_all,
        owned[0],
        owned[1],
        owned[2],
        owned[3],
        owned[4],
        key_total,
        value_total,
        owned[5],
        owned[6],
        owned[7],
        owned[8],
        owned[9],
        owned[10],
        owned[11],
        owned[12],
        owned[13],
        owned[14],
        owned[15],
    )


BF = jnp.bfloat16
F32 = jnp.float32
BOTH = ("dp", "tensor")
MESH_ID = pl.DeviceIdType.MESH


def cost(flops, moved):
    return pl.CostEstimate(flops=flops, bytes_accessed=moved, transcendentals=0)


def whole():
    return pl.BlockSpec(memory_space=pltpu.VMEM)


def anywhere():
    return pl.BlockSpec(memory_space=pl.ANY)


def roll_rows(value, distance, fill, row):
    size = value.shape[0]
    moved = pltpu.roll(value, distance % size, 0)
    outside = row < distance if distance > 0 else row >= size + distance
    return jnp.where(outside, fill, moved)


def doubling(factor, up, low, row, sign):
    size, step = factor.shape[0], 1
    while step < size:
        up = up + factor * roll_rows(up, sign * step, 0.0, row)
        low = low + factor * roll_rows(low, sign * step, 0.0, row)
        factor = factor * roll_rows(factor, sign * step, 1.0, row)
        step *= 2
    return factor, up, low


def row_copies(summary, arrived, send, recv, t, dp, size):
    return [
        pltpu.make_async_remote_copy(
            src_ref=summary,
            dst_ref=arrived.at[o],
            send_sem=send.at[o],
            recv_sem=recv.at[o],
            device_id=(dp, lax.rem(t + o, size)),
            device_id_type=MESH_ID,
        )
        for o in range(1, size)
    ]


def share_row(summary, arrived, send, recv, t, dp, size):
    copies = row_copies(summary, arrived, send, recv, t, dp, size)
    for copy in copies:
        copy.start()
    for copy in copies:
        copy.wait_recv()
    return copies


def lanes(j):
    return pl.ds(pl.multiple_of(j * 128, 128), 128)


def owner(i, x, y, c):
    first, second = i // 2, i % 2
    flip_x = first * c + second * (1 - c)
    flip_y = first * (1 - c) + second * c
    return x + flip_x - 2 * x * flip_x, y + flip_y - 2 * y * flip_y


def position(xx, yy, x, y, c):
    flip_x = x + xx - 2 * x * xx
    flip_y = y + yy - 2 * y * yy
    return 2 * (flip_x * c + flip_y * (1 - c)) + flip_x * (1 - c) + flip_y * c


class Links:
    def __init__(self, size):
        dp, t = lax.axis_index("dp"), lax.axis_index("tensor")
        x, c, z, y = dp // 2, dp % 2, t // 2, t % 2
        self.x, self.c, self.z, self.y, self.dp, self.t, self.size = x, c, z, y, dp, t, size
        over_x, over_y = ((1 - x) * 2 + c, t), (dp, z * 2 + 1 - y)
        self.over_x = over_x
        self.core = (x * 2 + 1 - c, t)
        self.first = (jnp.where(c == 0, over_y[0], over_x[0]), jnp.where(c == 0, over_y[1], over_x[1]))
        self.second = (jnp.where(c == 0, over_x[0], over_y[0]), jnp.where(c == 0, over_x[1], over_y[1]))
        self.along_z = [(dp, lax.rem(z + o, 4) * 2 + y) for o in (1, 2, 3)]
        self.over_y = over_y

    def row(self, o):
        return (self.dp, lax.rem(self.t + o, self.size))

    def greet(self, whole_row):
        peers = [self.row(o) for o in range(1, self.size)] if whole_row else self.along_z + [self.over_y]
        peers = peers + [self.over_x, self.core]
        barrier = pltpu.get_barrier_semaphore()
        for peer in peers:
            pl.semaphore_signal(barrier, inc=1, device_id=peer, device_id_type=MESH_ID)
        pl.semaphore_wait(barrier, len(peers))


def remote(source, target, send, recv, device):
    return pltpu.make_async_remote_copy(
        src_ref=source, dst_ref=target, send_sem=send, recv_sem=recv, device_id=device, device_id_type=MESH_ID
    )


def add_blocks(target, sources):
    count, rows = target.shape[:2]
    tile = min(rows, 32)
    per = rows // tile

    def turn(k, carry):
        n, at = k // per, pl.ds(pl.multiple_of(lax.rem(k, per) * tile, tile), tile)
        value = sources[0][n, at].astype(F32)
        for source in sources[1:]:
            value = value + source[n, at].astype(F32)
        target[n, at] = value.astype(target.dtype)
        return carry

    lax.fori_loop(0, count * per, turn, 0)


def dot_rows(target, left, right):
    tile = 256

    def turn(n, carry):
        at = pl.ds(pl.multiple_of(n * tile, tile), tile)
        target[:, at] = matmul_last(left[...], right[at, :])
        return carry

    lax.fori_loop(0, right.shape[0] // tile, turn, 0)


def norm_back_tiles(target, grads, normed, inverse, gain, base, sums, gain_row):
    tile = 32
    width = grads.shape[1]

    def turn(k, carry):
        at = pl.ds(pl.multiple_of(k * tile, tile), tile)
        grad, unit = grads[at, :], normed[at, :]
        scaled = grad * gain
        middle = jnp.sum(scaled, axis=-1, keepdims=True) * (1.0 / width)
        along = jnp.sum(scaled * unit, axis=-1, keepdims=True) * (1.0 / width)
        target[at, :] = base[at, :].astype(F32) + inverse[at, 0:1] * (scaled - middle - unit * along)
        sums[gain_row : gain_row + 1, :] += jnp.sum(grad * unit, axis=0, keepdims=True)
        sums[gain_row + 1 : gain_row + 2, :] += jnp.sum(grad, axis=0, keepdims=True)
        return carry

    lax.fori_loop(0, grads.shape[0] // tile, turn, 0)


GAIN_ONE, BIAS_ONE, GAIN_TWO, BIAS_TWO, MIX_KEY, MIX_VALUE, MIX_RECEPT, DECAY, PREMIUM, BLEND_KEY, BLEND_RECEPT = range(11)


def norm_tiles(source, unit, inverse):
    rows, width = source.shape
    tile = min(rows, 32)

    def turn(k, carry):
        at = pl.ds(pl.multiple_of(k * tile, tile), tile)
        value = source[at, :].astype(F32)
        center = value - jnp.sum(value, axis=-1, keepdims=True) * (1.0 / width)
        scale = lax.rsqrt(jnp.sum(center * center, axis=-1, keepdims=True) * (1.0 / width) + EPSILON)
        unit[at, :] = center * scale
        inverse[at, :] = jnp.broadcast_to(scale, (tile, 128))
        return carry

    lax.fori_loop(0, rows // tile, turn, 0)


def dot_columns(finish, left, right):
    tile = 256
    depth = left.shape[1]

    def turn(n, carry):
        at = pl.ds(pl.multiple_of(n * tile, tile), tile)
        finish(at, matmul(left[...], right[:, :, :, :, :, at].reshape(depth, tile)))
        return carry

    lax.fori_loop(0, right.shape[5] // tile, turn, 0)


SKEW = 2


def forward_kernel(
    tokens, cotangent, keep,
    own_vectors, own_key, own_value, own_recept, own_output, own_feedr, own_feed,
    all_vectors, all_key, all_value, all_recept, all_output, all_feedr, all_feed,
    result, table_out, rates_out, lefts, feed_in_out, grad_value_out, grad_gate_out, positive, spread_one_out,
    unit_one_out, inverse_one_out, spread_two_out, unit_two_out, inverse_two_out, keys_out, values_out, denom_out,
    mixed_out, prior_a_out, prior_b_out, recept_out,
    packed, table, rates, squares, feed_slot, positive_slot, left_parts, feed_in, grad_value, grad_gate, spread_one,
    unit_one, inverse_one, spread_two, unit_two, inverse_two, keys, values, gates, denom, mixed, prior_a, prior_b,
    cum, up, low, residual, total, halo_tokens, halo_unit, halo_inverse, summary, arrived, entering_rows, halo_out, halo_in,
    send, recv, own_sem, load_sem, out_sem, slot_sem, scan_send, scan_recv, halo_send, halo_recv,
):
    size = arrived.shape[0]
    links = Links(size)
    x, c, z, y, t, dp = links.x, links.c, links.z, links.y, links.t, links.dp
    count, width = tokens.shape
    micro, length = keep.shape[:2]
    ins = [own_vectors, own_key, own_value, own_recept, own_output, own_feedr, own_feed]
    outs = [all_vectors, all_key, all_value, all_recept, all_output, all_feedr, all_feed]
    piece = 16
    chunks = [(i, r) for i in range(7) for r in range(0, ins[i].shape[0], piece)]
    steps = len(chunks)
    feed_steps = ins[6].shape[0] // piece
    feed_base = steps - feed_steps
    x_first, y_first = jnp.where(c == 0, x, 1 - x), jnp.where(c == 0, 1 - y, y)
    first, second = links.first, links.second

    def place(n):
        if isinstance(n, int):
            i, start = chunks[n]
            return i, pl.ds(start, piece)
        return 6, pl.ds(pl.multiple_of((n - feed_base) * piece, piece), piece)

    def copy_z(n, o):
        i, at = place(n)
        return remote(ins[i].at[at], outs[i].at[x, c, z, y, at], send.at[n, o], recv.at[n, o], links.along_z[o])

    def copy_column(n, j, xx, yy, device):
        i, at = place(n)
        column = outs[i].at[xx, c, :, yy, at]
        return remote(column, column, send.at[n, j], recv.at[n, j], device)

    def copy_first(n):
        return copy_column(n, 3, x, y, first)

    def copy_second(n):
        return copy_column(n, 4, x, y, second)

    def copy_passed(n):
        return copy_column(n, 5, x_first, y_first, second)

    def copy_core(n):
        i, at = place(n)
        half = outs[i].at[:, c, :, :, at]
        return remote(half, half, send.at[n, 6], recv.at[n, 6], links.core)

    def step_a(n):
        for o in range(3):
            copy_z(n, o).wait_recv()
        copy_first(n).start()
        copy_second(n).start()

    def step_b(n):
        copy_first(n).wait_recv()
        copy_passed(n).start()

    def step_c(n):
        copy_second(n).wait_recv()
        copy_passed(n).wait_recv()
        copy_core(n).start()

    def advance(*numbers):
        for s in numbers:
            if s < steps:
                step_a(s)
            if 0 <= s - SKEW < steps:
                step_b(s - SKEW)
            if 0 <= s - 2 * SKEW < steps:
                step_c(s - 2 * SKEW)

    def load(k):
        return pltpu.make_async_copy(outs[1 + k], squares.at[k], load_sem.at[k])

    def ready(k):
        for n in (2 * k + 1, 2 * k + 2):
            copy_core(n).wait_recv()
        load(k).start()

    written = []

    def write(source, target):
        copy = pltpu.make_async_copy(source, target, out_sem.at[len(written)])
        copy.start()
        written.append(copy)

    owns = [pltpu.make_async_copy(ins[i], outs[i].at[x, c, z, y], own_sem.at[i]) for i in range(7)]
    for own in owns:
        own.start()
    links.greet(True)
    for n in range(steps):
        for o in range(3):
            copy_z(n, o).start()
    halo_copies = [
        remote(
            tokens.at[pl.ds((m + 1) * length - piece, piece)], halo_tokens.at[pl.ds(m * piece, piece)],
            halo_send.at[m], halo_recv.at[m], links.row(1),
        )
        for m in range(micro)
    ]
    for halo in halo_copies:
        halo.start()
    summary[...] = jnp.zeros_like(summary)
    halo_out[...] = jnp.zeros_like(halo_out)
    total[...] = jnp.zeros_like(total)
    for own in owns:
        own.wait()
    advance(0, 1)
    norm_tiles(tokens, unit_one, inverse_one)
    write(unit_one, unit_one_out)
    write(inverse_one, inverse_one_out)
    advance(2, 3, 4)
    for halo in halo_copies:
        halo.wait_recv()
    norm_tiles(halo_tokens, halo_unit, halo_inverse)
    copy_core(0).wait_recv()

    vector_load = pltpu.make_async_copy(all_vectors, packed, load_sem.at[5])
    vector_load.start()
    advance(5)
    vector_load.wait()
    share = width // 32
    per = 128 // share
    for j in range(width // 128):
        value = None
        for q in range(per):
            d = j * per + q
            part = packed[d // 16, (d // 8) % 2, (d // 2) % 4, d % 2].astype(F32)
            part = pltpu.roll(part, q * share, 1) if q else part
            value = part if value is None else value + part
        table[:, j * 128 : (j + 1) * 128] = value
    speed = jnp.exp(table[DECAY : DECAY + 1, :])
    rates[...] = jnp.broadcast_to(speed, rates.shape)
    table[DECAY : DECAY + 1, :] = jnp.exp(-speed)
    write(table, table_out)
    write(rates, rates_out)
    row = lax.broadcasted_iota(jnp.int32, (length, 128), 0)

    def vector(k, at):
        return table[k : k + 1, at]

    def normed(unit, gain, bias, at):
        return (unit * vector(gain, at) + vector(bias, at)).astype(BF).astype(F32)

    def blends(spread, unit, m, prior, gain, bias, mixes):
        rows_at = slice(m * length, (m + 1) * length)

        def turn(j, carry):
            at = lanes(j)
            now = normed(unit[rows_at, at], gain, bias, at)
            before = roll_rows(now, 1, jnp.where(t > 0, prior(at), 0.0), row) * keep[m]
            spread[rows_at, at] = now - before
            for target, mix in mixes:
                target[rows_at, at] = (now * vector(mix, at) + before * (1.0 - vector(mix, at))).astype(BF)
            return carry

        lax.fori_loop(0, width // 128, turn, 0)

    mixes = [(left_parts.at[2 + k], MIX_KEY + k) for k in range(3)]
    for m in range(micro):
        last = (m + 1) * piece - 1

        def prior(at, last=last):
            return normed(halo_unit[last : last + 1, at], GAIN_ONE, BIAS_ONE, at)

        blends(spread_one, unit_one, m, prior, GAIN_ONE, BIAS_ONE, mixes)
        advance(6 + m)
    write(spread_one, spread_one_out)
    for k in range(3):
        write(left_parts.at[2 + k], lefts.at[2 + k])

    def keep_in(target):
        def finish(at, value):
            target[:, at] = value

        return finish

    ready(0)
    advance(8)
    load(0).wait()
    dot_columns(keep_in(keys), left_parts.at[2], squares.at[0])
    write(keys, keys_out)
    ready(1)
    advance(9, 10)
    load(1).wait()
    dot_columns(keep_in(values), left_parts.at[3], squares.at[1])
    write(values, values_out)

    for m in range(micro):
        rows_at = slice(m * length, (m + 1) * length)

        def first_pass(j, carry, m=m, rows_at=rows_at):
            at = lanes(j)
            power = jnp.exp(keys[rows_at, at])
            f, a, b = doubling(keep[m] * vector(DECAY, at), power * values[rows_at, at], power, row, 1)
            cum[rows_at, at] = f
            up[rows_at, at] = a
            low[rows_at, at] = b
            summary[3 * m : 3 * m + 1, at] = f[length - 1 :]
            summary[3 * m + 1 : 3 * m + 2, at] = a[length - 1 :]
            summary[3 * m + 2 : 3 * m + 3, at] = b[length - 1 :]
            return carry

        lax.fori_loop(0, width // 128, first_pass, 0)
        advance(11 + m)
    scan_copies = row_copies(summary, arrived, scan_send, scan_recv, t, dp, size)
    for copy in scan_copies:
        copy.start()
    ready(2)
    load(2).wait()

    def finish_gate(at, value):
        gates[:, at] = jax.nn.sigmoid(value)

    dot_columns(finish_gate, left_parts.at[4], squares.at[2])
    write(gates, recept_out)
    for copy in scan_copies:
        copy.wait_recv()
    for m in range(micro):
        a = jnp.zeros((1, width), F32)
        b = jnp.zeros((1, width), F32)
        for o in range(size - 1, 0, -1):
            f = arrived[o, 3 * m : 3 * m + 1]
            a = jnp.where(t >= o, f * a + arrived[o, 3 * m + 1 : 3 * m + 2], a)
            b = jnp.where(t >= o, f * b + arrived[o, 3 * m + 2 : 3 * m + 3], b)
        entering_rows[2 * m : 2 * m + 1] = a
        entering_rows[2 * m + 1 : 2 * m + 2] = b
    advance(13)
    for m in range(micro):
        rows_at = slice(m * length, (m + 1) * length)

        def second_pass(j, carry, m=m, rows_at=rows_at):
            at = lanes(j)
            enter_a = entering_rows[2 * m : 2 * m + 1, at]
            enter_b = entering_rows[2 * m + 1 : 2 * m + 2, at]
            f = cum[rows_at, at]
            before_a = roll_rows(up[rows_at, at] + f * enter_a, 1, enter_a, row)
            before_b = roll_rows(low[rows_at, at] + f * enter_b, 1, enter_b, row)
            bonus = jnp.exp(vector(PREMIUM, at) + keys[rows_at, at])
            below = keep[m] * before_b + bonus
            blended = (keep[m] * before_a + bonus * values[rows_at, at]) / below
            left_parts[1, rows_at, at] = (gates[rows_at, at] * blended).astype(BF)
            denom[rows_at, at] = below
            mixed[rows_at, at] = blended
            prior_a[rows_at, at] = before_a
            prior_b[rows_at, at] = before_b
            return carry

        lax.fori_loop(0, width // 128, second_pass, 0)
    write(left_parts.at[1], lefts.at[1])
    write(denom, denom_out)
    write(mixed, mixed_out)
    write(prior_a, prior_a_out)
    write(prior_b, prior_b_out)
    ready(3)
    advance(14)
    load(3).wait()

    def finish_residual(at, value):
        residual[:, at] = tokens[:, at].astype(F32) + value

    dot_columns(finish_residual, left_parts.at[1], squares.at[3])
    norm_tiles(residual, unit_two, inverse_two)
    write(unit_two, unit_two_out)
    write(inverse_two, inverse_two_out)
    for m in range(micro):
        last = (m + 1) * length - 1
        halo_out[m : m + 1, :] = normed(unit_two[last : last + 1, :], GAIN_TWO, BIAS_TWO, slice(None))
    halo_two = remote(halo_out, halo_in, halo_send.at[micro], halo_recv.at[micro], links.row(1))
    halo_two.start()
    ready(4)
    advance(15)
    halo_two.wait_recv()
    mixes = [(feed_in, BLEND_KEY), (left_parts.at[0], BLEND_RECEPT)]
    for m in range(micro):

        def prior(at, m=m):
            return halo_in[m : m + 1, at]

        blends(spread_two, unit_two, m, prior, GAIN_TWO, BIAS_TWO, mixes)
    write(spread_two, spread_two_out)
    write(feed_in, feed_in_out)
    write(left_parts.at[0], lefts.at[0])
    advance(16)
    load(4).wait()

    def finish_second_gate(at, value):
        cum[:, at] = jax.nn.sigmoid(value)

    dot_columns(finish_second_gate, left_parts.at[0], squares.at[4])

    def arrive(s, carry):
        @pl.when(s + 2 * SKEW < feed_steps)
        def _():
            step_a(feed_base + s + 2 * SKEW)

        @pl.when(s + SKEW < feed_steps)
        def _():
            step_b(feed_base + s + SKEW)

        @pl.when(s < feed_steps)
        def _():
            step_c(feed_base + s)

        k = s - SKEW
        slot = lax.rem(s, 2)
        at = pl.ds(pl.multiple_of(k * piece, piece), piece)
        copy_core(feed_base + k).wait_recv()
        fetch = pltpu.make_async_copy(outs[6].at[:, :, :, :, at], feed_slot, slot_sem.at[0])
        fetch.start()

        def put(k, slot):
            at = pl.ds(pl.multiple_of(k * piece, piece), piece)
            return pltpu.make_async_copy(positive_slot.at[slot], positive.at[:, :, :, :, at], slot_sem.at[1 + slot])

        @pl.when(k >= 2)
        def _():
            put(k - 2, slot).wait()

        fetch.wait()
        units = 32 * piece
        hidden = jnp.maximum(matmul_last(feed_slot[:, :, :, :, :, :width].reshape(units, width), feed_in[...]), 0.0)
        positive_slot[slot] = hidden.reshape(positive_slot.shape[1:])
        put(k, slot).start()
        hidden_squares = (hidden * hidden).astype(BF)
        total[...] += matmul_lead(hidden_squares, feed_slot[:, :, :, :, :, width:].reshape(units, width))

        @pl.when(k == feed_steps - 1)
        def _():
            put(k - 1, 1 - slot).wait()
            put(k, slot).wait()

        return carry

    lax.fori_loop(SKEW, feed_steps + SKEW, arrive, 0)

    def last_pass(k, carry):
        at = pl.ds(pl.multiple_of(k * 32, 32), 32)
        gate, value_out, grad = cum[at, :], total[at, :], cotangent[at, :].astype(F32)
        residual[at, :] = residual[at, :] + gate * value_out
        grad_value[at, :] = (grad * gate).astype(BF)
        grad_gate[at, :] = (grad * value_out * gate * (1.0 - gate)).astype(BF)
        return carry

    lax.fori_loop(0, count // 32, last_pass, 0)
    write(residual, result)
    write(grad_value, grad_value_out)
    write(grad_gate, grad_gate_out)
    for n in range(steps):
        for o in range(3):
            copy_z(n, o).wait_send()
        for copy in (copy_first(n), copy_second(n), copy_passed(n), copy_core(n)):
            copy.wait_send()
    for copy in halo_copies + [halo_two] + scan_copies:
        copy.wait_send()
    for copy in written:
        copy.wait()


def forward(near, parts, size):
    count, width = near[0].shape
    rows = parts[6].shape[0]
    flat = lambda kind: jax.ShapeDtypeStruct((count, width), kind)
    narrow = jax.ShapeDtypeStruct((count, 128), F32)
    dma = pltpu.SemaphoreType.DMA
    big, low = pltpu.VMEM((count, width), F32), pltpu.VMEM((count, width), BF)
    lines = pltpu.VMEM((count, 128), F32)
    steps = sum(p.shape[0] // 16 for p in parts)
    eight = pltpu.VMEM((8, width), F32)
    return pl.pallas_call(
        forward_kernel,
        out_shape=[jax.ShapeDtypeStruct((2, 2, 4, 2) + p.shape, p.dtype) for p in parts]
        + [
            flat(F32), jax.ShapeDtypeStruct((16, width), F32), jax.ShapeDtypeStruct((8, width), F32),
            jax.ShapeDtypeStruct((5, count, width), BF), flat(BF), flat(BF), flat(BF),
            jax.ShapeDtypeStruct((2, 2, 4, 2, rows, count), F32), flat(F32), flat(F32), narrow, flat(F32), flat(F32), narrow,
        ]
        + [flat(F32)] * 7,
        in_specs=[whole()] * len(near) + [anywhere()] * len(parts),
        out_specs=[anywhere()] * 28,
        scratch_shapes=[
            pltpu.VMEM((2, 2, 4, 2, 16, 128), BF), pltpu.VMEM((16, width), F32), eight,
            pltpu.VMEM((5, 2, 2, 4, 2, width // 32, width), BF), pltpu.VMEM((2, 2, 4, 2, 16, 2 * width), BF),
            pltpu.VMEM((2, 2, 2, 4, 2, 16, count), F32), pltpu.VMEM((5, count, width), BF), low, low, low, big,
            big, lines, big, big, lines,
        ]
        + [big] * 12
        + [
            pltpu.VMEM((32, width), BF), pltpu.VMEM((32, width), F32), pltpu.VMEM((32, 128), F32), eight,
            pltpu.VMEM((size, 8, width), F32), eight, eight, eight,
            dma((steps, 7)), dma((steps, 7)), dma((7,)), dma((6,)), dma((24,)), dma((3,)), dma((size,)), dma((size,)),
            dma((3,)), dma((3,)),
        ],
        compiler_params=pltpu.CompilerParams(collective_id=0, has_side_effects=True, vmem_limit_bytes=66_000_000),
        cost_estimate=cost(6 * count * width * width + 4 * count * 32 * rows * width, 60_000_000),
        name="forward",
    )(*near, *parts)


def channel_backward_kernel(
    feed_in, grad_value, grad_gate, vectors, keep, inverse, cotangent,
    weights, positive, w_feedr, w_output, spread, unit, keys, values, denom, mixed, prior_a, prior_b, recept,
    feed_part, rights, grad_residual, sums,
    weight_slots, positive_slots, feedr, output, spread_in, unit_in, keys_in, values_in, denom_in, mixed_in,
    prior_a_in, prior_b_in, recept_in, value_part, key_part, outgoing, gathered, from_first, from_second,
    grad_in, grad_rin, grad_z, grad_w, cum, up, low, summary, arrived, entering_rows, halo_out, halo_in,
    slot_sem, load_sem, core_send, core_recv, first_send, first_recv, second_send, second_recv,
    scan_send, scan_recv, halo_send, halo_recv,
):
    size = arrived.shape[0]
    links = Links(size)
    x, c, z, y, t = links.x, links.c, links.z, links.y, links.t
    rows, width = weight_slots.shape[2], feed_in.shape[1]
    micro, length = keep.shape[:2]

    def fetches(s, slot):
        own = s // 4
        cc = own * c + (1 - own) * (1 - c)
        xx, yy = owner(3 - lax.rem(s, 4), x, y, cc)
        return (
            pltpu.make_async_copy(weights.at[xx, cc, :, yy], weight_slots.at[slot], slot_sem.at[0, slot]),
            pltpu.make_async_copy(positive.at[xx, cc, :, yy], positive_slots.at[slot], slot_sem.at[1, slot]),
        )

    for copy in fetches(0, 0):
        copy.start()
    late = [
        (w_feedr, feedr), (spread, spread_in), (unit, unit_in), (w_output, output), (recept, recept_in),
        (mixed, mixed_in), (denom, denom_in), (keys, keys_in), (values, values_in), (prior_a, prior_a_in),
        (prior_b, prior_b_in),
    ]
    loads = [pltpu.make_async_copy(source, target, load_sem.at[k]) for k, (source, target) in enumerate(late)]
    for load in loads:
        load.start()
    links.greet(True)
    grad_att, grad_keys, grad_values, grad_recept = [rights.at[n] for n in range(1, 5)]
    rights[0] = grad_gate[...]
    grad_in[...] = jnp.zeros_like(grad_in)
    sums[...] = jnp.zeros_like(sums)
    summary[...] = jnp.zeros_like(summary)
    halo_out[...] = jnp.zeros_like(halo_out)

    def to_core(i, slot):
        return remote(outgoing.at[slot], gathered.at[i], core_send.at[i], core_recv.at[i], links.core)

    def to_first(q, side):
        return remote(
            gathered.at[2 + q, side], from_first.at[q, side], first_send.at[q, side], first_recv.at[q, side], links.first
        )

    def column(s, carry):
        slot = lax.rem(s, 2)
        i = 3 - lax.rem(s, 4)
        for copy in fetches(s, slot):
            copy.wait()

        @pl.when(s < 7)
        def _():
            for copy in fetches(s + 1, 1 - slot):
                copy.start()

        hidden = positive_slots[slot].reshape(4 * rows, feed_in.shape[0])
        squares = (hidden * hidden).astype(BF)
        key_rows = weight_slots[slot, :, :, :width].reshape(4 * rows, width)
        value_rows = weight_slots[slot, :, :, width:].reshape(4 * rows, width)
        value_part[...] = matmul(squares, grad_value[...])
        grad_pre = (matmul_last(value_rows, grad_value[...]) * (2.0 * hidden)).astype(BF)
        key_part[...] = matmul(grad_pre, feed_in[...])
        grad_in[...] += matmul_lead(grad_pre, key_rows)

        @pl.when(s < 4)
        def _():
            @pl.when(s >= 2)
            def _():
                to_core(i + 2, slot).wait_send()

            for k in range(4):
                at = lax.rem(k + 4 - z, 4)
                outgoing[slot, 0, at] = value_part[k * rows : (k + 1) * rows].astype(BF)
                outgoing[slot, 1, at] = key_part[k * rows : (k + 1) * rows].astype(BF)
            to_core(i, slot).start()

        @pl.when(s >= 4)
        def _():
            to_core(i, slot).wait_recv()
            for side, part in ((0, value_part), (1, key_part)):
                for k in range(4):
                    at = lax.rem(k + 4 - z, 4)
                    total = gathered[i, side, at].astype(F32) + part[k * rows : (k + 1) * rows]
                    gathered[i, side, at] = total.astype(BF)

        @pl.when(jnp.logical_and(s >= 4, s < 6))
        def _():
            for side in (0, 1):
                to_first(i - 2, side).start()

        return carry

    lax.fori_loop(0, 8, column, 0)
    to_core(1, 0).wait_send()
    to_core(0, 1).wait_send()

    def to_second(side):
        return remote(
            gathered.at[1, side], from_second.at[side], second_send.at[side], second_recv.at[side], links.second
        )

    def pass_second(side):
        to_first(1, side).wait_recv()
        add_blocks(gathered.at[1, side], [gathered.at[1, side], from_first.at[1, side]])
        to_second(side).start()

    row = lax.broadcasted_iota(jnp.int32, (length, 128), 0)
    loads[0].wait()
    dot_rows(grad_rin, grad_gate, feedr)

    def shift_two(m, rows_at, at, keeping):
        return keeping * (
            grad_in[rows_at, at] * (1.0 - vectors[BLEND_KEY : BLEND_KEY + 1, at])
            + grad_rin[rows_at, at] * (1.0 - vectors[BLEND_RECEPT : BLEND_RECEPT + 1, at])
        )

    for m in range(micro):
        start = m * length
        halo_out[m : m + 1] = shift_two(m, slice(start, start + 1), slice(None), keep[m, 0:1, 0:1])
    halo = remote(halo_out, halo_in, halo_send.at[0], halo_recv.at[0], links.row(size - 1))
    halo.start()
    pass_second(0)
    loads[1].wait()
    halo.wait_recv()
    for m in range(micro):
        rows_at = slice(m * length, (m + 1) * length)

        def shift_pass(j, carry, m=m, rows_at=rows_at):
            at = lanes(j)
            after = jnp.where(t < size - 1, halo_in[m : m + 1, at], 0.0)
            shift = shift_two(m, rows_at, at, keep[m])
            from_in, from_rin, apart = grad_in[rows_at, at], grad_rin[rows_at, at], spread_in[rows_at, at]
            grad_z[rows_at, at] = (
                from_in * vectors[BLEND_KEY : BLEND_KEY + 1, at]
                + from_rin * vectors[BLEND_RECEPT : BLEND_RECEPT + 1, at]
                + roll_rows(shift, -1, after, row)
            )
            sums[BLEND_KEY : BLEND_KEY + 1, at] += jnp.sum(from_in * apart, axis=0, keepdims=True)
            sums[BLEND_RECEPT : BLEND_RECEPT + 1, at] += jnp.sum(from_rin * apart, axis=0, keepdims=True)
            return carry

        lax.fori_loop(0, width // 128, shift_pass, 0)
    loads[2].wait()
    norm_back_tiles(
        grad_residual, grad_z, unit_in, inverse, vectors[GAIN_TWO : GAIN_TWO + 1, :], cotangent, sums, GAIN_TWO
    )
    grad_att[...] = grad_residual[...].astype(BF)
    pass_second(1)

    loads[3].wait()
    dot_rows(grad_w, grad_att, output)
    for load in loads[4:]:
        load.wait()

    def quotient_grads(rows_at, at):
        gate = recept_in[rows_at, at]
        blended = mixed_in[rows_at, at]
        inner = grad_w[rows_at, at] * gate
        above = inner / denom_in[rows_at, at]
        return above, -above * blended, inner * blended * (1.0 - gate)

    for m in range(micro):
        rows_at = slice(m * length, (m + 1) * length)

        def first_pass(j, carry, m=m, rows_at=rows_at):
            at = lanes(j)
            above, below, rec = quotient_grads(rows_at, at)
            grad_recept[rows_at, at] = rec.astype(BF)
            factor = keep[m] * vectors[DECAY : DECAY + 1, at]
            f, a, b = doubling(factor, keep[m] * above, keep[m] * below, row, -1)
            cum[rows_at, at] = f
            up[rows_at, at] = a
            low[rows_at, at] = b
            summary[3 * m : 3 * m + 1, at] = f[:1]
            summary[3 * m + 1 : 3 * m + 2, at] = a[:1]
            summary[3 * m + 2 : 3 * m + 3, at] = b[:1]
            return carry

        lax.fori_loop(0, width // 128, first_pass, 0)
    copies = share_row(summary, arrived, scan_send, scan_recv, t, links.dp, size)
    for m in range(micro):
        a = jnp.zeros((1, width), F32)
        b = jnp.zeros((1, width), F32)
        for ahead in range(size - 1, 0, -1):
            o = size - ahead
            f = arrived[o, 3 * m : 3 * m + 1]
            a = jnp.where(t + ahead < size, f * a + arrived[o, 3 * m + 1 : 3 * m + 2], a)
            b = jnp.where(t + ahead < size, f * b + arrived[o, 3 * m + 2 : 3 * m + 3], b)
        entering_rows[2 * m : 2 * m + 1] = a
        entering_rows[2 * m + 1 : 2 * m + 2] = b
    for m in range(micro):
        rows_at = slice(m * length, (m + 1) * length)

        def second_pass(j, carry, m=m, rows_at=rows_at):
            at = lanes(j)
            enter_a = entering_rows[2 * m : 2 * m + 1, at]
            enter_b = entering_rows[2 * m + 1 : 2 * m + 2, at]
            f = cum[rows_at, at]
            alpha = roll_rows(up[rows_at, at] + f * enter_a, -1, enter_a, row)
            beta = roll_rows(low[rows_at, at] + f * enter_b, -1, enter_b, row)
            above, below, _ = quotient_grads(rows_at, at)
            key, value = keys_in[rows_at, at], values_in[rows_at, at]
            power = jnp.exp(key)
            bonus = jnp.exp(vectors[PREMIUM : PREMIUM + 1, at] + key)
            premium = bonus * (value * above + below)
            grad_values[rows_at, at] = (bonus * above + power * alpha).astype(BF)
            grad_keys[rows_at, at] = (premium + power * (value * alpha + beta)).astype(BF)
            fading = keep[m] * (alpha * prior_a_in[rows_at, at] + beta * prior_b_in[rows_at, at])
            sums[PREMIUM : PREMIUM + 1, at] += jnp.sum(premium, axis=0, keepdims=True)
            sums[DECAY : DECAY + 1, at] += jnp.sum(fading, axis=0, keepdims=True)
            return carry

        lax.fori_loop(0, width // 128, second_pass, 0)

    for side in (0, 1):
        to_first(0, side).wait_recv()
        to_second(side).wait_recv()
        add_blocks(
            feed_part.at[side], [gathered.at[0, side], from_first.at[0, side], from_second.at[side]]
        )
    for side in (0, 1):
        to_first(0, side).wait_send()
        to_first(1, side).wait_send()
        to_second(side).wait_send()
    halo.wait_send()
    for copy in copies:
        copy.wait_send()


def channel_backward(near, far, size):
    feed_in = near[0]
    weights = far[0]
    tokens, width = feed_in.shape
    micro, length = near[4].shape[:2]
    rows = weights.shape[4]
    flat_f32 = (tokens, width)
    dma = pltpu.SemaphoreType.DMA
    big = pltpu.VMEM(flat_f32, F32)
    return pl.pallas_call(
        channel_backward_kernel,
        out_shape=[
            jax.ShapeDtypeStruct((2, 4, rows, width), BF), jax.ShapeDtypeStruct((5, tokens, width), BF),
            jax.ShapeDtypeStruct(flat_f32, F32), jax.ShapeDtypeStruct((16, width), F32),
        ],
        in_specs=[whole()] * len(near) + [anywhere()] * len(far),
        out_specs=[whole()] * 4,
        scratch_shapes=[
            pltpu.VMEM((2, 4, rows, 2 * width), BF), pltpu.VMEM((2, 4, rows, tokens), F32),
            pltpu.VMEM((width, width), BF), pltpu.VMEM((width, width), BF),
        ]
        + [big] * 9
        + [
            pltpu.VMEM((4 * rows, width), F32), pltpu.VMEM((4 * rows, width), F32),
            pltpu.VMEM((2, 2, 4, rows, width), BF), pltpu.VMEM((4, 2, 4, rows, width), BF),
            pltpu.VMEM((2, 2, 4, rows, width), BF), pltpu.VMEM((2, 4, rows, width), BF),
        ]
        + [big] * 7
        + [
            pltpu.VMEM((8, width), F32), pltpu.VMEM((size, 8, width), F32), pltpu.VMEM((8, width), F32),
            pltpu.VMEM((8, width), F32), pltpu.VMEM((8, width), F32),
            dma((2, 2)), dma((11,)), dma((4,)), dma((4,)), dma((2, 2)), dma((2, 2)), dma((2,)), dma((2,)),
            dma((size,)), dma((size,)), dma((1,)), dma((1,)),
        ],
        compiler_params=pltpu.CompilerParams(
            collective_id=2, has_side_effects=True, vmem_limit_bytes=66_000_000
        ),
        cost_estimate=cost(8 * tokens * 32 * rows * width, 16 * 32 * rows * width),
        name="channel_backward",
    )(*near, *far)


def front_backward_kernel(
    feed_part, lefts, rights, vectors, keep, inverse, grad_residual, sums_in, rates,
    w_key, w_value, w_recept, spread, unit,
    square_grads, unit_key, unit_value, token_grads, vector_grads,
    key_in, value_in, recept_in, spread_in, unit_in, outgoing, gathered, from_first, from_second, from_z, feed_z,
    own_units, x_units, core_units, grad_key, grad_value, grad_recept, grad_z, sums, held, halo_out, halo_in,
    load_sem, core_send, core_recv, first_send, first_recv, second_send, second_recv, z_send, z_recv,
    feed_send, feed_recv, unit_send, unit_recv, halo_send, halo_recv, sum_send, sum_recv,
):
    links = Links(8)
    x, c, z, y, t, size = links.x, links.c, links.z, links.y, links.t, links.size
    count = lefts.shape[0]
    width = lefts.shape[2]
    rows = width // 32
    micro, length = keep.shape[:2]
    late = [(w_key, key_in), (w_value, value_in), (w_recept, recept_in), (spread, spread_in), (unit, unit_in)]
    loads = [pltpu.make_async_copy(source, target, load_sem.at[k]) for k, (source, target) in enumerate(late)]
    for load in loads:
        load.start()
    links.greet(True)
    feed_copies = {}
    for side in (0, 1):
        for o in (1, 2, 3):
            feed_copies[side, o] = remote(
                feed_part.at[side, o], feed_z.at[side, o - 1], feed_send.at[side, o - 1], feed_recv.at[side, o - 1],
                links.along_z[o - 1],
            )
            feed_copies[side, o].start()
    halo_out[...] = jnp.zeros_like(halo_out)
    sums[...] = sums_in[...]

    def part(n, cc, xx):
        at = pl.ds(pl.multiple_of((xx * 2 + cc) * 8 * rows, 8 * rows), 8 * rows)
        return matmul_lead(lefts[n, :, at], rights[n])

    def blocks():
        for zz in range(4):
            for yy in range(2):
                yield zz, yy, slice((zz * 2 + yy) * rows, (zz * 2 + yy + 1) * rows)

    def to_core(n):
        return remote(outgoing.at[n], gathered.at[n], core_send.at[n], core_recv.at[n], links.core)

    def to_first(n):
        return remote(
            gathered.at[n, pl.ds(2, 2)], from_first.at[n], first_send.at[n], first_recv.at[n], links.first
        )

    def to_second(n):
        return remote(gathered.at[n, 1], from_second.at[n], second_send.at[n], second_recv.at[n], links.second)

    def to_z(n, o):
        return remote(
            gathered.at[n, 0, o], from_z.at[n, o - 1], z_send.at[n, o - 1], z_recv.at[n, o - 1], links.along_z[o - 1]
        )

    def other(n, carry):
        for xx in range(2):
            value = part(n, 1 - c, xx)
            for zz, yy, at in blocks():
                outgoing[n, position(xx, yy, x, y, 1 - c), lax.rem(zz + 4 - z, 4)] = value[at].astype(BF)
        to_core(n).start()
        return carry

    def own(n, carry):
        to_core(n).wait_recv()
        for xx in range(2):
            value = part(n, c, xx)
            for zz, yy, at in blocks():
                i, o = position(xx, yy, x, y, c), lax.rem(zz + 4 - z, 4)
                gathered[n, i, o] = (gathered[n, i, o].astype(F32) + value[at]).astype(BF)
        to_first(n).start()
        return carry

    lax.fori_loop(0, count, other, 0)
    lax.fori_loop(0, count, own, 0)

    def pass_second(n):
        to_first(n).wait_recv()
        add_blocks(gathered.at[n, 1], [gathered.at[n, 1], from_first.at[n, 1]])
        to_second(n).start()

    def pass_z(n):
        to_second(n).wait_recv()
        add_blocks(gathered.at[n, 0], [gathered.at[n, 0], from_first.at[n, 0], from_second.at[n]])
        for o in (1, 2, 3):
            to_z(n, o).start()

    def finish(n):
        value = gathered[n, 0, 0].astype(F32)
        for o in (1, 2, 3):
            to_z(n, o).wait_recv()
            value = value + from_z[n, o - 1].astype(F32)
        square_grads[n] = value

    for side in (0, 1):
        for o in (1, 2, 3):
            feed_copies[side, o].wait_recv()
        for r in range(0, feed_part.shape[2], 32):
            at = slice(r, r + 32)
            value = feed_part[side, 0, at].astype(F32)
            for o in range(3):
                value = value + feed_z[side, o, at].astype(F32)
            own_units[side, at] = value.astype(BF)
    units_over_x = remote(own_units, x_units, unit_send.at[0], unit_recv.at[0], links.over_x)
    units_over_x.start()
    units_over_core = remote(own_units, core_units.at[0], unit_send.at[1], unit_recv.at[1], links.core)
    units_over_core.start()

    loads[0].wait()
    dot_rows(grad_key, rights.at[2], key_in)
    pass_second(0)
    loads[1].wait()
    dot_rows(grad_value, rights.at[3], value_in)
    pass_second(1)
    loads[2].wait()
    dot_rows(grad_recept, rights.at[4], recept_in)
    units_over_x.wait_recv()
    both_over_core = remote(x_units, core_units.at[1], unit_send.at[2], unit_recv.at[2], links.core)
    both_over_core.start()
    grads = ((grad_key, MIX_KEY), (grad_value, MIX_VALUE), (grad_recept, MIX_RECEPT))

    def shift_one(rows_at, at, keeping):
        return keeping * sum(g[rows_at, at] * (1.0 - vectors[k : k + 1, at]) for g, k in grads)

    for m in range(micro):
        start = m * length
        halo_out[m : m + 1] = shift_one(slice(start, start + 1), slice(None), keep[m, 0:1, 0:1])
    halo = remote(halo_out, halo_in, halo_send.at[0], halo_recv.at[0], links.row(size - 1))
    halo.start()
    pass_second(2)
    pass_z(0)
    loads[3].wait()
    halo.wait_recv()
    row = lax.broadcasted_iota(jnp.int32, (length, 128), 0)
    for m in range(micro):
        rows_at = slice(m * length, (m + 1) * length)

        def shift_pass(j, carry, m=m, rows_at=rows_at):
            at = lanes(j)
            after = jnp.where(t < size - 1, halo_in[m : m + 1, at], 0.0)
            apart = spread_in[rows_at, at]
            value = roll_rows(shift_one(rows_at, at, keep[m]), -1, after, row)
            for g, k in grads:
                value = value + g[rows_at, at] * vectors[k : k + 1, at]
                sums[k : k + 1, at] += jnp.sum(g[rows_at, at] * apart, axis=0, keepdims=True)
            grad_z[rows_at, at] = value
            return carry

        lax.fori_loop(0, width // 128, shift_pass, 0)
    pass_second(3)
    pass_z(1)
    loads[4].wait()
    norm_back_tiles(
        token_grads, grad_z, unit_in, inverse, vectors[GAIN_ONE : GAIN_ONE + 1, :], grad_residual, sums, GAIN_ONE
    )
    sums[DECAY : DECAY + 1, :] = -sums[DECAY : DECAY + 1, :] * rates[0:1, :] * vectors[DECAY : DECAY + 1, :]
    pass_second(4)

    stages = [[links.core], [links.over_x], [links.over_y], links.along_z]
    pending = []
    source, slot = sums, 0

    def begin(stage, source, slot):
        copies = [
            remote(source, held.at[slot + k], sum_send.at[slot + k], sum_recv.at[slot + k], peer)
            for k, peer in enumerate(stage)
        ]
        for copy in copies:
            copy.start()
        return copies

    def collect(copies, source, slot, target):
        value = source[...]
        for k, copy in enumerate(copies):
            copy.wait_recv()
            value = value + held[slot + k]
        target[...] = value

    copies = begin(stages[0], sums, 0)
    pending += copies
    pass_z(2)
    collect(copies, sums, 0, held.at[6])
    copies = begin(stages[1], held.at[6], 1)
    pending += copies
    pass_z(3)
    finish(0)
    collect(copies, held.at[6], 1, held.at[7])
    copies = begin(stages[2], held.at[7], 2)
    pending += copies
    pass_z(4)
    finish(1)
    collect(copies, held.at[7], 2, held.at[8])
    copies = begin(stages[3], held.at[8], 3)
    pending += copies
    units_over_core.wait_recv()
    both_over_core.wait_recv()
    for side, target in ((1, unit_key), (0, unit_value)):
        for d in range(4):
            for r in range(0, own_units.shape[1], 32):
                at = slice(r, r + 32)
                pick = jnp.where(links.dp == d ^ 1, core_units[0, side, at], core_units[1, side, at])
                pick = jnp.where(links.dp == d ^ 2, x_units[side, at], pick)
                pick = jnp.where(links.dp == d, own_units[side, at], pick)
                target[d, at] = pick.astype(F32)
    collect(copies, held.at[8], 3, vector_grads)
    finish(2)
    finish(3)
    finish(4)
    for n in range(count):
        to_core(n).wait_send()
        to_first(n).wait_send()
        to_second(n).wait_send()
        for o in (1, 2, 3):
            to_z(n, o).wait_send()
    for copy in pending + list(feed_copies.values()) + [units_over_x, units_over_core, both_over_core, halo]:
        copy.wait_send()


def front_backward(near, far):
    feed_part, lefts = near[:2]
    rows = feed_part.shape[2]
    count, tokens, width = lefts.shape
    own = width // 32
    dma = pltpu.SemaphoreType.DMA
    big = pltpu.VMEM((tokens, width), F32)
    square = pltpu.VMEM((width, width), BF)
    return pl.pallas_call(
        front_backward_kernel,
        out_shape=[
            jax.ShapeDtypeStruct((count, own, width), F32),
            jax.ShapeDtypeStruct((4, rows, width), F32), jax.ShapeDtypeStruct((4, rows, width), F32),
            jax.ShapeDtypeStruct((tokens, width), F32), jax.ShapeDtypeStruct((16, width), F32),
        ],
        in_specs=[whole()] * len(near) + [anywhere()] * len(far),
        out_specs=[whole()] * 5,
        scratch_shapes=[square] * 3
        + [big] * 2
        + [
            pltpu.VMEM((count, 4, 4, own, width), BF), pltpu.VMEM((count, 4, 4, own, width), BF),
            pltpu.VMEM((count, 2, 4, own, width), BF), pltpu.VMEM((count, 4, own, width), BF),
            pltpu.VMEM((count, 3, own, width), BF), pltpu.VMEM((2, 3, rows, width), BF),
            pltpu.VMEM((2, rows, width), BF), pltpu.VMEM((2, rows, width), BF), pltpu.VMEM((2, 2, rows, width), BF),
        ]
        + [big] * 4
        + [
            pltpu.VMEM((16, width), F32), pltpu.VMEM((9, 16, width), F32), pltpu.VMEM((8, width), F32),
            pltpu.VMEM((8, width), F32),
            dma((5,)), dma((count,)), dma((count,)), dma((count,)), dma((count,)), dma((count,)), dma((count,)),
            dma((count, 3)), dma((count, 3)), dma((2, 3)), dma((2, 3)), dma((3,)), dma((3,)), dma((1,)), dma((1,)),
            dma((6,)), dma((6,)),
        ],
        compiler_params=pltpu.CompilerParams(
            collective_id=3, has_side_effects=True, vmem_limit_bytes=66_000_000
        ),
        cost_estimate=cost(4 * count * tokens * width * width, 40 * width * width),
        name="front_backward",
    )(*near, *far)


def local_shards(tokens, resets, out_grads, *weights):
    (
        mixer_key, mixer_value, mixer_recept, mixer_output, feed_recept, feed_key, feed_value, *vector_shards
    ) = weights
    size = lax.axis_size("tensor")
    dp, t = lax.axis_index("dp"), lax.axis_index("tensor")
    micro, _, length, width = tokens.shape
    count = micro * length
    unit_rows = feed_key.shape[0] // 4
    feed_shard = jnp.concatenate(
        [lax.dynamic_slice_in_dim(w, dp * unit_rows, unit_rows, 0) for w in (feed_key, feed_value)], axis=1
    )
    share = vector_shards[0].shape[0]
    vector_pack = jnp.pad(jnp.stack(vector_shards), ((0, 16 - len(vector_shards)), (0, 128 - share)))
    keep = (1 - resets[:, 0]).astype(F32)[:, :, None]
    keep_lanes = jnp.broadcast_to(keep, (micro, length, 128))
    cotangent = out_grads.reshape(count, width)
    near = [tokens.reshape(count, width), cotangent, keep_lanes]
    parts = [vector_pack, mixer_key, mixer_value, mixer_recept, mixer_output, feed_recept, feed_shard]
    (
        _, all_key, all_value, all_recept, all_output, all_feedr, feed,
        result, table, rates, lefts, feed_in, grad_value, grad_gate, positive, spread_one, unit_one, inverse_one,
        spread_two, unit_two, inverse_two, keys, values, denom, mixed, prior_a, prior_b, recept,
    ) = forward(near, parts, size)
    w_key, w_value, w_recept, w_output, w_feedr = [
        w.reshape(width, width) for w in (all_key, all_value, all_recept, all_output, all_feedr)
    ]
    near = [feed_in, grad_value, grad_gate, table, keep_lanes, inverse_two, cotangent]
    far = [feed, positive, w_feedr, w_output, spread_two, unit_two, keys, values, denom, mixed, prior_a, prior_b, recept]
    feed_part, rights, grad_residual, sums = channel_backward(near, far, size)
    near = [feed_part, lefts, rights, table, keep_lanes, inverse_one, grad_residual, sums, rates]
    far = [w_key, w_value, w_recept, spread_one, unit_one]
    square_grads, unit_key, unit_value, token_grads, vector_grads = front_backward(near, far)
    mine = lax.dynamic_slice_in_dim(vector_grads, (dp * size + t) * share, share, 1)
    return (
        result.reshape(tokens.shape), token_grads.reshape(tokens.shape),
        square_grads[2], square_grads[3], square_grads[4], square_grads[1], square_grads[0],
        unit_key.reshape(feed_key.shape), unit_value.reshape(feed_value.shape),
    ) + tuple(mine[i] for i in range(len(vector_shards)))


def is_two_by_two_by_four(mesh):
    return mesh.shape["dp"] == 4 and mesh.shape["tensor"] == 8


def solution(mesh):
    return jax.shard_map(
        local_shards if is_two_by_two_by_four(mesh) else shards,
        mesh=mesh,
        in_specs=(
            P(None, "dp", "tensor", None),
            P(None, "dp", "tensor"),
            P(None, "dp", "tensor", None),
            P(("dp", "tensor"), None),
            P(("dp", "tensor"), None),
            P(("dp", "tensor"), None),
            P(("dp", "tensor"), None),
            P(("dp", "tensor"), None),
            P("tensor", None),
            P("tensor", None),
            P(("dp", "tensor")),
            P(("dp", "tensor")),
            P(("dp", "tensor")),
            P(("dp", "tensor")),
            P(("dp", "tensor")),
            P(("dp", "tensor")),
            P(("dp", "tensor")),
            P(("dp", "tensor")),
            P(("dp", "tensor")),
            P(("dp", "tensor")),
            P(("dp", "tensor")),
        ),
        out_specs=(
            P(None, "dp", "tensor", None),
            P(None, "dp", "tensor", None),
            P(("dp", "tensor"), None),
            P(("dp", "tensor"), None),
            P(("dp", "tensor"), None),
            P(("dp", "tensor"), None),
            P(("dp", "tensor"), None),
            P("tensor", None),
            P("tensor", None),
            P(("dp", "tensor")),
            P(("dp", "tensor")),
            P(("dp", "tensor")),
            P(("dp", "tensor")),
            P(("dp", "tensor")),
            P(("dp", "tensor")),
            P(("dp", "tensor")),
            P(("dp", "tensor")),
            P(("dp", "tensor")),
            P(("dp", "tensor")),
            P(("dp", "tensor")),
        ),
        check_vma=False,
    )
```

```python
import functools

import jax
import jax.numpy as jnp
from jax import lax
from jax.experimental import pallas as pl
from jax.experimental.pallas import tpu as pltpu
from jax.sharding import PartitionSpec as P

EPSILON = 1e-05


def entering(shard, axis, combine, identity, reverse):
    size, here = (lax.axis_size(axis), lax.axis_index(axis))
    everything = jax.tree.map(lambda part: lax.all_gather(part, axis), shard)
    start = jax.tree.map(
        lambda part, zero: jnp.broadcast_to(jnp.asarray(zero, part.dtype), part.shape),
        shard,
        identity,
    )

    def turn(k, before):
        at = size - 1 - k if reverse else k
        reached = at > here if reverse else at < here
        new = combine(before, jax.tree.map(lambda part: part[at], everything))
        return jax.tree.map(lambda a, b: jnp.where(reached, a, b), new, before)

    return lax.fori_loop(0, size, turn, start)


def shifted(block, axis, distance):
    devices = range(lax.axis_size(axis))
    route = [(i - distance, i) for i in devices if i - distance in devices]
    return lax.ppermute(block, axis, route)


def norm_rows(payload_series, gain, bias):
    center = payload_series - jnp.mean(payload_series, axis=-1, keepdims=True)
    inverse = lax.rsqrt(jnp.mean(center * center, axis=-1, keepdims=True) + EPSILON)
    normed = center * inverse
    return (normed * gain + bias, normed, inverse)


def norm_back(grad_out, normed, inverse, gain):
    scaled = grad_out * gain
    centred = scaled - jnp.mean(scaled, axis=-1, keepdims=True)
    grad_in = inverse * (centred - normed * jnp.mean(scaled * normed, axis=-1, keepdims=True))
    return (grad_in, jnp.sum(grad_out * normed, axis=0), jnp.sum(grad_out, axis=0))


def affine(earlier, later):
    return (
        earlier[0] * later[0],
        later[0] * earlier[1] + later[1],
        later[0] * earlier[2] + later[2],
    )


def carry_across(summary, backward):
    width = summary[0].shape[0]
    identity = (
        jnp.ones((width,), jnp.float32),
        jnp.zeros((width,), jnp.float32),
        jnp.zeros((width,), jnp.float32),
    )
    return entering(summary, "tensor", affine, identity, backward)


def matmul(left, right):
    return jnp.dot(left, right, preferred_element_type=jnp.float32)


def matmul_lead(left, right):
    return lax.dot_general(
        left, right, (((0,), (0,)), ((), ())), preferred_element_type=jnp.float32
    )


def matmul_last(left, right):
    return lax.dot_general(
        left, right, (((1,), (1,)), ((), ())), preferred_element_type=jnp.float32
    )


def shards(
    tokens,
    resets,
    out_grads,
    mixer_key,
    mixer_value,
    mixer_recept,
    mixer_output,
    feed_recept,
    feed_key,
    feed_value,
    first_gain,
    first_bias,
    second_gain,
    second_bias,
    mixing_key,
    mixing_value,
    mixing_recept,
    time_decay,
    time_first,
    feeding_key,
    feeding_recept,
):
    gathered = (
        lax.all_gather(mixer_key, ("dp", "tensor"), axis=0, tiled=True),
        lax.all_gather(mixer_value, ("dp", "tensor"), axis=0, tiled=True),
        lax.all_gather(mixer_recept, ("dp", "tensor"), axis=0, tiled=True),
        lax.all_gather(mixer_output, ("dp", "tensor"), axis=0, tiled=True),
        lax.all_gather(feed_recept, ("dp", "tensor"), axis=0, tiled=True),
        lax.all_gather(first_gain, ("dp", "tensor"), axis=0, tiled=True),
        lax.all_gather(first_bias, ("dp", "tensor"), axis=0, tiled=True),
        lax.all_gather(second_gain, ("dp", "tensor"), axis=0, tiled=True),
        lax.all_gather(second_bias, ("dp", "tensor"), axis=0, tiled=True),
        lax.all_gather(mixing_key, ("dp", "tensor"), axis=0, tiled=True),
        lax.all_gather(mixing_value, ("dp", "tensor"), axis=0, tiled=True),
        lax.all_gather(mixing_recept, ("dp", "tensor"), axis=0, tiled=True),
        lax.all_gather(time_decay, ("dp", "tensor"), axis=0, tiled=True),
        lax.all_gather(time_first, ("dp", "tensor"), axis=0, tiled=True),
        lax.all_gather(feeding_key, ("dp", "tensor"), axis=0, tiled=True),
        lax.all_gather(feeding_recept, ("dp", "tensor"), axis=0, tiled=True),
    )
    w_key, w_value, w_recept, w_output, w_feedr = (
        gathered[0],
        gathered[1],
        gathered[2],
        gathered[3],
        gathered[4],
    )
    parameter_vectors = [piece.astype(jnp.float32) for piece in gathered[5:]]
    gain_one, bias_one, gain_two, bias_two = (
        parameter_vectors[0],
        parameter_vectors[1],
        parameter_vectors[2],
        parameter_vectors[3],
    )
    mix_key, mix_value, mix_recept = (
        parameter_vectors[4],
        parameter_vectors[5],
        parameter_vectors[6],
    )
    (
        fading_speed_logarithm,
        opening_premium_logarithm,
        channel_lookup_blend,
        channel_gating_blend,
    ) = (parameter_vectors[7], parameter_vectors[8], parameter_vectors[9], parameter_vectors[10])
    rates = jnp.exp(fading_speed_logarithm)
    fading_multiplier = jnp.exp(-rates)
    micro_count = tokens.shape[0]
    width = tokens.shape[3]
    grad_keyw = jnp.zeros(feed_key.shape, jnp.float32)
    grad_valuew = jnp.zeros(feed_value.shape, jnp.float32)
    square_grads = [jnp.zeros((width, width), jnp.float32) for index_one in range(5)]
    parameter_vector_gradients = [jnp.zeros((width,), jnp.float32) for index_two in range(11)]
    results = []
    input_grads = []
    for micro_index in range(micro_count):
        inputs = tokens[micro_index, 0].astype(jnp.float32)
        restart_retain_flags = (1 - resets[micro_index, 0]).astype(jnp.float32)[:, None]
        cotangent = out_grads[micro_index, 0].astype(jnp.float32)
        normed_one, unit_one, inverse_one = norm_rows(inputs, gain_one, bias_one)
        z_one = normed_one.astype(jnp.bfloat16)
        prior_one = shifted(z_one[-1:], "tensor", 1)
        before_one = (
            jnp.concatenate([prior_one, z_one[:-1]], axis=0).astype(jnp.float32)
            * restart_retain_flags
        )
        z_onef = z_one.astype(jnp.float32)
        in_key = (z_onef * mix_key + before_one * (1.0 - mix_key)).astype(jnp.bfloat16)
        in_value = (z_onef * mix_value + before_one * (1.0 - mix_value)).astype(jnp.bfloat16)
        in_recept = (z_onef * mix_recept + before_one * (1.0 - mix_recept)).astype(jnp.bfloat16)
        lookup_series = matmul(in_key, w_key)
        payload_series = matmul(in_value, w_value)
        recept = jax.nn.sigmoid(matmul(in_recept, w_recept))
        powered_lookup = jnp.exp(lookup_series)
        premium_plus_lookup = jnp.exp(opening_premium_logarithm + lookup_series)
        factor = restart_retain_flags * fading_multiplier
        cum_factor, local_a, local_b = lax.associative_scan(
            affine, (factor, powered_lookup * payload_series, powered_lookup), axis=0
        )
        incoming = carry_across((cum_factor[-1], local_a[-1], local_b[-1]), False)
        upper_running_state = local_a + cum_factor * incoming[1]
        lower_running_state = local_b + cum_factor * incoming[2]
        earlier_upper_state = jnp.concatenate([incoming[1][None], upper_running_state[:-1]], axis=0)
        earlier_lower_state = jnp.concatenate([incoming[2][None], lower_running_state[:-1]], axis=0)
        lower_quotient_part = restart_retain_flags * earlier_lower_state + premium_plus_lookup
        blended = (
            restart_retain_flags * earlier_upper_state + premium_plus_lookup * payload_series
        ) / lower_quotient_part
        weighted = (recept * blended).astype(jnp.bfloat16)
        residual = inputs + matmul(weighted, w_output)
        normed_two, unit_two, inverse_two = norm_rows(residual, gain_two, bias_two)
        z_two = normed_two.astype(jnp.bfloat16)
        prior_two = shifted(z_two[-1:], "tensor", 1)
        before_two = (
            jnp.concatenate([prior_two, z_two[:-1]], axis=0).astype(jnp.float32)
            * restart_retain_flags
        )
        z_twof = z_two.astype(jnp.float32)
        feed_in = (
            z_twof * channel_lookup_blend + before_two * (1.0 - channel_lookup_blend)
        ).astype(jnp.bfloat16)
        feed_rin = (
            z_twof * channel_gating_blend + before_two * (1.0 - channel_gating_blend)
        ).astype(jnp.bfloat16)
        gate = jax.nn.sigmoid(matmul(feed_rin, w_feedr))
        all_in = lax.all_gather(feed_in, "tensor", axis=0, tiled=True)
        hidden_pre = matmul_last(feed_key, all_in)
        hidden = jnp.square(jnp.maximum(hidden_pre, 0.0)).astype(jnp.bfloat16)
        value_out = lax.psum_scatter(
            matmul_lead(hidden, feed_value), "tensor", scatter_dimension=0, tiled=True
        )
        results.append(residual + gate * value_out)
        grad_value = (cotangent * gate).astype(jnp.bfloat16)
        grad_gate = (cotangent * value_out * gate * (1.0 - gate)).astype(jnp.bfloat16)
        square_grads[4] = square_grads[4] + matmul_lead(feed_rin, grad_gate)
        grad_rin = matmul_last(grad_gate, w_feedr)
        relu_twice = 2.0 * jnp.maximum(hidden_pre, 0.0)
        add_piece = lax.all_gather(grad_value, "tensor", axis=0, tiled=True)
        rows_total = matmul(hidden, add_piece)
        block = matmul_last(feed_value, add_piece)
        grad_valuew = grad_valuew + rows_total
        grad_pre = (block * relu_twice).astype(jnp.bfloat16)
        grad_keyw = grad_keyw + matmul(grad_pre, all_in)
        grad_in = lax.psum_scatter(
            matmul_lead(grad_pre, feed_key), "tensor", scatter_dimension=0, tiled=True
        )
        parameter_vector_gradients[9] = parameter_vector_gradients[9] + jnp.sum(
            grad_in * (z_twof - before_two), axis=0
        )
        parameter_vector_gradients[10] = parameter_vector_gradients[10] + jnp.sum(
            grad_rin * (z_twof - before_two), axis=0
        )
        shift_two = restart_retain_flags * (
            grad_in * (1.0 - channel_lookup_blend) + grad_rin * (1.0 - channel_gating_blend)
        )
        after_two = shifted(shift_two[:1], "tensor", -1)
        grad_z_two = (
            grad_in * channel_lookup_blend
            + grad_rin * channel_gating_blend
            + jnp.concatenate([shift_two[1:], after_two], axis=0)
        )
        back_two, gain_part, bias_part = norm_back(grad_z_two, unit_two, inverse_two, gain_two)
        parameter_vector_gradients[2] = parameter_vector_gradients[2] + gain_part
        parameter_vector_gradients[3] = parameter_vector_gradients[3] + bias_part
        grad_residual = cotangent + back_two
        grad_att = grad_residual.astype(jnp.bfloat16)
        square_grads[3] = square_grads[3] + matmul_lead(weighted, grad_att)
        grad_weighted = matmul_last(grad_att, w_output)
        grad_mixed = grad_weighted * recept
        grad_recept = (grad_weighted * blended * recept * (1.0 - recept)).astype(jnp.bfloat16)
        upper_adjoint = grad_mixed / lower_quotient_part
        denominator_gradient = -grad_mixed * blended / lower_quotient_part
        cum_back, local_xa, local_xb = lax.associative_scan(
            affine,
            (
                factor,
                restart_retain_flags * upper_adjoint,
                restart_retain_flags * denominator_gradient,
            ),
            reverse=True,
            axis=0,
        )
        beyond = carry_across((cum_back[0], local_xa[0], local_xb[0]), True)
        adjoint_a = local_xa + cum_back * beyond[1]
        adjoint_b = local_xb + cum_back * beyond[2]
        running_upper_total = jnp.concatenate([adjoint_a[1:], beyond[1][None]], axis=0)
        running_lower_total = jnp.concatenate([adjoint_b[1:], beyond[2][None]], axis=0)
        premium_power = premium_plus_lookup * (
            payload_series * upper_adjoint + denominator_gradient
        )
        adjoint_payloads = (
            premium_plus_lookup * upper_adjoint + powered_lookup * running_upper_total
        ).astype(jnp.bfloat16)
        key_gradient_rows = (
            premium_power
            + powered_lookup * (payload_series * running_upper_total + running_lower_total)
        ).astype(jnp.bfloat16)
        parameter_vector_gradients[8] = parameter_vector_gradients[8] + jnp.sum(
            premium_power, axis=0
        )
        decay_sum = jnp.sum(
            restart_retain_flags
            * (
                running_upper_total * earlier_upper_state
                + running_lower_total * earlier_lower_state
            ),
            axis=0,
        )
        parameter_vector_gradients[7] = (
            parameter_vector_gradients[7] - rates * fading_multiplier * decay_sum
        )
        square_grads[0] = square_grads[0] + matmul_lead(in_key, key_gradient_rows)
        square_grads[1] = square_grads[1] + matmul_lead(in_value, adjoint_payloads)
        square_grads[2] = square_grads[2] + matmul_lead(in_recept, grad_recept)
        grad_inkey = matmul_last(key_gradient_rows, w_key)
        grad_invalue = matmul_last(adjoint_payloads, w_value)
        grad_inrecept = matmul_last(grad_recept, w_recept)
        spread_one = z_onef - before_one
        parameter_vector_gradients[4] = parameter_vector_gradients[4] + jnp.sum(
            grad_inkey * spread_one, axis=0
        )
        parameter_vector_gradients[5] = parameter_vector_gradients[5] + jnp.sum(
            grad_invalue * spread_one, axis=0
        )
        parameter_vector_gradients[6] = parameter_vector_gradients[6] + jnp.sum(
            grad_inrecept * spread_one, axis=0
        )
        shift_one = restart_retain_flags * (
            grad_inkey * (1.0 - mix_key)
            + grad_invalue * (1.0 - mix_value)
            + grad_inrecept * (1.0 - mix_recept)
        )
        after_one = shifted(shift_one[:1], "tensor", -1)
        grad_z_one = (
            grad_inkey * mix_key
            + grad_invalue * mix_value
            + grad_inrecept * mix_recept
            + jnp.concatenate([shift_one[1:], after_one], axis=0)
        )
        back_one, gain_first, bias_first = norm_back(grad_z_one, unit_one, inverse_one, gain_one)
        parameter_vector_gradients[0] = parameter_vector_gradients[0] + gain_first
        parameter_vector_gradients[1] = parameter_vector_gradients[1] + bias_first
        input_grads.append(grad_residual + back_one)
    owned = (
        lax.psum_scatter(square_grads[0], ("dp", "tensor"), scatter_dimension=0, tiled=True),
        lax.psum_scatter(square_grads[1], ("dp", "tensor"), scatter_dimension=0, tiled=True),
        lax.psum_scatter(square_grads[2], ("dp", "tensor"), scatter_dimension=0, tiled=True),
        lax.psum_scatter(square_grads[3], ("dp", "tensor"), scatter_dimension=0, tiled=True),
        lax.psum_scatter(square_grads[4], ("dp", "tensor"), scatter_dimension=0, tiled=True),
        lax.psum_scatter(
            parameter_vector_gradients[0], ("dp", "tensor"), scatter_dimension=0, tiled=True
        ),
        lax.psum_scatter(
            parameter_vector_gradients[1], ("dp", "tensor"), scatter_dimension=0, tiled=True
        ),
        lax.psum_scatter(
            parameter_vector_gradients[2], ("dp", "tensor"), scatter_dimension=0, tiled=True
        ),
        lax.psum_scatter(
            parameter_vector_gradients[3], ("dp", "tensor"), scatter_dimension=0, tiled=True
        ),
        lax.psum_scatter(
            parameter_vector_gradients[4], ("dp", "tensor"), scatter_dimension=0, tiled=True
        ),
        lax.psum_scatter(
            parameter_vector_gradients[5], ("dp", "tensor"), scatter_dimension=0, tiled=True
        ),
        lax.psum_scatter(
            parameter_vector_gradients[6], ("dp", "tensor"), scatter_dimension=0, tiled=True
        ),
        lax.psum_scatter(
            parameter_vector_gradients[7], ("dp", "tensor"), scatter_dimension=0, tiled=True
        ),
        lax.psum_scatter(
            parameter_vector_gradients[8], ("dp", "tensor"), scatter_dimension=0, tiled=True
        ),
        lax.psum_scatter(
            parameter_vector_gradients[9], ("dp", "tensor"), scatter_dimension=0, tiled=True
        ),
        lax.psum_scatter(
            parameter_vector_gradients[10], ("dp", "tensor"), scatter_dimension=0, tiled=True
        ),
    )
    key_rows, value_rows_grad = (grad_keyw, grad_valuew)
    key_total, value_total = (
        lax.psum(key_rows.astype(jnp.bfloat16), "dp").astype(jnp.float32),
        lax.psum(value_rows_grad.astype(jnp.bfloat16), "dp").astype(jnp.float32),
    )
    result_all = jnp.stack(results)[:, None]
    grads_all = jnp.stack(input_grads)[:, None]
    return (
        result_all,
        grads_all,
        owned[0],
        owned[1],
        owned[2],
        owned[3],
        owned[4],
        key_total,
        value_total,
        owned[5],
        owned[6],
        owned[7],
        owned[8],
        owned[9],
        owned[10],
        owned[11],
        owned[12],
        owned[13],
        owned[14],
        owned[15],
    )


BF = jnp.bfloat16
F32 = jnp.float32
BOTH = ("dp", "tensor")
MESH_ID = pl.DeviceIdType.MESH


def cost(flops, moved):
    return pl.CostEstimate(flops=flops, bytes_accessed=moved, transcendentals=0)


def whole():
    return pl.BlockSpec(memory_space=pltpu.VMEM)


def anywhere():
    return pl.BlockSpec(memory_space=pl.ANY)


def roll_rows(value, distance, fill, row):
    size = value.shape[0]
    moved = pltpu.roll(value, distance % size, 0)
    outside = row < distance if distance > 0 else row >= size + distance
    return jnp.where(outside, fill, moved)


def doubling(factor, up, low, row, sign):
    size, step = factor.shape[0], 1
    while step < size:
        up = up + factor * roll_rows(up, sign * step, 0.0, row)
        low = low + factor * roll_rows(low, sign * step, 0.0, row)
        factor = factor * roll_rows(factor, sign * step, 1.0, row)
        step *= 2
    return factor, up, low


def row_copies(summary, arrived, send, recv, t, dp, size):
    return [
        pltpu.make_async_remote_copy(
            src_ref=summary,
            dst_ref=arrived.at[o],
            send_sem=send.at[o],
            recv_sem=recv.at[o],
            device_id=(dp, lax.rem(t + o, size)),
            device_id_type=MESH_ID,
        )
        for o in range(1, size)
    ]


def share_row(summary, arrived, send, recv, t, dp, size):
    copies = row_copies(summary, arrived, send, recv, t, dp, size)
    for copy in copies:
        copy.start()
    for copy in copies:
        copy.wait_recv()
    return copies


def lanes(j):
    return pl.ds(pl.multiple_of(j * 128, 128), 128)


def owner(i, x, y, c):
    first, second = i // 2, i % 2
    flip_x = first * c + second * (1 - c)
    flip_y = first * (1 - c) + second * c
    return x + flip_x - 2 * x * flip_x, y + flip_y - 2 * y * flip_y


def position(xx, yy, x, y, c):
    flip_x = x + xx - 2 * x * xx
    flip_y = y + yy - 2 * y * yy
    return 2 * (flip_x * c + flip_y * (1 - c)) + flip_x * (1 - c) + flip_y * c


class Links:
    def __init__(self, size):
        dp, t = lax.axis_index("dp"), lax.axis_index("tensor")
        x, c, z, y = dp // 2, dp % 2, t // 2, t % 2
        self.x, self.c, self.z, self.y, self.dp, self.t, self.size = x, c, z, y, dp, t, size
        over_x, over_y = ((1 - x) * 2 + c, t), (dp, z * 2 + 1 - y)
        self.over_x = over_x
        self.core = (x * 2 + 1 - c, t)
        self.first = (jnp.where(c == 0, over_y[0], over_x[0]), jnp.where(c == 0, over_y[1], over_x[1]))
        self.second = (jnp.where(c == 0, over_x[0], over_y[0]), jnp.where(c == 0, over_x[1], over_y[1]))
        self.along_z = [(dp, lax.rem(z + o, 4) * 2 + y) for o in (1, 2, 3)]
        self.over_y = over_y

    def row(self, o):
        return (self.dp, lax.rem(self.t + o, self.size))

    def greet(self, whole_row):
        peers = [self.row(o) for o in range(1, self.size)] if whole_row else self.along_z + [self.over_y]
        peers = peers + [self.over_x, self.core]
        barrier = pltpu.get_barrier_semaphore()
        for peer in peers:
            pl.semaphore_signal(barrier, inc=1, device_id=peer, device_id_type=MESH_ID)
        pl.semaphore_wait(barrier, len(peers))


def remote(source, target, send, recv, device):
    return pltpu.make_async_remote_copy(
        src_ref=source, dst_ref=target, send_sem=send, recv_sem=recv, device_id=device, device_id_type=MESH_ID
    )


def add_blocks(target, sources):
    count, rows = target.shape[:2]
    tile = min(rows, 32)
    per = rows // tile

    def turn(k, carry):
        n, at = k // per, pl.ds(pl.multiple_of(lax.rem(k, per) * tile, tile), tile)
        value = sources[0][n, at].astype(F32)
        for source in sources[1:]:
            value = value + source[n, at].astype(F32)
        target[n, at] = value.astype(target.dtype)
        return carry

    lax.fori_loop(0, count * per, turn, 0)


def dot_rows(target, left, right):
    tile = 256

    def turn(n, carry):
        at = pl.ds(pl.multiple_of(n * tile, tile), tile)
        target[:, at] = matmul_last(left[...], right[at, :])
        return carry

    lax.fori_loop(0, right.shape[0] // tile, turn, 0)


def norm_back_tiles(target, grads, normed, inverse, gain, base, sums, gain_row):
    tile = 32
    width = grads.shape[1]

    def turn(k, carry):
        at = pl.ds(pl.multiple_of(k * tile, tile), tile)
        grad, unit = grads[at, :], normed[at, :]
        scaled = grad * gain
        middle = jnp.sum(scaled, axis=-1, keepdims=True) * (1.0 / width)
        along = jnp.sum(scaled * unit, axis=-1, keepdims=True) * (1.0 / width)
        target[at, :] = base[at, :].astype(F32) + inverse[at, 0:1] * (scaled - middle - unit * along)
        sums[gain_row : gain_row + 1, :] += jnp.sum(grad * unit, axis=0, keepdims=True)
        sums[gain_row + 1 : gain_row + 2, :] += jnp.sum(grad, axis=0, keepdims=True)
        return carry

    lax.fori_loop(0, grads.shape[0] // tile, turn, 0)


GAIN_ONE, BIAS_ONE, GAIN_TWO, BIAS_TWO, MIX_KEY, MIX_VALUE, MIX_RECEPT, DECAY, PREMIUM, BLEND_KEY, BLEND_RECEPT = range(11)


def norm_tiles(source, unit, inverse):
    rows, width = source.shape
    tile = min(rows, 32)

    def turn(k, carry):
        at = pl.ds(pl.multiple_of(k * tile, tile), tile)
        value = source[at, :].astype(F32)
        center = value - jnp.sum(value, axis=-1, keepdims=True) * (1.0 / width)
        scale = lax.rsqrt(jnp.sum(center * center, axis=-1, keepdims=True) * (1.0 / width) + EPSILON)
        unit[at, :] = center * scale
        inverse[at, :] = jnp.broadcast_to(scale, (tile, 128))
        return carry

    lax.fori_loop(0, rows // tile, turn, 0)


def dot_columns(finish, left, right):
    tile = 256
    depth = left.shape[1]

    def turn(n, carry):
        at = pl.ds(pl.multiple_of(n * tile, tile), tile)
        finish(at, matmul(left[...], right[:, :, :, :, :, at].reshape(depth, tile)))
        return carry

    lax.fori_loop(0, right.shape[5] // tile, turn, 0)


AHEAD = 3


def forward_kernel(
    tokens, cotangent, keep,
    own_vectors, own_key, own_value, own_recept, own_output, own_feedr, own_feed,
    all_vectors, all_key, all_value, all_recept, all_output, all_feedr, all_feed,
    result, table_out, rates_out, lefts, feed_in_out, grad_value_out, grad_gate_out, positive, spread_one_out,
    unit_one_out, inverse_one_out, spread_two_out, unit_two_out, inverse_two_out, keys_out, values_out, denom_out,
    mixed_out, prior_a_out, prior_b_out, recept_out,
    packed, table, rates, squares, feed_slot, positive_slot, left_parts, feed_in, grad_value, grad_gate, spread_one,
    unit_one, inverse_one, spread_two, unit_two, inverse_two, keys, values, gates, denom, mixed, prior_a, prior_b,
    cum, up, low, residual, total, halo_tokens, halo_unit, halo_inverse, summary, arrived, entering_rows, halo_out, halo_in,
    send, recv, own_sem, load_sem, out_sem, slot_sem, scan_send, scan_recv, halo_send, halo_recv,
):
    size = arrived.shape[0]
    links = Links(size)
    x, c, z, y, t, dp = links.x, links.c, links.z, links.y, links.t, links.dp
    count, width = tokens.shape
    micro, length = keep.shape[:2]
    ins = [own_vectors, own_key, own_value, own_recept, own_output, own_feedr, own_feed]
    outs = [all_vectors, all_key, all_value, all_recept, all_output, all_feedr, all_feed]
    piece = 16
    chunks = [(i, r) for i in range(7) for r in range(0, ins[i].shape[0], piece)]
    steps = len(chunks)
    feed_steps = ins[6].shape[0] // piece
    feed_base = steps - feed_steps
    x_first, y_first = jnp.where(c == 0, x, 1 - x), jnp.where(c == 0, 1 - y, y)
    first, second = links.first, links.second

    def place(n):
        if isinstance(n, int):
            i, start = chunks[n]
            return i, pl.ds(start, piece)
        return 6, pl.ds(pl.multiple_of((n - feed_base) * piece, piece), piece)

    def copy_z(n, o):
        i, at = place(n)
        return remote(ins[i].at[at], outs[i].at[x, c, z, y, at], send.at[n, o], recv.at[n, o], links.along_z[o])

    def copy_column(n, j, xx, yy, device):
        i, at = place(n)
        column = outs[i].at[xx, c, :, yy, at]
        return remote(column, column, send.at[n, j], recv.at[n, j], device)

    def copy_first(n):
        return copy_column(n, 3, x, y, first)

    def copy_second(n):
        return copy_column(n, 4, x, y, second)

    def copy_passed(n):
        return copy_column(n, 5, x_first, y_first, second)

    def copy_core(n):
        i, at = place(n)
        half = outs[i].at[:, c, :, :, at]
        return remote(half, half, send.at[n, 6], recv.at[n, 6], links.core)

    def step_z(n):
        for o in range(3):
            copy_z(n, o).start()

    def step_a(n):
        for o in range(3):
            copy_z(n, o).wait_recv()
        copy_first(n).start()
        copy_second(n).start()

    def step_b(n):
        copy_first(n).wait_recv()
        copy_passed(n).start()

    def step_c(n):
        copy_second(n).wait_recv()
        copy_passed(n).wait_recv()
        copy_core(n).start()

    def advance(*numbers):
        for s in numbers:
            if s + AHEAD < steps:
                step_z(s + AHEAD)
            if s < steps:
                step_a(s)
            if 0 <= s - 1 < steps:
                step_b(s - 1)
            if 0 <= s - 2 < steps:
                step_c(s - 2)

    def load(k):
        return pltpu.make_async_copy(outs[1 + k], squares.at[k], load_sem.at[k])

    def ready(k):
        for n in (2 * k + 1, 2 * k + 2):
            copy_core(n).wait_recv()
        load(k).start()

    written = []

    def write(source, target):
        copy = pltpu.make_async_copy(source, target, out_sem.at[len(written)])
        copy.start()
        written.append(copy)

    owns = [pltpu.make_async_copy(ins[i], outs[i].at[x, c, z, y], own_sem.at[i]) for i in range(7)]
    for own in owns:
        own.start()
    links.greet(True)
    halo_copies = [
        remote(
            tokens.at[pl.ds((m + 1) * length - piece, piece)], halo_tokens.at[pl.ds(m * piece, piece)],
            halo_send.at[m], halo_recv.at[m], links.row(1),
        )
        for m in range(micro)
    ]
    for halo in halo_copies:
        halo.start()
    for n in range(AHEAD):
        step_z(n)
    summary[...] = jnp.zeros_like(summary)
    halo_out[...] = jnp.zeros_like(halo_out)
    total[...] = jnp.zeros_like(total)
    for own in owns:
        own.wait()
    advance(0)
    norm_tiles(tokens, unit_one, inverse_one)
    write(unit_one, unit_one_out)
    write(inverse_one, inverse_one_out)
    advance(1, 2)
    for halo in halo_copies:
        halo.wait_recv()
    norm_tiles(halo_tokens, halo_unit, halo_inverse)
    copy_core(0).wait_recv()

    vector_load = pltpu.make_async_copy(all_vectors, packed, load_sem.at[5])
    vector_load.start()
    advance(3)
    vector_load.wait()
    share = width // 32
    per = 128 // share
    for j in range(width // 128):
        value = None
        for q in range(per):
            d = j * per + q
            part = packed[d // 16, (d // 8) % 2, (d // 2) % 4, d % 2].astype(F32)
            part = pltpu.roll(part, q * share, 1) if q else part
            value = part if value is None else value + part
        table[:, j * 128 : (j + 1) * 128] = value
    speed = jnp.exp(table[DECAY : DECAY + 1, :])
    rates[...] = jnp.broadcast_to(speed, rates.shape)
    table[DECAY : DECAY + 1, :] = jnp.exp(-speed)
    write(table, table_out)
    write(rates, rates_out)
    row = lax.broadcasted_iota(jnp.int32, (length, 128), 0)

    def vector(k, at):
        return table[k : k + 1, at]

    def normed(unit, gain, bias, at):
        return (unit * vector(gain, at) + vector(bias, at)).astype(BF).astype(F32)

    def blends(spread, unit, m, prior, gain, bias, mixes):
        rows_at = slice(m * length, (m + 1) * length)

        def turn(j, carry):
            at = lanes(j)
            now = normed(unit[rows_at, at], gain, bias, at)
            before = roll_rows(now, 1, jnp.where(t > 0, prior(at), 0.0), row) * keep[m]
            spread[rows_at, at] = now - before
            for target, mix in mixes:
                target[rows_at, at] = (now * vector(mix, at) + before * (1.0 - vector(mix, at))).astype(BF)
            return carry

        lax.fori_loop(0, width // 128, turn, 0)

    mixes = [(left_parts.at[2 + k], MIX_KEY + k) for k in range(3)]
    for m in range(micro):
        last = (m + 1) * piece - 1

        def prior(at, last=last):
            return normed(halo_unit[last : last + 1, at], GAIN_ONE, BIAS_ONE, at)

        blends(spread_one, unit_one, m, prior, GAIN_ONE, BIAS_ONE, mixes)
        advance(4 + m)
    write(spread_one, spread_one_out)
    for k in range(3):
        write(left_parts.at[2 + k], lefts.at[2 + k])

    def keep_in(target):
        def finish(at, value):
            target[:, at] = value

        return finish

    ready(0)
    advance(6)
    load(0).wait()
    dot_columns(keep_in(keys), left_parts.at[2], squares.at[0])
    write(keys, keys_out)
    ready(1)
    advance(7)
    load(1).wait()
    dot_columns(keep_in(values), left_parts.at[3], squares.at[1])
    write(values, values_out)

    for m in range(micro):
        rows_at = slice(m * length, (m + 1) * length)

        def first_pass(j, carry, m=m, rows_at=rows_at):
            at = lanes(j)
            power = jnp.exp(keys[rows_at, at])
            f, a, b = doubling(keep[m] * vector(DECAY, at), power * values[rows_at, at], power, row, 1)
            cum[rows_at, at] = f
            up[rows_at, at] = a
            low[rows_at, at] = b
            summary[3 * m : 3 * m + 1, at] = f[length - 1 :]
            summary[3 * m + 1 : 3 * m + 2, at] = a[length - 1 :]
            summary[3 * m + 2 : 3 * m + 3, at] = b[length - 1 :]
            return carry

        lax.fori_loop(0, width // 128, first_pass, 0)
        advance(8 + m)
    scan_copies = row_copies(summary, arrived, scan_send, scan_recv, t, dp, size)
    for copy in scan_copies:
        copy.start()
    ready(2)
    load(2).wait()

    def finish_gate(at, value):
        gates[:, at] = jax.nn.sigmoid(value)

    dot_columns(finish_gate, left_parts.at[4], squares.at[2])
    write(gates, recept_out)
    advance(10, 11)
    for copy in scan_copies:
        copy.wait_recv()
    for m in range(micro):
        a = jnp.zeros((1, width), F32)
        b = jnp.zeros((1, width), F32)
        for o in range(size - 1, 0, -1):
            f = arrived[o, 3 * m : 3 * m + 1]
            a = jnp.where(t >= o, f * a + arrived[o, 3 * m + 1 : 3 * m + 2], a)
            b = jnp.where(t >= o, f * b + arrived[o, 3 * m + 2 : 3 * m + 3], b)
        entering_rows[2 * m : 2 * m + 1] = a
        entering_rows[2 * m + 1 : 2 * m + 2] = b
    for m in range(micro):
        rows_at = slice(m * length, (m + 1) * length)

        def second_pass(j, carry, m=m, rows_at=rows_at):
            at = lanes(j)
            enter_a = entering_rows[2 * m : 2 * m + 1, at]
            enter_b = entering_rows[2 * m + 1 : 2 * m + 2, at]
            f = cum[rows_at, at]
            before_a = roll_rows(up[rows_at, at] + f * enter_a, 1, enter_a, row)
            before_b = roll_rows(low[rows_at, at] + f * enter_b, 1, enter_b, row)
            bonus = jnp.exp(vector(PREMIUM, at) + keys[rows_at, at])
            below = keep[m] * before_b + bonus
            blended = (keep[m] * before_a + bonus * values[rows_at, at]) / below
            left_parts[1, rows_at, at] = (gates[rows_at, at] * blended).astype(BF)
            denom[rows_at, at] = below
            mixed[rows_at, at] = blended
            prior_a[rows_at, at] = before_a
            prior_b[rows_at, at] = before_b
            return carry

        lax.fori_loop(0, width // 128, second_pass, 0)
    write(left_parts.at[1], lefts.at[1])
    write(denom, denom_out)
    write(mixed, mixed_out)
    write(prior_a, prior_a_out)
    write(prior_b, prior_b_out)
    ready(3)
    advance(12)
    load(3).wait()

    def finish_residual(at, value):
        residual[:, at] = tokens[:, at].astype(F32) + value

    dot_columns(finish_residual, left_parts.at[1], squares.at[3])
    norm_tiles(residual, unit_two, inverse_two)
    write(unit_two, unit_two_out)
    write(inverse_two, inverse_two_out)
    for m in range(micro):
        last = (m + 1) * length - 1
        halo_out[m : m + 1, :] = normed(unit_two[last : last + 1, :], GAIN_TWO, BIAS_TWO, slice(None))
    halo_two = remote(halo_out, halo_in, halo_send.at[micro], halo_recv.at[micro], links.row(1))
    halo_two.start()
    ready(4)
    advance(13)
    halo_two.wait_recv()
    mixes = [(feed_in, BLEND_KEY), (left_parts.at[0], BLEND_RECEPT)]
    for m in range(micro):

        def prior(at, m=m):
            return halo_in[m : m + 1, at]

        blends(spread_two, unit_two, m, prior, GAIN_TWO, BIAS_TWO, mixes)
    write(spread_two, spread_two_out)
    write(feed_in, feed_in_out)
    write(left_parts.at[0], lefts.at[0])
    advance(14)
    load(4).wait()

    def finish_second_gate(at, value):
        cum[:, at] = jax.nn.sigmoid(value)

    dot_columns(finish_second_gate, left_parts.at[0], squares.at[4])

    advance(15)
    later = {0: 16, 1: 17, 3: 18, 5: 19, 7: 20}

    def arrive(k, carry):
        for turn, number in later.items():
            pl.when(k == turn)(functools.partial(advance, number))
        slot = lax.rem(k, 2)
        at = pl.ds(pl.multiple_of(k * piece, piece), piece)
        copy_core(feed_base + k).wait_recv()
        fetch = pltpu.make_async_copy(outs[6].at[:, :, :, :, at], feed_slot, slot_sem.at[0])
        fetch.start()

        def put(k, slot):
            at = pl.ds(pl.multiple_of(k * piece, piece), piece)
            return pltpu.make_async_copy(positive_slot.at[slot], positive.at[:, :, :, :, at], slot_sem.at[1 + slot])

        @pl.when(k >= 2)
        def _():
            put(k - 2, slot).wait()

        fetch.wait()
        units = 32 * piece
        hidden = jnp.maximum(matmul_last(feed_slot[:, :, :, :, :, :width].reshape(units, width), feed_in[...]), 0.0)
        positive_slot[slot] = hidden.reshape(positive_slot.shape[1:])
        put(k, slot).start()
        hidden_squares = (hidden * hidden).astype(BF)
        total[...] += matmul_lead(hidden_squares, feed_slot[:, :, :, :, :, width:].reshape(units, width))

        @pl.when(k == feed_steps - 1)
        def _():
            put(k - 1, 1 - slot).wait()
            put(k, slot).wait()

        return carry

    lax.fori_loop(0, feed_steps, arrive, 0)

    def last_pass(k, carry):
        at = pl.ds(pl.multiple_of(k * 32, 32), 32)
        gate, value_out, grad = cum[at, :], total[at, :], cotangent[at, :].astype(F32)
        residual[at, :] = residual[at, :] + gate * value_out
        grad_value[at, :] = (grad * gate).astype(BF)
        grad_gate[at, :] = (grad * value_out * gate * (1.0 - gate)).astype(BF)
        return carry

    lax.fori_loop(0, count // 32, last_pass, 0)
    write(residual, result)
    write(grad_value, grad_value_out)
    write(grad_gate, grad_gate_out)
    for n in range(steps):
        for o in range(3):
            copy_z(n, o).wait_send()
        for copy in (copy_first(n), copy_second(n), copy_passed(n), copy_core(n)):
            copy.wait_send()
    for copy in halo_copies + [halo_two] + scan_copies:
        copy.wait_send()
    for copy in written:
        copy.wait()


def forward(near, parts, size):
    count, width = near[0].shape
    rows = parts[6].shape[0]
    flat = lambda kind: jax.ShapeDtypeStruct((count, width), kind)
    narrow = jax.ShapeDtypeStruct((count, 128), F32)
    dma = pltpu.SemaphoreType.DMA
    big, low = pltpu.VMEM((count, width), F32), pltpu.VMEM((count, width), BF)
    lines = pltpu.VMEM((count, 128), F32)
    steps = sum(p.shape[0] // 16 for p in parts)
    eight = pltpu.VMEM((8, width), F32)
    return pl.pallas_call(
        forward_kernel,
        out_shape=[jax.ShapeDtypeStruct((2, 2, 4, 2) + p.shape, p.dtype) for p in parts]
        + [
            flat(F32), jax.ShapeDtypeStruct((16, width), F32), jax.ShapeDtypeStruct((8, width), F32),
            jax.ShapeDtypeStruct((5, count, width), BF), flat(BF), flat(BF), flat(BF),
            jax.ShapeDtypeStruct((2, 2, 4, 2, rows, count), F32), flat(F32), flat(F32), narrow, flat(F32), flat(F32), narrow,
        ]
        + [flat(F32)] * 7,
        in_specs=[whole()] * (len(near) + len(parts)),
        out_specs=[anywhere()] * 28,
        scratch_shapes=[
            pltpu.VMEM((2, 2, 4, 2, 16, 128), BF), pltpu.VMEM((16, width), F32), eight,
            pltpu.VMEM((5, 2, 2, 4, 2, width // 32, width), BF), pltpu.VMEM((2, 2, 4, 2, 16, 2 * width), BF),
            pltpu.VMEM((2, 2, 2, 4, 2, 16, count), F32), pltpu.VMEM((5, count, width), BF), low, low, low, big,
            big, lines, big, big, lines,
        ]
        + [big] * 12
        + [
            pltpu.VMEM((32, width), BF), pltpu.VMEM((32, width), F32), pltpu.VMEM((32, 128), F32), eight,
            pltpu.VMEM((size, 8, width), F32), eight, eight, eight,
            dma((steps, 7)), dma((steps, 7)), dma((7,)), dma((6,)), dma((24,)), dma((3,)), dma((size,)), dma((size,)),
            dma((3,)), dma((3,)),
        ],
        compiler_params=pltpu.CompilerParams(collective_id=0, has_side_effects=True, vmem_limit_bytes=66_000_000),
        cost_estimate=cost(6 * count * width * width + 4 * count * 32 * rows * width, 60_000_000),
        name="forward",
    )(*near, *parts)


def channel_backward_kernel(
    feed_in, grad_value, grad_gate, vectors, keep, inverse, cotangent,
    weights, positive, w_feedr, w_output, spread, unit, keys, values, denom, mixed, prior_a, prior_b, recept,
    feed_part, rights, grad_residual, sums,
    weight_slots, positive_slots, feedr, output, spread_in, unit_in, keys_in, values_in, denom_in, mixed_in,
    prior_a_in, prior_b_in, recept_in, value_part, key_part, outgoing, gathered, from_first, from_second,
    grad_in, grad_rin, grad_z, grad_w, cum, up, low, summary, arrived, entering_rows, halo_out, halo_in,
    slot_sem, load_sem, core_send, core_recv, first_send, first_recv, second_send, second_recv,
    scan_send, scan_recv, halo_send, halo_recv,
):
    size = arrived.shape[0]
    links = Links(size)
    x, c, z, y, t = links.x, links.c, links.z, links.y, links.t
    rows, width = weight_slots.shape[2], feed_in.shape[1]
    micro, length = keep.shape[:2]

    def fetches(s, slot):
        own = s // 4
        cc = own * c + (1 - own) * (1 - c)
        xx, yy = owner(3 - lax.rem(s, 4), x, y, cc)
        return (
            pltpu.make_async_copy(weights.at[xx, cc, :, yy], weight_slots.at[slot], slot_sem.at[0, slot]),
            pltpu.make_async_copy(positive.at[xx, cc, :, yy], positive_slots.at[slot], slot_sem.at[1, slot]),
        )

    for copy in fetches(0, 0):
        copy.start()
    late = [
        (w_feedr, feedr), (spread, spread_in), (unit, unit_in), (w_output, output), (recept, recept_in),
        (mixed, mixed_in), (denom, denom_in), (keys, keys_in), (values, values_in), (prior_a, prior_a_in),
        (prior_b, prior_b_in),
    ]
    loads = [pltpu.make_async_copy(source, target, load_sem.at[k]) for k, (source, target) in enumerate(late)]
    for load in loads:
        load.start()
    links.greet(True)
    grad_att, grad_keys, grad_values, grad_recept = [rights.at[n] for n in range(1, 5)]
    rights[0] = grad_gate[...]
    grad_in[...] = jnp.zeros_like(grad_in)
    sums[...] = jnp.zeros_like(sums)
    summary[...] = jnp.zeros_like(summary)
    halo_out[...] = jnp.zeros_like(halo_out)

    def to_core(i, slot):
        return remote(outgoing.at[slot], gathered.at[i], core_send.at[i], core_recv.at[i], links.core)

    def to_first(q, side):
        return remote(
            gathered.at[2 + q, side], from_first.at[q, side], first_send.at[q, side], first_recv.at[q, side], links.first
        )

    def column(s, carry):
        slot = lax.rem(s, 2)
        i = 3 - lax.rem(s, 4)
        for copy in fetches(s, slot):
            copy.wait()

        @pl.when(s < 7)
        def _():
            for copy in fetches(s + 1, 1 - slot):
                copy.start()

        hidden = positive_slots[slot].reshape(4 * rows, feed_in.shape[0])
        squares = (hidden * hidden).astype(BF)
        key_rows = weight_slots[slot, :, :, :width].reshape(4 * rows, width)
        value_rows = weight_slots[slot, :, :, width:].reshape(4 * rows, width)
        value_part[...] = matmul(squares, grad_value[...])
        grad_pre = (matmul_last(value_rows, grad_value[...]) * (2.0 * hidden)).astype(BF)
        key_part[...] = matmul(grad_pre, feed_in[...])
        grad_in[...] += matmul_lead(grad_pre, key_rows)

        @pl.when(s < 4)
        def _():
            @pl.when(s >= 2)
            def _():
                to_core(i + 2, slot).wait_send()

            for k in range(4):
                at = lax.rem(k + 4 - z, 4)
                outgoing[slot, 0, at] = value_part[k * rows : (k + 1) * rows].astype(BF)
                outgoing[slot, 1, at] = key_part[k * rows : (k + 1) * rows].astype(BF)
            to_core(i, slot).start()

        @pl.when(s >= 4)
        def _():
            to_core(i, slot).wait_recv()
            for side, part in ((0, value_part), (1, key_part)):
                for k in range(4):
                    at = lax.rem(k + 4 - z, 4)
                    total = gathered[i, side, at].astype(F32) + part[k * rows : (k + 1) * rows]
                    gathered[i, side, at] = total.astype(BF)

        @pl.when(jnp.logical_and(s >= 4, s < 6))
        def _():
            for side in (0, 1):
                to_first(i - 2, side).start()

        return carry

    lax.fori_loop(0, 8, column, 0)
    to_core(1, 0).wait_send()
    to_core(0, 1).wait_send()

    def to_second(side):
        return remote(
            gathered.at[1, side], from_second.at[side], second_send.at[side], second_recv.at[side], links.second
        )

    def pass_second(side):
        to_first(1, side).wait_recv()
        add_blocks(gathered.at[1, side], [gathered.at[1, side], from_first.at[1, side]])
        to_second(side).start()

    row = lax.broadcasted_iota(jnp.int32, (length, 128), 0)
    loads[0].wait()
    dot_rows(grad_rin, grad_gate, feedr)

    def shift_two(m, rows_at, at, keeping):
        return keeping * (
            grad_in[rows_at, at] * (1.0 - vectors[BLEND_KEY : BLEND_KEY + 1, at])
            + grad_rin[rows_at, at] * (1.0 - vectors[BLEND_RECEPT : BLEND_RECEPT + 1, at])
        )

    for m in range(micro):
        start = m * length
        halo_out[m : m + 1] = shift_two(m, slice(start, start + 1), slice(None), keep[m, 0:1, 0:1])
    halo = remote(halo_out, halo_in, halo_send.at[0], halo_recv.at[0], links.row(size - 1))
    halo.start()
    pass_second(0)
    loads[1].wait()
    halo.wait_recv()
    for m in range(micro):
        rows_at = slice(m * length, (m + 1) * length)

        def shift_pass(j, carry, m=m, rows_at=rows_at):
            at = lanes(j)
            after = jnp.where(t < size - 1, halo_in[m : m + 1, at], 0.0)
            shift = shift_two(m, rows_at, at, keep[m])
            from_in, from_rin, apart = grad_in[rows_at, at], grad_rin[rows_at, at], spread_in[rows_at, at]
            grad_z[rows_at, at] = (
                from_in * vectors[BLEND_KEY : BLEND_KEY + 1, at]
                + from_rin * vectors[BLEND_RECEPT : BLEND_RECEPT + 1, at]
                + roll_rows(shift, -1, after, row)
            )
            sums[BLEND_KEY : BLEND_KEY + 1, at] += jnp.sum(from_in * apart, axis=0, keepdims=True)
            sums[BLEND_RECEPT : BLEND_RECEPT + 1, at] += jnp.sum(from_rin * apart, axis=0, keepdims=True)
            return carry

        lax.fori_loop(0, width // 128, shift_pass, 0)
    loads[2].wait()
    norm_back_tiles(
        grad_residual, grad_z, unit_in, inverse, vectors[GAIN_TWO : GAIN_TWO + 1, :], cotangent, sums, GAIN_TWO
    )
    grad_att[...] = grad_residual[...].astype(BF)
    pass_second(1)

    loads[3].wait()
    dot_rows(grad_w, grad_att, output)
    for load in loads[4:]:
        load.wait()

    def quotient_grads(rows_at, at):
        gate = recept_in[rows_at, at]
        blended = mixed_in[rows_at, at]
        inner = grad_w[rows_at, at] * gate
        above = inner / denom_in[rows_at, at]
        return above, -above * blended, inner * blended * (1.0 - gate)

    for m in range(micro):
        rows_at = slice(m * length, (m + 1) * length)

        def first_pass(j, carry, m=m, rows_at=rows_at):
            at = lanes(j)
            above, below, rec = quotient_grads(rows_at, at)
            grad_recept[rows_at, at] = rec.astype(BF)
            factor = keep[m] * vectors[DECAY : DECAY + 1, at]
            f, a, b = doubling(factor, keep[m] * above, keep[m] * below, row, -1)
            cum[rows_at, at] = f
            up[rows_at, at] = a
            low[rows_at, at] = b
            summary[3 * m : 3 * m + 1, at] = f[:1]
            summary[3 * m + 1 : 3 * m + 2, at] = a[:1]
            summary[3 * m + 2 : 3 * m + 3, at] = b[:1]
            return carry

        lax.fori_loop(0, width // 128, first_pass, 0)
    copies = share_row(summary, arrived, scan_send, scan_recv, t, links.dp, size)
    for m in range(micro):
        a = jnp.zeros((1, width), F32)
        b = jnp.zeros((1, width), F32)
        for ahead in range(size - 1, 0, -1):
            o = size - ahead
            f = arrived[o, 3 * m : 3 * m + 1]
            a = jnp.where(t + ahead < size, f * a + arrived[o, 3 * m + 1 : 3 * m + 2], a)
            b = jnp.where(t + ahead < size, f * b + arrived[o, 3 * m + 2 : 3 * m + 3], b)
        entering_rows[2 * m : 2 * m + 1] = a
        entering_rows[2 * m + 1 : 2 * m + 2] = b
    for m in range(micro):
        rows_at = slice(m * length, (m + 1) * length)

        def second_pass(j, carry, m=m, rows_at=rows_at):
            at = lanes(j)
            enter_a = entering_rows[2 * m : 2 * m + 1, at]
            enter_b = entering_rows[2 * m + 1 : 2 * m + 2, at]
            f = cum[rows_at, at]
            alpha = roll_rows(up[rows_at, at] + f * enter_a, -1, enter_a, row)
            beta = roll_rows(low[rows_at, at] + f * enter_b, -1, enter_b, row)
            above, below, _ = quotient_grads(rows_at, at)
            key, value = keys_in[rows_at, at], values_in[rows_at, at]
            power = jnp.exp(key)
            bonus = jnp.exp(vectors[PREMIUM : PREMIUM + 1, at] + key)
            premium = bonus * (value * above + below)
            grad_values[rows_at, at] = (bonus * above + power * alpha).astype(BF)
            grad_keys[rows_at, at] = (premium + power * (value * alpha + beta)).astype(BF)
            fading = keep[m] * (alpha * prior_a_in[rows_at, at] + beta * prior_b_in[rows_at, at])
            sums[PREMIUM : PREMIUM + 1, at] += jnp.sum(premium, axis=0, keepdims=True)
            sums[DECAY : DECAY + 1, at] += jnp.sum(fading, axis=0, keepdims=True)
            return carry

        lax.fori_loop(0, width // 128, second_pass, 0)

    for side in (0, 1):
        to_first(0, side).wait_recv()
        to_second(side).wait_recv()
        add_blocks(
            feed_part.at[side], [gathered.at[0, side], from_first.at[0, side], from_second.at[side]]
        )
    for side in (0, 1):
        to_first(0, side).wait_send()
        to_first(1, side).wait_send()
        to_second(side).wait_send()
    halo.wait_send()
    for copy in copies:
        copy.wait_send()


def channel_backward(near, far, size):
    feed_in = near[0]
    weights = far[0]
    tokens, width = feed_in.shape
    micro, length = near[4].shape[:2]
    rows = weights.shape[4]
    flat_f32 = (tokens, width)
    dma = pltpu.SemaphoreType.DMA
    big = pltpu.VMEM(flat_f32, F32)
    return pl.pallas_call(
        channel_backward_kernel,
        out_shape=[
            jax.ShapeDtypeStruct((2, 4, rows, width), BF), jax.ShapeDtypeStruct((5, tokens, width), BF),
            jax.ShapeDtypeStruct(flat_f32, F32), jax.ShapeDtypeStruct((16, width), F32),
        ],
        in_specs=[whole()] * len(near) + [anywhere()] * len(far),
        out_specs=[whole()] * 4,
        scratch_shapes=[
            pltpu.VMEM((2, 4, rows, 2 * width), BF), pltpu.VMEM((2, 4, rows, tokens), F32),
            pltpu.VMEM((width, width), BF), pltpu.VMEM((width, width), BF),
        ]
        + [big] * 9
        + [
            pltpu.VMEM((4 * rows, width), F32), pltpu.VMEM((4 * rows, width), F32),
            pltpu.VMEM((2, 2, 4, rows, width), BF), pltpu.VMEM((4, 2, 4, rows, width), BF),
            pltpu.VMEM((2, 2, 4, rows, width), BF), pltpu.VMEM((2, 4, rows, width), BF),
        ]
        + [big] * 7
        + [
            pltpu.VMEM((8, width), F32), pltpu.VMEM((size, 8, width), F32), pltpu.VMEM((8, width), F32),
            pltpu.VMEM((8, width), F32), pltpu.VMEM((8, width), F32),
            dma((2, 2)), dma((11,)), dma((4,)), dma((4,)), dma((2, 2)), dma((2, 2)), dma((2,)), dma((2,)),
            dma((size,)), dma((size,)), dma((1,)), dma((1,)),
        ],
        compiler_params=pltpu.CompilerParams(
            collective_id=2, has_side_effects=True, vmem_limit_bytes=66_000_000
        ),
        cost_estimate=cost(8 * tokens * 32 * rows * width, 16 * 32 * rows * width),
        name="channel_backward",
    )(*near, *far)


def front_backward_kernel(
    feed_part, lefts, rights, vectors, keep, inverse, grad_residual, sums_in, rates,
    w_key, w_value, w_recept, spread, unit,
    square_grads, unit_key, unit_value, token_grads, vector_grads,
    key_in, value_in, recept_in, spread_in, unit_in, outgoing, gathered, from_first, from_second, from_z, feed_z,
    own_units, x_units, core_units, grad_key, grad_value, grad_recept, grad_z, sums, held, halo_out, halo_in,
    load_sem, core_send, core_recv, first_send, first_recv, second_send, second_recv, z_send, z_recv,
    feed_send, feed_recv, unit_send, unit_recv, halo_send, halo_recv, sum_send, sum_recv,
):
    links = Links(8)
    x, c, z, y, t, size = links.x, links.c, links.z, links.y, links.t, links.size
    count = lefts.shape[0]
    width = lefts.shape[2]
    rows = width // 32
    micro, length = keep.shape[:2]
    late = [(w_key, key_in), (w_value, value_in), (w_recept, recept_in), (spread, spread_in), (unit, unit_in)]
    loads = [pltpu.make_async_copy(source, target, load_sem.at[k]) for k, (source, target) in enumerate(late)]
    for load in loads:
        load.start()
    links.greet(True)
    feed_copies = {}
    for side in (0, 1):
        for o in (1, 2, 3):
            feed_copies[side, o] = remote(
                feed_part.at[side, o], feed_z.at[side, o - 1], feed_send.at[side, o - 1], feed_recv.at[side, o - 1],
                links.along_z[o - 1],
            )
            feed_copies[side, o].start()
    halo_out[...] = jnp.zeros_like(halo_out)
    sums[...] = sums_in[...]

    def part(n, cc, xx):
        at = pl.ds(pl.multiple_of((xx * 2 + cc) * 8 * rows, 8 * rows), 8 * rows)
        return matmul_lead(lefts[n, :, at], rights[n])

    def blocks():
        for zz in range(4):
            for yy in range(2):
                yield zz, yy, slice((zz * 2 + yy) * rows, (zz * 2 + yy + 1) * rows)

    def to_core(n):
        return remote(outgoing.at[n], gathered.at[n], core_send.at[n], core_recv.at[n], links.core)

    def to_first(n):
        return remote(
            gathered.at[n, pl.ds(2, 2)], from_first.at[n], first_send.at[n], first_recv.at[n], links.first
        )

    def to_second(n):
        return remote(gathered.at[n, 1], from_second.at[n], second_send.at[n], second_recv.at[n], links.second)

    def to_z(n, o):
        return remote(
            gathered.at[n, 0, o], from_z.at[n, o - 1], z_send.at[n, o - 1], z_recv.at[n, o - 1], links.along_z[o - 1]
        )

    def other(n, carry):
        for xx in range(2):
            value = part(n, 1 - c, xx)
            for zz, yy, at in blocks():
                outgoing[n, position(xx, yy, x, y, 1 - c), lax.rem(zz + 4 - z, 4)] = value[at].astype(BF)
        to_core(n).start()
        return carry

    def own(n, carry):
        to_core(n).wait_recv()
        for xx in range(2):
            value = part(n, c, xx)
            for zz, yy, at in blocks():
                i, o = position(xx, yy, x, y, c), lax.rem(zz + 4 - z, 4)
                gathered[n, i, o] = (gathered[n, i, o].astype(F32) + value[at]).astype(BF)
        to_first(n).start()
        return carry

    lax.fori_loop(0, count, other, 0)
    lax.fori_loop(0, count, own, 0)

    def pass_second(n):
        to_first(n).wait_recv()
        add_blocks(gathered.at[n, 1], [gathered.at[n, 1], from_first.at[n, 1]])
        to_second(n).start()

    def pass_z(n):
        to_second(n).wait_recv()
        add_blocks(gathered.at[n, 0], [gathered.at[n, 0], from_first.at[n, 0], from_second.at[n]])
        for o in (1, 2, 3):
            to_z(n, o).start()

    def finish(n):
        value = gathered[n, 0, 0].astype(F32)
        for o in (1, 2, 3):
            to_z(n, o).wait_recv()
            value = value + from_z[n, o - 1].astype(F32)
        square_grads[n] = value

    for side in (0, 1):
        for o in (1, 2, 3):
            feed_copies[side, o].wait_recv()
        for r in range(0, feed_part.shape[2], 32):
            at = slice(r, r + 32)
            value = feed_part[side, 0, at].astype(F32)
            for o in range(3):
                value = value + feed_z[side, o, at].astype(F32)
            own_units[side, at] = value.astype(BF)
    units_over_x = remote(own_units, x_units, unit_send.at[0], unit_recv.at[0], links.over_x)
    units_over_x.start()
    units_over_core = remote(own_units, core_units.at[0], unit_send.at[1], unit_recv.at[1], links.core)
    units_over_core.start()

    loads[0].wait()
    dot_rows(grad_key, rights.at[2], key_in)
    pass_second(0)
    loads[1].wait()
    dot_rows(grad_value, rights.at[3], value_in)
    pass_second(1)
    loads[2].wait()
    dot_rows(grad_recept, rights.at[4], recept_in)
    units_over_x.wait_recv()
    both_over_core = remote(x_units, core_units.at[1], unit_send.at[2], unit_recv.at[2], links.core)
    both_over_core.start()
    grads = ((grad_key, MIX_KEY), (grad_value, MIX_VALUE), (grad_recept, MIX_RECEPT))

    def shift_one(rows_at, at, keeping):
        return keeping * sum(g[rows_at, at] * (1.0 - vectors[k : k + 1, at]) for g, k in grads)

    for m in range(micro):
        start = m * length
        halo_out[m : m + 1] = shift_one(slice(start, start + 1), slice(None), keep[m, 0:1, 0:1])
    halo = remote(halo_out, halo_in, halo_send.at[0], halo_recv.at[0], links.row(size - 1))
    halo.start()
    pass_second(2)
    pass_z(0)
    loads[3].wait()
    halo.wait_recv()
    row = lax.broadcasted_iota(jnp.int32, (length, 128), 0)
    for m in range(micro):
        rows_at = slice(m * length, (m + 1) * length)

        def shift_pass(j, carry, m=m, rows_at=rows_at):
            at = lanes(j)
            after = jnp.where(t < size - 1, halo_in[m : m + 1, at], 0.0)
            apart = spread_in[rows_at, at]
            value = roll_rows(shift_one(rows_at, at, keep[m]), -1, after, row)
            for g, k in grads:
                value = value + g[rows_at, at] * vectors[k : k + 1, at]
                sums[k : k + 1, at] += jnp.sum(g[rows_at, at] * apart, axis=0, keepdims=True)
            grad_z[rows_at, at] = value
            return carry

        lax.fori_loop(0, width // 128, shift_pass, 0)
    pass_second(3)
    pass_z(1)
    loads[4].wait()
    norm_back_tiles(
        token_grads, grad_z, unit_in, inverse, vectors[GAIN_ONE : GAIN_ONE + 1, :], grad_residual, sums, GAIN_ONE
    )
    sums[DECAY : DECAY + 1, :] = -sums[DECAY : DECAY + 1, :] * rates[0:1, :] * vectors[DECAY : DECAY + 1, :]
    pass_second(4)

    stages = [[links.core], [links.over_x], [links.over_y], links.along_z]
    pending = []
    source, slot = sums, 0

    def begin(stage, source, slot):
        copies = [
            remote(source, held.at[slot + k], sum_send.at[slot + k], sum_recv.at[slot + k], peer)
            for k, peer in enumerate(stage)
        ]
        for copy in copies:
            copy.start()
        return copies

    def collect(copies, source, slot, target):
        value = source[...]
        for k, copy in enumerate(copies):
            copy.wait_recv()
            value = value + held[slot + k]
        target[...] = value

    copies = begin(stages[0], sums, 0)
    pending += copies
    pass_z(2)
    collect(copies, sums, 0, held.at[6])
    copies = begin(stages[1], held.at[6], 1)
    pending += copies
    pass_z(3)
    finish(0)
    collect(copies, held.at[6], 1, held.at[7])
    copies = begin(stages[2], held.at[7], 2)
    pending += copies
    pass_z(4)
    finish(1)
    collect(copies, held.at[7], 2, held.at[8])
    copies = begin(stages[3], held.at[8], 3)
    pending += copies
    units_over_core.wait_recv()
    both_over_core.wait_recv()
    for side, target in ((1, unit_key), (0, unit_value)):
        for d in range(4):
            for r in range(0, own_units.shape[1], 32):
                at = slice(r, r + 32)
                pick = jnp.where(links.dp == d ^ 1, core_units[0, side, at], core_units[1, side, at])
                pick = jnp.where(links.dp == d ^ 2, x_units[side, at], pick)
                pick = jnp.where(links.dp == d, own_units[side, at], pick)
                target[d, at] = pick.astype(F32)
    collect(copies, held.at[8], 3, vector_grads)
    finish(2)
    finish(3)
    finish(4)
    for n in range(count):
        to_core(n).wait_send()
        to_first(n).wait_send()
        to_second(n).wait_send()
        for o in (1, 2, 3):
            to_z(n, o).wait_send()
    for copy in pending + list(feed_copies.values()) + [units_over_x, units_over_core, both_over_core, halo]:
        copy.wait_send()


def front_backward(near, far):
    feed_part, lefts = near[:2]
    rows = feed_part.shape[2]
    count, tokens, width = lefts.shape
    own = width // 32
    dma = pltpu.SemaphoreType.DMA
    big = pltpu.VMEM((tokens, width), F32)
    square = pltpu.VMEM((width, width), BF)
    return pl.pallas_call(
        front_backward_kernel,
        out_shape=[
            jax.ShapeDtypeStruct((count, own, width), F32),
            jax.ShapeDtypeStruct((4, rows, width), F32), jax.ShapeDtypeStruct((4, rows, width), F32),
            jax.ShapeDtypeStruct((tokens, width), F32), jax.ShapeDtypeStruct((16, width), F32),
        ],
        in_specs=[whole()] * len(near) + [anywhere()] * len(far),
        out_specs=[whole()] * 5,
        scratch_shapes=[square] * 3
        + [big] * 2
        + [
            pltpu.VMEM((count, 4, 4, own, width), BF), pltpu.VMEM((count, 4, 4, own, width), BF),
            pltpu.VMEM((count, 2, 4, own, width), BF), pltpu.VMEM((count, 4, own, width), BF),
            pltpu.VMEM((count, 3, own, width), BF), pltpu.VMEM((2, 3, rows, width), BF),
            pltpu.VMEM((2, rows, width), BF), pltpu.VMEM((2, rows, width), BF), pltpu.VMEM((2, 2, rows, width), BF),
        ]
        + [big] * 4
        + [
            pltpu.VMEM((16, width), F32), pltpu.VMEM((9, 16, width), F32), pltpu.VMEM((8, width), F32),
            pltpu.VMEM((8, width), F32),
            dma((5,)), dma((count,)), dma((count,)), dma((count,)), dma((count,)), dma((count,)), dma((count,)),
            dma((count, 3)), dma((count, 3)), dma((2, 3)), dma((2, 3)), dma((3,)), dma((3,)), dma((1,)), dma((1,)),
            dma((6,)), dma((6,)),
        ],
        compiler_params=pltpu.CompilerParams(
            collective_id=3, has_side_effects=True, vmem_limit_bytes=66_000_000
        ),
        cost_estimate=cost(4 * count * tokens * width * width, 40 * width * width),
        name="front_backward",
    )(*near, *far)


def local_shards(tokens, resets, out_grads, *weights):
    (
        mixer_key, mixer_value, mixer_recept, mixer_output, feed_recept, feed_key, feed_value, *vector_shards
    ) = weights
    size = lax.axis_size("tensor")
    dp, t = lax.axis_index("dp"), lax.axis_index("tensor")
    micro, _, length, width = tokens.shape
    count = micro * length
    unit_rows = feed_key.shape[0] // 4
    feed_shard = jnp.concatenate(
        [lax.dynamic_slice_in_dim(w, dp * unit_rows, unit_rows, 0) for w in (feed_key, feed_value)], axis=1
    )
    share = vector_shards[0].shape[0]
    vector_pack = jnp.pad(jnp.stack(vector_shards), ((0, 16 - len(vector_shards)), (0, 128 - share)))
    keep = (1 - resets[:, 0]).astype(F32)[:, :, None]
    keep_lanes = jnp.broadcast_to(keep, (micro, length, 128))
    cotangent = out_grads.reshape(count, width)
    near = [tokens.reshape(count, width), cotangent, keep_lanes]
    parts = [vector_pack, mixer_key, mixer_value, mixer_recept, mixer_output, feed_recept, feed_shard]
    (
        _, all_key, all_value, all_recept, all_output, all_feedr, feed,
        result, table, rates, lefts, feed_in, grad_value, grad_gate, positive, spread_one, unit_one, inverse_one,
        spread_two, unit_two, inverse_two, keys, values, denom, mixed, prior_a, prior_b, recept,
    ) = forward(near, parts, size)
    w_key, w_value, w_recept, w_output, w_feedr = [
        w.reshape(width, width) for w in (all_key, all_value, all_recept, all_output, all_feedr)
    ]
    near = [feed_in, grad_value, grad_gate, table, keep_lanes, inverse_two, cotangent]
    far = [feed, positive, w_feedr, w_output, spread_two, unit_two, keys, values, denom, mixed, prior_a, prior_b, recept]
    feed_part, rights, grad_residual, sums = channel_backward(near, far, size)
    near = [feed_part, lefts, rights, table, keep_lanes, inverse_one, grad_residual, sums, rates]
    far = [w_key, w_value, w_recept, spread_one, unit_one]
    square_grads, unit_key, unit_value, token_grads, vector_grads = front_backward(near, far)
    mine = lax.dynamic_slice_in_dim(vector_grads, (dp * size + t) * share, share, 1)
    return (
        result.reshape(tokens.shape), token_grads.reshape(tokens.shape),
        square_grads[2], square_grads[3], square_grads[4], square_grads[1], square_grads[0],
        unit_key.reshape(feed_key.shape), unit_value.reshape(feed_value.shape),
    ) + tuple(mine[i] for i in range(len(vector_shards)))


def is_two_by_two_by_four(mesh):
    return mesh.shape["dp"] == 4 and mesh.shape["tensor"] == 8


def solution(mesh):
    return jax.shard_map(
        local_shards if is_two_by_two_by_four(mesh) else shards,
        mesh=mesh,
        in_specs=(
            P(None, "dp", "tensor", None),
            P(None, "dp", "tensor"),
            P(None, "dp", "tensor", None),
            P(("dp", "tensor"), None),
            P(("dp", "tensor"), None),
            P(("dp", "tensor"), None),
            P(("dp", "tensor"), None),
            P(("dp", "tensor"), None),
            P("tensor", None),
            P("tensor", None),
            P(("dp", "tensor")),
            P(("dp", "tensor")),
            P(("dp", "tensor")),
            P(("dp", "tensor")),
            P(("dp", "tensor")),
            P(("dp", "tensor")),
            P(("dp", "tensor")),
            P(("dp", "tensor")),
            P(("dp", "tensor")),
            P(("dp", "tensor")),
            P(("dp", "tensor")),
        ),
        out_specs=(
            P(None, "dp", "tensor", None),
            P(None, "dp", "tensor", None),
            P(("dp", "tensor"), None),
            P(("dp", "tensor"), None),
            P(("dp", "tensor"), None),
            P(("dp", "tensor"), None),
            P(("dp", "tensor"), None),
            P("tensor", None),
            P("tensor", None),
            P(("dp", "tensor")),
            P(("dp", "tensor")),
            P(("dp", "tensor")),
            P(("dp", "tensor")),
            P(("dp", "tensor")),
            P(("dp", "tensor")),
            P(("dp", "tensor")),
            P(("dp", "tensor")),
            P(("dp", "tensor")),
            P(("dp", "tensor")),
            P(("dp", "tensor")),
        ),
        check_vma=False,
    )
```

```python
import functools

import jax
import jax.numpy as jnp
from jax import lax
from jax.experimental import pallas as pl
from jax.experimental.pallas import tpu as pltpu
from jax.sharding import PartitionSpec as P

EPSILON = 1e-05


def entering(shard, axis, combine, identity, reverse):
    size, here = (lax.axis_size(axis), lax.axis_index(axis))
    everything = jax.tree.map(lambda part: lax.all_gather(part, axis), shard)
    start = jax.tree.map(
        lambda part, zero: jnp.broadcast_to(jnp.asarray(zero, part.dtype), part.shape),
        shard,
        identity,
    )

    def turn(k, before):
        at = size - 1 - k if reverse else k
        reached = at > here if reverse else at < here
        new = combine(before, jax.tree.map(lambda part: part[at], everything))
        return jax.tree.map(lambda a, b: jnp.where(reached, a, b), new, before)

    return lax.fori_loop(0, size, turn, start)


def shifted(block, axis, distance):
    devices = range(lax.axis_size(axis))
    route = [(i - distance, i) for i in devices if i - distance in devices]
    return lax.ppermute(block, axis, route)


def norm_rows(payload_series, gain, bias):
    center = payload_series - jnp.mean(payload_series, axis=-1, keepdims=True)
    inverse = lax.rsqrt(jnp.mean(center * center, axis=-1, keepdims=True) + EPSILON)
    normed = center * inverse
    return (normed * gain + bias, normed, inverse)


def norm_back(grad_out, normed, inverse, gain):
    scaled = grad_out * gain
    centred = scaled - jnp.mean(scaled, axis=-1, keepdims=True)
    grad_in = inverse * (centred - normed * jnp.mean(scaled * normed, axis=-1, keepdims=True))
    return (grad_in, jnp.sum(grad_out * normed, axis=0), jnp.sum(grad_out, axis=0))


def affine(earlier, later):
    return (
        earlier[0] * later[0],
        later[0] * earlier[1] + later[1],
        later[0] * earlier[2] + later[2],
    )


def carry_across(summary, backward):
    width = summary[0].shape[0]
    identity = (
        jnp.ones((width,), jnp.float32),
        jnp.zeros((width,), jnp.float32),
        jnp.zeros((width,), jnp.float32),
    )
    return entering(summary, "tensor", affine, identity, backward)


def matmul(left, right):
    return jnp.dot(left, right, preferred_element_type=jnp.float32)


def matmul_lead(left, right):
    return lax.dot_general(
        left, right, (((0,), (0,)), ((), ())), preferred_element_type=jnp.float32
    )


def matmul_last(left, right):
    return lax.dot_general(
        left, right, (((1,), (1,)), ((), ())), preferred_element_type=jnp.float32
    )


def shards(
    tokens,
    resets,
    out_grads,
    mixer_key,
    mixer_value,
    mixer_recept,
    mixer_output,
    feed_recept,
    feed_key,
    feed_value,
    first_gain,
    first_bias,
    second_gain,
    second_bias,
    mixing_key,
    mixing_value,
    mixing_recept,
    time_decay,
    time_first,
    feeding_key,
    feeding_recept,
):
    gathered = (
        lax.all_gather(mixer_key, ("dp", "tensor"), axis=0, tiled=True),
        lax.all_gather(mixer_value, ("dp", "tensor"), axis=0, tiled=True),
        lax.all_gather(mixer_recept, ("dp", "tensor"), axis=0, tiled=True),
        lax.all_gather(mixer_output, ("dp", "tensor"), axis=0, tiled=True),
        lax.all_gather(feed_recept, ("dp", "tensor"), axis=0, tiled=True),
        lax.all_gather(first_gain, ("dp", "tensor"), axis=0, tiled=True),
        lax.all_gather(first_bias, ("dp", "tensor"), axis=0, tiled=True),
        lax.all_gather(second_gain, ("dp", "tensor"), axis=0, tiled=True),
        lax.all_gather(second_bias, ("dp", "tensor"), axis=0, tiled=True),
        lax.all_gather(mixing_key, ("dp", "tensor"), axis=0, tiled=True),
        lax.all_gather(mixing_value, ("dp", "tensor"), axis=0, tiled=True),
        lax.all_gather(mixing_recept, ("dp", "tensor"), axis=0, tiled=True),
        lax.all_gather(time_decay, ("dp", "tensor"), axis=0, tiled=True),
        lax.all_gather(time_first, ("dp", "tensor"), axis=0, tiled=True),
        lax.all_gather(feeding_key, ("dp", "tensor"), axis=0, tiled=True),
        lax.all_gather(feeding_recept, ("dp", "tensor"), axis=0, tiled=True),
    )
    w_key, w_value, w_recept, w_output, w_feedr = (
        gathered[0],
        gathered[1],
        gathered[2],
        gathered[3],
        gathered[4],
    )
    parameter_vectors = [piece.astype(jnp.float32) for piece in gathered[5:]]
    gain_one, bias_one, gain_two, bias_two = (
        parameter_vectors[0],
        parameter_vectors[1],
        parameter_vectors[2],
        parameter_vectors[3],
    )
    mix_key, mix_value, mix_recept = (
        parameter_vectors[4],
        parameter_vectors[5],
        parameter_vectors[6],
    )
    (
        fading_speed_logarithm,
        opening_premium_logarithm,
        channel_lookup_blend,
        channel_gating_blend,
    ) = (parameter_vectors[7], parameter_vectors[8], parameter_vectors[9], parameter_vectors[10])
    rates = jnp.exp(fading_speed_logarithm)
    fading_multiplier = jnp.exp(-rates)
    micro_count = tokens.shape[0]
    width = tokens.shape[3]
    grad_keyw = jnp.zeros(feed_key.shape, jnp.float32)
    grad_valuew = jnp.zeros(feed_value.shape, jnp.float32)
    square_grads = [jnp.zeros((width, width), jnp.float32) for index_one in range(5)]
    parameter_vector_gradients = [jnp.zeros((width,), jnp.float32) for index_two in range(11)]
    results = []
    input_grads = []
    for micro_index in range(micro_count):
        inputs = tokens[micro_index, 0].astype(jnp.float32)
        restart_retain_flags = (1 - resets[micro_index, 0]).astype(jnp.float32)[:, None]
        cotangent = out_grads[micro_index, 0].astype(jnp.float32)
        normed_one, unit_one, inverse_one = norm_rows(inputs, gain_one, bias_one)
        z_one = normed_one.astype(jnp.bfloat16)
        prior_one = shifted(z_one[-1:], "tensor", 1)
        before_one = (
            jnp.concatenate([prior_one, z_one[:-1]], axis=0).astype(jnp.float32)
            * restart_retain_flags
        )
        z_onef = z_one.astype(jnp.float32)
        in_key = (z_onef * mix_key + before_one * (1.0 - mix_key)).astype(jnp.bfloat16)
        in_value = (z_onef * mix_value + before_one * (1.0 - mix_value)).astype(jnp.bfloat16)
        in_recept = (z_onef * mix_recept + before_one * (1.0 - mix_recept)).astype(jnp.bfloat16)
        lookup_series = matmul(in_key, w_key)
        payload_series = matmul(in_value, w_value)
        recept = jax.nn.sigmoid(matmul(in_recept, w_recept))
        powered_lookup = jnp.exp(lookup_series)
        premium_plus_lookup = jnp.exp(opening_premium_logarithm + lookup_series)
        factor = restart_retain_flags * fading_multiplier
        cum_factor, local_a, local_b = lax.associative_scan(
            affine, (factor, powered_lookup * payload_series, powered_lookup), axis=0
        )
        incoming = carry_across((cum_factor[-1], local_a[-1], local_b[-1]), False)
        upper_running_state = local_a + cum_factor * incoming[1]
        lower_running_state = local_b + cum_factor * incoming[2]
        earlier_upper_state = jnp.concatenate([incoming[1][None], upper_running_state[:-1]], axis=0)
        earlier_lower_state = jnp.concatenate([incoming[2][None], lower_running_state[:-1]], axis=0)
        lower_quotient_part = restart_retain_flags * earlier_lower_state + premium_plus_lookup
        blended = (
            restart_retain_flags * earlier_upper_state + premium_plus_lookup * payload_series
        ) / lower_quotient_part
        weighted = (recept * blended).astype(jnp.bfloat16)
        residual = inputs + matmul(weighted, w_output)
        normed_two, unit_two, inverse_two = norm_rows(residual, gain_two, bias_two)
        z_two = normed_two.astype(jnp.bfloat16)
        prior_two = shifted(z_two[-1:], "tensor", 1)
        before_two = (
            jnp.concatenate([prior_two, z_two[:-1]], axis=0).astype(jnp.float32)
            * restart_retain_flags
        )
        z_twof = z_two.astype(jnp.float32)
        feed_in = (
            z_twof * channel_lookup_blend + before_two * (1.0 - channel_lookup_blend)
        ).astype(jnp.bfloat16)
        feed_rin = (
            z_twof * channel_gating_blend + before_two * (1.0 - channel_gating_blend)
        ).astype(jnp.bfloat16)
        gate = jax.nn.sigmoid(matmul(feed_rin, w_feedr))
        all_in = lax.all_gather(feed_in, "tensor", axis=0, tiled=True)
        hidden_pre = matmul_last(feed_key, all_in)
        hidden = jnp.square(jnp.maximum(hidden_pre, 0.0)).astype(jnp.bfloat16)
        value_out = lax.psum_scatter(
            matmul_lead(hidden, feed_value), "tensor", scatter_dimension=0, tiled=True
        )
        results.append(residual + gate * value_out)
        grad_value = (cotangent * gate).astype(jnp.bfloat16)
        grad_gate = (cotangent * value_out * gate * (1.0 - gate)).astype(jnp.bfloat16)
        square_grads[4] = square_grads[4] + matmul_lead(feed_rin, grad_gate)
        grad_rin = matmul_last(grad_gate, w_feedr)
        relu_twice = 2.0 * jnp.maximum(hidden_pre, 0.0)
        add_piece = lax.all_gather(grad_value, "tensor", axis=0, tiled=True)
        rows_total = matmul(hidden, add_piece)
        block = matmul_last(feed_value, add_piece)
        grad_valuew = grad_valuew + rows_total
        grad_pre = (block * relu_twice).astype(jnp.bfloat16)
        grad_keyw = grad_keyw + matmul(grad_pre, all_in)
        grad_in = lax.psum_scatter(
            matmul_lead(grad_pre, feed_key), "tensor", scatter_dimension=0, tiled=True
        )
        parameter_vector_gradients[9] = parameter_vector_gradients[9] + jnp.sum(
            grad_in * (z_twof - before_two), axis=0
        )
        parameter_vector_gradients[10] = parameter_vector_gradients[10] + jnp.sum(
            grad_rin * (z_twof - before_two), axis=0
        )
        shift_two = restart_retain_flags * (
            grad_in * (1.0 - channel_lookup_blend) + grad_rin * (1.0 - channel_gating_blend)
        )
        after_two = shifted(shift_two[:1], "tensor", -1)
        grad_z_two = (
            grad_in * channel_lookup_blend
            + grad_rin * channel_gating_blend
            + jnp.concatenate([shift_two[1:], after_two], axis=0)
        )
        back_two, gain_part, bias_part = norm_back(grad_z_two, unit_two, inverse_two, gain_two)
        parameter_vector_gradients[2] = parameter_vector_gradients[2] + gain_part
        parameter_vector_gradients[3] = parameter_vector_gradients[3] + bias_part
        grad_residual = cotangent + back_two
        grad_att = grad_residual.astype(jnp.bfloat16)
        square_grads[3] = square_grads[3] + matmul_lead(weighted, grad_att)
        grad_weighted = matmul_last(grad_att, w_output)
        grad_mixed = grad_weighted * recept
        grad_recept = (grad_weighted * blended * recept * (1.0 - recept)).astype(jnp.bfloat16)
        upper_adjoint = grad_mixed / lower_quotient_part
        denominator_gradient = -grad_mixed * blended / lower_quotient_part
        cum_back, local_xa, local_xb = lax.associative_scan(
            affine,
            (
                factor,
                restart_retain_flags * upper_adjoint,
                restart_retain_flags * denominator_gradient,
            ),
            reverse=True,
            axis=0,
        )
        beyond = carry_across((cum_back[0], local_xa[0], local_xb[0]), True)
        adjoint_a = local_xa + cum_back * beyond[1]
        adjoint_b = local_xb + cum_back * beyond[2]
        running_upper_total = jnp.concatenate([adjoint_a[1:], beyond[1][None]], axis=0)
        running_lower_total = jnp.concatenate([adjoint_b[1:], beyond[2][None]], axis=0)
        premium_power = premium_plus_lookup * (
            payload_series * upper_adjoint + denominator_gradient
        )
        adjoint_payloads = (
            premium_plus_lookup * upper_adjoint + powered_lookup * running_upper_total
        ).astype(jnp.bfloat16)
        key_gradient_rows = (
            premium_power
            + powered_lookup * (payload_series * running_upper_total + running_lower_total)
        ).astype(jnp.bfloat16)
        parameter_vector_gradients[8] = parameter_vector_gradients[8] + jnp.sum(
            premium_power, axis=0
        )
        decay_sum = jnp.sum(
            restart_retain_flags
            * (
                running_upper_total * earlier_upper_state
                + running_lower_total * earlier_lower_state
            ),
            axis=0,
        )
        parameter_vector_gradients[7] = (
            parameter_vector_gradients[7] - rates * fading_multiplier * decay_sum
        )
        square_grads[0] = square_grads[0] + matmul_lead(in_key, key_gradient_rows)
        square_grads[1] = square_grads[1] + matmul_lead(in_value, adjoint_payloads)
        square_grads[2] = square_grads[2] + matmul_lead(in_recept, grad_recept)
        grad_inkey = matmul_last(key_gradient_rows, w_key)
        grad_invalue = matmul_last(adjoint_payloads, w_value)
        grad_inrecept = matmul_last(grad_recept, w_recept)
        spread_one = z_onef - before_one
        parameter_vector_gradients[4] = parameter_vector_gradients[4] + jnp.sum(
            grad_inkey * spread_one, axis=0
        )
        parameter_vector_gradients[5] = parameter_vector_gradients[5] + jnp.sum(
            grad_invalue * spread_one, axis=0
        )
        parameter_vector_gradients[6] = parameter_vector_gradients[6] + jnp.sum(
            grad_inrecept * spread_one, axis=0
        )
        shift_one = restart_retain_flags * (
            grad_inkey * (1.0 - mix_key)
            + grad_invalue * (1.0 - mix_value)
            + grad_inrecept * (1.0 - mix_recept)
        )
        after_one = shifted(shift_one[:1], "tensor", -1)
        grad_z_one = (
            grad_inkey * mix_key
            + grad_invalue * mix_value
            + grad_inrecept * mix_recept
            + jnp.concatenate([shift_one[1:], after_one], axis=0)
        )
        back_one, gain_first, bias_first = norm_back(grad_z_one, unit_one, inverse_one, gain_one)
        parameter_vector_gradients[0] = parameter_vector_gradients[0] + gain_first
        parameter_vector_gradients[1] = parameter_vector_gradients[1] + bias_first
        input_grads.append(grad_residual + back_one)
    owned = (
        lax.psum_scatter(square_grads[0], ("dp", "tensor"), scatter_dimension=0, tiled=True),
        lax.psum_scatter(square_grads[1], ("dp", "tensor"), scatter_dimension=0, tiled=True),
        lax.psum_scatter(square_grads[2], ("dp", "tensor"), scatter_dimension=0, tiled=True),
        lax.psum_scatter(square_grads[3], ("dp", "tensor"), scatter_dimension=0, tiled=True),
        lax.psum_scatter(square_grads[4], ("dp", "tensor"), scatter_dimension=0, tiled=True),
        lax.psum_scatter(
            parameter_vector_gradients[0], ("dp", "tensor"), scatter_dimension=0, tiled=True
        ),
        lax.psum_scatter(
            parameter_vector_gradients[1], ("dp", "tensor"), scatter_dimension=0, tiled=True
        ),
        lax.psum_scatter(
            parameter_vector_gradients[2], ("dp", "tensor"), scatter_dimension=0, tiled=True
        ),
        lax.psum_scatter(
            parameter_vector_gradients[3], ("dp", "tensor"), scatter_dimension=0, tiled=True
        ),
        lax.psum_scatter(
            parameter_vector_gradients[4], ("dp", "tensor"), scatter_dimension=0, tiled=True
        ),
        lax.psum_scatter(
            parameter_vector_gradients[5], ("dp", "tensor"), scatter_dimension=0, tiled=True
        ),
        lax.psum_scatter(
            parameter_vector_gradients[6], ("dp", "tensor"), scatter_dimension=0, tiled=True
        ),
        lax.psum_scatter(
            parameter_vector_gradients[7], ("dp", "tensor"), scatter_dimension=0, tiled=True
        ),
        lax.psum_scatter(
            parameter_vector_gradients[8], ("dp", "tensor"), scatter_dimension=0, tiled=True
        ),
        lax.psum_scatter(
            parameter_vector_gradients[9], ("dp", "tensor"), scatter_dimension=0, tiled=True
        ),
        lax.psum_scatter(
            parameter_vector_gradients[10], ("dp", "tensor"), scatter_dimension=0, tiled=True
        ),
    )
    key_rows, value_rows_grad = (grad_keyw, grad_valuew)
    key_total, value_total = (
        lax.psum(key_rows.astype(jnp.bfloat16), "dp").astype(jnp.float32),
        lax.psum(value_rows_grad.astype(jnp.bfloat16), "dp").astype(jnp.float32),
    )
    result_all = jnp.stack(results)[:, None]
    grads_all = jnp.stack(input_grads)[:, None]
    return (
        result_all,
        grads_all,
        owned[0],
        owned[1],
        owned[2],
        owned[3],
        owned[4],
        key_total,
        value_total,
        owned[5],
        owned[6],
        owned[7],
        owned[8],
        owned[9],
        owned[10],
        owned[11],
        owned[12],
        owned[13],
        owned[14],
        owned[15],
    )


BF = jnp.bfloat16
F32 = jnp.float32
BOTH = ("dp", "tensor")
MESH_ID = pl.DeviceIdType.MESH


def cost(flops, moved):
    return pl.CostEstimate(flops=flops, bytes_accessed=moved, transcendentals=0)


def whole():
    return pl.BlockSpec(memory_space=pltpu.VMEM)


def anywhere():
    return pl.BlockSpec(memory_space=pl.ANY)


def roll_rows(value, distance, fill, row):
    size = value.shape[0]
    moved = pltpu.roll(value, distance % size, 0)
    outside = row < distance if distance > 0 else row >= size + distance
    return jnp.where(outside, fill, moved)


def doubling(factor, up, low, row, sign):
    size, step = factor.shape[0], 1
    while step < size:
        up = up + factor * roll_rows(up, sign * step, 0.0, row)
        low = low + factor * roll_rows(low, sign * step, 0.0, row)
        factor = factor * roll_rows(factor, sign * step, 1.0, row)
        step *= 2
    return factor, up, low


def row_copies(summary, arrived, send, recv, t, dp, size):
    return [
        pltpu.make_async_remote_copy(
            src_ref=summary,
            dst_ref=arrived.at[o],
            send_sem=send.at[o],
            recv_sem=recv.at[o],
            device_id=(dp, lax.rem(t + o, size)),
            device_id_type=MESH_ID,
        )
        for o in range(1, size)
    ]


def lanes(j):
    return pl.ds(pl.multiple_of(j * 128, 128), 128)


def owner(i, x, y, c):
    first, second = i // 2, i % 2
    flip_x = first * c + second * (1 - c)
    flip_y = first * (1 - c) + second * c
    return x + flip_x - 2 * x * flip_x, y + flip_y - 2 * y * flip_y


def position(xx, yy, x, y, c):
    flip_x = x + xx - 2 * x * xx
    flip_y = y + yy - 2 * y * yy
    return 2 * (flip_x * c + flip_y * (1 - c)) + flip_x * (1 - c) + flip_y * c


class Links:
    def __init__(self, size):
        dp, t = lax.axis_index("dp"), lax.axis_index("tensor")
        x, c, z, y = dp // 2, dp % 2, t // 2, t % 2
        self.x, self.c, self.z, self.y, self.dp, self.t, self.size = x, c, z, y, dp, t, size
        over_x, over_y = ((1 - x) * 2 + c, t), (dp, z * 2 + 1 - y)
        self.over_x = over_x
        self.core = (x * 2 + 1 - c, t)
        self.first = (jnp.where(c == 0, over_y[0], over_x[0]), jnp.where(c == 0, over_y[1], over_x[1]))
        self.second = (jnp.where(c == 0, over_x[0], over_y[0]), jnp.where(c == 0, over_x[1], over_y[1]))
        self.along_z = [(dp, lax.rem(z + o, 4) * 2 + y) for o in (1, 2, 3)]
        self.over_y = over_y

    def row(self, o):
        return (self.dp, lax.rem(self.t + o, self.size))

    def greet(self, whole_row):
        peers = [self.row(o) for o in range(1, self.size)] if whole_row else self.along_z + [self.over_y]
        peers = peers + [self.over_x, self.core]
        barrier = pltpu.get_barrier_semaphore()
        for peer in peers:
            pl.semaphore_signal(barrier, inc=1, device_id=peer, device_id_type=MESH_ID)
        pl.semaphore_wait(barrier, len(peers))


def remote(source, target, send, recv, device):
    return pltpu.make_async_remote_copy(
        src_ref=source, dst_ref=target, send_sem=send, recv_sem=recv, device_id=device, device_id_type=MESH_ID
    )


def add_blocks(target, sources):
    count, rows = target.shape[:2]
    tile = min(rows, 32)
    per = rows // tile

    def turn(k, carry):
        n, at = k // per, pl.ds(pl.multiple_of(lax.rem(k, per) * tile, tile), tile)
        value = sources[0][n, at].astype(F32)
        for source in sources[1:]:
            value = value + source[n, at].astype(F32)
        target[n, at] = value.astype(target.dtype)
        return carry

    lax.fori_loop(0, count * per, turn, 0)


def dot_rows(target, left, right):
    tile = 256

    def turn(n, carry):
        at = pl.ds(pl.multiple_of(n * tile, tile), tile)
        target[:, at] = matmul_last(left[...], right[at, :])
        return carry

    lax.fori_loop(0, right.shape[0] // tile, turn, 0)


def norm_back_tiles(target, grads, normed, inverse, gain, base, sums, gain_row):
    tile = 32
    width = grads.shape[1]

    def turn(k, carry):
        at = pl.ds(pl.multiple_of(k * tile, tile), tile)
        grad, unit = grads[at, :], normed[at, :]
        scaled = grad * gain
        middle = jnp.sum(scaled, axis=-1, keepdims=True) * (1.0 / width)
        along = jnp.sum(scaled * unit, axis=-1, keepdims=True) * (1.0 / width)
        target[at, :] = base[at, :].astype(F32) + inverse[at, 0:1] * (scaled - middle - unit * along)
        sums[gain_row : gain_row + 1, :] += jnp.sum(grad * unit, axis=0, keepdims=True)
        sums[gain_row + 1 : gain_row + 2, :] += jnp.sum(grad, axis=0, keepdims=True)
        return carry

    lax.fori_loop(0, grads.shape[0] // tile, turn, 0)


GAIN_ONE, BIAS_ONE, GAIN_TWO, BIAS_TWO, MIX_KEY, MIX_VALUE, MIX_RECEPT, DECAY, PREMIUM, BLEND_KEY, BLEND_RECEPT = range(11)


def norm_tiles(source, unit, inverse):
    rows, width = source.shape
    tile = min(rows, 32)

    def turn(k, carry):
        at = pl.ds(pl.multiple_of(k * tile, tile), tile)
        value = source[at, :].astype(F32)
        center = value - jnp.sum(value, axis=-1, keepdims=True) * (1.0 / width)
        scale = lax.rsqrt(jnp.sum(center * center, axis=-1, keepdims=True) * (1.0 / width) + EPSILON)
        unit[at, :] = center * scale
        inverse[at, :] = jnp.broadcast_to(scale, (tile, 128))
        return carry

    lax.fori_loop(0, rows // tile, turn, 0)


def dot_columns(finish, left, right):
    tile = 256
    depth = left.shape[1]

    def turn(n, carry):
        at = pl.ds(pl.multiple_of(n * tile, tile), tile)
        finish(at, matmul(left[...], right[:, :, :, :, :, at].reshape(depth, tile)))
        return carry

    lax.fori_loop(0, right.shape[5] // tile, turn, 0)


AHEAD = 3


def forward_kernel(
    tokens, cotangent, keep,
    own_vectors, own_key, own_value, own_recept, own_output, own_feedr, own_feed,
    all_vectors, all_key, all_value, all_recept, all_output, all_feedr, all_feed,
    result, table_out, rates_out, lefts, feed_in_out, grad_value_out, grad_gate_out, positive, spread_one_out,
    unit_one_out, inverse_one_out, spread_two_out, unit_two_out, inverse_two_out, keys_out, values_out, denom_out,
    mixed_out, prior_a_out, prior_b_out, recept_out,
    packed, table, rates, squares, feed_slot, positive_slot, left_parts, feed_in, grad_value, grad_gate, spread_one,
    unit_one, inverse_one, spread_two, unit_two, inverse_two, keys, values, gates, denom, mixed, prior_a, prior_b,
    cum, up, low, residual, total, halo_tokens, halo_unit, halo_inverse, summary, arrived, entering_rows, halo_out, halo_in,
    send, recv, own_sem, load_sem, out_sem, slot_sem, scan_send, scan_recv, halo_send, halo_recv,
):
    size = arrived.shape[0]
    links = Links(size)
    x, c, z, y, t, dp = links.x, links.c, links.z, links.y, links.t, links.dp
    count, width = tokens.shape
    micro, length = keep.shape[:2]
    ins = [own_vectors, own_key, own_value, own_recept, own_output, own_feedr, own_feed]
    outs = [all_vectors, all_key, all_value, all_recept, all_output, all_feedr, all_feed]
    piece = 16
    chunks = [(i, r) for i in range(7) for r in range(0, ins[i].shape[0], piece)]
    steps = len(chunks)
    feed_steps = ins[6].shape[0] // piece
    feed_base = steps - feed_steps
    x_first, y_first = jnp.where(c == 0, x, 1 - x), jnp.where(c == 0, 1 - y, y)
    first, second = links.first, links.second

    def place(n):
        if isinstance(n, int):
            i, start = chunks[n]
            return i, pl.ds(start, piece)
        return 6, pl.ds(pl.multiple_of((n - feed_base) * piece, piece), piece)

    def copy_z(n, o):
        i, at = place(n)
        return remote(ins[i].at[at], outs[i].at[x, c, z, y, at], send.at[n, o], recv.at[n, o], links.along_z[o])

    def copy_column(n, j, xx, yy, device):
        i, at = place(n)
        column = outs[i].at[xx, c, :, yy, at]
        return remote(column, column, send.at[n, j], recv.at[n, j], device)

    def copy_first(n):
        return copy_column(n, 3, x, y, first)

    def copy_second(n):
        return copy_column(n, 4, x, y, second)

    def copy_passed(n):
        return copy_column(n, 5, x_first, y_first, second)

    def copy_core(n):
        i, at = place(n)
        half = outs[i].at[:, c, :, :, at]
        return remote(half, half, send.at[n, 6], recv.at[n, 6], links.core)

    def step_z(n):
        for o in range(3):
            copy_z(n, o).start()

    def step_a(n):
        for o in range(3):
            copy_z(n, o).wait_recv()
        copy_first(n).start()
        copy_second(n).start()

    def step_b(n):
        copy_first(n).wait_recv()
        copy_passed(n).start()

    def step_c(n):
        copy_second(n).wait_recv()
        copy_passed(n).wait_recv()
        copy_core(n).start()

    def advance(*numbers):
        for s in numbers:
            if s + AHEAD < steps:
                step_z(s + AHEAD)
            if s < steps:
                step_a(s)
            if 0 <= s - 1 < steps:
                step_b(s - 1)
            if 0 <= s - 2 < steps:
                step_c(s - 2)

    def load(k):
        return pltpu.make_async_copy(outs[1 + k], squares.at[k], load_sem.at[k])

    def ready(k):
        for n in (2 * k + 1, 2 * k + 2):
            copy_core(n).wait_recv()
        load(k).start()

    written = []

    def write(source, target):
        copy = pltpu.make_async_copy(source, target, out_sem.at[len(written)])
        copy.start()
        written.append(copy)

    owns = [pltpu.make_async_copy(ins[i], outs[i].at[x, c, z, y], own_sem.at[i]) for i in range(7)]
    for own in owns:
        own.start()
    links.greet(True)
    halo_copies = [
        remote(
            tokens.at[pl.ds((m + 1) * length - piece, piece)], halo_tokens.at[pl.ds(m * piece, piece)],
            halo_send.at[m], halo_recv.at[m], links.row(1),
        )
        for m in range(micro)
    ]
    for halo in halo_copies:
        halo.start()
    for n in range(AHEAD):
        step_z(n)
    summary[...] = jnp.zeros_like(summary)
    halo_out[...] = jnp.zeros_like(halo_out)
    total[...] = jnp.zeros_like(total)
    for own in owns:
        own.wait()
    advance(0)
    norm_tiles(tokens, unit_one, inverse_one)
    write(unit_one, unit_one_out)
    write(inverse_one, inverse_one_out)
    advance(1, 2)
    for halo in halo_copies:
        halo.wait_recv()
    norm_tiles(halo_tokens, halo_unit, halo_inverse)
    copy_core(0).wait_recv()

    vector_load = pltpu.make_async_copy(all_vectors, packed, load_sem.at[5])
    vector_load.start()
    advance(3)
    vector_load.wait()
    share = width // 32
    per = 128 // share
    for j in range(width // 128):
        value = None
        for q in range(per):
            d = j * per + q
            part = packed[d // 16, (d // 8) % 2, (d // 2) % 4, d % 2].astype(F32)
            part = pltpu.roll(part, q * share, 1) if q else part
            value = part if value is None else value + part
        table[:, j * 128 : (j + 1) * 128] = value
    speed = jnp.exp(table[DECAY : DECAY + 1, :])
    rates[...] = jnp.broadcast_to(speed, rates.shape)
    table[DECAY : DECAY + 1, :] = jnp.exp(-speed)
    write(table, table_out)
    write(rates, rates_out)
    row = lax.broadcasted_iota(jnp.int32, (length, 128), 0)

    def vector(k, at):
        return table[k : k + 1, at]

    def normed(unit, gain, bias, at):
        return (unit * vector(gain, at) + vector(bias, at)).astype(BF).astype(F32)

    def blends(spread, unit, m, prior, gain, bias, mixes):
        rows_at = slice(m * length, (m + 1) * length)

        def turn(j, carry):
            at = lanes(j)
            now = normed(unit[rows_at, at], gain, bias, at)
            before = roll_rows(now, 1, jnp.where(t > 0, prior(at), 0.0), row) * keep[m]
            spread[rows_at, at] = now - before
            for target, mix in mixes:
                target[rows_at, at] = (now * vector(mix, at) + before * (1.0 - vector(mix, at))).astype(BF)
            return carry

        lax.fori_loop(0, width // 128, turn, 0)

    mixes = [(left_parts.at[2 + k], MIX_KEY + k) for k in range(3)]
    for m in range(micro):
        last = (m + 1) * piece - 1

        def prior(at, last=last):
            return normed(halo_unit[last : last + 1, at], GAIN_ONE, BIAS_ONE, at)

        blends(spread_one, unit_one, m, prior, GAIN_ONE, BIAS_ONE, mixes)
        advance(4 + m)
    write(spread_one, spread_one_out)
    for k in range(3):
        write(left_parts.at[2 + k], lefts.at[2 + k])

    def keep_in(target):
        def finish(at, value):
            target[:, at] = value

        return finish

    ready(0)
    advance(6)
    load(0).wait()
    dot_columns(keep_in(keys), left_parts.at[2], squares.at[0])
    write(keys, keys_out)
    ready(1)
    advance(7)
    load(1).wait()
    dot_columns(keep_in(values), left_parts.at[3], squares.at[1])
    write(values, values_out)

    for m in range(micro):
        rows_at = slice(m * length, (m + 1) * length)

        def first_pass(j, carry, m=m, rows_at=rows_at):
            at = lanes(j)
            power = jnp.exp(keys[rows_at, at])
            f, a, b = doubling(keep[m] * vector(DECAY, at), power * values[rows_at, at], power, row, 1)
            cum[rows_at, at] = f
            up[rows_at, at] = a
            low[rows_at, at] = b
            summary[3 * m : 3 * m + 1, at] = f[length - 1 :]
            summary[3 * m + 1 : 3 * m + 2, at] = a[length - 1 :]
            summary[3 * m + 2 : 3 * m + 3, at] = b[length - 1 :]
            return carry

        lax.fori_loop(0, width // 128, first_pass, 0)
        advance(8 + m)
    scan_copies = row_copies(summary, arrived, scan_send, scan_recv, t, dp, size)
    for copy in scan_copies:
        copy.start()
    ready(2)
    load(2).wait()

    def finish_gate(at, value):
        gates[:, at] = jax.nn.sigmoid(value)

    dot_columns(finish_gate, left_parts.at[4], squares.at[2])
    write(gates, recept_out)
    advance(10, 11)
    for copy in scan_copies:
        copy.wait_recv()
    for m in range(micro):
        a = jnp.zeros((1, width), F32)
        b = jnp.zeros((1, width), F32)
        for o in range(size - 1, 0, -1):
            f = arrived[o, 3 * m : 3 * m + 1]
            a = jnp.where(t >= o, f * a + arrived[o, 3 * m + 1 : 3 * m + 2], a)
            b = jnp.where(t >= o, f * b + arrived[o, 3 * m + 2 : 3 * m + 3], b)
        entering_rows[2 * m : 2 * m + 1] = a
        entering_rows[2 * m + 1 : 2 * m + 2] = b
    for m in range(micro):
        rows_at = slice(m * length, (m + 1) * length)

        def second_pass(j, carry, m=m, rows_at=rows_at):
            at = lanes(j)
            enter_a = entering_rows[2 * m : 2 * m + 1, at]
            enter_b = entering_rows[2 * m + 1 : 2 * m + 2, at]
            f = cum[rows_at, at]
            before_a = roll_rows(up[rows_at, at] + f * enter_a, 1, enter_a, row)
            before_b = roll_rows(low[rows_at, at] + f * enter_b, 1, enter_b, row)
            bonus = jnp.exp(vector(PREMIUM, at) + keys[rows_at, at])
            below = keep[m] * before_b + bonus
            blended = (keep[m] * before_a + bonus * values[rows_at, at]) / below
            left_parts[1, rows_at, at] = (gates[rows_at, at] * blended).astype(BF)
            denom[rows_at, at] = below
            mixed[rows_at, at] = blended
            prior_a[rows_at, at] = before_a
            prior_b[rows_at, at] = before_b
            return carry

        lax.fori_loop(0, width // 128, second_pass, 0)
    write(left_parts.at[1], lefts.at[1])
    write(denom, denom_out)
    write(mixed, mixed_out)
    write(prior_a, prior_a_out)
    write(prior_b, prior_b_out)
    ready(3)
    advance(12)
    load(3).wait()

    def finish_residual(at, value):
        residual[:, at] = tokens[:, at].astype(F32) + value

    dot_columns(finish_residual, left_parts.at[1], squares.at[3])
    norm_tiles(residual, unit_two, inverse_two)
    write(unit_two, unit_two_out)
    write(inverse_two, inverse_two_out)
    for m in range(micro):
        last = (m + 1) * length - 1
        halo_out[m : m + 1, :] = normed(unit_two[last : last + 1, :], GAIN_TWO, BIAS_TWO, slice(None))
    halo_two = remote(halo_out, halo_in, halo_send.at[micro], halo_recv.at[micro], links.row(1))
    halo_two.start()
    ready(4)
    advance(13)
    halo_two.wait_recv()
    mixes = [(feed_in, BLEND_KEY), (left_parts.at[0], BLEND_RECEPT)]
    for m in range(micro):

        def prior(at, m=m):
            return halo_in[m : m + 1, at]

        blends(spread_two, unit_two, m, prior, GAIN_TWO, BIAS_TWO, mixes)
    write(spread_two, spread_two_out)
    write(feed_in, feed_in_out)
    write(left_parts.at[0], lefts.at[0])
    advance(14)
    load(4).wait()

    def finish_second_gate(at, value):
        cum[:, at] = jax.nn.sigmoid(value)

    dot_columns(finish_second_gate, left_parts.at[0], squares.at[4])

    advance(15)
    later = {0: 16, 1: 17, 3: 18, 5: 19, 7: 20}

    def arrive(k, carry):
        for turn, number in later.items():
            pl.when(k == turn)(functools.partial(advance, number))
        slot = lax.rem(k, 2)
        at = pl.ds(pl.multiple_of(k * piece, piece), piece)
        copy_core(feed_base + k).wait_recv()
        fetch = pltpu.make_async_copy(outs[6].at[:, :, :, :, at], feed_slot, slot_sem.at[0])
        fetch.start()

        def put(k, slot):
            at = pl.ds(pl.multiple_of(k * piece, piece), piece)
            return pltpu.make_async_copy(positive_slot.at[slot], positive.at[:, :, :, :, at], slot_sem.at[1 + slot])

        @pl.when(k >= 2)
        def _():
            put(k - 2, slot).wait()

        fetch.wait()
        units = 32 * piece
        hidden = jnp.maximum(matmul_last(feed_slot[:, :, :, :, :, :width].reshape(units, width), feed_in[...]), 0.0)
        positive_slot[slot] = hidden.reshape(positive_slot.shape[1:])
        put(k, slot).start()
        hidden_squares = (hidden * hidden).astype(BF)
        total[...] += matmul_lead(hidden_squares, feed_slot[:, :, :, :, :, width:].reshape(units, width))

        @pl.when(k == feed_steps - 1)
        def _():
            put(k - 1, 1 - slot).wait()
            put(k, slot).wait()

        return carry

    lax.fori_loop(0, feed_steps, arrive, 0)

    def last_pass(k, carry):
        at = pl.ds(pl.multiple_of(k * 32, 32), 32)
        gate, value_out, grad = cum[at, :], total[at, :], cotangent[at, :].astype(F32)
        residual[at, :] = residual[at, :] + gate * value_out
        grad_value[at, :] = (grad * gate).astype(BF)
        grad_gate[at, :] = (grad * value_out * gate * (1.0 - gate)).astype(BF)
        return carry

    lax.fori_loop(0, count // 32, last_pass, 0)
    write(residual, result)
    write(grad_value, grad_value_out)
    write(grad_gate, grad_gate_out)
    for n in range(steps):
        for o in range(3):
            copy_z(n, o).wait_send()
        for copy in (copy_first(n), copy_second(n), copy_passed(n), copy_core(n)):
            copy.wait_send()
    for copy in halo_copies + [halo_two] + scan_copies:
        copy.wait_send()
    for copy in written:
        copy.wait()


def forward(near, parts, size):
    count, width = near[0].shape
    rows = parts[6].shape[0]
    flat = lambda kind: jax.ShapeDtypeStruct((count, width), kind)
    narrow = jax.ShapeDtypeStruct((count, 128), F32)
    dma = pltpu.SemaphoreType.DMA
    big, low = pltpu.VMEM((count, width), F32), pltpu.VMEM((count, width), BF)
    lines = pltpu.VMEM((count, 128), F32)
    steps = sum(p.shape[0] // 16 for p in parts)
    eight = pltpu.VMEM((8, width), F32)
    return pl.pallas_call(
        forward_kernel,
        out_shape=[jax.ShapeDtypeStruct((2, 2, 4, 2) + p.shape, p.dtype) for p in parts]
        + [
            flat(F32), jax.ShapeDtypeStruct((16, width), F32), jax.ShapeDtypeStruct((8, width), F32),
            jax.ShapeDtypeStruct((5, count, width), BF), flat(BF), flat(BF), flat(BF),
            jax.ShapeDtypeStruct((2, 2, 4, 2, rows, count), F32), flat(F32), flat(F32), narrow, flat(F32), flat(F32), narrow,
        ]
        + [flat(F32)] * 7,
        in_specs=[whole()] * (len(near) + len(parts)),
        out_specs=[anywhere()] * 28,
        scratch_shapes=[
            pltpu.VMEM((2, 2, 4, 2, 16, 128), BF), pltpu.VMEM((16, width), F32), eight,
            pltpu.VMEM((5, 2, 2, 4, 2, width // 32, width), BF), pltpu.VMEM((2, 2, 4, 2, 16, 2 * width), BF),
            pltpu.VMEM((2, 2, 2, 4, 2, 16, count), F32), pltpu.VMEM((5, count, width), BF), low, low, low, big,
            big, lines, big, big, lines,
        ]
        + [big] * 12
        + [
            pltpu.VMEM((32, width), BF), pltpu.VMEM((32, width), F32), pltpu.VMEM((32, 128), F32), eight,
            pltpu.VMEM((size, 8, width), F32), eight, eight, eight,
            dma((steps, 7)), dma((steps, 7)), dma((7,)), dma((6,)), dma((24,)), dma((3,)), dma((size,)), dma((size,)),
            dma((3,)), dma((3,)),
        ],
        compiler_params=pltpu.CompilerParams(collective_id=0, has_side_effects=True, vmem_limit_bytes=66_000_000),
        cost_estimate=cost(6 * count * width * width + 4 * count * 32 * rows * width, 60_000_000),
        name="forward",
    )(*near, *parts)


def channel_backward_kernel(
    feed_in, grad_value, grad_gate, vectors, keep, inverse, cotangent,
    weights, positive, w_feedr, w_output, spread, unit, keys, values, denom, mixed, prior_a, prior_b, recept,
    own_units, rights, grad_residual, sums,
    weight_slots, positive_slots, feedr, output, spread_in, unit_in, keys_in, values_in, denom_in, mixed_in,
    prior_a_in, prior_b_in, recept_in, value_part, key_part, outgoing, gathered, from_first, from_second, feed_part, feed_z,
    grad_in, grad_rin, grad_z, grad_w, cum, up, low, summary, arrived, entering_rows, halo_out, halo_in,
    slot_sem, load_sem, core_send, core_recv, first_send, first_recv, second_send, second_recv, feed_send, feed_recv,
    scan_send, scan_recv, halo_send, halo_recv,
):
    size = arrived.shape[0]
    links = Links(size)
    x, c, z, y, t = links.x, links.c, links.z, links.y, links.t
    rows, width = weight_slots.shape[2], feed_in.shape[1]
    micro, length = keep.shape[:2]

    def which(s):
        return lax.rem(s // 2, 2), 3 - 2 * (s // 4) - lax.rem(s, 2)

    def fetches(s, slot):
        own, i = which(s)
        cc = own * c + (1 - own) * (1 - c)
        xx, yy = owner(i, x, y, cc)
        return (
            pltpu.make_async_copy(weights.at[xx, cc, :, yy], weight_slots.at[slot], slot_sem.at[0, slot]),
            pltpu.make_async_copy(positive.at[xx, cc, :, yy], positive_slots.at[slot], slot_sem.at[1, slot]),
        )

    for copy in fetches(0, 0):
        copy.start()
    late = [
        (w_feedr, feedr), (spread, spread_in), (unit, unit_in), (w_output, output), (recept, recept_in),
        (mixed, mixed_in), (denom, denom_in), (keys, keys_in), (values, values_in), (prior_a, prior_a_in),
        (prior_b, prior_b_in),
    ]
    loads = [pltpu.make_async_copy(source, target, load_sem.at[k]) for k, (source, target) in enumerate(late)]
    for load in loads:
        load.start()
    links.greet(True)
    grad_att, grad_keys, grad_values, grad_recept = [rights.at[n] for n in range(1, 5)]
    rights[0] = grad_gate[...]
    grad_in[...] = jnp.zeros_like(grad_in)
    sums[...] = jnp.zeros_like(sums)
    summary[...] = jnp.zeros_like(summary)
    halo_out[...] = jnp.zeros_like(halo_out)

    def to_core(i, slot):
        return remote(outgoing.at[slot], gathered.at[i], core_send.at[i], core_recv.at[i], links.core)

    half = rows // 2

    def piece(ref, u, *first):
        return ref.at[(*first, u // 2, slice(None), slice((u % 2) * half, (u % 2 + 1) * half))]

    def to_first(q, u):
        return remote(
            piece(gathered, u, 2 + q), piece(from_first, u, q), first_send.at[q, u], first_recv.at[q, u], links.first
        )

    def column(s, carry):
        slot = lax.rem(s, 2)
        own, i = which(s)
        for copy in fetches(s, slot):
            copy.wait()

        @pl.when(s < 7)
        def _():
            for copy in fetches(s + 1, 1 - slot):
                copy.start()

        hidden = positive_slots[slot].reshape(4 * rows, feed_in.shape[0])
        squares = (hidden * hidden).astype(BF)
        key_rows = weight_slots[slot, :, :, :width].reshape(4 * rows, width)
        value_rows = weight_slots[slot, :, :, width:].reshape(4 * rows, width)
        value_part[...] = matmul(squares, grad_value[...])
        grad_pre = (matmul_last(value_rows, grad_value[...]) * (2.0 * hidden)).astype(BF)
        key_part[...] = matmul(grad_pre, feed_in[...])
        grad_in[...] += matmul_lead(grad_pre, key_rows)

        @pl.when(own == 0)
        def _():
            @pl.when(s >= 4)
            def _():
                to_core(i + 2, slot).wait_send()

            for k in range(4):
                at = lax.rem(k + 4 - z, 4)
                outgoing[slot, 0, at] = value_part[k * rows : (k + 1) * rows].astype(BF)
                outgoing[slot, 1, at] = key_part[k * rows : (k + 1) * rows].astype(BF)
            to_core(i, slot).start()

        @pl.when(own == 1)
        def _():
            to_core(i, slot).wait_recv()
            for side, part in ((0, value_part), (1, key_part)):
                for k in range(4):
                    at = lax.rem(k + 4 - z, 4)
                    total = gathered[i, side, at].astype(F32) + part[k * rows : (k + 1) * rows]
                    gathered[i, side, at] = total.astype(BF)

        for turn, q in ((2, 1), (3, 0)):

            @pl.when(s == turn)
            def _(q=q):
                to_first(q, 0).start()
                to_first(q, 1).start()

        return carry

    lax.fori_loop(0, 8, column, 0)
    to_core(1, 0).wait_send()
    to_core(0, 1).wait_send()

    def to_second(u):
        return remote(
            piece(gathered, u, 1), piece(from_second, u), second_send.at[u], second_recv.at[u], links.second
        )

    def to_z(u, o):
        at = slice((u % 2) * half, (u % 2 + 1) * half)
        return remote(
            feed_part.at[u // 2, o, at], feed_z.at[u // 2, o - 1, at], feed_send.at[u, o - 1], feed_recv.at[u, o - 1],
            links.along_z[o - 1],
        )

    def pass_first(u):
        to_first(1, u).start()
        to_first(0, u).start()

    def pass_second(u):
        to_first(1, u).wait_recv()
        add_blocks(piece(gathered, u, 1), [piece(gathered, u, 1), piece(from_first, u, 1)])
        to_second(u).start()

    def pass_z(u):
        to_first(0, u).wait_recv()
        to_second(u).wait_recv()
        add_blocks(piece(feed_part, u), [piece(gathered, u, 0), piece(from_first, u, 0), piece(from_second, u)])
        for o in (1, 2, 3):
            to_z(u, o).start()

    def finish(u):
        for o in (1, 2, 3):
            to_z(u, o).wait_recv()
        for r in range((u % 2) * half, (u % 2 + 1) * half, 32):
            at = slice(r, r + 32)
            value = feed_part[u // 2, 0, at].astype(F32)
            for o in range(3):
                value = value + feed_z[u // 2, o, at].astype(F32)
            own_units[u // 2, at] = value.astype(BF)

    row = lax.broadcasted_iota(jnp.int32, (length, 128), 0)
    loads[0].wait()
    dot_rows(grad_rin, grad_gate, feedr)

    def shift_two(m, rows_at, at, keeping):
        return keeping * (
            grad_in[rows_at, at] * (1.0 - vectors[BLEND_KEY : BLEND_KEY + 1, at])
            + grad_rin[rows_at, at] * (1.0 - vectors[BLEND_RECEPT : BLEND_RECEPT + 1, at])
        )

    for m in range(micro):
        start = m * length
        halo_out[m : m + 1] = shift_two(m, slice(start, start + 1), slice(None), keep[m, 0:1, 0:1])
    halo = remote(halo_out, halo_in, halo_send.at[0], halo_recv.at[0], links.row(size - 1))
    halo.start()
    pass_second(0)
    pass_first(2)
    pass_second(1)
    loads[1].wait()
    halo.wait_recv()
    for m in range(micro):
        rows_at = slice(m * length, (m + 1) * length)

        def shift_pass(j, carry, m=m, rows_at=rows_at):
            at = lanes(j)
            after = jnp.where(t < size - 1, halo_in[m : m + 1, at], 0.0)
            shift = shift_two(m, rows_at, at, keep[m])
            from_in, from_rin, apart = grad_in[rows_at, at], grad_rin[rows_at, at], spread_in[rows_at, at]
            grad_z[rows_at, at] = (
                from_in * vectors[BLEND_KEY : BLEND_KEY + 1, at]
                + from_rin * vectors[BLEND_RECEPT : BLEND_RECEPT + 1, at]
                + roll_rows(shift, -1, after, row)
            )
            sums[BLEND_KEY : BLEND_KEY + 1, at] += jnp.sum(from_in * apart, axis=0, keepdims=True)
            sums[BLEND_RECEPT : BLEND_RECEPT + 1, at] += jnp.sum(from_rin * apart, axis=0, keepdims=True)
            return carry

        lax.fori_loop(0, width // 128, shift_pass, 0)
    loads[2].wait()
    norm_back_tiles(
        grad_residual, grad_z, unit_in, inverse, vectors[GAIN_TWO : GAIN_TWO + 1, :], cotangent, sums, GAIN_TWO
    )
    grad_att[...] = grad_residual[...].astype(BF)

    loads[3].wait()
    dot_rows(grad_w, grad_att, output)
    for load in loads[4:]:
        load.wait()
    pass_z(0)

    def quotient_grads(rows_at, at):
        gate = recept_in[rows_at, at]
        blended = mixed_in[rows_at, at]
        inner = grad_w[rows_at, at] * gate
        above = inner / denom_in[rows_at, at]
        return above, -above * blended, inner * blended * (1.0 - gate)

    for m in range(micro):
        rows_at = slice(m * length, (m + 1) * length)

        def first_pass(j, carry, m=m, rows_at=rows_at):
            at = lanes(j)
            above, below, rec = quotient_grads(rows_at, at)
            grad_recept[rows_at, at] = rec.astype(BF)
            factor = keep[m] * vectors[DECAY : DECAY + 1, at]
            f, a, b = doubling(factor, keep[m] * above, keep[m] * below, row, -1)
            cum[rows_at, at] = f
            up[rows_at, at] = a
            low[rows_at, at] = b
            summary[3 * m : 3 * m + 1, at] = f[:1]
            summary[3 * m + 1 : 3 * m + 2, at] = a[:1]
            summary[3 * m + 2 : 3 * m + 3, at] = b[:1]
            return carry

        lax.fori_loop(0, width // 128, first_pass, 0)
    copies = row_copies(summary, arrived, scan_send, scan_recv, t, links.dp, size)
    for copy in copies:
        copy.start()
    pass_first(3)
    pass_second(2)
    pass_z(1)
    for copy in copies:
        copy.wait_recv()
    for m in range(micro):
        a = jnp.zeros((1, width), F32)
        b = jnp.zeros((1, width), F32)
        for ahead in range(size - 1, 0, -1):
            o = size - ahead
            f = arrived[o, 3 * m : 3 * m + 1]
            a = jnp.where(t + ahead < size, f * a + arrived[o, 3 * m + 1 : 3 * m + 2], a)
            b = jnp.where(t + ahead < size, f * b + arrived[o, 3 * m + 2 : 3 * m + 3], b)
        entering_rows[2 * m : 2 * m + 1] = a
        entering_rows[2 * m + 1 : 2 * m + 2] = b
    for m in range(micro):
        rows_at = slice(m * length, (m + 1) * length)

        def second_pass(j, carry, m=m, rows_at=rows_at):
            at = lanes(j)
            enter_a = entering_rows[2 * m : 2 * m + 1, at]
            enter_b = entering_rows[2 * m + 1 : 2 * m + 2, at]
            f = cum[rows_at, at]
            alpha = roll_rows(up[rows_at, at] + f * enter_a, -1, enter_a, row)
            beta = roll_rows(low[rows_at, at] + f * enter_b, -1, enter_b, row)
            above, below, _ = quotient_grads(rows_at, at)
            key, value = keys_in[rows_at, at], values_in[rows_at, at]
            power = jnp.exp(key)
            bonus = jnp.exp(vectors[PREMIUM : PREMIUM + 1, at] + key)
            premium = bonus * (value * above + below)
            grad_values[rows_at, at] = (bonus * above + power * alpha).astype(BF)
            grad_keys[rows_at, at] = (premium + power * (value * alpha + beta)).astype(BF)
            fading = keep[m] * (alpha * prior_a_in[rows_at, at] + beta * prior_b_in[rows_at, at])
            sums[PREMIUM : PREMIUM + 1, at] += jnp.sum(premium, axis=0, keepdims=True)
            sums[DECAY : DECAY + 1, at] += jnp.sum(fading, axis=0, keepdims=True)
            return carry

        lax.fori_loop(0, width // 128, second_pass, 0)
        if m == 0:
            pass_second(3)

    pass_z(2)
    finish(0)
    finish(1)
    pass_z(3)
    finish(2)
    finish(3)
    for u in range(4):
        to_first(0, u).wait_send()
        to_first(1, u).wait_send()
        to_second(u).wait_send()
        for o in (1, 2, 3):
            to_z(u, o).wait_send()
    halo.wait_send()
    for copy in copies:
        copy.wait_send()


def channel_backward(near, far, size):
    feed_in = near[0]
    weights = far[0]
    tokens, width = feed_in.shape
    micro, length = near[4].shape[:2]
    rows = weights.shape[4]
    flat_f32 = (tokens, width)
    dma = pltpu.SemaphoreType.DMA
    big = pltpu.VMEM(flat_f32, F32)
    return pl.pallas_call(
        channel_backward_kernel,
        out_shape=[
            jax.ShapeDtypeStruct((2, rows, width), BF), jax.ShapeDtypeStruct((5, tokens, width), BF),
            jax.ShapeDtypeStruct(flat_f32, F32), jax.ShapeDtypeStruct((16, width), F32),
        ],
        in_specs=[whole()] * len(near) + [anywhere()] * len(far),
        out_specs=[whole()] * 4,
        scratch_shapes=[
            pltpu.VMEM((2, 4, rows, 2 * width), BF), pltpu.VMEM((2, 4, rows, tokens), F32),
            pltpu.VMEM((width, width), BF), pltpu.VMEM((width, width), BF),
        ]
        + [big] * 9
        + [
            pltpu.VMEM((4 * rows, width), F32), pltpu.VMEM((4 * rows, width), F32),
            pltpu.VMEM((2, 2, 4, rows, width), BF), pltpu.VMEM((4, 2, 4, rows, width), BF),
            pltpu.VMEM((2, 2, 4, rows, width), BF), pltpu.VMEM((2, 4, rows, width), BF),
            pltpu.VMEM((2, 4, rows, width), BF), pltpu.VMEM((2, 3, rows, width), BF),
        ]
        + [big] * 7
        + [
            pltpu.VMEM((8, width), F32), pltpu.VMEM((size, 8, width), F32), pltpu.VMEM((8, width), F32),
            pltpu.VMEM((8, width), F32), pltpu.VMEM((8, width), F32),
            dma((2, 2)), dma((11,)), dma((4,)), dma((4,)), dma((2, 4)), dma((2, 4)), dma((4,)), dma((4,)),
            dma((4, 3)), dma((4, 3)),
            dma((size,)), dma((size,)), dma((1,)), dma((1,)),
        ],
        compiler_params=pltpu.CompilerParams(
            collective_id=2, has_side_effects=True, vmem_limit_bytes=66_000_000
        ),
        cost_estimate=cost(8 * tokens * 32 * rows * width, 16 * 32 * rows * width),
        name="channel_backward",
    )(*near, *far)


def front_backward_kernel(
    own_units, lefts, rights, vectors, keep, inverse, grad_residual, sums_in, rates,
    w_key, w_value, w_recept, spread, unit,
    square_grads, unit_key, unit_value, token_grads, vector_grads,
    key_in, value_in, recept_in, spread_in, unit_in, outgoing, gathered, from_first, from_second, from_z,
    x_units, core_units, grad_key, grad_value, grad_recept, grad_z, sums, held, halo_out, halo_in,
    load_sem, core_send, core_recv, first_send, first_recv, second_send, second_recv, z_send, z_recv,
    unit_send, unit_recv, halo_send, halo_recv, sum_send, sum_recv,
):
    links = Links(8)
    x, c, z, y, t, size = links.x, links.c, links.z, links.y, links.t, links.size
    count = lefts.shape[0]
    width = lefts.shape[2]
    rows = width // 32
    micro, length = keep.shape[:2]
    late = [(w_key, key_in), (w_value, value_in), (w_recept, recept_in), (spread, spread_in), (unit, unit_in)]
    loads = [pltpu.make_async_copy(source, target, load_sem.at[k]) for k, (source, target) in enumerate(late)]
    for load in loads:
        load.start()
    links.greet(True)
    units_over_x = remote(own_units, x_units, unit_send.at[0], unit_recv.at[0], links.over_x)
    pl.when(c == 0)(units_over_x.start)
    units_over_core = remote(own_units, core_units.at[0], unit_send.at[1], unit_recv.at[1], links.core)
    units_over_core.start()
    halo_out[...] = jnp.zeros_like(halo_out)
    sums[...] = sums_in[...]

    def part(n, cc, xx):
        at = pl.ds(pl.multiple_of((xx * 2 + cc) * 8 * rows, 8 * rows), 8 * rows)
        return matmul_lead(lefts[n, :, at], rights[n])

    def blocks():
        for zz in range(4):
            for yy in range(2):
                yield zz, yy, slice((zz * 2 + yy) * rows, (zz * 2 + yy + 1) * rows)

    def to_core(n):
        return remote(outgoing.at[n], gathered.at[n], core_send.at[n], core_recv.at[n], links.core)

    def to_first(n):
        return remote(
            gathered.at[n, pl.ds(2, 2)], from_first.at[n], first_send.at[n], first_recv.at[n], links.first
        )

    def to_second(n):
        return remote(gathered.at[n, 1], from_second.at[n], second_send.at[n], second_recv.at[n], links.second)

    def to_z(n, o):
        return remote(
            gathered.at[n, 0, o], from_z.at[n, o - 1], z_send.at[n, o - 1], z_recv.at[n, o - 1], links.along_z[o - 1]
        )

    def other(n, carry):
        for xx in range(2):
            value = part(n, 1 - c, xx)
            for zz, yy, at in blocks():
                outgoing[n, position(xx, yy, x, y, 1 - c), lax.rem(zz + 4 - z, 4)] = value[at].astype(BF)
        to_core(n).start()

    def own(n, carry):
        to_core(n).wait_recv()
        for xx in range(2):
            value = part(n, c, xx)
            for zz, yy, at in blocks():
                i, o = position(xx, yy, x, y, c), lax.rem(zz + 4 - z, 4)
                gathered[n, i, o] = (gathered[n, i, o].astype(F32) + value[at]).astype(BF)
        to_first(n).start()

    def both(n, carry):
        pl.when(n < count)(lambda: other(n, None))
        pl.when(n >= 1)(lambda: own(n - 1, None))
        return carry

    lax.fori_loop(0, count + 1, both, 0)
    pl.when(c == 1)(units_over_x.start)

    def pass_second(n):
        to_first(n).wait_recv()
        add_blocks(gathered.at[n, 1], [gathered.at[n, 1], from_first.at[n, 1]])
        to_second(n).start()

    def pass_z(n):
        to_second(n).wait_recv()
        add_blocks(gathered.at[n, 0], [gathered.at[n, 0], from_first.at[n, 0], from_second.at[n]])
        for o in (1, 2, 3):
            to_z(n, o).start()

    def finish(n):
        value = gathered[n, 0, 0].astype(F32)
        for o in (1, 2, 3):
            to_z(n, o).wait_recv()
            value = value + from_z[n, o - 1].astype(F32)
        square_grads[n] = value

    loads[0].wait()
    dot_rows(grad_key, rights.at[2], key_in)
    pass_second(0)
    loads[1].wait()
    dot_rows(grad_value, rights.at[3], value_in)
    pass_second(1)
    loads[2].wait()
    dot_rows(grad_recept, rights.at[4], recept_in)
    both_over_core = remote(x_units, core_units.at[1], unit_send.at[2], unit_recv.at[2], links.core)
    grads = ((grad_key, MIX_KEY), (grad_value, MIX_VALUE), (grad_recept, MIX_RECEPT))

    def shift_one(rows_at, at, keeping):
        return keeping * sum(g[rows_at, at] * (1.0 - vectors[k : k + 1, at]) for g, k in grads)

    for m in range(micro):
        start = m * length
        halo_out[m : m + 1] = shift_one(slice(start, start + 1), slice(None), keep[m, 0:1, 0:1])
    halo = remote(halo_out, halo_in, halo_send.at[0], halo_recv.at[0], links.row(size - 1))
    halo.start()
    pass_second(2)
    pass_z(0)
    pass_second(3)
    pass_z(1)
    pass_second(4)
    loads[3].wait()
    halo.wait_recv()
    row = lax.broadcasted_iota(jnp.int32, (length, 128), 0)
    for m in range(micro):
        rows_at = slice(m * length, (m + 1) * length)

        def shift_pass(j, carry, m=m, rows_at=rows_at):
            at = lanes(j)
            after = jnp.where(t < size - 1, halo_in[m : m + 1, at], 0.0)
            apart = spread_in[rows_at, at]
            value = roll_rows(shift_one(rows_at, at, keep[m]), -1, after, row)
            for g, k in grads:
                value = value + g[rows_at, at] * vectors[k : k + 1, at]
                sums[k : k + 1, at] += jnp.sum(g[rows_at, at] * apart, axis=0, keepdims=True)
            grad_z[rows_at, at] = value
            return carry

        lax.fori_loop(0, width // 128, shift_pass, 0)
    pass_z(2)
    loads[4].wait()
    norm_back_tiles(
        token_grads, grad_z, unit_in, inverse, vectors[GAIN_ONE : GAIN_ONE + 1, :], grad_residual, sums, GAIN_ONE
    )
    sums[DECAY : DECAY + 1, :] = -sums[DECAY : DECAY + 1, :] * rates[0:1, :] * vectors[DECAY : DECAY + 1, :]

    stages = [[links.core], [links.over_x], [links.over_y], links.along_z]
    pending = []
    source, slot = sums, 0

    def begin(stage, source, slot):
        copies = [
            remote(source, held.at[slot + k], sum_send.at[slot + k], sum_recv.at[slot + k], peer)
            for k, peer in enumerate(stage)
        ]
        for copy in copies:
            copy.start()
        return copies

    def collect(copies, source, slot, target):
        value = source[...]
        for k, copy in enumerate(copies):
            copy.wait_recv()
            value = value + held[slot + k]
        target[...] = value

    copies = begin(stages[0], sums, 0)
    pending += copies
    pass_z(3)
    finish(0)
    collect(copies, sums, 0, held.at[6])
    copies = begin(stages[1], held.at[6], 1)
    pending += copies
    pass_z(4)
    finish(1)
    collect(copies, held.at[6], 1, held.at[7])
    copies = begin(stages[2], held.at[7], 2)
    pending += copies
    units_over_x.wait_recv()
    both_over_core.start()
    finish(2)
    collect(copies, held.at[7], 2, held.at[8])
    copies = begin(stages[3], held.at[8], 3)
    pending += copies
    units_over_core.wait_recv()
    both_over_core.wait_recv()
    for side, target in ((1, unit_key), (0, unit_value)):
        for d in range(4):
            for r in range(0, own_units.shape[1], 32):
                at = slice(r, r + 32)
                pick = jnp.where(links.dp == d ^ 1, core_units[0, side, at], core_units[1, side, at])
                pick = jnp.where(links.dp == d ^ 2, x_units[side, at], pick)
                pick = jnp.where(links.dp == d, own_units[side, at], pick)
                target[d, at] = pick.astype(F32)
    finish(3)
    collect(copies, held.at[8], 3, vector_grads)
    finish(4)
    for n in range(count):
        to_core(n).wait_send()
        to_first(n).wait_send()
        to_second(n).wait_send()
        for o in (1, 2, 3):
            to_z(n, o).wait_send()
    for copy in pending + [units_over_x, units_over_core, both_over_core, halo]:
        copy.wait_send()


def front_backward(near, far):
    own_units, lefts = near[:2]
    rows = own_units.shape[1]
    count, tokens, width = lefts.shape
    own = width // 32
    dma = pltpu.SemaphoreType.DMA
    big = pltpu.VMEM((tokens, width), F32)
    square = pltpu.VMEM((width, width), BF)
    return pl.pallas_call(
        front_backward_kernel,
        out_shape=[
            jax.ShapeDtypeStruct((count, own, width), F32),
            jax.ShapeDtypeStruct((4, rows, width), F32), jax.ShapeDtypeStruct((4, rows, width), F32),
            jax.ShapeDtypeStruct((tokens, width), F32), jax.ShapeDtypeStruct((16, width), F32),
        ],
        in_specs=[whole()] * len(near) + [anywhere()] * len(far),
        out_specs=[whole()] * 5,
        scratch_shapes=[square] * 3
        + [big] * 2
        + [
            pltpu.VMEM((count, 4, 4, own, width), BF), pltpu.VMEM((count, 4, 4, own, width), BF),
            pltpu.VMEM((count, 2, 4, own, width), BF), pltpu.VMEM((count, 4, own, width), BF),
            pltpu.VMEM((count, 3, own, width), BF), pltpu.VMEM((2, rows, width), BF), pltpu.VMEM((2, 2, rows, width), BF),
        ]
        + [big] * 4
        + [
            pltpu.VMEM((16, width), F32), pltpu.VMEM((9, 16, width), F32), pltpu.VMEM((8, width), F32),
            pltpu.VMEM((8, width), F32),
            dma((5,)), dma((count,)), dma((count,)), dma((count,)), dma((count,)), dma((count,)), dma((count,)),
            dma((count, 3)), dma((count, 3)), dma((3,)), dma((3,)), dma((1,)), dma((1,)),
            dma((6,)), dma((6,)),
        ],
        compiler_params=pltpu.CompilerParams(
            collective_id=3, has_side_effects=True, vmem_limit_bytes=66_000_000
        ),
        cost_estimate=cost(4 * count * tokens * width * width, 40 * width * width),
        name="front_backward",
    )(*near, *far)


def local_shards(tokens, resets, out_grads, *weights):
    (
        mixer_key, mixer_value, mixer_recept, mixer_output, feed_recept, feed_key, feed_value, *vector_shards
    ) = weights
    size = lax.axis_size("tensor")
    dp, t = lax.axis_index("dp"), lax.axis_index("tensor")
    micro, _, length, width = tokens.shape
    count = micro * length
    unit_rows = feed_key.shape[0] // 4
    feed_shard = jnp.concatenate(
        [lax.dynamic_slice_in_dim(w, dp * unit_rows, unit_rows, 0) for w in (feed_key, feed_value)], axis=1
    )
    share = vector_shards[0].shape[0]
    vector_pack = jnp.pad(jnp.stack(vector_shards), ((0, 16 - len(vector_shards)), (0, 128 - share)))
    keep = (1 - resets[:, 0]).astype(F32)[:, :, None]
    keep_lanes = jnp.broadcast_to(keep, (micro, length, 128))
    cotangent = out_grads.reshape(count, width)
    near = [tokens.reshape(count, width), cotangent, keep_lanes]
    parts = [vector_pack, mixer_key, mixer_value, mixer_recept, mixer_output, feed_recept, feed_shard]
    (
        _, all_key, all_value, all_recept, all_output, all_feedr, feed,
        result, table, rates, lefts, feed_in, grad_value, grad_gate, positive, spread_one, unit_one, inverse_one,
        spread_two, unit_two, inverse_two, keys, values, denom, mixed, prior_a, prior_b, recept,
    ) = forward(near, parts, size)
    w_key, w_value, w_recept, w_output, w_feedr = [
        w.reshape(width, width) for w in (all_key, all_value, all_recept, all_output, all_feedr)
    ]
    near = [feed_in, grad_value, grad_gate, table, keep_lanes, inverse_two, cotangent]
    far = [feed, positive, w_feedr, w_output, spread_two, unit_two, keys, values, denom, mixed, prior_a, prior_b, recept]
    own_units, rights, grad_residual, sums = channel_backward(near, far, size)
    near = [own_units, lefts, rights, table, keep_lanes, inverse_one, grad_residual, sums, rates]
    far = [w_key, w_value, w_recept, spread_one, unit_one]
    square_grads, unit_key, unit_value, token_grads, vector_grads = front_backward(near, far)
    mine = lax.dynamic_slice_in_dim(vector_grads, (dp * size + t) * share, share, 1)
    return (
        result.reshape(tokens.shape), token_grads.reshape(tokens.shape),
        square_grads[2], square_grads[3], square_grads[4], square_grads[1], square_grads[0],
        unit_key.reshape(feed_key.shape), unit_value.reshape(feed_value.shape),
    ) + tuple(mine[i] for i in range(len(vector_shards)))


def is_two_by_two_by_four(mesh):
    return mesh.shape["dp"] == 4 and mesh.shape["tensor"] == 8


def solution(mesh):
    return jax.shard_map(
        local_shards if is_two_by_two_by_four(mesh) else shards,
        mesh=mesh,
        in_specs=(
            P(None, "dp", "tensor", None),
            P(None, "dp", "tensor"),
            P(None, "dp", "tensor", None),
            P(("dp", "tensor"), None),
            P(("dp", "tensor"), None),
            P(("dp", "tensor"), None),
            P(("dp", "tensor"), None),
            P(("dp", "tensor"), None),
            P("tensor", None),
            P("tensor", None),
            P(("dp", "tensor")),
            P(("dp", "tensor")),
            P(("dp", "tensor")),
            P(("dp", "tensor")),
            P(("dp", "tensor")),
            P(("dp", "tensor")),
            P(("dp", "tensor")),
            P(("dp", "tensor")),
            P(("dp", "tensor")),
            P(("dp", "tensor")),
            P(("dp", "tensor")),
        ),
        out_specs=(
            P(None, "dp", "tensor", None),
            P(None, "dp", "tensor", None),
            P(("dp", "tensor"), None),
            P(("dp", "tensor"), None),
            P(("dp", "tensor"), None),
            P(("dp", "tensor"), None),
            P(("dp", "tensor"), None),
            P("tensor", None),
            P("tensor", None),
            P(("dp", "tensor")),
            P(("dp", "tensor")),
            P(("dp", "tensor")),
            P(("dp", "tensor")),
            P(("dp", "tensor")),
            P(("dp", "tensor")),
            P(("dp", "tensor")),
            P(("dp", "tensor")),
            P(("dp", "tensor")),
            P(("dp", "tensor")),
            P(("dp", "tensor")),
        ),
        check_vma=False,
    )
```

```python
import functools

import jax
import jax.numpy as jnp
from jax import lax
from jax.experimental import pallas as pl
from jax.experimental.pallas import tpu as pltpu
from jax.sharding import PartitionSpec as P

EPSILON = 1e-05


def entering(shard, axis, combine, identity, reverse):
    size, here = (lax.axis_size(axis), lax.axis_index(axis))
    everything = jax.tree.map(lambda part: lax.all_gather(part, axis), shard)
    start = jax.tree.map(
        lambda part, zero: jnp.broadcast_to(jnp.asarray(zero, part.dtype), part.shape),
        shard,
        identity,
    )

    def turn(k, before):
        at = size - 1 - k if reverse else k
        reached = at > here if reverse else at < here
        new = combine(before, jax.tree.map(lambda part: part[at], everything))
        return jax.tree.map(lambda a, b: jnp.where(reached, a, b), new, before)

    return lax.fori_loop(0, size, turn, start)


def shifted(block, axis, distance):
    devices = range(lax.axis_size(axis))
    route = [(i - distance, i) for i in devices if i - distance in devices]
    return lax.ppermute(block, axis, route)


def norm_rows(payload_series, gain, bias):
    center = payload_series - jnp.mean(payload_series, axis=-1, keepdims=True)
    inverse = lax.rsqrt(jnp.mean(center * center, axis=-1, keepdims=True) + EPSILON)
    normed = center * inverse
    return (normed * gain + bias, normed, inverse)


def norm_back(grad_out, normed, inverse, gain):
    scaled = grad_out * gain
    centred = scaled - jnp.mean(scaled, axis=-1, keepdims=True)
    grad_in = inverse * (centred - normed * jnp.mean(scaled * normed, axis=-1, keepdims=True))
    return (grad_in, jnp.sum(grad_out * normed, axis=0), jnp.sum(grad_out, axis=0))


def affine(earlier, later):
    return (
        earlier[0] * later[0],
        later[0] * earlier[1] + later[1],
        later[0] * earlier[2] + later[2],
    )


def carry_across(summary, backward):
    width = summary[0].shape[0]
    identity = (
        jnp.ones((width,), jnp.float32),
        jnp.zeros((width,), jnp.float32),
        jnp.zeros((width,), jnp.float32),
    )
    return entering(summary, "tensor", affine, identity, backward)


def matmul(left, right):
    return jnp.dot(left, right, preferred_element_type=jnp.float32)


def matmul_lead(left, right):
    return lax.dot_general(
        left, right, (((0,), (0,)), ((), ())), preferred_element_type=jnp.float32
    )


def matmul_last(left, right):
    return lax.dot_general(
        left, right, (((1,), (1,)), ((), ())), preferred_element_type=jnp.float32
    )


def shards(
    tokens,
    resets,
    out_grads,
    mixer_key,
    mixer_value,
    mixer_recept,
    mixer_output,
    feed_recept,
    feed_key,
    feed_value,
    first_gain,
    first_bias,
    second_gain,
    second_bias,
    mixing_key,
    mixing_value,
    mixing_recept,
    time_decay,
    time_first,
    feeding_key,
    feeding_recept,
):
    gathered = (
        lax.all_gather(mixer_key, ("dp", "tensor"), axis=0, tiled=True),
        lax.all_gather(mixer_value, ("dp", "tensor"), axis=0, tiled=True),
        lax.all_gather(mixer_recept, ("dp", "tensor"), axis=0, tiled=True),
        lax.all_gather(mixer_output, ("dp", "tensor"), axis=0, tiled=True),
        lax.all_gather(feed_recept, ("dp", "tensor"), axis=0, tiled=True),
        lax.all_gather(first_gain, ("dp", "tensor"), axis=0, tiled=True),
        lax.all_gather(first_bias, ("dp", "tensor"), axis=0, tiled=True),
        lax.all_gather(second_gain, ("dp", "tensor"), axis=0, tiled=True),
        lax.all_gather(second_bias, ("dp", "tensor"), axis=0, tiled=True),
        lax.all_gather(mixing_key, ("dp", "tensor"), axis=0, tiled=True),
        lax.all_gather(mixing_value, ("dp", "tensor"), axis=0, tiled=True),
        lax.all_gather(mixing_recept, ("dp", "tensor"), axis=0, tiled=True),
        lax.all_gather(time_decay, ("dp", "tensor"), axis=0, tiled=True),
        lax.all_gather(time_first, ("dp", "tensor"), axis=0, tiled=True),
        lax.all_gather(feeding_key, ("dp", "tensor"), axis=0, tiled=True),
        lax.all_gather(feeding_recept, ("dp", "tensor"), axis=0, tiled=True),
    )
    w_key, w_value, w_recept, w_output, w_feedr = (
        gathered[0],
        gathered[1],
        gathered[2],
        gathered[3],
        gathered[4],
    )
    parameter_vectors = [piece.astype(jnp.float32) for piece in gathered[5:]]
    gain_one, bias_one, gain_two, bias_two = (
        parameter_vectors[0],
        parameter_vectors[1],
        parameter_vectors[2],
        parameter_vectors[3],
    )
    mix_key, mix_value, mix_recept = (
        parameter_vectors[4],
        parameter_vectors[5],
        parameter_vectors[6],
    )
    (
        fading_speed_logarithm,
        opening_premium_logarithm,
        channel_lookup_blend,
        channel_gating_blend,
    ) = (parameter_vectors[7], parameter_vectors[8], parameter_vectors[9], parameter_vectors[10])
    rates = jnp.exp(fading_speed_logarithm)
    fading_multiplier = jnp.exp(-rates)
    micro_count = tokens.shape[0]
    width = tokens.shape[3]
    grad_keyw = jnp.zeros(feed_key.shape, jnp.float32)
    grad_valuew = jnp.zeros(feed_value.shape, jnp.float32)
    square_grads = [jnp.zeros((width, width), jnp.float32) for index_one in range(5)]
    parameter_vector_gradients = [jnp.zeros((width,), jnp.float32) for index_two in range(11)]
    results = []
    input_grads = []
    for micro_index in range(micro_count):
        inputs = tokens[micro_index, 0].astype(jnp.float32)
        restart_retain_flags = (1 - resets[micro_index, 0]).astype(jnp.float32)[:, None]
        cotangent = out_grads[micro_index, 0].astype(jnp.float32)
        normed_one, unit_one, inverse_one = norm_rows(inputs, gain_one, bias_one)
        z_one = normed_one.astype(jnp.bfloat16)
        prior_one = shifted(z_one[-1:], "tensor", 1)
        before_one = (
            jnp.concatenate([prior_one, z_one[:-1]], axis=0).astype(jnp.float32)
            * restart_retain_flags
        )
        z_onef = z_one.astype(jnp.float32)
        in_key = (z_onef * mix_key + before_one * (1.0 - mix_key)).astype(jnp.bfloat16)
        in_value = (z_onef * mix_value + before_one * (1.0 - mix_value)).astype(jnp.bfloat16)
        in_recept = (z_onef * mix_recept + before_one * (1.0 - mix_recept)).astype(jnp.bfloat16)
        lookup_series = matmul(in_key, w_key)
        payload_series = matmul(in_value, w_value)
        recept = jax.nn.sigmoid(matmul(in_recept, w_recept))
        powered_lookup = jnp.exp(lookup_series)
        premium_plus_lookup = jnp.exp(opening_premium_logarithm + lookup_series)
        factor = restart_retain_flags * fading_multiplier
        cum_factor, local_a, local_b = lax.associative_scan(
            affine, (factor, powered_lookup * payload_series, powered_lookup), axis=0
        )
        incoming = carry_across((cum_factor[-1], local_a[-1], local_b[-1]), False)
        upper_running_state = local_a + cum_factor * incoming[1]
        lower_running_state = local_b + cum_factor * incoming[2]
        earlier_upper_state = jnp.concatenate([incoming[1][None], upper_running_state[:-1]], axis=0)
        earlier_lower_state = jnp.concatenate([incoming[2][None], lower_running_state[:-1]], axis=0)
        lower_quotient_part = restart_retain_flags * earlier_lower_state + premium_plus_lookup
        blended = (
            restart_retain_flags * earlier_upper_state + premium_plus_lookup * payload_series
        ) / lower_quotient_part
        weighted = (recept * blended).astype(jnp.bfloat16)
        residual = inputs + matmul(weighted, w_output)
        normed_two, unit_two, inverse_two = norm_rows(residual, gain_two, bias_two)
        z_two = normed_two.astype(jnp.bfloat16)
        prior_two = shifted(z_two[-1:], "tensor", 1)
        before_two = (
            jnp.concatenate([prior_two, z_two[:-1]], axis=0).astype(jnp.float32)
            * restart_retain_flags
        )
        z_twof = z_two.astype(jnp.float32)
        feed_in = (
            z_twof * channel_lookup_blend + before_two * (1.0 - channel_lookup_blend)
        ).astype(jnp.bfloat16)
        feed_rin = (
            z_twof * channel_gating_blend + before_two * (1.0 - channel_gating_blend)
        ).astype(jnp.bfloat16)
        gate = jax.nn.sigmoid(matmul(feed_rin, w_feedr))
        all_in = lax.all_gather(feed_in, "tensor", axis=0, tiled=True)
        hidden_pre = matmul_last(feed_key, all_in)
        hidden = jnp.square(jnp.maximum(hidden_pre, 0.0)).astype(jnp.bfloat16)
        value_out = lax.psum_scatter(
            matmul_lead(hidden, feed_value), "tensor", scatter_dimension=0, tiled=True
        )
        results.append(residual + gate * value_out)
        grad_value = (cotangent * gate).astype(jnp.bfloat16)
        grad_gate = (cotangent * value_out * gate * (1.0 - gate)).astype(jnp.bfloat16)
        square_grads[4] = square_grads[4] + matmul_lead(feed_rin, grad_gate)
        grad_rin = matmul_last(grad_gate, w_feedr)
        relu_twice = 2.0 * jnp.maximum(hidden_pre, 0.0)
        add_piece = lax.all_gather(grad_value, "tensor", axis=0, tiled=True)
        rows_total = matmul(hidden, add_piece)
        block = matmul_last(feed_value, add_piece)
        grad_valuew = grad_valuew + rows_total
        grad_pre = (block * relu_twice).astype(jnp.bfloat16)
        grad_keyw = grad_keyw + matmul(grad_pre, all_in)
        grad_in = lax.psum_scatter(
            matmul_lead(grad_pre, feed_key), "tensor", scatter_dimension=0, tiled=True
        )
        parameter_vector_gradients[9] = parameter_vector_gradients[9] + jnp.sum(
            grad_in * (z_twof - before_two), axis=0
        )
        parameter_vector_gradients[10] = parameter_vector_gradients[10] + jnp.sum(
            grad_rin * (z_twof - before_two), axis=0
        )
        shift_two = restart_retain_flags * (
            grad_in * (1.0 - channel_lookup_blend) + grad_rin * (1.0 - channel_gating_blend)
        )
        after_two = shifted(shift_two[:1], "tensor", -1)
        grad_z_two = (
            grad_in * channel_lookup_blend
            + grad_rin * channel_gating_blend
            + jnp.concatenate([shift_two[1:], after_two], axis=0)
        )
        back_two, gain_part, bias_part = norm_back(grad_z_two, unit_two, inverse_two, gain_two)
        parameter_vector_gradients[2] = parameter_vector_gradients[2] + gain_part
        parameter_vector_gradients[3] = parameter_vector_gradients[3] + bias_part
        grad_residual = cotangent + back_two
        grad_att = grad_residual.astype(jnp.bfloat16)
        square_grads[3] = square_grads[3] + matmul_lead(weighted, grad_att)
        grad_weighted = matmul_last(grad_att, w_output)
        grad_mixed = grad_weighted * recept
        grad_recept = (grad_weighted * blended * recept * (1.0 - recept)).astype(jnp.bfloat16)
        upper_adjoint = grad_mixed / lower_quotient_part
        denominator_gradient = -grad_mixed * blended / lower_quotient_part
        cum_back, local_xa, local_xb = lax.associative_scan(
            affine,
            (
                factor,
                restart_retain_flags * upper_adjoint,
                restart_retain_flags * denominator_gradient,
            ),
            reverse=True,
            axis=0,
        )
        beyond = carry_across((cum_back[0], local_xa[0], local_xb[0]), True)
        adjoint_a = local_xa + cum_back * beyond[1]
        adjoint_b = local_xb + cum_back * beyond[2]
        running_upper_total = jnp.concatenate([adjoint_a[1:], beyond[1][None]], axis=0)
        running_lower_total = jnp.concatenate([adjoint_b[1:], beyond[2][None]], axis=0)
        premium_power = premium_plus_lookup * (
            payload_series * upper_adjoint + denominator_gradient
        )
        adjoint_payloads = (
            premium_plus_lookup * upper_adjoint + powered_lookup * running_upper_total
        ).astype(jnp.bfloat16)
        key_gradient_rows = (
            premium_power
            + powered_lookup * (payload_series * running_upper_total + running_lower_total)
        ).astype(jnp.bfloat16)
        parameter_vector_gradients[8] = parameter_vector_gradients[8] + jnp.sum(
            premium_power, axis=0
        )
        decay_sum = jnp.sum(
            restart_retain_flags
            * (
                running_upper_total * earlier_upper_state
                + running_lower_total * earlier_lower_state
            ),
            axis=0,
        )
        parameter_vector_gradients[7] = (
            parameter_vector_gradients[7] - rates * fading_multiplier * decay_sum
        )
        square_grads[0] = square_grads[0] + matmul_lead(in_key, key_gradient_rows)
        square_grads[1] = square_grads[1] + matmul_lead(in_value, adjoint_payloads)
        square_grads[2] = square_grads[2] + matmul_lead(in_recept, grad_recept)
        grad_inkey = matmul_last(key_gradient_rows, w_key)
        grad_invalue = matmul_last(adjoint_payloads, w_value)
        grad_inrecept = matmul_last(grad_recept, w_recept)
        spread_one = z_onef - before_one
        parameter_vector_gradients[4] = parameter_vector_gradients[4] + jnp.sum(
            grad_inkey * spread_one, axis=0
        )
        parameter_vector_gradients[5] = parameter_vector_gradients[5] + jnp.sum(
            grad_invalue * spread_one, axis=0
        )
        parameter_vector_gradients[6] = parameter_vector_gradients[6] + jnp.sum(
            grad_inrecept * spread_one, axis=0
        )
        shift_one = restart_retain_flags * (
            grad_inkey * (1.0 - mix_key)
            + grad_invalue * (1.0 - mix_value)
            + grad_inrecept * (1.0 - mix_recept)
        )
        after_one = shifted(shift_one[:1], "tensor", -1)
        grad_z_one = (
            grad_inkey * mix_key
            + grad_invalue * mix_value
            + grad_inrecept * mix_recept
            + jnp.concatenate([shift_one[1:], after_one], axis=0)
        )
        back_one, gain_first, bias_first = norm_back(grad_z_one, unit_one, inverse_one, gain_one)
        parameter_vector_gradients[0] = parameter_vector_gradients[0] + gain_first
        parameter_vector_gradients[1] = parameter_vector_gradients[1] + bias_first
        input_grads.append(grad_residual + back_one)
    owned = (
        lax.psum_scatter(square_grads[0], ("dp", "tensor"), scatter_dimension=0, tiled=True),
        lax.psum_scatter(square_grads[1], ("dp", "tensor"), scatter_dimension=0, tiled=True),
        lax.psum_scatter(square_grads[2], ("dp", "tensor"), scatter_dimension=0, tiled=True),
        lax.psum_scatter(square_grads[3], ("dp", "tensor"), scatter_dimension=0, tiled=True),
        lax.psum_scatter(square_grads[4], ("dp", "tensor"), scatter_dimension=0, tiled=True),
        lax.psum_scatter(
            parameter_vector_gradients[0], ("dp", "tensor"), scatter_dimension=0, tiled=True
        ),
        lax.psum_scatter(
            parameter_vector_gradients[1], ("dp", "tensor"), scatter_dimension=0, tiled=True
        ),
        lax.psum_scatter(
            parameter_vector_gradients[2], ("dp", "tensor"), scatter_dimension=0, tiled=True
        ),
        lax.psum_scatter(
            parameter_vector_gradients[3], ("dp", "tensor"), scatter_dimension=0, tiled=True
        ),
        lax.psum_scatter(
            parameter_vector_gradients[4], ("dp", "tensor"), scatter_dimension=0, tiled=True
        ),
        lax.psum_scatter(
            parameter_vector_gradients[5], ("dp", "tensor"), scatter_dimension=0, tiled=True
        ),
        lax.psum_scatter(
            parameter_vector_gradients[6], ("dp", "tensor"), scatter_dimension=0, tiled=True
        ),
        lax.psum_scatter(
            parameter_vector_gradients[7], ("dp", "tensor"), scatter_dimension=0, tiled=True
        ),
        lax.psum_scatter(
            parameter_vector_gradients[8], ("dp", "tensor"), scatter_dimension=0, tiled=True
        ),
        lax.psum_scatter(
            parameter_vector_gradients[9], ("dp", "tensor"), scatter_dimension=0, tiled=True
        ),
        lax.psum_scatter(
            parameter_vector_gradients[10], ("dp", "tensor"), scatter_dimension=0, tiled=True
        ),
    )
    key_rows, value_rows_grad = (grad_keyw, grad_valuew)
    key_total, value_total = (
        lax.psum(key_rows.astype(jnp.bfloat16), "dp").astype(jnp.float32),
        lax.psum(value_rows_grad.astype(jnp.bfloat16), "dp").astype(jnp.float32),
    )
    result_all = jnp.stack(results)[:, None]
    grads_all = jnp.stack(input_grads)[:, None]
    return (
        result_all,
        grads_all,
        owned[0],
        owned[1],
        owned[2],
        owned[3],
        owned[4],
        key_total,
        value_total,
        owned[5],
        owned[6],
        owned[7],
        owned[8],
        owned[9],
        owned[10],
        owned[11],
        owned[12],
        owned[13],
        owned[14],
        owned[15],
    )


BF = jnp.bfloat16
F32 = jnp.float32
BOTH = ("dp", "tensor")
MESH_ID = pl.DeviceIdType.MESH


def cost(flops, moved):
    return pl.CostEstimate(flops=flops, bytes_accessed=moved, transcendentals=0)


def whole():
    return pl.BlockSpec(memory_space=pltpu.VMEM)


def anywhere():
    return pl.BlockSpec(memory_space=pl.ANY)


def roll_rows(value, distance, fill, row):
    size = value.shape[0]
    moved = pltpu.roll(value, distance % size, 0)
    outside = row < distance if distance > 0 else row >= size + distance
    return jnp.where(outside, fill, moved)


def doubling(factor, up, low, row, sign):
    size, step = factor.shape[0], 1
    while step < size:
        up = up + factor * roll_rows(up, sign * step, 0.0, row)
        low = low + factor * roll_rows(low, sign * step, 0.0, row)
        factor = factor * roll_rows(factor, sign * step, 1.0, row)
        step *= 2
    return factor, up, low


def row_copies(summary, arrived, send, recv, t, dp, size):
    return [
        pltpu.make_async_remote_copy(
            src_ref=summary,
            dst_ref=arrived.at[o],
            send_sem=send.at[o],
            recv_sem=recv.at[o],
            device_id=(dp, lax.rem(t + o, size)),
            device_id_type=MESH_ID,
        )
        for o in range(1, size)
    ]


def lanes(j):
    return pl.ds(pl.multiple_of(j * 128, 128), 128)


def owner(i, x, y, c):
    first, second = i // 2, i % 2
    flip_x = first * c + second * (1 - c)
    flip_y = first * (1 - c) + second * c
    return x + flip_x - 2 * x * flip_x, y + flip_y - 2 * y * flip_y


def position(xx, yy, x, y, c):
    flip_x = x + xx - 2 * x * xx
    flip_y = y + yy - 2 * y * yy
    return 2 * (flip_x * c + flip_y * (1 - c)) + flip_x * (1 - c) + flip_y * c


class Links:
    def __init__(self, size):
        dp, t = lax.axis_index("dp"), lax.axis_index("tensor")
        x, c, z, y = dp // 2, dp % 2, t // 2, t % 2
        self.x, self.c, self.z, self.y, self.dp, self.t, self.size = x, c, z, y, dp, t, size
        over_x, over_y = ((1 - x) * 2 + c, t), (dp, z * 2 + 1 - y)
        self.over_x = over_x
        self.core = (x * 2 + 1 - c, t)
        self.first = (jnp.where(c == 0, over_y[0], over_x[0]), jnp.where(c == 0, over_y[1], over_x[1]))
        self.second = (jnp.where(c == 0, over_x[0], over_y[0]), jnp.where(c == 0, over_x[1], over_y[1]))
        self.along_z = [(dp, lax.rem(z + o, 4) * 2 + y) for o in (1, 2, 3)]
        self.over_y = over_y

    def row(self, o):
        return (self.dp, lax.rem(self.t + o, self.size))

    def greet(self, whole_row):
        peers = [self.row(o) for o in range(1, self.size)] if whole_row else self.along_z + [self.over_y]
        peers = peers + [self.over_x, self.core]
        barrier = pltpu.get_barrier_semaphore()
        for peer in peers:
            pl.semaphore_signal(barrier, inc=1, device_id=peer, device_id_type=MESH_ID)
        pl.semaphore_wait(barrier, len(peers))


def remote(source, target, send, recv, device):
    return pltpu.make_async_remote_copy(
        src_ref=source, dst_ref=target, send_sem=send, recv_sem=recv, device_id=device, device_id_type=MESH_ID
    )


def add_blocks(target, sources):
    count, rows = target.shape[:2]
    tile = min(rows, 32)
    per = rows // tile

    def turn(k, carry):
        n, at = k // per, pl.ds(pl.multiple_of(lax.rem(k, per) * tile, tile), tile)
        value = sources[0][n, at].astype(F32)
        for source in sources[1:]:
            value = value + source[n, at].astype(F32)
        target[n, at] = value.astype(target.dtype)
        return carry

    lax.fori_loop(0, count * per, turn, 0)


def dot_rows(target, left, right):
    tile = 256

    def turn(n, carry):
        at = pl.ds(pl.multiple_of(n * tile, tile), tile)
        target[:, at] = matmul_last(left[...], right[at, :])
        return carry

    lax.fori_loop(0, right.shape[0] // tile, turn, 0)


def norm_back_tiles(target, grads, normed, inverse, gain, base, sums, gain_row):
    tile = 32
    width = grads.shape[1]

    def turn(k, carry):
        at = pl.ds(pl.multiple_of(k * tile, tile), tile)
        grad, unit = grads[at, :], normed[at, :]
        scaled = grad * gain
        middle = jnp.sum(scaled, axis=-1, keepdims=True) * (1.0 / width)
        along = jnp.sum(scaled * unit, axis=-1, keepdims=True) * (1.0 / width)
        target[at, :] = base[at, :].astype(F32) + inverse[at, 0:1] * (scaled - middle - unit * along)
        sums[gain_row : gain_row + 1, :] += jnp.sum(grad * unit, axis=0, keepdims=True)
        sums[gain_row + 1 : gain_row + 2, :] += jnp.sum(grad, axis=0, keepdims=True)
        return carry

    lax.fori_loop(0, grads.shape[0] // tile, turn, 0)


GAIN_ONE, BIAS_ONE, GAIN_TWO, BIAS_TWO, MIX_KEY, MIX_VALUE, MIX_RECEPT, DECAY, PREMIUM, BLEND_KEY, BLEND_RECEPT = range(11)


def norm_tiles(source, unit, inverse):
    rows, width = source.shape
    tile = min(rows, 32)

    def turn(k, carry):
        at = pl.ds(pl.multiple_of(k * tile, tile), tile)
        value = source[at, :].astype(F32)
        center = value - jnp.sum(value, axis=-1, keepdims=True) * (1.0 / width)
        scale = lax.rsqrt(jnp.sum(center * center, axis=-1, keepdims=True) * (1.0 / width) + EPSILON)
        unit[at, :] = center * scale
        inverse[at, :] = jnp.broadcast_to(scale, (tile, 128))
        return carry

    lax.fori_loop(0, rows // tile, turn, 0)


def dot_columns(finish, left, right):
    tile = 256
    depth = left.shape[1]

    def turn(n, carry):
        at = pl.ds(pl.multiple_of(n * tile, tile), tile)
        finish(at, matmul(left[...], right[:, :, :, :, :, at].reshape(depth, tile)))
        return carry

    lax.fori_loop(0, right.shape[5] // tile, turn, 0)


AHEAD = 3


def forward_kernel(
    tokens, cotangent, keep,
    own_vectors, own_key, own_value, own_recept, own_output, own_feedr,
    feed_key, feed_value,
    all_vectors, all_key, all_value, all_recept, all_output, all_feedr, all_feed,
    result, table_out, rates_out, lefts, feed_in_out, grad_value_out, grad_gate_out, positive, spread_one_out,
    unit_one_out, inverse_one_out, spread_two_out, unit_two_out, inverse_two_out, keys_out, values_out, denom_out,
    mixed_out, prior_a_out, prior_b_out, recept_out,
    own_feed, packed, table, rates, squares, feed_slot, positive_slot, left_parts, feed_in, grad_value, grad_gate, spread_one,
    unit_one, inverse_one, spread_two, unit_two, inverse_two, keys, values, gates, denom, mixed, prior_a, prior_b,
    cum, up, low, residual, total, halo_tokens, halo_unit, halo_inverse, summary, arrived, entering_rows, halo_out, halo_in,
    send, recv, own_sem, feed_sem, load_sem, out_sem, slot_sem, scan_send, scan_recv, halo_send, halo_recv,
):
    size = arrived.shape[0]
    links = Links(size)
    x, c, z, y, t, dp = links.x, links.c, links.z, links.y, links.t, links.dp
    count, width = tokens.shape
    micro, length = keep.shape[:2]
    ins = [own_vectors, own_key, own_value, own_recept, own_output, own_feedr, own_feed]
    outs = [all_vectors, all_key, all_value, all_recept, all_output, all_feedr, all_feed]
    piece = 16
    chunks = [(i, r) for i in range(7) for r in range(0, ins[i].shape[0], piece)]
    steps = len(chunks)
    feed_steps = ins[6].shape[0] // piece
    feed_base = steps - feed_steps
    x_first, y_first = jnp.where(c == 0, x, 1 - x), jnp.where(c == 0, 1 - y, y)
    first, second = links.first, links.second

    def place(n):
        if isinstance(n, int):
            i, start = chunks[n]
            return i, pl.ds(start, piece)
        return 6, pl.ds(pl.multiple_of((n - feed_base) * piece, piece), piece)

    def copy_z(n, o):
        i, at = place(n)
        return remote(ins[i].at[at], outs[i].at[x, c, z, y, at], send.at[n, o], recv.at[n, o], links.along_z[o])

    def copy_column(n, j, xx, yy, device):
        i, at = place(n)
        column = outs[i].at[xx, c, :, yy, at]
        return remote(column, column, send.at[n, j], recv.at[n, j], device)

    def copy_first(n):
        return copy_column(n, 3, x, y, first)

    def copy_second(n):
        return copy_column(n, 4, x, y, second)

    def copy_passed(n):
        return copy_column(n, 5, x_first, y_first, second)

    def copy_core(n):
        i, at = place(n)
        half = outs[i].at[:, c, :, :, at]
        return remote(half, half, send.at[n, 6], recv.at[n, 6], links.core)

    def step_z(n):
        for o in range(3):
            copy_z(n, o).start()

    def step_a(n):
        for o in range(3):
            copy_z(n, o).wait_recv()
        copy_first(n).start()
        copy_second(n).start()

    def step_b(n):
        copy_first(n).wait_recv()
        copy_passed(n).start()

    def step_c(n):
        copy_second(n).wait_recv()
        copy_passed(n).wait_recv()
        copy_core(n).start()

    def advance(*numbers):
        for s in numbers:
            if s + AHEAD < steps:
                step_z(s + AHEAD)
            if s < steps:
                step_a(s)
            if 0 <= s - 1 < steps:
                step_b(s - 1)
            if 0 <= s - 2 < steps:
                step_c(s - 2)

    def load(k):
        return pltpu.make_async_copy(outs[1 + k], squares.at[k], load_sem.at[k])

    def ready(k):
        for n in (2 * k + 1, 2 * k + 2):
            copy_core(n).wait_recv()
        load(k).start()

    written = []

    def write(source, target):
        copy = pltpu.make_async_copy(source, target, out_sem.at[len(written)])
        copy.start()
        written.append(copy)

    owns = [pltpu.make_async_copy(ins[i], outs[i].at[x, c, z, y], own_sem.at[i]) for i in range(7)]
    for own in owns[:6]:
        own.start()
    share_rows = own_feed.shape[0]
    mine = pl.ds(pl.multiple_of(dp * share_rows, share_rows), share_rows)
    feed_loads = [
        pltpu.make_async_copy(feed_key.at[mine], own_feed.at[:, :width], feed_sem.at[0]),
        pltpu.make_async_copy(feed_value.at[mine], own_feed.at[:, width:], feed_sem.at[1]),
    ]
    for copy in feed_loads:
        copy.start()
    links.greet(True)
    halo_copies = [
        remote(
            tokens.at[pl.ds((m + 1) * length - piece, piece)], halo_tokens.at[pl.ds(m * piece, piece)],
            halo_send.at[m], halo_recv.at[m], links.row(1),
        )
        for m in range(micro)
    ]
    for halo in halo_copies:
        halo.start()
    for n in range(AHEAD):
        step_z(n)
    summary[...] = jnp.zeros_like(summary)
    halo_out[...] = jnp.zeros_like(halo_out)
    total[...] = jnp.zeros_like(total)
    for own in owns[:6]:
        own.wait()
    advance(0)
    norm_tiles(tokens, unit_one, inverse_one)
    write(unit_one, unit_one_out)
    write(inverse_one, inverse_one_out)
    for copy in feed_loads:
        copy.wait()
    owns[6].start()
    advance(1, 2)
    for halo in halo_copies:
        halo.wait_recv()
    norm_tiles(halo_tokens, halo_unit, halo_inverse)
    copy_core(0).wait_recv()

    vector_load = pltpu.make_async_copy(all_vectors, packed, load_sem.at[5])
    vector_load.start()
    advance(3)
    owns[6].wait()
    vector_load.wait()
    share = width // 32
    per = 128 // share
    for j in range(width // 128):
        value = None
        for q in range(per):
            d = j * per + q
            part = packed[d // 16, (d // 8) % 2, (d // 2) % 4, d % 2].astype(F32)
            part = pltpu.roll(part, q * share, 1) if q else part
            value = part if value is None else value + part
        table[:, j * 128 : (j + 1) * 128] = value
    speed = jnp.exp(table[DECAY : DECAY + 1, :])
    rates[...] = jnp.broadcast_to(speed, rates.shape)
    table[DECAY : DECAY + 1, :] = jnp.exp(-speed)
    write(table, table_out)
    write(rates, rates_out)
    row = lax.broadcasted_iota(jnp.int32, (length, 128), 0)

    def vector(k, at):
        return table[k : k + 1, at]

    def normed(unit, gain, bias, at):
        return (unit * vector(gain, at) + vector(bias, at)).astype(BF).astype(F32)

    def blends(spread, unit, m, prior, gain, bias, mixes):
        rows_at = slice(m * length, (m + 1) * length)

        def turn(j, carry):
            at = lanes(j)
            now = normed(unit[rows_at, at], gain, bias, at)
            before = roll_rows(now, 1, jnp.where(t > 0, prior(at), 0.0), row) * keep[m]
            spread[rows_at, at] = now - before
            for target, mix in mixes:
                target[rows_at, at] = (now * vector(mix, at) + before * (1.0 - vector(mix, at))).astype(BF)
            return carry

        lax.fori_loop(0, width // 128, turn, 0)

    mixes = [(left_parts.at[2 + k], MIX_KEY + k) for k in range(3)]
    for m in range(micro):
        last = (m + 1) * piece - 1

        def prior(at, last=last):
            return normed(halo_unit[last : last + 1, at], GAIN_ONE, BIAS_ONE, at)

        blends(spread_one, unit_one, m, prior, GAIN_ONE, BIAS_ONE, mixes)
        advance(4 + m)
    write(spread_one, spread_one_out)
    for k in range(3):
        write(left_parts.at[2 + k], lefts.at[2 + k])

    def keep_in(target):
        def finish(at, value):
            target[:, at] = value

        return finish

    ready(0)
    advance(6)
    load(0).wait()
    dot_columns(keep_in(keys), left_parts.at[2], squares.at[0])
    write(keys, keys_out)
    ready(1)
    advance(7)
    load(1).wait()
    dot_columns(keep_in(values), left_parts.at[3], squares.at[1])
    write(values, values_out)

    for m in range(micro):
        rows_at = slice(m * length, (m + 1) * length)

        def first_pass(j, carry, m=m, rows_at=rows_at):
            at = lanes(j)
            power = jnp.exp(keys[rows_at, at])
            f, a, b = doubling(keep[m] * vector(DECAY, at), power * values[rows_at, at], power, row, 1)
            cum[rows_at, at] = f
            up[rows_at, at] = a
            low[rows_at, at] = b
            summary[3 * m : 3 * m + 1, at] = f[length - 1 :]
            summary[3 * m + 1 : 3 * m + 2, at] = a[length - 1 :]
            summary[3 * m + 2 : 3 * m + 3, at] = b[length - 1 :]
            return carry

        lax.fori_loop(0, width // 128, first_pass, 0)
        advance(8 + m)
    scan_copies = row_copies(summary, arrived, scan_send, scan_recv, t, dp, size)
    for copy in scan_copies:
        copy.start()
    ready(2)
    load(2).wait()

    def finish_gate(at, value):
        gates[:, at] = jax.nn.sigmoid(value)

    dot_columns(finish_gate, left_parts.at[4], squares.at[2])
    write(gates, recept_out)
    advance(10, 11, 12)
    for copy in scan_copies:
        copy.wait_recv()
    for m in range(micro):
        a = jnp.zeros((1, width), F32)
        b = jnp.zeros((1, width), F32)
        for o in range(size - 1, 0, -1):
            f = arrived[o, 3 * m : 3 * m + 1]
            a = jnp.where(t >= o, f * a + arrived[o, 3 * m + 1 : 3 * m + 2], a)
            b = jnp.where(t >= o, f * b + arrived[o, 3 * m + 2 : 3 * m + 3], b)
        entering_rows[2 * m : 2 * m + 1] = a
        entering_rows[2 * m + 1 : 2 * m + 2] = b
    for m in range(micro):
        rows_at = slice(m * length, (m + 1) * length)

        def second_pass(j, carry, m=m, rows_at=rows_at):
            at = lanes(j)
            enter_a = entering_rows[2 * m : 2 * m + 1, at]
            enter_b = entering_rows[2 * m + 1 : 2 * m + 2, at]
            f = cum[rows_at, at]
            before_a = roll_rows(up[rows_at, at] + f * enter_a, 1, enter_a, row)
            before_b = roll_rows(low[rows_at, at] + f * enter_b, 1, enter_b, row)
            bonus = jnp.exp(vector(PREMIUM, at) + keys[rows_at, at])
            below = keep[m] * before_b + bonus
            blended = (keep[m] * before_a + bonus * values[rows_at, at]) / below
            left_parts[1, rows_at, at] = (gates[rows_at, at] * blended).astype(BF)
            denom[rows_at, at] = below
            mixed[rows_at, at] = blended
            prior_a[rows_at, at] = before_a
            prior_b[rows_at, at] = before_b
            return carry

        lax.fori_loop(0, width // 128, second_pass, 0)
    write(left_parts.at[1], lefts.at[1])
    write(denom, denom_out)
    write(mixed, mixed_out)
    write(prior_a, prior_a_out)
    write(prior_b, prior_b_out)
    ready(3)
    load(3).wait()

    def finish_residual(at, value):
        residual[:, at] = tokens[:, at].astype(F32) + value

    dot_columns(finish_residual, left_parts.at[1], squares.at[3])
    norm_tiles(residual, unit_two, inverse_two)
    write(unit_two, unit_two_out)
    write(inverse_two, inverse_two_out)
    for m in range(micro):
        last = (m + 1) * length - 1
        halo_out[m : m + 1, :] = normed(unit_two[last : last + 1, :], GAIN_TWO, BIAS_TWO, slice(None))
    halo_two = remote(halo_out, halo_in, halo_send.at[micro], halo_recv.at[micro], links.row(1))
    halo_two.start()
    ready(4)
    advance(13, 14)
    halo_two.wait_recv()
    mixes = [(feed_in, BLEND_KEY), (left_parts.at[0], BLEND_RECEPT)]
    for m in range(micro):

        def prior(at, m=m):
            return halo_in[m : m + 1, at]

        blends(spread_two, unit_two, m, prior, GAIN_TWO, BIAS_TWO, mixes)
    write(spread_two, spread_two_out)
    write(feed_in, feed_in_out)
    write(left_parts.at[0], lefts.at[0])
    load(4).wait()

    def finish_second_gate(at, value):
        cum[:, at] = jax.nn.sigmoid(value)

    dot_columns(finish_second_gate, left_parts.at[0], squares.at[4])

    advance(15)
    later = {0: 16, 1: 17, 3: 18, 5: 19, 7: 20}

    def arrive(k, carry):
        for turn, number in later.items():
            pl.when(k == turn)(functools.partial(advance, number))
        slot = lax.rem(k, 2)
        at = pl.ds(pl.multiple_of(k * piece, piece), piece)
        copy_core(feed_base + k).wait_recv()
        fetch = pltpu.make_async_copy(outs[6].at[:, :, :, :, at], feed_slot, slot_sem.at[0])
        fetch.start()

        def put(k, slot):
            at = pl.ds(pl.multiple_of(k * piece, piece), piece)
            return pltpu.make_async_copy(positive_slot.at[slot], positive.at[:, :, :, :, at], slot_sem.at[1 + slot])

        @pl.when(k >= 2)
        def _():
            put(k - 2, slot).wait()

        fetch.wait()
        units = 32 * piece
        hidden = jnp.maximum(matmul_last(feed_slot[:, :, :, :, :, :width].reshape(units, width), feed_in[...]), 0.0)
        positive_slot[slot] = hidden.reshape(positive_slot.shape[1:])
        put(k, slot).start()
        hidden_squares = (hidden * hidden).astype(BF)
        total[...] += matmul_lead(hidden_squares, feed_slot[:, :, :, :, :, width:].reshape(units, width))

        @pl.when(k == feed_steps - 1)
        def _():
            put(k - 1, 1 - slot).wait()
            put(k, slot).wait()

        return carry

    lax.fori_loop(0, feed_steps, arrive, 0)

    def last_pass(k, carry):
        at = pl.ds(pl.multiple_of(k * 32, 32), 32)
        gate, value_out, grad = cum[at, :], total[at, :], cotangent[at, :].astype(F32)
        residual[at, :] = residual[at, :] + gate * value_out
        grad_value[at, :] = (grad * gate).astype(BF)
        grad_gate[at, :] = (grad * value_out * gate * (1.0 - gate)).astype(BF)
        return carry

    lax.fori_loop(0, count // 32, last_pass, 0)
    write(residual, result)
    write(grad_value, grad_value_out)
    write(grad_gate, grad_gate_out)
    for n in range(steps):
        for o in range(3):
            copy_z(n, o).wait_send()
        for copy in (copy_first(n), copy_second(n), copy_passed(n), copy_core(n)):
            copy.wait_send()
    for copy in halo_copies + [halo_two] + scan_copies:
        copy.wait_send()
    for copy in written:
        copy.wait()


def forward(near, parts, far, size):
    count, width = near[0].shape
    rows = far[0].shape[0] // 4
    whole_parts = [(p.shape, p.dtype) for p in parts] + [((rows, 2 * width), BF)]
    flat = lambda kind: jax.ShapeDtypeStruct((count, width), kind)
    narrow = jax.ShapeDtypeStruct((count, 128), F32)
    dma = pltpu.SemaphoreType.DMA
    big, low = pltpu.VMEM((count, width), F32), pltpu.VMEM((count, width), BF)
    lines = pltpu.VMEM((count, 128), F32)
    steps = sum(shape[0] // 16 for shape, _ in whole_parts)
    eight = pltpu.VMEM((8, width), F32)
    return pl.pallas_call(
        forward_kernel,
        out_shape=[jax.ShapeDtypeStruct((2, 2, 4, 2) + shape, kind) for shape, kind in whole_parts]
        + [
            flat(F32), jax.ShapeDtypeStruct((16, width), F32), jax.ShapeDtypeStruct((8, width), F32),
            jax.ShapeDtypeStruct((5, count, width), BF), flat(BF), flat(BF), flat(BF),
            jax.ShapeDtypeStruct((2, 2, 4, 2, rows, count), F32), flat(F32), flat(F32), narrow, flat(F32), flat(F32), narrow,
        ]
        + [flat(F32)] * 7,
        in_specs=[whole()] * (len(near) + len(parts)) + [anywhere()] * 2,
        out_specs=[anywhere()] * 28,
        scratch_shapes=[
            pltpu.VMEM((rows, 2 * width), BF),
            pltpu.VMEM((2, 2, 4, 2, 16, 128), BF), pltpu.VMEM((16, width), F32), eight,
            pltpu.VMEM((5, 2, 2, 4, 2, width // 32, width), BF), pltpu.VMEM((2, 2, 4, 2, 16, 2 * width), BF),
            pltpu.VMEM((2, 2, 2, 4, 2, 16, count), F32), pltpu.VMEM((5, count, width), BF), low, low, low, big,
            big, lines, big, big, lines,
        ]
        + [big] * 12
        + [
            pltpu.VMEM((32, width), BF), pltpu.VMEM((32, width), F32), pltpu.VMEM((32, 128), F32), eight,
            pltpu.VMEM((size, 8, width), F32), eight, eight, eight,
            dma((steps, 7)), dma((steps, 7)), dma((7,)), dma((2,)), dma((6,)), dma((24,)), dma((3,)), dma((size,)), dma((size,)),
            dma((3,)), dma((3,)),
        ],
        compiler_params=pltpu.CompilerParams(collective_id=0, has_side_effects=True, vmem_limit_bytes=66_000_000),
        cost_estimate=cost(6 * count * width * width + 4 * count * 32 * rows * width, 60_000_000),
        name="forward",
    )(*near, *parts, *far)


def channel_backward_kernel(
    feed_in, grad_value, grad_gate, vectors, keep, inverse, cotangent,
    weights, positive, w_feedr, w_output, spread, unit, keys, values, denom, mixed, prior_a, prior_b, recept,
    own_units, rights, grad_residual, sums,
    weight_slots, positive_slots, feedr, output, spread_in, unit_in, keys_in, values_in, denom_in, mixed_in,
    prior_a_in, prior_b_in, recept_in, value_part, key_part, outgoing, gathered, from_first, from_second, feed_part, feed_z,
    grad_in, grad_rin, grad_z, grad_w, cum, up, low, summary, arrived, entering_rows, halo_out, halo_in,
    slot_sem, load_sem, core_send, core_recv, first_send, first_recv, second_send, second_recv, feed_send, feed_recv,
    scan_send, scan_recv, halo_send, halo_recv,
):
    size = arrived.shape[0]
    links = Links(size)
    x, c, z, y, t = links.x, links.c, links.z, links.y, links.t
    rows, width = weight_slots.shape[2], feed_in.shape[1]
    micro, length = keep.shape[:2]

    def which(s):
        return lax.rem(s, 2), 3 - s // 2

    def fetches(s, slot):
        own, i = which(s)
        cc = own * c + (1 - own) * (1 - c)
        xx, yy = owner(i, x, y, cc)
        return (
            pltpu.make_async_copy(weights.at[xx, cc, :, yy], weight_slots.at[slot], slot_sem.at[0, slot]),
            pltpu.make_async_copy(positive.at[xx, cc, :, yy], positive_slots.at[slot], slot_sem.at[1, slot]),
        )

    for copy in fetches(0, 0):
        copy.start()
    late = [
        (w_feedr, feedr), (spread, spread_in), (unit, unit_in), (w_output, output), (recept, recept_in),
        (mixed, mixed_in), (denom, denom_in), (keys, keys_in), (values, values_in), (prior_a, prior_a_in),
        (prior_b, prior_b_in),
    ]
    loads = [pltpu.make_async_copy(source, target, load_sem.at[k]) for k, (source, target) in enumerate(late)]
    for load in loads:
        load.start()
    links.greet(True)
    grad_att, grad_keys, grad_values, grad_recept = [rights.at[n] for n in range(1, 5)]
    rights[0] = grad_gate[...]
    grad_in[...] = jnp.zeros_like(grad_in)
    sums[...] = jnp.zeros_like(sums)
    summary[...] = jnp.zeros_like(summary)
    halo_out[...] = jnp.zeros_like(halo_out)

    def to_core(i, slot):
        return remote(outgoing.at[slot], gathered.at[i], core_send.at[i], core_recv.at[i], links.core)

    spans = [(0, rows // 2), (rows // 2, rows)] * 2

    def piece(ref, u, *first):
        return ref.at[(*first, u // 2, slice(None), slice(*spans[u]))]

    def to_first(q, u):
        return remote(
            piece(gathered, u, 2 + q), piece(from_first, u, q), first_send.at[q, u], first_recv.at[q, u], links.first
        )

    def to_second(u):
        return remote(
            piece(gathered, u, 1), piece(from_second, u), second_send.at[u], second_recv.at[u], links.second
        )

    def to_z(u, o):
        at = slice(*spans[u])
        return remote(
            feed_part.at[u // 2, o, at], feed_z.at[u // 2, o - 1, at], feed_send.at[u, o - 1], feed_recv.at[u, o - 1],
            links.along_z[o - 1],
        )

    def pass_first(u):
        to_first(1, u).start()
        to_first(0, u).start()

    def pass_second(u):
        to_first(1, u).wait_recv()
        add_blocks(piece(gathered, u, 1), [piece(gathered, u, 1), piece(from_first, u, 1)])
        to_second(u).start()

    def pass_z(u):
        to_first(0, u).wait_recv()
        to_second(u).wait_recv()
        add_blocks(piece(feed_part, u), [piece(gathered, u, 0), piece(from_first, u, 0), piece(from_second, u)])
        for o in (1, 2, 3):
            to_z(u, o).start()

    def finish(u):
        for o in (1, 2, 3):
            to_z(u, o).wait_recv()
        for r in range(*spans[u], 32):
            at = slice(r, r + 32)
            value = feed_part[u // 2, 0, at].astype(F32)
            for o in range(3):
                value = value + feed_z[u // 2, o, at].astype(F32)
            own_units[u // 2, at] = value.astype(BF)

    def column(s, carry):
        slot = lax.rem(s, 2)
        own, i = which(s)
        for copy in fetches(s, slot):
            copy.wait()

        @pl.when(s < 7)
        def _():
            for copy in fetches(s + 1, 1 - slot):
                copy.start()

        hidden = positive_slots[slot].reshape(4 * rows, feed_in.shape[0])
        squares = (hidden * hidden).astype(BF)
        key_rows = weight_slots[slot, :, :, :width].reshape(4 * rows, width)
        value_rows = weight_slots[slot, :, :, width:].reshape(4 * rows, width)
        value_part[...] = matmul(squares, grad_value[...])
        grad_pre = (matmul_last(value_rows, grad_value[...]) * (2.0 * hidden)).astype(BF)
        key_part[...] = matmul(grad_pre, feed_in[...])
        grad_in[...] += matmul_lead(grad_pre, key_rows)

        turn_slot = lax.rem(s // 2, 2)

        @pl.when(own == 0)
        def _():
            @pl.when(s >= 4)
            def _():
                to_core(i + 2, turn_slot).wait_send()

            for k in range(4):
                at = lax.rem(k + 4 - z, 4)
                outgoing[turn_slot, 0, at] = value_part[k * rows : (k + 1) * rows].astype(BF)
                outgoing[turn_slot, 1, at] = key_part[k * rows : (k + 1) * rows].astype(BF)
            to_core(i, turn_slot).start()

        @pl.when(own == 1)
        def _():
            to_core(i, turn_slot).wait_recv()
            for side, part in ((0, value_part), (1, key_part)):
                for k in range(4):
                    at = lax.rem(k + 4 - z, 4)
                    total = gathered[i, side, at].astype(F32) + part[k * rows : (k + 1) * rows]
                    gathered[i, side, at] = total.astype(BF)

        for turn, q in ((1, 1), (3, 0)):

            @pl.when(s == turn)
            def _(q=q):
                to_first(q, 0).start()
                to_first(q, 1).start()

        pl.when(s == 5)(lambda: pass_second(0))
        pl.when(s == 6)(lambda: pass_second(1))
        return carry

    lax.fori_loop(0, 8, column, 0)
    to_core(1, 0).wait_send()
    to_core(0, 1).wait_send()

    row = lax.broadcasted_iota(jnp.int32, (length, 128), 0)
    loads[0].wait()
    dot_rows(grad_rin, grad_gate, feedr)

    def shift_two(m, rows_at, at, keeping):
        return keeping * (
            grad_in[rows_at, at] * (1.0 - vectors[BLEND_KEY : BLEND_KEY + 1, at])
            + grad_rin[rows_at, at] * (1.0 - vectors[BLEND_RECEPT : BLEND_RECEPT + 1, at])
        )

    for m in range(micro):
        start = m * length
        halo_out[m : m + 1] = shift_two(m, slice(start, start + 1), slice(None), keep[m, 0:1, 0:1])
    halo = remote(halo_out, halo_in, halo_send.at[0], halo_recv.at[0], links.row(size - 1))
    halo.start()
    pass_first(2)
    loads[1].wait()
    pass_z(0)
    halo.wait_recv()
    for m in range(micro):
        rows_at = slice(m * length, (m + 1) * length)

        def shift_pass(j, carry, m=m, rows_at=rows_at):
            at = lanes(j)
            after = jnp.where(t < size - 1, halo_in[m : m + 1, at], 0.0)
            shift = shift_two(m, rows_at, at, keep[m])
            from_in, from_rin, apart = grad_in[rows_at, at], grad_rin[rows_at, at], spread_in[rows_at, at]
            grad_z[rows_at, at] = (
                from_in * vectors[BLEND_KEY : BLEND_KEY + 1, at]
                + from_rin * vectors[BLEND_RECEPT : BLEND_RECEPT + 1, at]
                + roll_rows(shift, -1, after, row)
            )
            sums[BLEND_KEY : BLEND_KEY + 1, at] += jnp.sum(from_in * apart, axis=0, keepdims=True)
            sums[BLEND_RECEPT : BLEND_RECEPT + 1, at] += jnp.sum(from_rin * apart, axis=0, keepdims=True)
            return carry

        lax.fori_loop(0, width // 128, shift_pass, 0)
    loads[2].wait()
    norm_back_tiles(
        grad_residual, grad_z, unit_in, inverse, vectors[GAIN_TWO : GAIN_TWO + 1, :], cotangent, sums, GAIN_TWO
    )
    grad_att[...] = grad_residual[...].astype(BF)

    loads[3].wait()
    dot_rows(grad_w, grad_att, output)
    for load in loads[4:]:
        load.wait()
    pass_z(1)

    def quotient_grads(rows_at, at):
        gate = recept_in[rows_at, at]
        blended = mixed_in[rows_at, at]
        inner = grad_w[rows_at, at] * gate
        above = inner / denom_in[rows_at, at]
        return above, -above * blended, inner * blended * (1.0 - gate)

    for m in range(micro):
        rows_at = slice(m * length, (m + 1) * length)

        def first_pass(j, carry, m=m, rows_at=rows_at):
            at = lanes(j)
            above, below, rec = quotient_grads(rows_at, at)
            grad_recept[rows_at, at] = rec.astype(BF)
            factor = keep[m] * vectors[DECAY : DECAY + 1, at]
            f, a, b = doubling(factor, keep[m] * above, keep[m] * below, row, -1)
            cum[rows_at, at] = f
            up[rows_at, at] = a
            low[rows_at, at] = b
            summary[3 * m : 3 * m + 1, at] = f[:1]
            summary[3 * m + 1 : 3 * m + 2, at] = a[:1]
            summary[3 * m + 2 : 3 * m + 3, at] = b[:1]
            return carry

        lax.fori_loop(0, width // 128, first_pass, 0)
    copies = row_copies(summary, arrived, scan_send, scan_recv, t, links.dp, size)
    for copy in copies:
        copy.start()
    pass_first(3)
    pass_second(2)
    pass_second(3)
    for copy in copies:
        copy.wait_recv()
    for m in range(micro):
        a = jnp.zeros((1, width), F32)
        b = jnp.zeros((1, width), F32)
        for ahead in range(size - 1, 0, -1):
            o = size - ahead
            f = arrived[o, 3 * m : 3 * m + 1]
            a = jnp.where(t + ahead < size, f * a + arrived[o, 3 * m + 1 : 3 * m + 2], a)
            b = jnp.where(t + ahead < size, f * b + arrived[o, 3 * m + 2 : 3 * m + 3], b)
        entering_rows[2 * m : 2 * m + 1] = a
        entering_rows[2 * m + 1 : 2 * m + 2] = b
    for m in range(micro):
        rows_at = slice(m * length, (m + 1) * length)

        def second_pass(j, carry, m=m, rows_at=rows_at):
            at = lanes(j)
            enter_a = entering_rows[2 * m : 2 * m + 1, at]
            enter_b = entering_rows[2 * m + 1 : 2 * m + 2, at]
            f = cum[rows_at, at]
            alpha = roll_rows(up[rows_at, at] + f * enter_a, -1, enter_a, row)
            beta = roll_rows(low[rows_at, at] + f * enter_b, -1, enter_b, row)
            above, below, _ = quotient_grads(rows_at, at)
            key, value = keys_in[rows_at, at], values_in[rows_at, at]
            power = jnp.exp(key)
            bonus = jnp.exp(vectors[PREMIUM : PREMIUM + 1, at] + key)
            premium = bonus * (value * above + below)
            grad_values[rows_at, at] = (bonus * above + power * alpha).astype(BF)
            grad_keys[rows_at, at] = (premium + power * (value * alpha + beta)).astype(BF)
            fading = keep[m] * (alpha * prior_a_in[rows_at, at] + beta * prior_b_in[rows_at, at])
            sums[PREMIUM : PREMIUM + 1, at] += jnp.sum(premium, axis=0, keepdims=True)
            sums[DECAY : DECAY + 1, at] += jnp.sum(fading, axis=0, keepdims=True)
            return carry

        lax.fori_loop(0, width // 128, second_pass, 0)
        if m == 0:
            pass_z(2)

    finish(0)
    finish(1)
    pass_z(3)
    finish(2)
    finish(3)
    for u in range(4):
        to_first(0, u).wait_send()
        to_first(1, u).wait_send()
        to_second(u).wait_send()
        for o in (1, 2, 3):
            to_z(u, o).wait_send()
    halo.wait_send()
    for copy in copies:
        copy.wait_send()


def channel_backward(near, far, size):
    feed_in = near[0]
    weights = far[0]
    tokens, width = feed_in.shape
    micro, length = near[4].shape[:2]
    rows = weights.shape[4]
    flat_f32 = (tokens, width)
    dma = pltpu.SemaphoreType.DMA
    big = pltpu.VMEM(flat_f32, F32)
    return pl.pallas_call(
        channel_backward_kernel,
        out_shape=[
            jax.ShapeDtypeStruct((2, rows, width), BF),
            jax.ShapeDtypeStruct((5, tokens, width), BF),
            jax.ShapeDtypeStruct(flat_f32, F32), jax.ShapeDtypeStruct((16, width), F32),
        ],
        in_specs=[whole()] * len(near) + [anywhere()] * len(far),
        out_specs=[whole()] * 4,
        scratch_shapes=[
            pltpu.VMEM((2, 4, rows, 2 * width), BF), pltpu.VMEM((2, 4, rows, tokens), F32),
            pltpu.VMEM((width, width), BF), pltpu.VMEM((width, width), BF),
        ]
        + [big] * 9
        + [
            pltpu.VMEM((4 * rows, width), F32), pltpu.VMEM((4 * rows, width), F32),
            pltpu.VMEM((2, 2, 4, rows, width), BF), pltpu.VMEM((4, 2, 4, rows, width), BF),
            pltpu.VMEM((2, 2, 4, rows, width), BF), pltpu.VMEM((2, 4, rows, width), BF),
            pltpu.VMEM((2, 4, rows, width), BF), pltpu.VMEM((2, 3, rows, width), BF),
        ]
        + [big] * 7
        + [
            pltpu.VMEM((8, width), F32), pltpu.VMEM((size, 8, width), F32), pltpu.VMEM((8, width), F32),
            pltpu.VMEM((8, width), F32), pltpu.VMEM((8, width), F32),
            dma((2, 2)), dma((11,)), dma((4,)), dma((4,)), dma((2, 4)), dma((2, 4)), dma((4,)), dma((4,)),
            dma((4, 3)), dma((4, 3)),
            dma((size,)), dma((size,)), dma((1,)), dma((1,)),
        ],
        compiler_params=pltpu.CompilerParams(
            collective_id=2, has_side_effects=True, vmem_limit_bytes=66_000_000
        ),
        cost_estimate=cost(8 * tokens * 32 * rows * width, 16 * 32 * rows * width),
        name="channel_backward",
    )(*near, *far)


def front_backward_kernel(
    own_units, vectors, keep, inverse, sums_in, rates,
    lefts_far, rights_far, grad_residual_far, w_key, w_value, w_recept, spread, unit,
    square_grads, units, token_grads, vector_grads,
    lefts, rights, grad_residual, key_in, value_in, recept_in, spread_in, unit_in, outgoing, gathered, from_first, from_second, from_z,
    grad_key, grad_value, grad_recept, grad_z, sums, held, halo_out, halo_in,
    load_sem, core_send, core_recv, first_send, first_recv, second_send, second_recv, z_send, z_recv,
    unit_send, unit_recv, halo_send, halo_recv, sum_send, sum_recv, keep_sem, pair_sem,
):
    links = Links(8)
    x, c, z, y, t, size = links.x, links.c, links.z, links.y, links.t, links.size
    count = lefts.shape[0]
    width = lefts.shape[2]
    rows = width // 32
    micro, length = keep.shape[:2]
    late = [(w_key, key_in), (w_value, value_in), (w_recept, recept_in), (spread, spread_in), (unit, unit_in)]
    late += [(grad_residual_far, grad_residual)]
    loads = [pltpu.make_async_copy(source, target, load_sem.at[k]) for k, (source, target) in enumerate(late)]

    def pair(n):
        return (
            pltpu.make_async_copy(lefts_far.at[n], lefts.at[n], pair_sem.at[0, n]),
            pltpu.make_async_copy(rights_far.at[n], rights.at[n], pair_sem.at[1, n]),
        )

    for n in range(count):
        for copy in pair(n):
            copy.start()
    for load in loads:
        load.start()
    links.greet(True)
    dp = links.dp
    over = (1 - x) * 2 + c
    kept = pltpu.make_async_copy(own_units, units.at[dp], keep_sem.at[0])
    kept.start()
    units_over_x = remote(own_units, units.at[dp], unit_send.at[0], unit_recv.at[0], links.over_x)
    pl.when(c == 0)(units_over_x.start)
    units_over_core = remote(own_units, units.at[dp], unit_send.at[1], unit_recv.at[1], links.core)
    units_over_core.start()
    halo_out[...] = jnp.zeros_like(halo_out)
    sums[...] = sums_in[...]

    def part(n, cc, xx):
        at = pl.ds(pl.multiple_of((xx * 2 + cc) * 8 * rows, 8 * rows), 8 * rows)
        return matmul_lead(lefts[n, :, at], rights[n])

    def blocks():
        for zz in range(4):
            for yy in range(2):
                yield zz, yy, slice((zz * 2 + yy) * rows, (zz * 2 + yy + 1) * rows)

    def to_core(n):
        return remote(outgoing.at[n], gathered.at[n], core_send.at[n], core_recv.at[n], links.core)

    def to_first(n):
        return remote(
            gathered.at[n, pl.ds(2, 2)], from_first.at[n], first_send.at[n], first_recv.at[n], links.first
        )

    def to_second(n):
        return remote(gathered.at[n, 1], from_second.at[n], second_send.at[n], second_recv.at[n], links.second)

    def to_z(n, o):
        return remote(
            gathered.at[n, 0, o], from_z.at[n, o - 1], z_send.at[n, o - 1], z_recv.at[n, o - 1], links.along_z[o - 1]
        )

    def other(n, carry):
        for copy in pair(n):
            copy.wait()
        for xx in range(2):
            value = part(n, 1 - c, xx)
            for zz, yy, at in blocks():
                outgoing[n, position(xx, yy, x, y, 1 - c), lax.rem(zz + 4 - z, 4)] = value[at].astype(BF)
        to_core(n).start()

    def own(n, carry):
        to_core(n).wait_recv()
        for xx in range(2):
            value = part(n, c, xx)
            for zz, yy, at in blocks():
                i, o = position(xx, yy, x, y, c), lax.rem(zz + 4 - z, 4)
                gathered[n, i, o] = (gathered[n, i, o].astype(F32) + value[at]).astype(BF)
        to_first(n).start()

    def both(n, carry):
        pl.when(n < count)(lambda: other(n, None))
        pl.when(n >= 1)(lambda: own(n - 1, None))
        return carry

    lax.fori_loop(0, count + 1, both, 0)
    pl.when(c == 1)(units_over_x.start)

    def pass_second(n):
        to_first(n).wait_recv()
        add_blocks(gathered.at[n, 1], [gathered.at[n, 1], from_first.at[n, 1]])
        to_second(n).start()

    def pass_z(n):
        to_second(n).wait_recv()
        add_blocks(gathered.at[n, 0], [gathered.at[n, 0], from_first.at[n, 0], from_second.at[n]])
        for o in (1, 2, 3):
            to_z(n, o).start()

    def finish(n):
        value = gathered[n, 0, 0].astype(F32)
        for o in (1, 2, 3):
            to_z(n, o).wait_recv()
            value = value + from_z[n, o - 1].astype(F32)
        square_grads[n] = value

    loads[0].wait()
    dot_rows(grad_key, rights.at[2], key_in)
    pass_second(0)
    loads[1].wait()
    dot_rows(grad_value, rights.at[3], value_in)
    pass_second(1)
    loads[2].wait()
    dot_rows(grad_recept, rights.at[4], recept_in)
    last_over_core = remote(units.at[over], units.at[over], unit_send.at[2], unit_recv.at[2], links.core)
    grads = ((grad_key, MIX_KEY), (grad_value, MIX_VALUE), (grad_recept, MIX_RECEPT))

    def shift_one(rows_at, at, keeping):
        return keeping * sum(g[rows_at, at] * (1.0 - vectors[k : k + 1, at]) for g, k in grads)

    for m in range(micro):
        start = m * length
        halo_out[m : m + 1] = shift_one(slice(start, start + 1), slice(None), keep[m, 0:1, 0:1])
    halo = remote(halo_out, halo_in, halo_send.at[0], halo_recv.at[0], links.row(size - 1))
    halo.start()
    pass_second(2)
    pass_z(0)
    pass_second(3)
    pass_z(1)
    pass_second(4)
    loads[3].wait()
    halo.wait_recv()
    row = lax.broadcasted_iota(jnp.int32, (length, 128), 0)
    for m in range(micro):
        rows_at = slice(m * length, (m + 1) * length)

        def shift_pass(j, carry, m=m, rows_at=rows_at):
            at = lanes(j)
            after = jnp.where(t < size - 1, halo_in[m : m + 1, at], 0.0)
            apart = spread_in[rows_at, at]
            value = roll_rows(shift_one(rows_at, at, keep[m]), -1, after, row)
            for g, k in grads:
                value = value + g[rows_at, at] * vectors[k : k + 1, at]
                sums[k : k + 1, at] += jnp.sum(g[rows_at, at] * apart, axis=0, keepdims=True)
            grad_z[rows_at, at] = value
            return carry

        lax.fori_loop(0, width // 128, shift_pass, 0)
    pass_z(2)
    loads[4].wait()
    loads[5].wait()
    norm_back_tiles(
        token_grads, grad_z, unit_in, inverse, vectors[GAIN_ONE : GAIN_ONE + 1, :], grad_residual, sums, GAIN_ONE
    )
    sums[DECAY : DECAY + 1, :] = -sums[DECAY : DECAY + 1, :] * rates[0:1, :] * vectors[DECAY : DECAY + 1, :]

    stages = [[links.core], [links.over_x], [links.over_y], links.along_z]
    pending = []
    source, slot = sums, 0

    def begin(stage, source, slot):
        copies = [
            remote(source, held.at[slot + k], sum_send.at[slot + k], sum_recv.at[slot + k], peer)
            for k, peer in enumerate(stage)
        ]
        for copy in copies:
            copy.start()
        return copies

    def collect(copies, source, slot, target):
        value = source[...]
        for k, copy in enumerate(copies):
            copy.wait_recv()
            value = value + held[slot + k]
        target[...] = value

    copies = begin(stages[0], sums, 0)
    pending += copies
    pass_z(3)
    finish(0)
    collect(copies, sums, 0, held.at[6])
    copies = begin(stages[1], held.at[6], 1)
    pending += copies
    pass_z(4)
    finish(1)
    collect(copies, held.at[6], 1, held.at[7])
    copies = begin(stages[2], held.at[7], 2)
    pending += copies
    units_over_x.wait_recv()
    last_over_core.start()
    finish(2)
    collect(copies, held.at[7], 2, held.at[8])
    copies = begin(stages[3], held.at[8], 3)
    pending += copies
    finish(3)
    collect(copies, held.at[8], 3, vector_grads)
    finish(4)
    for copy in (units_over_core, last_over_core):
        copy.wait_recv()
    kept.wait()
    for n in range(count):
        to_core(n).wait_send()
        to_first(n).wait_send()
        to_second(n).wait_send()
        for o in (1, 2, 3):
            to_z(n, o).wait_send()
    for copy in pending + [units_over_x, units_over_core, last_over_core, halo]:
        copy.wait_send()


def front_backward(near, far):
    own_units, lefts = near[0], far[0]
    rows = own_units.shape[1]
    count, tokens, width = lefts.shape
    own = width // 32
    dma = pltpu.SemaphoreType.DMA
    big = pltpu.VMEM((tokens, width), F32)
    square = pltpu.VMEM((width, width), BF)
    return pl.pallas_call(
        front_backward_kernel,
        out_shape=[
            jax.ShapeDtypeStruct((count, own, width), F32),
            jax.ShapeDtypeStruct((4, 2, rows, width), BF),
            jax.ShapeDtypeStruct((tokens, width), F32), jax.ShapeDtypeStruct((16, width), F32),
        ],
        in_specs=[whole()] * len(near) + [anywhere()] * len(far),
        out_specs=[whole(), anywhere(), whole(), whole()],
        scratch_shapes=[pltpu.VMEM(lefts.shape, BF), pltpu.VMEM(lefts.shape, BF), big]
        + [square] * 3
        + [big] * 2
        + [
            pltpu.VMEM((count, 4, 4, own, width), BF), pltpu.VMEM((count, 4, 4, own, width), BF),
            pltpu.VMEM((count, 2, 4, own, width), BF), pltpu.VMEM((count, 4, own, width), BF),
            pltpu.VMEM((count, 3, own, width), BF),
        ]
        + [big] * 4
        + [
            pltpu.VMEM((16, width), F32), pltpu.VMEM((9, 16, width), F32), pltpu.VMEM((8, width), F32),
            pltpu.VMEM((8, width), F32),
            dma((6,)), dma((count,)), dma((count,)), dma((count,)), dma((count,)), dma((count,)), dma((count,)),
            dma((count, 3)), dma((count, 3)), dma((3,)), dma((3,)), dma((1,)), dma((1,)),
            dma((6,)), dma((6,)), dma((1,)), dma((2, count)),
        ],
        compiler_params=pltpu.CompilerParams(
            collective_id=3, has_side_effects=True, vmem_limit_bytes=66_000_000
        ),
        cost_estimate=cost(4 * count * tokens * width * width, 40 * width * width),
        name="front_backward",
    )(*near, *far)


def local_shards(tokens, resets, out_grads, *weights):
    (
        mixer_key, mixer_value, mixer_recept, mixer_output, feed_recept, feed_key, feed_value, *vector_shards
    ) = weights
    size = lax.axis_size("tensor")
    dp, t = lax.axis_index("dp"), lax.axis_index("tensor")
    micro, _, length, width = tokens.shape
    count = micro * length
    share = vector_shards[0].shape[0]
    vector_pack = jnp.pad(jnp.stack(vector_shards), ((0, 16 - len(vector_shards)), (0, 128 - share)))
    keep = (1 - resets[:, 0]).astype(F32)[:, :, None]
    keep_lanes = jnp.broadcast_to(keep, (micro, length, 128))
    cotangent = out_grads.reshape(count, width)
    near = [tokens.reshape(count, width), cotangent, keep_lanes]
    parts = [vector_pack, mixer_key, mixer_value, mixer_recept, mixer_output, feed_recept]
    (
        _, all_key, all_value, all_recept, all_output, all_feedr, feed,
        result, table, rates, lefts, feed_in, grad_value, grad_gate, positive, spread_one, unit_one, inverse_one,
        spread_two, unit_two, inverse_two, keys, values, denom, mixed, prior_a, prior_b, recept,
    ) = forward(near, parts, [feed_key, feed_value], size)
    w_key, w_value, w_recept, w_output, w_feedr = [
        w.reshape(width, width) for w in (all_key, all_value, all_recept, all_output, all_feedr)
    ]
    near = [feed_in, grad_value, grad_gate, table, keep_lanes, inverse_two, cotangent]
    far = [feed, positive, w_feedr, w_output, spread_two, unit_two, keys, values, denom, mixed, prior_a, prior_b, recept]
    own_units, rights, grad_residual, sums = channel_backward(near, far, size)
    near = [own_units, table, keep_lanes, inverse_one, sums, rates]
    far = [lefts, rights, grad_residual, w_key, w_value, w_recept, spread_one, unit_one]
    square_grads, units, token_grads, vector_grads = front_backward(near, far)
    mine = lax.dynamic_slice_in_dim(vector_grads, (dp * size + t) * share, share, 1)
    return (
        result.reshape(tokens.shape), token_grads.reshape(tokens.shape),
        square_grads[2], square_grads[3], square_grads[4], square_grads[1], square_grads[0],
        units[:, 1].reshape(feed_key.shape).astype(F32), units[:, 0].reshape(feed_value.shape).astype(F32),
    ) + tuple(mine[i] for i in range(len(vector_shards)))


def is_two_by_two_by_four(mesh):
    return mesh.shape["dp"] == 4 and mesh.shape["tensor"] == 8


def solution(mesh):
    return jax.shard_map(
        local_shards if is_two_by_two_by_four(mesh) else shards,
        mesh=mesh,
        in_specs=(
            P(None, "dp", "tensor", None),
            P(None, "dp", "tensor"),
            P(None, "dp", "tensor", None),
            P(("dp", "tensor"), None),
            P(("dp", "tensor"), None),
            P(("dp", "tensor"), None),
            P(("dp", "tensor"), None),
            P(("dp", "tensor"), None),
            P("tensor", None),
            P("tensor", None),
            P(("dp", "tensor")),
            P(("dp", "tensor")),
            P(("dp", "tensor")),
            P(("dp", "tensor")),
            P(("dp", "tensor")),
            P(("dp", "tensor")),
            P(("dp", "tensor")),
            P(("dp", "tensor")),
            P(("dp", "tensor")),
            P(("dp", "tensor")),
            P(("dp", "tensor")),
        ),
        out_specs=(
            P(None, "dp", "tensor", None),
            P(None, "dp", "tensor", None),
            P(("dp", "tensor"), None),
            P(("dp", "tensor"), None),
            P(("dp", "tensor"), None),
            P(("dp", "tensor"), None),
            P(("dp", "tensor"), None),
            P("tensor", None),
            P("tensor", None),
            P(("dp", "tensor")),
            P(("dp", "tensor")),
            P(("dp", "tensor")),
            P(("dp", "tensor")),
            P(("dp", "tensor")),
            P(("dp", "tensor")),
            P(("dp", "tensor")),
            P(("dp", "tensor")),
            P(("dp", "tensor")),
            P(("dp", "tensor")),
            P(("dp", "tensor")),
        ),
        check_vma=False,
    )
```

```python
import functools

import jax
import jax.numpy as jnp
from jax import lax
from jax.experimental import pallas as pl
from jax.experimental.pallas import tpu as pltpu
from jax.sharding import PartitionSpec as P

EPSILON = 1e-05


def entering(shard, axis, combine, identity, reverse):
    size, here = (lax.axis_size(axis), lax.axis_index(axis))
    everything = jax.tree.map(lambda part: lax.all_gather(part, axis), shard)
    start = jax.tree.map(
        lambda part, zero: jnp.broadcast_to(jnp.asarray(zero, part.dtype), part.shape),
        shard,
        identity,
    )

    def turn(k, before):
        at = size - 1 - k if reverse else k
        reached = at > here if reverse else at < here
        new = combine(before, jax.tree.map(lambda part: part[at], everything))
        return jax.tree.map(lambda a, b: jnp.where(reached, a, b), new, before)

    return lax.fori_loop(0, size, turn, start)


def shifted(block, axis, distance):
    devices = range(lax.axis_size(axis))
    route = [(i - distance, i) for i in devices if i - distance in devices]
    return lax.ppermute(block, axis, route)


def norm_rows(payload_series, gain, bias):
    center = payload_series - jnp.mean(payload_series, axis=-1, keepdims=True)
    inverse = lax.rsqrt(jnp.mean(center * center, axis=-1, keepdims=True) + EPSILON)
    normed = center * inverse
    return (normed * gain + bias, normed, inverse)


def norm_back(grad_out, normed, inverse, gain):
    scaled = grad_out * gain
    centred = scaled - jnp.mean(scaled, axis=-1, keepdims=True)
    grad_in = inverse * (centred - normed * jnp.mean(scaled * normed, axis=-1, keepdims=True))
    return (grad_in, jnp.sum(grad_out * normed, axis=0), jnp.sum(grad_out, axis=0))


def affine(earlier, later):
    return (
        earlier[0] * later[0],
        later[0] * earlier[1] + later[1],
        later[0] * earlier[2] + later[2],
    )


def carry_across(summary, backward):
    width = summary[0].shape[0]
    identity = (
        jnp.ones((width,), jnp.float32),
        jnp.zeros((width,), jnp.float32),
        jnp.zeros((width,), jnp.float32),
    )
    return entering(summary, "tensor", affine, identity, backward)


def matmul(left, right):
    return jnp.dot(left, right, preferred_element_type=jnp.float32)


def matmul_lead(left, right):
    return lax.dot_general(
        left, right, (((0,), (0,)), ((), ())), preferred_element_type=jnp.float32
    )


def matmul_last(left, right):
    return lax.dot_general(
        left, right, (((1,), (1,)), ((), ())), preferred_element_type=jnp.float32
    )


def shards(
    tokens,
    resets,
    out_grads,
    mixer_key,
    mixer_value,
    mixer_recept,
    mixer_output,
    feed_recept,
    feed_key,
    feed_value,
    first_gain,
    first_bias,
    second_gain,
    second_bias,
    mixing_key,
    mixing_value,
    mixing_recept,
    time_decay,
    time_first,
    feeding_key,
    feeding_recept,
):
    gathered = (
        lax.all_gather(mixer_key, ("dp", "tensor"), axis=0, tiled=True),
        lax.all_gather(mixer_value, ("dp", "tensor"), axis=0, tiled=True),
        lax.all_gather(mixer_recept, ("dp", "tensor"), axis=0, tiled=True),
        lax.all_gather(mixer_output, ("dp", "tensor"), axis=0, tiled=True),
        lax.all_gather(feed_recept, ("dp", "tensor"), axis=0, tiled=True),
        lax.all_gather(first_gain, ("dp", "tensor"), axis=0, tiled=True),
        lax.all_gather(first_bias, ("dp", "tensor"), axis=0, tiled=True),
        lax.all_gather(second_gain, ("dp", "tensor"), axis=0, tiled=True),
        lax.all_gather(second_bias, ("dp", "tensor"), axis=0, tiled=True),
        lax.all_gather(mixing_key, ("dp", "tensor"), axis=0, tiled=True),
        lax.all_gather(mixing_value, ("dp", "tensor"), axis=0, tiled=True),
        lax.all_gather(mixing_recept, ("dp", "tensor"), axis=0, tiled=True),
        lax.all_gather(time_decay, ("dp", "tensor"), axis=0, tiled=True),
        lax.all_gather(time_first, ("dp", "tensor"), axis=0, tiled=True),
        lax.all_gather(feeding_key, ("dp", "tensor"), axis=0, tiled=True),
        lax.all_gather(feeding_recept, ("dp", "tensor"), axis=0, tiled=True),
    )
    w_key, w_value, w_recept, w_output, w_feedr = (
        gathered[0],
        gathered[1],
        gathered[2],
        gathered[3],
        gathered[4],
    )
    parameter_vectors = [piece.astype(jnp.float32) for piece in gathered[5:]]
    gain_one, bias_one, gain_two, bias_two = (
        parameter_vectors[0],
        parameter_vectors[1],
        parameter_vectors[2],
        parameter_vectors[3],
    )
    mix_key, mix_value, mix_recept = (
        parameter_vectors[4],
        parameter_vectors[5],
        parameter_vectors[6],
    )
    (
        fading_speed_logarithm,
        opening_premium_logarithm,
        channel_lookup_blend,
        channel_gating_blend,
    ) = (parameter_vectors[7], parameter_vectors[8], parameter_vectors[9], parameter_vectors[10])
    rates = jnp.exp(fading_speed_logarithm)
    fading_multiplier = jnp.exp(-rates)
    micro_count = tokens.shape[0]
    width = tokens.shape[3]
    grad_keyw = jnp.zeros(feed_key.shape, jnp.float32)
    grad_valuew = jnp.zeros(feed_value.shape, jnp.float32)
    square_grads = [jnp.zeros((width, width), jnp.float32) for index_one in range(5)]
    parameter_vector_gradients = [jnp.zeros((width,), jnp.float32) for index_two in range(11)]
    results = []
    input_grads = []
    for micro_index in range(micro_count):
        inputs = tokens[micro_index, 0].astype(jnp.float32)
        restart_retain_flags = (1 - resets[micro_index, 0]).astype(jnp.float32)[:, None]
        cotangent = out_grads[micro_index, 0].astype(jnp.float32)
        normed_one, unit_one, inverse_one = norm_rows(inputs, gain_one, bias_one)
        z_one = normed_one.astype(jnp.bfloat16)
        prior_one = shifted(z_one[-1:], "tensor", 1)
        before_one = (
            jnp.concatenate([prior_one, z_one[:-1]], axis=0).astype(jnp.float32)
            * restart_retain_flags
        )
        z_onef = z_one.astype(jnp.float32)
        in_key = (z_onef * mix_key + before_one * (1.0 - mix_key)).astype(jnp.bfloat16)
        in_value = (z_onef * mix_value + before_one * (1.0 - mix_value)).astype(jnp.bfloat16)
        in_recept = (z_onef * mix_recept + before_one * (1.0 - mix_recept)).astype(jnp.bfloat16)
        lookup_series = matmul(in_key, w_key)
        payload_series = matmul(in_value, w_value)
        recept = jax.nn.sigmoid(matmul(in_recept, w_recept))
        powered_lookup = jnp.exp(lookup_series)
        premium_plus_lookup = jnp.exp(opening_premium_logarithm + lookup_series)
        factor = restart_retain_flags * fading_multiplier
        cum_factor, local_a, local_b = lax.associative_scan(
            affine, (factor, powered_lookup * payload_series, powered_lookup), axis=0
        )
        incoming = carry_across((cum_factor[-1], local_a[-1], local_b[-1]), False)
        upper_running_state = local_a + cum_factor * incoming[1]
        lower_running_state = local_b + cum_factor * incoming[2]
        earlier_upper_state = jnp.concatenate([incoming[1][None], upper_running_state[:-1]], axis=0)
        earlier_lower_state = jnp.concatenate([incoming[2][None], lower_running_state[:-1]], axis=0)
        lower_quotient_part = restart_retain_flags * earlier_lower_state + premium_plus_lookup
        blended = (
            restart_retain_flags * earlier_upper_state + premium_plus_lookup * payload_series
        ) / lower_quotient_part
        weighted = (recept * blended).astype(jnp.bfloat16)
        residual = inputs + matmul(weighted, w_output)
        normed_two, unit_two, inverse_two = norm_rows(residual, gain_two, bias_two)
        z_two = normed_two.astype(jnp.bfloat16)
        prior_two = shifted(z_two[-1:], "tensor", 1)
        before_two = (
            jnp.concatenate([prior_two, z_two[:-1]], axis=0).astype(jnp.float32)
            * restart_retain_flags
        )
        z_twof = z_two.astype(jnp.float32)
        feed_in = (
            z_twof * channel_lookup_blend + before_two * (1.0 - channel_lookup_blend)
        ).astype(jnp.bfloat16)
        feed_rin = (
            z_twof * channel_gating_blend + before_two * (1.0 - channel_gating_blend)
        ).astype(jnp.bfloat16)
        gate = jax.nn.sigmoid(matmul(feed_rin, w_feedr))
        all_in = lax.all_gather(feed_in, "tensor", axis=0, tiled=True)
        hidden_pre = matmul_last(feed_key, all_in)
        hidden = jnp.square(jnp.maximum(hidden_pre, 0.0)).astype(jnp.bfloat16)
        value_out = lax.psum_scatter(
            matmul_lead(hidden, feed_value), "tensor", scatter_dimension=0, tiled=True
        )
        results.append(residual + gate * value_out)
        grad_value = (cotangent * gate).astype(jnp.bfloat16)
        grad_gate = (cotangent * value_out * gate * (1.0 - gate)).astype(jnp.bfloat16)
        square_grads[4] = square_grads[4] + matmul_lead(feed_rin, grad_gate)
        grad_rin = matmul_last(grad_gate, w_feedr)
        relu_twice = 2.0 * jnp.maximum(hidden_pre, 0.0)
        add_piece = lax.all_gather(grad_value, "tensor", axis=0, tiled=True)
        rows_total = matmul(hidden, add_piece)
        block = matmul_last(feed_value, add_piece)
        grad_valuew = grad_valuew + rows_total
        grad_pre = (block * relu_twice).astype(jnp.bfloat16)
        grad_keyw = grad_keyw + matmul(grad_pre, all_in)
        grad_in = lax.psum_scatter(
            matmul_lead(grad_pre, feed_key), "tensor", scatter_dimension=0, tiled=True
        )
        parameter_vector_gradients[9] = parameter_vector_gradients[9] + jnp.sum(
            grad_in * (z_twof - before_two), axis=0
        )
        parameter_vector_gradients[10] = parameter_vector_gradients[10] + jnp.sum(
            grad_rin * (z_twof - before_two), axis=0
        )
        shift_two = restart_retain_flags * (
            grad_in * (1.0 - channel_lookup_blend) + grad_rin * (1.0 - channel_gating_blend)
        )
        after_two = shifted(shift_two[:1], "tensor", -1)
        grad_z_two = (
            grad_in * channel_lookup_blend
            + grad_rin * channel_gating_blend
            + jnp.concatenate([shift_two[1:], after_two], axis=0)
        )
        back_two, gain_part, bias_part = norm_back(grad_z_two, unit_two, inverse_two, gain_two)
        parameter_vector_gradients[2] = parameter_vector_gradients[2] + gain_part
        parameter_vector_gradients[3] = parameter_vector_gradients[3] + bias_part
        grad_residual = cotangent + back_two
        grad_att = grad_residual.astype(jnp.bfloat16)
        square_grads[3] = square_grads[3] + matmul_lead(weighted, grad_att)
        grad_weighted = matmul_last(grad_att, w_output)
        grad_mixed = grad_weighted * recept
        grad_recept = (grad_weighted * blended * recept * (1.0 - recept)).astype(jnp.bfloat16)
        upper_adjoint = grad_mixed / lower_quotient_part
        denominator_gradient = -grad_mixed * blended / lower_quotient_part
        cum_back, local_xa, local_xb = lax.associative_scan(
            affine,
            (
                factor,
                restart_retain_flags * upper_adjoint,
                restart_retain_flags * denominator_gradient,
            ),
            reverse=True,
            axis=0,
        )
        beyond = carry_across((cum_back[0], local_xa[0], local_xb[0]), True)
        adjoint_a = local_xa + cum_back * beyond[1]
        adjoint_b = local_xb + cum_back * beyond[2]
        running_upper_total = jnp.concatenate([adjoint_a[1:], beyond[1][None]], axis=0)
        running_lower_total = jnp.concatenate([adjoint_b[1:], beyond[2][None]], axis=0)
        premium_power = premium_plus_lookup * (
            payload_series * upper_adjoint + denominator_gradient
        )
        adjoint_payloads = (
            premium_plus_lookup * upper_adjoint + powered_lookup * running_upper_total
        ).astype(jnp.bfloat16)
        key_gradient_rows = (
            premium_power
            + powered_lookup * (payload_series * running_upper_total + running_lower_total)
        ).astype(jnp.bfloat16)
        parameter_vector_gradients[8] = parameter_vector_gradients[8] + jnp.sum(
            premium_power, axis=0
        )
        decay_sum = jnp.sum(
            restart_retain_flags
            * (
                running_upper_total * earlier_upper_state
                + running_lower_total * earlier_lower_state
            ),
            axis=0,
        )
        parameter_vector_gradients[7] = (
            parameter_vector_gradients[7] - rates * fading_multiplier * decay_sum
        )
        square_grads[0] = square_grads[0] + matmul_lead(in_key, key_gradient_rows)
        square_grads[1] = square_grads[1] + matmul_lead(in_value, adjoint_payloads)
        square_grads[2] = square_grads[2] + matmul_lead(in_recept, grad_recept)
        grad_inkey = matmul_last(key_gradient_rows, w_key)
        grad_invalue = matmul_last(adjoint_payloads, w_value)
        grad_inrecept = matmul_last(grad_recept, w_recept)
        spread_one = z_onef - before_one
        parameter_vector_gradients[4] = parameter_vector_gradients[4] + jnp.sum(
            grad_inkey * spread_one, axis=0
        )
        parameter_vector_gradients[5] = parameter_vector_gradients[5] + jnp.sum(
            grad_invalue * spread_one, axis=0
        )
        parameter_vector_gradients[6] = parameter_vector_gradients[6] + jnp.sum(
            grad_inrecept * spread_one, axis=0
        )
        shift_one = restart_retain_flags * (
            grad_inkey * (1.0 - mix_key)
            + grad_invalue * (1.0 - mix_value)
            + grad_inrecept * (1.0 - mix_recept)
        )
        after_one = shifted(shift_one[:1], "tensor", -1)
        grad_z_one = (
            grad_inkey * mix_key
            + grad_invalue * mix_value
            + grad_inrecept * mix_recept
            + jnp.concatenate([shift_one[1:], after_one], axis=0)
        )
        back_one, gain_first, bias_first = norm_back(grad_z_one, unit_one, inverse_one, gain_one)
        parameter_vector_gradients[0] = parameter_vector_gradients[0] + gain_first
        parameter_vector_gradients[1] = parameter_vector_gradients[1] + bias_first
        input_grads.append(grad_residual + back_one)
    owned = (
        lax.psum_scatter(square_grads[0], ("dp", "tensor"), scatter_dimension=0, tiled=True),
        lax.psum_scatter(square_grads[1], ("dp", "tensor"), scatter_dimension=0, tiled=True),
        lax.psum_scatter(square_grads[2], ("dp", "tensor"), scatter_dimension=0, tiled=True),
        lax.psum_scatter(square_grads[3], ("dp", "tensor"), scatter_dimension=0, tiled=True),
        lax.psum_scatter(square_grads[4], ("dp", "tensor"), scatter_dimension=0, tiled=True),
        lax.psum_scatter(
            parameter_vector_gradients[0], ("dp", "tensor"), scatter_dimension=0, tiled=True
        ),
        lax.psum_scatter(
            parameter_vector_gradients[1], ("dp", "tensor"), scatter_dimension=0, tiled=True
        ),
        lax.psum_scatter(
            parameter_vector_gradients[2], ("dp", "tensor"), scatter_dimension=0, tiled=True
        ),
        lax.psum_scatter(
            parameter_vector_gradients[3], ("dp", "tensor"), scatter_dimension=0, tiled=True
        ),
        lax.psum_scatter(
            parameter_vector_gradients[4], ("dp", "tensor"), scatter_dimension=0, tiled=True
        ),
        lax.psum_scatter(
            parameter_vector_gradients[5], ("dp", "tensor"), scatter_dimension=0, tiled=True
        ),
        lax.psum_scatter(
            parameter_vector_gradients[6], ("dp", "tensor"), scatter_dimension=0, tiled=True
        ),
        lax.psum_scatter(
            parameter_vector_gradients[7], ("dp", "tensor"), scatter_dimension=0, tiled=True
        ),
        lax.psum_scatter(
            parameter_vector_gradients[8], ("dp", "tensor"), scatter_dimension=0, tiled=True
        ),
        lax.psum_scatter(
            parameter_vector_gradients[9], ("dp", "tensor"), scatter_dimension=0, tiled=True
        ),
        lax.psum_scatter(
            parameter_vector_gradients[10], ("dp", "tensor"), scatter_dimension=0, tiled=True
        ),
    )
    key_rows, value_rows_grad = (grad_keyw, grad_valuew)
    key_total, value_total = (
        lax.psum(key_rows.astype(jnp.bfloat16), "dp").astype(jnp.float32),
        lax.psum(value_rows_grad.astype(jnp.bfloat16), "dp").astype(jnp.float32),
    )
    result_all = jnp.stack(results)[:, None]
    grads_all = jnp.stack(input_grads)[:, None]
    return (
        result_all,
        grads_all,
        owned[0],
        owned[1],
        owned[2],
        owned[3],
        owned[4],
        key_total,
        value_total,
        owned[5],
        owned[6],
        owned[7],
        owned[8],
        owned[9],
        owned[10],
        owned[11],
        owned[12],
        owned[13],
        owned[14],
        owned[15],
    )


BF = jnp.bfloat16
F32 = jnp.float32
BOTH = ("dp", "tensor")
MESH_ID = pl.DeviceIdType.MESH


def cost(flops, moved):
    return pl.CostEstimate(flops=flops, bytes_accessed=moved, transcendentals=0)


def whole():
    return pl.BlockSpec(memory_space=pltpu.VMEM)


def anywhere():
    return pl.BlockSpec(memory_space=pl.ANY)


def roll_rows(value, distance, fill, row):
    size = value.shape[0]
    moved = pltpu.roll(value, distance % size, 0)
    outside = row < distance if distance > 0 else row >= size + distance
    return jnp.where(outside, fill, moved)


def doubling(factor, up, low, row, sign):
    size, step = factor.shape[0], 1
    while step < size:
        up = up + factor * roll_rows(up, sign * step, 0.0, row)
        low = low + factor * roll_rows(low, sign * step, 0.0, row)
        factor = factor * roll_rows(factor, sign * step, 1.0, row)
        step *= 2
    return factor, up, low


def row_copies(summary, arrived, send, recv, t, dp, size):
    return [
        pltpu.make_async_remote_copy(
            src_ref=summary,
            dst_ref=arrived.at[o],
            send_sem=send.at[o],
            recv_sem=recv.at[o],
            device_id=(dp, lax.rem(t + o, size)),
            device_id_type=MESH_ID,
        )
        for o in range(1, size)
    ]


def lanes(j):
    return pl.ds(pl.multiple_of(j * 128, 128), 128)


def owner(i, x, y, c):
    first, second = i // 2, i % 2
    flip_x = first * c + second * (1 - c)
    flip_y = first * (1 - c) + second * c
    return x + flip_x - 2 * x * flip_x, y + flip_y - 2 * y * flip_y


def position(xx, yy, x, y, c):
    flip_x = x + xx - 2 * x * xx
    flip_y = y + yy - 2 * y * yy
    return 2 * (flip_x * c + flip_y * (1 - c)) + flip_x * (1 - c) + flip_y * c


class Links:
    def __init__(self, size):
        dp, t = lax.axis_index("dp"), lax.axis_index("tensor")
        x, c, z, y = dp // 2, dp % 2, t // 2, t % 2
        self.x, self.c, self.z, self.y, self.dp, self.t, self.size = x, c, z, y, dp, t, size
        over_x, over_y = ((1 - x) * 2 + c, t), (dp, z * 2 + 1 - y)
        self.over_x = over_x
        self.core = (x * 2 + 1 - c, t)
        self.first = (jnp.where(c == 0, over_y[0], over_x[0]), jnp.where(c == 0, over_y[1], over_x[1]))
        self.second = (jnp.where(c == 0, over_x[0], over_y[0]), jnp.where(c == 0, over_x[1], over_y[1]))
        self.along_z = [(dp, lax.rem(z + o, 4) * 2 + y) for o in (1, 2, 3)]
        self.over_y = over_y

    def row(self, o):
        return (self.dp, lax.rem(self.t + o, self.size))

    def greet(self, whole_row):
        peers = [self.row(o) for o in range(1, self.size)] if whole_row else self.along_z + [self.over_y]
        peers = peers + [self.over_x, self.core]
        barrier = pltpu.get_barrier_semaphore()
        for peer in peers:
            pl.semaphore_signal(barrier, inc=1, device_id=peer, device_id_type=MESH_ID)
        pl.semaphore_wait(barrier, len(peers))


def remote(source, target, send, recv, device):
    return pltpu.make_async_remote_copy(
        src_ref=source, dst_ref=target, send_sem=send, recv_sem=recv, device_id=device, device_id_type=MESH_ID
    )


def add_blocks(target, sources):
    count, rows = target.shape[:2]
    tile = min(rows, 32)
    per = rows // tile

    def turn(k, carry):
        n, at = k // per, pl.ds(pl.multiple_of(lax.rem(k, per) * tile, tile), tile)
        value = sources[0][n, at].astype(F32)
        for source in sources[1:]:
            value = value + source[n, at].astype(F32)
        target[n, at] = value.astype(target.dtype)
        return carry

    lax.fori_loop(0, count * per, turn, 0)


def dot_rows(target, left, right):
    tile = 256

    def turn(n, carry):
        at = pl.ds(pl.multiple_of(n * tile, tile), tile)
        target[:, at] = matmul_last(left[...], right[at, :])
        return carry

    lax.fori_loop(0, right.shape[0] // tile, turn, 0)


def norm_back_tiles(target, grads, normed, inverse, gain, base, sums, gain_row):
    tile = 32
    width = grads.shape[1]

    def turn(k, carry):
        at = pl.ds(pl.multiple_of(k * tile, tile), tile)
        grad, unit = grads[at, :], normed[at, :]
        scaled = grad * gain
        middle = jnp.sum(scaled, axis=-1, keepdims=True) * (1.0 / width)
        along = jnp.sum(scaled * unit, axis=-1, keepdims=True) * (1.0 / width)
        target[at, :] = base[at, :].astype(F32) + inverse[at, 0:1] * (scaled - middle - unit * along)
        sums[gain_row : gain_row + 1, :] += jnp.sum(grad * unit, axis=0, keepdims=True)
        sums[gain_row + 1 : gain_row + 2, :] += jnp.sum(grad, axis=0, keepdims=True)
        return carry

    lax.fori_loop(0, grads.shape[0] // tile, turn, 0)


GAIN_ONE, BIAS_ONE, GAIN_TWO, BIAS_TWO, MIX_KEY, MIX_VALUE, MIX_RECEPT, DECAY, PREMIUM, BLEND_KEY, BLEND_RECEPT = range(11)


def norm_tiles(source, unit, inverse):
    rows, width = source.shape
    tile = min(rows, 32)

    def turn(k, carry):
        at = pl.ds(pl.multiple_of(k * tile, tile), tile)
        value = source[at, :].astype(F32)
        center = value - jnp.sum(value, axis=-1, keepdims=True) * (1.0 / width)
        scale = lax.rsqrt(jnp.sum(center * center, axis=-1, keepdims=True) * (1.0 / width) + EPSILON)
        unit[at, :] = center * scale
        inverse[at, :] = jnp.broadcast_to(scale, (tile, 128))
        return carry

    lax.fori_loop(0, rows // tile, turn, 0)


def dot_columns(finish, left, right):
    tile = 256
    depth = left.shape[1]

    def turn(n, carry):
        at = pl.ds(pl.multiple_of(n * tile, tile), tile)
        finish(at, matmul(left[...], right[:, :, :, :, :, at].reshape(depth, tile)))
        return carry

    lax.fori_loop(0, right.shape[5] // tile, turn, 0)


AHEAD = 3


def forward_kernel(
    tokens, cotangent, keep,
    own_vectors, own_key, own_value, own_recept, own_output, own_feedr,
    feed_key, feed_value,
    all_vectors, all_key, all_value, all_recept, all_output, all_feedr, all_feed,
    result, table_out, rates_out, lefts, feed_in_out, grad_value_out, grad_gate_out, positive, spread_one_out,
    unit_one_out, inverse_one_out, spread_two_out, unit_two_out, inverse_two_out, keys_out, values_out, denom_out,
    mixed_out, prior_a_out, prior_b_out, recept_out,
    own_feed, packed, table, rates, squares, feed_slot, positive_slot, left_parts, feed_in, grad_value, grad_gate, spread_one,
    unit_one, inverse_one, spread_two, unit_two, inverse_two, keys, values, gates, denom, mixed, prior_a, prior_b,
    cum, up, low, residual, total, halo_tokens, halo_unit, halo_inverse, summary, arrived, entering_rows, halo_out, halo_in,
    send, recv, own_sem, feed_sem, load_sem, out_sem, slot_sem, scan_send, scan_recv, halo_send, halo_recv,
):
    size = arrived.shape[0]
    links = Links(size)
    x, c, z, y, t, dp = links.x, links.c, links.z, links.y, links.t, links.dp
    count, width = tokens.shape
    micro, length = keep.shape[:2]
    ins = [own_vectors, own_key, own_value, own_recept, own_output, own_feedr, own_feed]
    outs = [all_vectors, all_key, all_value, all_recept, all_output, all_feedr, all_feed]
    piece = 16
    chunks = [(i, r) for i in range(7) for r in range(0, ins[i].shape[0], piece)]
    steps = len(chunks)
    feed_steps = ins[6].shape[0] // piece
    feed_base = steps - feed_steps
    x_first, y_first = jnp.where(c == 0, x, 1 - x), jnp.where(c == 0, 1 - y, y)
    first, second = links.first, links.second

    def place(n):
        if isinstance(n, int):
            i, start = chunks[n]
            return i, pl.ds(start, piece)
        return 6, pl.ds(pl.multiple_of((n - feed_base) * piece, piece), piece)

    def copy_z(n, o):
        i, at = place(n)
        return remote(ins[i].at[at], outs[i].at[x, c, z, y, at], send.at[n, o], recv.at[n, o], links.along_z[o])

    def copy_column(n, j, xx, yy, device):
        i, at = place(n)
        column = outs[i].at[xx, c, :, yy, at]
        return remote(column, column, send.at[n, j], recv.at[n, j], device)

    def copy_first(n):
        return copy_column(n, 3, x, y, first)

    def copy_second(n):
        return copy_column(n, 4, x, y, second)

    def copy_passed(n):
        return copy_column(n, 5, x_first, y_first, second)

    def copy_core(n):
        i, at = place(n)
        half = outs[i].at[:, c, :, :, at]
        return remote(half, half, send.at[n, 6], recv.at[n, 6], links.core)

    def step_z(n):
        for o in range(3):
            copy_z(n, o).start()

    def step_a(n):
        for o in range(3):
            copy_z(n, o).wait_recv()
        copy_first(n).start()
        copy_second(n).start()

    def step_b(n):
        copy_first(n).wait_recv()
        copy_passed(n).start()

    def step_c(n):
        copy_second(n).wait_recv()
        copy_passed(n).wait_recv()
        copy_core(n).start()

    def advance(*numbers):
        for s in numbers:
            if s + AHEAD < steps:
                step_z(s + AHEAD)
            if s < steps:
                step_a(s)
            if 0 <= s - 1 < steps:
                step_b(s - 1)
            if 0 <= s - 2 < steps:
                step_c(s - 2)

    def load(k):
        return pltpu.make_async_copy(outs[1 + k], squares.at[k], load_sem.at[k])

    def ready(k):
        for n in (2 * k + 1, 2 * k + 2):
            copy_core(n).wait_recv()
        load(k).start()

    written = []

    def write(source, target):
        copy = pltpu.make_async_copy(source, target, out_sem.at[len(written)])
        copy.start()
        written.append(copy)

    owns = [pltpu.make_async_copy(ins[i], outs[i].at[x, c, z, y], own_sem.at[i]) for i in range(7)]
    for own in owns[:6]:
        own.start()
    share_rows = own_feed.shape[0]
    mine = pl.ds(pl.multiple_of(dp * share_rows, share_rows), share_rows)
    feed_loads = [
        pltpu.make_async_copy(feed_key.at[mine], own_feed.at[:, :width], feed_sem.at[0]),
        pltpu.make_async_copy(feed_value.at[mine], own_feed.at[:, width:], feed_sem.at[1]),
    ]
    for copy in feed_loads:
        copy.start()
    links.greet(True)
    halo_copies = [
        remote(
            tokens.at[pl.ds((m + 1) * length - piece, piece)], halo_tokens.at[pl.ds(m * piece, piece)],
            halo_send.at[m], halo_recv.at[m], links.row(1),
        )
        for m in range(micro)
    ]
    for halo in halo_copies:
        halo.start()
    for n in range(AHEAD):
        step_z(n)
    summary[...] = jnp.zeros_like(summary)
    halo_out[...] = jnp.zeros_like(halo_out)
    total[...] = jnp.zeros_like(total)
    for own in owns[:6]:
        own.wait()
    advance(0)
    norm_tiles(tokens, unit_one, inverse_one)
    write(unit_one, unit_one_out)
    write(inverse_one, inverse_one_out)
    for copy in feed_loads:
        copy.wait()
    owns[6].start()
    advance(1, 2)
    for halo in halo_copies:
        halo.wait_recv()
    norm_tiles(halo_tokens, halo_unit, halo_inverse)
    copy_core(0).wait_recv()

    vector_load = pltpu.make_async_copy(all_vectors, packed, load_sem.at[5])
    vector_load.start()
    advance(3)
    owns[6].wait()
    vector_load.wait()
    share = width // 32
    per = 128 // share
    for j in range(width // 128):
        value = None
        for q in range(per):
            d = j * per + q
            part = packed[d // 16, (d // 8) % 2, (d // 2) % 4, d % 2].astype(F32)
            part = pltpu.roll(part, q * share, 1) if q else part
            value = part if value is None else value + part
        table[:, j * 128 : (j + 1) * 128] = value
    speed = jnp.exp(table[DECAY : DECAY + 1, :])
    rates[...] = jnp.broadcast_to(speed, rates.shape)
    table[DECAY : DECAY + 1, :] = jnp.exp(-speed)
    write(table, table_out)
    write(rates, rates_out)
    row = lax.broadcasted_iota(jnp.int32, (length, 128), 0)

    def vector(k, at):
        return table[k : k + 1, at]

    def normed(unit, gain, bias, at):
        return (unit * vector(gain, at) + vector(bias, at)).astype(BF).astype(F32)

    def blends(spread, unit, m, prior, gain, bias, mixes):
        rows_at = slice(m * length, (m + 1) * length)

        def turn(j, carry):
            at = lanes(j)
            now = normed(unit[rows_at, at], gain, bias, at)
            before = roll_rows(now, 1, jnp.where(t > 0, prior(at), 0.0), row) * keep[m]
            spread[rows_at, at] = now - before
            for target, mix in mixes:
                target[rows_at, at] = (now * vector(mix, at) + before * (1.0 - vector(mix, at))).astype(BF)
            return carry

        lax.fori_loop(0, width // 128, turn, 0)

    mixes = [(left_parts.at[2 + k], MIX_KEY + k) for k in range(3)]
    for m in range(micro):
        last = (m + 1) * piece - 1

        def prior(at, last=last):
            return normed(halo_unit[last : last + 1, at], GAIN_ONE, BIAS_ONE, at)

        blends(spread_one, unit_one, m, prior, GAIN_ONE, BIAS_ONE, mixes)
        advance(4 + m)
    write(spread_one, spread_one_out)
    for k in range(3):
        write(left_parts.at[2 + k], lefts.at[2 + k])

    def keep_in(target):
        def finish(at, value):
            target[:, at] = value

        return finish

    ready(0)
    advance(6)
    load(0).wait()
    dot_columns(keep_in(keys), left_parts.at[2], squares.at[0])
    write(keys, keys_out)
    ready(1)
    advance(7)
    load(1).wait()
    dot_columns(keep_in(values), left_parts.at[3], squares.at[1])
    write(values, values_out)

    for m in range(micro):
        rows_at = slice(m * length, (m + 1) * length)

        def first_pass(j, carry, m=m, rows_at=rows_at):
            at = lanes(j)
            power = jnp.exp(keys[rows_at, at])
            f, a, b = doubling(keep[m] * vector(DECAY, at), power * values[rows_at, at], power, row, 1)
            cum[rows_at, at] = f
            up[rows_at, at] = a
            low[rows_at, at] = b
            summary[3 * m : 3 * m + 1, at] = f[length - 1 :]
            summary[3 * m + 1 : 3 * m + 2, at] = a[length - 1 :]
            summary[3 * m + 2 : 3 * m + 3, at] = b[length - 1 :]
            return carry

        lax.fori_loop(0, width // 128, first_pass, 0)
        advance(8 + m)
    scan_copies = row_copies(summary, arrived, scan_send, scan_recv, t, dp, size)
    for copy in scan_copies:
        copy.start()
    ready(2)
    load(2).wait()

    def finish_gate(at, value):
        gates[:, at] = jax.nn.sigmoid(value)

    dot_columns(finish_gate, left_parts.at[4], squares.at[2])
    write(gates, recept_out)
    advance(10, 11, 12)
    for copy in scan_copies:
        copy.wait_recv()
    for m in range(micro):
        a = jnp.zeros((1, width), F32)
        b = jnp.zeros((1, width), F32)
        for o in range(size - 1, 0, -1):
            f = arrived[o, 3 * m : 3 * m + 1]
            a = jnp.where(t >= o, f * a + arrived[o, 3 * m + 1 : 3 * m + 2], a)
            b = jnp.where(t >= o, f * b + arrived[o, 3 * m + 2 : 3 * m + 3], b)
        entering_rows[2 * m : 2 * m + 1] = a
        entering_rows[2 * m + 1 : 2 * m + 2] = b
    for m in range(micro):
        rows_at = slice(m * length, (m + 1) * length)

        def second_pass(j, carry, m=m, rows_at=rows_at):
            at = lanes(j)
            enter_a = entering_rows[2 * m : 2 * m + 1, at]
            enter_b = entering_rows[2 * m + 1 : 2 * m + 2, at]
            f = cum[rows_at, at]
            before_a = roll_rows(up[rows_at, at] + f * enter_a, 1, enter_a, row)
            before_b = roll_rows(low[rows_at, at] + f * enter_b, 1, enter_b, row)
            bonus = jnp.exp(vector(PREMIUM, at) + keys[rows_at, at])
            below = keep[m] * before_b + bonus
            blended = (keep[m] * before_a + bonus * values[rows_at, at]) / below
            left_parts[1, rows_at, at] = (gates[rows_at, at] * blended).astype(BF)
            denom[rows_at, at] = below
            mixed[rows_at, at] = blended
            prior_a[rows_at, at] = before_a
            prior_b[rows_at, at] = before_b
            return carry

        lax.fori_loop(0, width // 128, second_pass, 0)
    write(left_parts.at[1], lefts.at[1])
    write(denom, denom_out)
    write(mixed, mixed_out)
    write(prior_a, prior_a_out)
    write(prior_b, prior_b_out)
    ready(3)
    load(3).wait()

    def finish_residual(at, value):
        residual[:, at] = tokens[:, at].astype(F32) + value

    dot_columns(finish_residual, left_parts.at[1], squares.at[3])
    norm_tiles(residual, unit_two, inverse_two)
    write(unit_two, unit_two_out)
    write(inverse_two, inverse_two_out)
    for m in range(micro):
        last = (m + 1) * length - 1
        halo_out[m : m + 1, :] = normed(unit_two[last : last + 1, :], GAIN_TWO, BIAS_TWO, slice(None))
    halo_two = remote(halo_out, halo_in, halo_send.at[micro], halo_recv.at[micro], links.row(1))
    halo_two.start()
    ready(4)
    advance(13, 14)
    halo_two.wait_recv()
    mixes = [(feed_in, BLEND_KEY), (left_parts.at[0], BLEND_RECEPT)]
    for m in range(micro):

        def prior(at, m=m):
            return halo_in[m : m + 1, at]

        blends(spread_two, unit_two, m, prior, GAIN_TWO, BIAS_TWO, mixes)
    write(spread_two, spread_two_out)
    write(feed_in, feed_in_out)
    write(left_parts.at[0], lefts.at[0])
    load(4).wait()

    def finish_second_gate(at, value):
        cum[:, at] = jax.nn.sigmoid(value)

    dot_columns(finish_second_gate, left_parts.at[0], squares.at[4])

    advance(15)
    later = {0: 16, 1: 17, 3: 18, 5: 19, 7: 20}

    def arrive(k, carry):
        for turn, number in later.items():
            pl.when(k == turn)(functools.partial(advance, number))
        slot = lax.rem(k, 2)
        at = pl.ds(pl.multiple_of(k * piece, piece), piece)
        copy_core(feed_base + k).wait_recv()
        fetch = pltpu.make_async_copy(outs[6].at[:, :, :, :, at], feed_slot, slot_sem.at[0])
        fetch.start()

        def put(k, slot):
            at = pl.ds(pl.multiple_of(k * piece, piece), piece)
            return pltpu.make_async_copy(positive_slot.at[slot], positive.at[:, :, :, :, at], slot_sem.at[1 + slot])

        @pl.when(k >= 2)
        def _():
            put(k - 2, slot).wait()

        fetch.wait()
        units = 32 * piece
        hidden = jnp.maximum(matmul_last(feed_slot[:, :, :, :, :, :width].reshape(units, width), feed_in[...]), 0.0)
        positive_slot[slot] = hidden.reshape(positive_slot.shape[1:])
        put(k, slot).start()
        hidden_squares = (hidden * hidden).astype(BF)
        total[...] += matmul_lead(hidden_squares, feed_slot[:, :, :, :, :, width:].reshape(units, width))

        @pl.when(k == feed_steps - 1)
        def _():
            put(k - 1, 1 - slot).wait()
            put(k, slot).wait()

        return carry

    lax.fori_loop(0, feed_steps, arrive, 0)

    def last_pass(k, carry):
        at = pl.ds(pl.multiple_of(k * 32, 32), 32)
        gate, value_out, grad = cum[at, :], total[at, :], cotangent[at, :].astype(F32)
        residual[at, :] = residual[at, :] + gate * value_out
        grad_value[at, :] = (grad * gate).astype(BF)
        grad_gate[at, :] = (grad * value_out * gate * (1.0 - gate)).astype(BF)
        return carry

    lax.fori_loop(0, count // 32, last_pass, 0)
    write(residual, result)
    write(grad_value, grad_value_out)
    write(grad_gate, grad_gate_out)
    for n in range(steps):
        for o in range(3):
            copy_z(n, o).wait_send()
        for copy in (copy_first(n), copy_second(n), copy_passed(n), copy_core(n)):
            copy.wait_send()
    for copy in halo_copies + [halo_two] + scan_copies:
        copy.wait_send()
    for copy in written:
        copy.wait()


def forward(near, parts, far, size):
    count, width = near[0].shape
    rows = far[0].shape[0] // 4
    whole_parts = [(p.shape, p.dtype) for p in parts] + [((rows, 2 * width), BF)]
    flat = lambda kind: jax.ShapeDtypeStruct((count, width), kind)
    narrow = jax.ShapeDtypeStruct((count, 128), F32)
    dma = pltpu.SemaphoreType.DMA
    big, low = pltpu.VMEM((count, width), F32), pltpu.VMEM((count, width), BF)
    lines = pltpu.VMEM((count, 128), F32)
    steps = sum(shape[0] // 16 for shape, _ in whole_parts)
    eight = pltpu.VMEM((8, width), F32)
    return pl.pallas_call(
        forward_kernel,
        out_shape=[jax.ShapeDtypeStruct((2, 2, 4, 2) + shape, kind) for shape, kind in whole_parts]
        + [
            flat(F32), jax.ShapeDtypeStruct((16, width), F32), jax.ShapeDtypeStruct((8, width), F32),
            jax.ShapeDtypeStruct((5, count, width), BF), flat(BF), flat(BF), flat(BF),
            jax.ShapeDtypeStruct((2, 2, 4, 2, rows, count), F32), flat(F32), flat(F32), narrow, flat(F32), flat(F32), narrow,
        ]
        + [flat(F32)] * 7,
        in_specs=[whole()] * (len(near) + len(parts)) + [anywhere()] * 2,
        out_specs=[anywhere()] * 28,
        scratch_shapes=[
            pltpu.VMEM((rows, 2 * width), BF),
            pltpu.VMEM((2, 2, 4, 2, 16, 128), BF), pltpu.VMEM((16, width), F32), eight,
            pltpu.VMEM((5, 2, 2, 4, 2, width // 32, width), BF), pltpu.VMEM((2, 2, 4, 2, 16, 2 * width), BF),
            pltpu.VMEM((2, 2, 2, 4, 2, 16, count), F32), pltpu.VMEM((5, count, width), BF), low, low, low, big,
            big, lines, big, big, lines,
        ]
        + [big] * 12
        + [
            pltpu.VMEM((32, width), BF), pltpu.VMEM((32, width), F32), pltpu.VMEM((32, 128), F32), eight,
            pltpu.VMEM((size, 8, width), F32), eight, eight, eight,
            dma((steps, 7)), dma((steps, 7)), dma((7,)), dma((2,)), dma((6,)), dma((24,)), dma((3,)), dma((size,)), dma((size,)),
            dma((3,)), dma((3,)),
        ],
        compiler_params=pltpu.CompilerParams(collective_id=0, has_side_effects=True, vmem_limit_bytes=66_000_000),
        cost_estimate=cost(6 * count * width * width + 4 * count * 32 * rows * width, 60_000_000),
        name="forward",
    )(*near, *parts, *far)


def channel_backward_kernel(
    feed_in, grad_value, grad_gate, vectors, keep, inverse, cotangent,
    weights, positive, w_feedr, w_output, spread, unit, keys, values, denom, mixed, prior_a, prior_b, recept,
    own_units, sums, rights_far, grad_residual_far,
    rights, grad_residual,
    weight_slots, positive_slots, feedr, output, spread_in, unit_in, keys_in, values_in, denom_in, mixed_in,
    prior_a_in, prior_b_in, recept_in, value_part, key_part, outgoing, gathered, from_first, from_second, feed_part, feed_z,
    grad_in, grad_rin, grad_z, grad_w, cum, up, low, summary, arrived, entering_rows, halo_out, halo_in,
    slot_sem, load_sem, core_send, core_recv, first_send, first_recv, second_send, second_recv, feed_send, feed_recv,
    scan_send, scan_recv, halo_send, halo_recv, out_sem,
):
    size = arrived.shape[0]
    links = Links(size)
    x, c, z, y, t = links.x, links.c, links.z, links.y, links.t
    rows, width = weight_slots.shape[2], feed_in.shape[1]
    micro, length = keep.shape[:2]

    def which(s):
        return lax.rem(s, 2), 3 - s // 2

    def fetches(s, slot):
        own, i = which(s)
        cc = own * c + (1 - own) * (1 - c)
        xx, yy = owner(i, x, y, cc)
        return (
            pltpu.make_async_copy(weights.at[xx, cc, :, yy], weight_slots.at[slot], slot_sem.at[0, slot]),
            pltpu.make_async_copy(positive.at[xx, cc, :, yy], positive_slots.at[slot], slot_sem.at[1, slot]),
        )

    for copy in fetches(0, 0):
        copy.start()
    late = [
        (w_feedr, feedr), (spread, spread_in), (unit, unit_in), (w_output, output), (recept, recept_in),
        (mixed, mixed_in), (denom, denom_in), (keys, keys_in), (values, values_in), (prior_a, prior_a_in),
        (prior_b, prior_b_in),
    ]
    loads = [pltpu.make_async_copy(source, target, load_sem.at[k]) for k, (source, target) in enumerate(late)]
    for load in loads:
        load.start()
    links.greet(True)
    grad_att, grad_keys, grad_values, grad_recept = [rights.at[n] for n in range(1, 5)]
    rights[0] = grad_gate[...]
    puts = [pltpu.make_async_copy(rights.at[n], rights_far.at[n], out_sem.at[n]) for n in range(5)]
    puts.append(pltpu.make_async_copy(grad_residual, grad_residual_far, out_sem.at[5]))
    puts[0].start()
    grad_in[...] = jnp.zeros_like(grad_in)
    sums[...] = jnp.zeros_like(sums)
    summary[...] = jnp.zeros_like(summary)
    halo_out[...] = jnp.zeros_like(halo_out)

    def to_core(i, slot):
        return remote(outgoing.at[slot], gathered.at[i], core_send.at[i], core_recv.at[i], links.core)

    spans = [(0, rows // 2), (rows // 2, rows)] * 2

    def piece(ref, u, *first):
        return ref.at[(*first, u // 2, slice(None), slice(*spans[u]))]

    def to_first(q, u):
        return remote(
            piece(gathered, u, 2 + q), piece(from_first, u, q), first_send.at[q, u], first_recv.at[q, u], links.first
        )

    def to_second(u):
        return remote(
            piece(gathered, u, 1), piece(from_second, u), second_send.at[u], second_recv.at[u], links.second
        )

    def to_z(u, o):
        at = slice(*spans[u])
        return remote(
            feed_part.at[u // 2, o, at], feed_z.at[u // 2, o - 1, at], feed_send.at[u, o - 1], feed_recv.at[u, o - 1],
            links.along_z[o - 1],
        )

    def pass_first(u):
        to_first(1, u).start()
        to_first(0, u).start()

    def pass_second(u):
        to_first(1, u).wait_recv()
        add_blocks(piece(gathered, u, 1), [piece(gathered, u, 1), piece(from_first, u, 1)])
        to_second(u).start()

    def pass_z(u):
        to_first(0, u).wait_recv()
        to_second(u).wait_recv()
        add_blocks(piece(feed_part, u), [piece(gathered, u, 0), piece(from_first, u, 0), piece(from_second, u)])
        for o in (1, 2, 3):
            to_z(u, o).start()

    def finish(u):
        for o in (1, 2, 3):
            to_z(u, o).wait_recv()
        for r in range(*spans[u], 32):
            at = slice(r, r + 32)
            value = feed_part[u // 2, 0, at].astype(F32)
            for o in range(3):
                value = value + feed_z[u // 2, o, at].astype(F32)
            own_units[u // 2, at] = value.astype(BF)

    def column(s, carry):
        slot = lax.rem(s, 2)
        own, i = which(s)
        for copy in fetches(s, slot):
            copy.wait()

        @pl.when(s < 7)
        def _():
            for copy in fetches(s + 1, 1 - slot):
                copy.start()

        hidden = positive_slots[slot].reshape(4 * rows, feed_in.shape[0])
        squares = (hidden * hidden).astype(BF)
        key_rows = weight_slots[slot, :, :, :width].reshape(4 * rows, width)
        value_rows = weight_slots[slot, :, :, width:].reshape(4 * rows, width)
        value_part[...] = matmul(squares, grad_value[...])
        grad_pre = (matmul_last(value_rows, grad_value[...]) * (2.0 * hidden)).astype(BF)
        key_part[...] = matmul(grad_pre, feed_in[...])
        grad_in[...] += matmul_lead(grad_pre, key_rows)

        turn_slot = lax.rem(s // 2, 2)

        @pl.when(own == 0)
        def _():
            @pl.when(s >= 4)
            def _():
                to_core(i + 2, turn_slot).wait_send()

            for k in range(4):
                at = lax.rem(k + 4 - z, 4)
                outgoing[turn_slot, 0, at] = value_part[k * rows : (k + 1) * rows].astype(BF)
                outgoing[turn_slot, 1, at] = key_part[k * rows : (k + 1) * rows].astype(BF)
            to_core(i, turn_slot).start()

        @pl.when(own == 1)
        def _():
            to_core(i, turn_slot).wait_recv()
            for side, part in ((0, value_part), (1, key_part)):
                for k in range(4):
                    at = lax.rem(k + 4 - z, 4)
                    total = gathered[i, side, at].astype(F32) + part[k * rows : (k + 1) * rows]
                    gathered[i, side, at] = total.astype(BF)

        for turn, q in ((1, 1), (3, 0)):

            @pl.when(s == turn)
            def _(q=q):
                to_first(q, 0).start()
                to_first(q, 1).start()

        pl.when(s == 5)(lambda: pass_second(0))
        pl.when(s == 6)(lambda: pass_second(1))
        return carry

    lax.fori_loop(0, 8, column, 0)
    to_core(1, 0).wait_send()
    to_core(0, 1).wait_send()

    row = lax.broadcasted_iota(jnp.int32, (length, 128), 0)
    loads[0].wait()
    dot_rows(grad_rin, grad_gate, feedr)

    def shift_two(m, rows_at, at, keeping):
        return keeping * (
            grad_in[rows_at, at] * (1.0 - vectors[BLEND_KEY : BLEND_KEY + 1, at])
            + grad_rin[rows_at, at] * (1.0 - vectors[BLEND_RECEPT : BLEND_RECEPT + 1, at])
        )

    for m in range(micro):
        start = m * length
        halo_out[m : m + 1] = shift_two(m, slice(start, start + 1), slice(None), keep[m, 0:1, 0:1])
    halo = remote(halo_out, halo_in, halo_send.at[0], halo_recv.at[0], links.row(size - 1))
    halo.start()
    pass_first(2)
    loads[1].wait()
    pass_z(0)
    halo.wait_recv()
    for m in range(micro):
        rows_at = slice(m * length, (m + 1) * length)

        def shift_pass(j, carry, m=m, rows_at=rows_at):
            at = lanes(j)
            after = jnp.where(t < size - 1, halo_in[m : m + 1, at], 0.0)
            shift = shift_two(m, rows_at, at, keep[m])
            from_in, from_rin, apart = grad_in[rows_at, at], grad_rin[rows_at, at], spread_in[rows_at, at]
            grad_z[rows_at, at] = (
                from_in * vectors[BLEND_KEY : BLEND_KEY + 1, at]
                + from_rin * vectors[BLEND_RECEPT : BLEND_RECEPT + 1, at]
                + roll_rows(shift, -1, after, row)
            )
            sums[BLEND_KEY : BLEND_KEY + 1, at] += jnp.sum(from_in * apart, axis=0, keepdims=True)
            sums[BLEND_RECEPT : BLEND_RECEPT + 1, at] += jnp.sum(from_rin * apart, axis=0, keepdims=True)
            return carry

        lax.fori_loop(0, width // 128, shift_pass, 0)
    loads[2].wait()
    norm_back_tiles(
        grad_residual, grad_z, unit_in, inverse, vectors[GAIN_TWO : GAIN_TWO + 1, :], cotangent, sums, GAIN_TWO
    )
    grad_att[...] = grad_residual[...].astype(BF)
    puts[1].start()
    puts[5].start()

    loads[3].wait()
    dot_rows(grad_w, grad_att, output)
    for load in loads[4:]:
        load.wait()
    pass_z(1)

    def quotient_grads(rows_at, at):
        gate = recept_in[rows_at, at]
        blended = mixed_in[rows_at, at]
        inner = grad_w[rows_at, at] * gate
        above = inner / denom_in[rows_at, at]
        return above, -above * blended, inner * blended * (1.0 - gate)

    for m in range(micro):
        rows_at = slice(m * length, (m + 1) * length)

        def first_pass(j, carry, m=m, rows_at=rows_at):
            at = lanes(j)
            above, below, rec = quotient_grads(rows_at, at)
            grad_recept[rows_at, at] = rec.astype(BF)
            factor = keep[m] * vectors[DECAY : DECAY + 1, at]
            f, a, b = doubling(factor, keep[m] * above, keep[m] * below, row, -1)
            cum[rows_at, at] = f
            up[rows_at, at] = a
            low[rows_at, at] = b
            summary[3 * m : 3 * m + 1, at] = f[:1]
            summary[3 * m + 1 : 3 * m + 2, at] = a[:1]
            summary[3 * m + 2 : 3 * m + 3, at] = b[:1]
            return carry

        lax.fori_loop(0, width // 128, first_pass, 0)
    copies = row_copies(summary, arrived, scan_send, scan_recv, t, links.dp, size)
    for copy in copies:
        copy.start()
    pass_first(3)
    pass_second(2)
    pass_second(3)
    for copy in copies:
        copy.wait_recv()
    for m in range(micro):
        a = jnp.zeros((1, width), F32)
        b = jnp.zeros((1, width), F32)
        for ahead in range(size - 1, 0, -1):
            o = size - ahead
            f = arrived[o, 3 * m : 3 * m + 1]
            a = jnp.where(t + ahead < size, f * a + arrived[o, 3 * m + 1 : 3 * m + 2], a)
            b = jnp.where(t + ahead < size, f * b + arrived[o, 3 * m + 2 : 3 * m + 3], b)
        entering_rows[2 * m : 2 * m + 1] = a
        entering_rows[2 * m + 1 : 2 * m + 2] = b
    for m in range(micro):
        rows_at = slice(m * length, (m + 1) * length)

        def second_pass(j, carry, m=m, rows_at=rows_at):
            at = lanes(j)
            enter_a = entering_rows[2 * m : 2 * m + 1, at]
            enter_b = entering_rows[2 * m + 1 : 2 * m + 2, at]
            f = cum[rows_at, at]
            alpha = roll_rows(up[rows_at, at] + f * enter_a, -1, enter_a, row)
            beta = roll_rows(low[rows_at, at] + f * enter_b, -1, enter_b, row)
            above, below, _ = quotient_grads(rows_at, at)
            key, value = keys_in[rows_at, at], values_in[rows_at, at]
            power = jnp.exp(key)
            bonus = jnp.exp(vectors[PREMIUM : PREMIUM + 1, at] + key)
            premium = bonus * (value * above + below)
            grad_values[rows_at, at] = (bonus * above + power * alpha).astype(BF)
            grad_keys[rows_at, at] = (premium + power * (value * alpha + beta)).astype(BF)
            fading = keep[m] * (alpha * prior_a_in[rows_at, at] + beta * prior_b_in[rows_at, at])
            sums[PREMIUM : PREMIUM + 1, at] += jnp.sum(premium, axis=0, keepdims=True)
            sums[DECAY : DECAY + 1, at] += jnp.sum(fading, axis=0, keepdims=True)
            return carry

        lax.fori_loop(0, width // 128, second_pass, 0)
        if m == 0:
            pass_z(2)
    for n in (2, 3, 4):
        puts[n].start()

    finish(0)
    finish(1)
    pass_z(3)
    finish(2)
    finish(3)
    for u in range(4):
        to_first(0, u).wait_send()
        to_first(1, u).wait_send()
        to_second(u).wait_send()
        for o in (1, 2, 3):
            to_z(u, o).wait_send()
    halo.wait_send()
    for copy in copies:
        copy.wait_send()
    for copy in puts:
        copy.wait()


def channel_backward(near, far, size):
    feed_in = near[0]
    weights = far[0]
    tokens, width = feed_in.shape
    micro, length = near[4].shape[:2]
    rows = weights.shape[4]
    flat_f32 = (tokens, width)
    dma = pltpu.SemaphoreType.DMA
    big = pltpu.VMEM(flat_f32, F32)
    return pl.pallas_call(
        channel_backward_kernel,
        out_shape=[
            jax.ShapeDtypeStruct((2, rows, width), BF), jax.ShapeDtypeStruct((16, width), F32),
            jax.ShapeDtypeStruct((5, tokens, width), BF), jax.ShapeDtypeStruct(flat_f32, F32),
        ],
        in_specs=[whole()] * len(near) + [anywhere()] * len(far),
        out_specs=[whole()] * 2 + [anywhere()] * 2,
        scratch_shapes=[
            pltpu.VMEM((5, tokens, width), BF), big,
            pltpu.VMEM((2, 4, rows, 2 * width), BF), pltpu.VMEM((2, 4, rows, tokens), F32),
            pltpu.VMEM((width, width), BF), pltpu.VMEM((width, width), BF),
        ]
        + [big] * 9
        + [
            pltpu.VMEM((4 * rows, width), F32), pltpu.VMEM((4 * rows, width), F32),
            pltpu.VMEM((2, 2, 4, rows, width), BF), pltpu.VMEM((4, 2, 4, rows, width), BF),
            pltpu.VMEM((2, 2, 4, rows, width), BF), pltpu.VMEM((2, 4, rows, width), BF),
            pltpu.VMEM((2, 4, rows, width), BF), pltpu.VMEM((2, 3, rows, width), BF),
        ]
        + [big] * 7
        + [
            pltpu.VMEM((8, width), F32), pltpu.VMEM((size, 8, width), F32), pltpu.VMEM((8, width), F32),
            pltpu.VMEM((8, width), F32), pltpu.VMEM((8, width), F32),
            dma((2, 2)), dma((11,)), dma((4,)), dma((4,)), dma((2, 4)), dma((2, 4)), dma((4,)), dma((4,)),
            dma((4, 3)), dma((4, 3)),
            dma((size,)), dma((size,)), dma((1,)), dma((1,)), dma((6,)),
        ],
        compiler_params=pltpu.CompilerParams(
            collective_id=2, has_side_effects=True, vmem_limit_bytes=66_000_000
        ),
        cost_estimate=cost(8 * tokens * 32 * rows * width, 16 * 32 * rows * width),
        name="channel_backward",
    )(*near, *far)


def front_backward_kernel(
    own_units, vectors, keep, inverse, sums_in, rates,
    lefts_far, rights_far, grad_residual_far, w_key, w_value, w_recept, spread, unit,
    square_grads, units, token_grads, vector_grads,
    lefts, rights, grad_residual, key_in, value_in, recept_in, spread_in, unit_in, outgoing, gathered, from_first, from_second, from_z,
    grad_key, grad_value, grad_recept, grad_z, sums, held, halo_out, halo_in,
    load_sem, core_send, core_recv, first_send, first_recv, second_send, second_recv, z_send, z_recv,
    unit_send, unit_recv, halo_send, halo_recv, sum_send, sum_recv, keep_sem, pair_sem,
):
    links = Links(8)
    x, c, z, y, t, size = links.x, links.c, links.z, links.y, links.t, links.size
    count = lefts.shape[0]
    width = lefts.shape[2]
    rows = width // 32
    micro, length = keep.shape[:2]
    late = [(w_key, key_in), (w_value, value_in), (w_recept, recept_in), (spread, spread_in), (unit, unit_in)]
    late += [(grad_residual_far, grad_residual)]
    loads = [pltpu.make_async_copy(source, target, load_sem.at[k]) for k, (source, target) in enumerate(late)]

    def pair(n):
        return (
            pltpu.make_async_copy(lefts_far.at[n], lefts.at[n], pair_sem.at[0, n]),
            pltpu.make_async_copy(rights_far.at[n], rights.at[n], pair_sem.at[1, n]),
        )

    for n in range(count):
        for copy in pair(n):
            copy.start()
    for load in loads:
        load.start()
    links.greet(True)
    dp = links.dp
    over = (1 - x) * 2 + c
    kept = pltpu.make_async_copy(own_units, units.at[dp], keep_sem.at[0])
    kept.start()
    units_over_x = remote(own_units, units.at[dp], unit_send.at[0], unit_recv.at[0], links.over_x)
    pl.when(c == 0)(units_over_x.start)
    units_over_core = remote(own_units, units.at[dp], unit_send.at[1], unit_recv.at[1], links.core)
    units_over_core.start()
    halo_out[...] = jnp.zeros_like(halo_out)
    sums[...] = sums_in[...]

    def part(n, cc, xx):
        at = pl.ds(pl.multiple_of((xx * 2 + cc) * 8 * rows, 8 * rows), 8 * rows)
        return matmul_lead(lefts[n, :, at], rights[n])

    def blocks():
        for zz in range(4):
            for yy in range(2):
                yield zz, yy, slice((zz * 2 + yy) * rows, (zz * 2 + yy + 1) * rows)

    def to_core(n):
        return remote(outgoing.at[n], gathered.at[n], core_send.at[n], core_recv.at[n], links.core)

    def to_first(n):
        return remote(
            gathered.at[n, pl.ds(2, 2)], from_first.at[n], first_send.at[n], first_recv.at[n], links.first
        )

    def to_second(n):
        return remote(gathered.at[n, 1], from_second.at[n], second_send.at[n], second_recv.at[n], links.second)

    def to_z(n, o):
        return remote(
            gathered.at[n, 0, o], from_z.at[n, o - 1], z_send.at[n, o - 1], z_recv.at[n, o - 1], links.along_z[o - 1]
        )

    def other(n, carry):
        for copy in pair(n):
            copy.wait()
        for xx in range(2):
            value = part(n, 1 - c, xx)
            for zz, yy, at in blocks():
                outgoing[n, position(xx, yy, x, y, 1 - c), lax.rem(zz + 4 - z, 4)] = value[at].astype(BF)
        to_core(n).start()

    def own(n, carry):
        to_core(n).wait_recv()
        for xx in range(2):
            value = part(n, c, xx)
            for zz, yy, at in blocks():
                i, o = position(xx, yy, x, y, c), lax.rem(zz + 4 - z, 4)
                gathered[n, i, o] = (gathered[n, i, o].astype(F32) + value[at]).astype(BF)
        to_first(n).start()

    def both(n, carry):
        pl.when(n < count)(lambda: other(n, None))
        pl.when(n >= 1)(lambda: own(n - 1, None))
        return carry

    lax.fori_loop(0, count + 1, both, 0)
    pl.when(c == 1)(units_over_x.start)

    def pass_second(n):
        to_first(n).wait_recv()
        add_blocks(gathered.at[n, 1], [gathered.at[n, 1], from_first.at[n, 1]])
        to_second(n).start()

    def pass_z(n):
        to_second(n).wait_recv()
        add_blocks(gathered.at[n, 0], [gathered.at[n, 0], from_first.at[n, 0], from_second.at[n]])
        for o in (1, 2, 3):
            to_z(n, o).start()

    def finish(n):
        value = gathered[n, 0, 0].astype(F32)
        for o in (1, 2, 3):
            to_z(n, o).wait_recv()
            value = value + from_z[n, o - 1].astype(F32)
        square_grads[n] = value

    loads[0].wait()
    dot_rows(grad_key, rights.at[2], key_in)
    pass_second(0)
    loads[1].wait()
    dot_rows(grad_value, rights.at[3], value_in)
    pass_second(1)
    loads[2].wait()
    dot_rows(grad_recept, rights.at[4], recept_in)
    last_over_core = remote(units.at[over], units.at[over], unit_send.at[2], unit_recv.at[2], links.core)
    grads = ((grad_key, MIX_KEY), (grad_value, MIX_VALUE), (grad_recept, MIX_RECEPT))

    def shift_one(rows_at, at, keeping):
        return keeping * sum(g[rows_at, at] * (1.0 - vectors[k : k + 1, at]) for g, k in grads)

    for m in range(micro):
        start = m * length
        halo_out[m : m + 1] = shift_one(slice(start, start + 1), slice(None), keep[m, 0:1, 0:1])
    halo = remote(halo_out, halo_in, halo_send.at[0], halo_recv.at[0], links.row(size - 1))
    halo.start()
    pass_second(2)
    pass_z(0)
    pass_second(3)
    pass_z(1)
    pass_second(4)
    loads[3].wait()
    halo.wait_recv()
    row = lax.broadcasted_iota(jnp.int32, (length, 128), 0)
    for m in range(micro):
        rows_at = slice(m * length, (m + 1) * length)

        def shift_pass(j, carry, m=m, rows_at=rows_at):
            at = lanes(j)
            after = jnp.where(t < size - 1, halo_in[m : m + 1, at], 0.0)
            apart = spread_in[rows_at, at]
            value = roll_rows(shift_one(rows_at, at, keep[m]), -1, after, row)
            for g, k in grads:
                value = value + g[rows_at, at] * vectors[k : k + 1, at]
                sums[k : k + 1, at] += jnp.sum(g[rows_at, at] * apart, axis=0, keepdims=True)
            grad_z[rows_at, at] = value
            return carry

        lax.fori_loop(0, width // 128, shift_pass, 0)
    pass_z(2)
    loads[4].wait()
    loads[5].wait()
    norm_back_tiles(
        token_grads, grad_z, unit_in, inverse, vectors[GAIN_ONE : GAIN_ONE + 1, :], grad_residual, sums, GAIN_ONE
    )
    sums[DECAY : DECAY + 1, :] = -sums[DECAY : DECAY + 1, :] * rates[0:1, :] * vectors[DECAY : DECAY + 1, :]

    stages = [[links.core], [links.over_x], [links.over_y]]
    pending = []
    source, slot = sums, 0

    def begin(stage, source, slot):
        copies = [
            remote(source, held.at[slot + k], sum_send.at[slot + k], sum_recv.at[slot + k], peer)
            for k, peer in enumerate(stage)
        ]
        for copy in copies:
            copy.start()
        return copies

    def collect(copies, source, slot, target):
        value = source[...]
        for k, copy in enumerate(copies):
            copy.wait_recv()
            value = value + held[slot + k]
        target[...] = value

    copies = begin(stages[0], sums, 0)
    pending += copies
    pass_z(3)
    finish(0)
    collect(copies, sums, 0, held.at[6])
    copies = begin(stages[1], held.at[6], 1)
    pending += copies
    pass_z(4)
    finish(1)
    collect(copies, held.at[6], 1, held.at[7])
    copies = begin(stages[2], held.at[7], 2)
    pending += copies
    units_over_x.wait_recv()
    last_over_core.start()
    finish(2)
    collect(copies, held.at[7], 2, held.at[8])

    def block(zz):
        return pl.ds(pl.multiple_of((dp * 2 + zz // 2) * 128, 128), 128)

    copies = []
    for k, peer in enumerate(links.along_z):
        at = block(lax.rem(z + k + 1, 4))
        copies.append(
            remote(held.at[8, :, at], held.at[3 + k, :, at], sum_send.at[3 + k], sum_recv.at[3 + k], peer)
        )
        copies[-1].start()
    pending += copies
    finish(3)
    own_lanes = block(z)
    value = held[8, :, own_lanes]
    for k, copy in enumerate(copies):
        copy.wait_recv()
        value = value + held[3 + k, :, own_lanes]
    vector_grads[...] = jnp.zeros_like(vector_grads)
    vector_grads[:, own_lanes] = value
    finish(4)
    for copy in (units_over_core, last_over_core):
        copy.wait_recv()
    kept.wait()
    for n in range(count):
        to_core(n).wait_send()
        to_first(n).wait_send()
        to_second(n).wait_send()
        for o in (1, 2, 3):
            to_z(n, o).wait_send()
    for copy in pending + [units_over_x, units_over_core, last_over_core, halo]:
        copy.wait_send()


def front_backward(near, far):
    own_units, lefts = near[0], far[0]
    rows = own_units.shape[1]
    count, tokens, width = lefts.shape
    own = width // 32
    dma = pltpu.SemaphoreType.DMA
    big = pltpu.VMEM((tokens, width), F32)
    square = pltpu.VMEM((width, width), BF)
    return pl.pallas_call(
        front_backward_kernel,
        out_shape=[
            jax.ShapeDtypeStruct((count, own, width), F32),
            jax.ShapeDtypeStruct((4, 2, rows, width), BF),
            jax.ShapeDtypeStruct((tokens, width), F32), jax.ShapeDtypeStruct((16, width), F32),
        ],
        in_specs=[whole()] * len(near) + [anywhere()] * len(far),
        out_specs=[whole(), anywhere(), whole(), whole()],
        scratch_shapes=[pltpu.VMEM(lefts.shape, BF), pltpu.VMEM(lefts.shape, BF), big]
        + [square] * 3
        + [big] * 2
        + [
            pltpu.VMEM((count, 4, 4, own, width), BF), pltpu.VMEM((count, 4, 4, own, width), BF),
            pltpu.VMEM((count, 2, 4, own, width), BF), pltpu.VMEM((count, 4, own, width), BF),
            pltpu.VMEM((count, 3, own, width), BF),
        ]
        + [big] * 4
        + [
            pltpu.VMEM((16, width), F32), pltpu.VMEM((9, 16, width), F32), pltpu.VMEM((8, width), F32),
            pltpu.VMEM((8, width), F32),
            dma((6,)), dma((count,)), dma((count,)), dma((count,)), dma((count,)), dma((count,)), dma((count,)),
            dma((count, 3)), dma((count, 3)), dma((3,)), dma((3,)), dma((1,)), dma((1,)),
            dma((6,)), dma((6,)), dma((1,)), dma((2, count)),
        ],
        compiler_params=pltpu.CompilerParams(
            collective_id=3, has_side_effects=True, vmem_limit_bytes=66_000_000
        ),
        cost_estimate=cost(4 * count * tokens * width * width, 40 * width * width),
        name="front_backward",
    )(*near, *far)


def local_shards(tokens, resets, out_grads, *weights):
    (
        mixer_key, mixer_value, mixer_recept, mixer_output, feed_recept, feed_key, feed_value, *vector_shards
    ) = weights
    size = lax.axis_size("tensor")
    dp, t = lax.axis_index("dp"), lax.axis_index("tensor")
    micro, _, length, width = tokens.shape
    count = micro * length
    share = vector_shards[0].shape[0]
    vector_pack = jnp.pad(jnp.stack(vector_shards), ((0, 16 - len(vector_shards)), (0, 128 - share)))
    keep = (1 - resets[:, 0]).astype(F32)[:, :, None]
    keep_lanes = jnp.broadcast_to(keep, (micro, length, 128))
    cotangent = out_grads.reshape(count, width)
    near = [tokens.reshape(count, width), cotangent, keep_lanes]
    parts = [vector_pack, mixer_key, mixer_value, mixer_recept, mixer_output, feed_recept]
    (
        _, all_key, all_value, all_recept, all_output, all_feedr, feed,
        result, table, rates, lefts, feed_in, grad_value, grad_gate, positive, spread_one, unit_one, inverse_one,
        spread_two, unit_two, inverse_two, keys, values, denom, mixed, prior_a, prior_b, recept,
    ) = forward(near, parts, [feed_key, feed_value], size)
    w_key, w_value, w_recept, w_output, w_feedr = [
        w.reshape(width, width) for w in (all_key, all_value, all_recept, all_output, all_feedr)
    ]
    near = [feed_in, grad_value, grad_gate, table, keep_lanes, inverse_two, cotangent]
    far = [feed, positive, w_feedr, w_output, spread_two, unit_two, keys, values, denom, mixed, prior_a, prior_b, recept]
    own_units, sums, rights, grad_residual = channel_backward(near, far, size)
    near = [own_units, table, keep_lanes, inverse_one, sums, rates]
    far = [lefts, rights, grad_residual, w_key, w_value, w_recept, spread_one, unit_one]
    square_grads, units, token_grads, vector_grads = front_backward(near, far)
    mine = lax.dynamic_slice_in_dim(vector_grads, (dp * size + t) * share, share, 1)
    return (
        result.reshape(tokens.shape), token_grads.reshape(tokens.shape),
        square_grads[2], square_grads[3], square_grads[4], square_grads[1], square_grads[0],
        units[:, 1].reshape(feed_key.shape).astype(F32), units[:, 0].reshape(feed_value.shape).astype(F32),
    ) + tuple(mine[i] for i in range(len(vector_shards)))


def is_two_by_two_by_four(mesh):
    return mesh.shape["dp"] == 4 and mesh.shape["tensor"] == 8


def solution(mesh):
    return jax.shard_map(
        local_shards if is_two_by_two_by_four(mesh) else shards,
        mesh=mesh,
        in_specs=(
            P(None, "dp", "tensor", None),
            P(None, "dp", "tensor"),
            P(None, "dp", "tensor", None),
            P(("dp", "tensor"), None),
            P(("dp", "tensor"), None),
            P(("dp", "tensor"), None),
            P(("dp", "tensor"), None),
            P(("dp", "tensor"), None),
            P("tensor", None),
            P("tensor", None),
            P(("dp", "tensor")),
            P(("dp", "tensor")),
            P(("dp", "tensor")),
            P(("dp", "tensor")),
            P(("dp", "tensor")),
            P(("dp", "tensor")),
            P(("dp", "tensor")),
            P(("dp", "tensor")),
            P(("dp", "tensor")),
            P(("dp", "tensor")),
            P(("dp", "tensor")),
        ),
        out_specs=(
            P(None, "dp", "tensor", None),
            P(None, "dp", "tensor", None),
            P(("dp", "tensor"), None),
            P(("dp", "tensor"), None),
            P(("dp", "tensor"), None),
            P(("dp", "tensor"), None),
            P(("dp", "tensor"), None),
            P("tensor", None),
            P("tensor", None),
            P(("dp", "tensor")),
            P(("dp", "tensor")),
            P(("dp", "tensor")),
            P(("dp", "tensor")),
            P(("dp", "tensor")),
            P(("dp", "tensor")),
            P(("dp", "tensor")),
            P(("dp", "tensor")),
            P(("dp", "tensor")),
            P(("dp", "tensor")),
            P(("dp", "tensor")),
        ),
        check_vma=False,
    )
```
